8 devices in a mesh: dp: 1 (over z), ty: 2 (over y), tx: 4 (over x, core).
Axes of the slice: x: 2, y: 2, z: 1, core: 2. Of those that a mesh axis runs over, the one named last changes fastest.
Arguments:
- x_in: bfloat16 [1, 256, 2048], P('dp', None, 'tx')
- positions: int32 [1, 256], P('dp')
- d_y: bfloat16 [1, 256, 2048], P('dp', None, 'tx')
- ln_gamma: float32 [2048], P('tx')
- w_q: bfloat16 [2048, 2048], P('tx', 'ty')
- w_g: bfloat16 [2048, 8192], P('tx', 'ty')
- w_u: bfloat16 [2048, 8192], P('tx', 'ty')
- w_k: bfloat16 [2048, 256], P('tx')
- w_v: bfloat16 [2048, 256], P('tx')
- w_o: bfloat16 [2048, 2048], P('ty', 'tx')
- w_d: bfloat16 [8192, 2048], P('ty', 'tx')
Outputs:
- output 1: bfloat16 [1, 256, 2048], P('dp', None, 'tx')
- output 2: bfloat16 [1, 256, 2048], P('dp', None, 'tx')
- output 3: float32 [2048], P(('dp', 'tx'))
- output 4: float32 [2048, 2048], P(('dp', 'tx'), 'ty')
- output 5: float32 [2048, 8192], P(('dp', 'tx'), 'ty')
- output 6: float32 [2048, 8192], P(('dp', 'tx'), 'ty')
- output 7: float32 [2048, 256], P(('dp', 'tx'))
- output 8: float32 [2048, 256], P(('dp', 'tx'))
- output 9: float32 [2048, 2048], P(('dp', 'ty'), 'tx')
- output 10: float32 [8192, 2048], P(('dp', 'ty'), 'tx')
All inputs are finite; a program needn't handle non-finite values.
Results may differ from the reference program's by a relative error of at most 0.02.
Values are sent between devices in bfloat16 or wider.
A program may use at most 1 GiB of HBM per device.

```python
import functools
import jax
import jax.numpy as jnp
from jax import lax

D_MODEL = 2048
N_HEADS = 8
HEAD_DIM = 256
D_FF = 8192
SEQ_LEN = 256
N_SEQS = 1
TOKENS = N_SEQS * SEQ_LEN
Q_WIDTH = N_HEADS * HEAD_DIM
EPS = 1e-6
ROPE_BASE = 10000.0
SCORE_SCALE = HEAD_DIM ** -0.5


def setup_inputs(seed: int = 0, part: int = 0) -> dict:
    part_key = jax.random.fold_in(jax.random.key(seed), part)
    k_x, k_rows, k_ramp, k_start, k_steps, k_dy = jax.random.split(part_key, 6)
    shared = jax.random.split(jax.random.key(seed + 1), 8)
    width_ramp = jnp.linspace(-1.0, 1.0, D_MODEL, dtype=jnp.float32)
    row_scale = jax.random.uniform(k_rows, (N_SEQS, SEQ_LEN, 1), jnp.float32, 0.5, 1.5)
    ramp_size = jax.random.uniform(k_ramp, (N_SEQS, SEQ_LEN, 1), jnp.float32, -1.5, 1.5)
    x_in = jax.random.normal(k_x, (N_SEQS, SEQ_LEN, D_MODEL), jnp.float32) * row_scale + ramp_size * width_ramp
    pos_start = jax.random.randint(k_start, (N_SEQS, 1), 0, SEQ_LEN, dtype=jnp.int32)
    pos_steps = jax.random.randint(k_steps, (N_SEQS, SEQ_LEN), 1, 4, dtype=jnp.int32)
    positions = (pos_start + jnp.cumsum(pos_steps, axis=1, dtype=jnp.int32) - pos_steps[:, 0:1]).astype(jnp.int32)
    d_y = jax.random.normal(k_dy, (N_SEQS, SEQ_LEN, D_MODEL), jnp.float32)
    ln_gamma = 1.0 + 0.3 * jax.random.normal(shared[0], (D_MODEL,), jnp.float32)
    in_scale = D_MODEL ** -0.5
    return {
        'x_in': x_in.astype(jnp.bfloat16),
        'positions': positions,
        'd_y': d_y.astype(jnp.bfloat16),
        'ln_gamma': ln_gamma,
        'w_q': (jax.random.normal(shared[1], (D_MODEL, Q_WIDTH), jnp.float32) * in_scale).astype(jnp.bfloat16),
        'w_g': (jax.random.normal(shared[2], (D_MODEL, D_FF), jnp.float32) * in_scale).astype(jnp.bfloat16),
        'w_u': (jax.random.normal(shared[3], (D_MODEL, D_FF), jnp.float32) * in_scale).astype(jnp.bfloat16),
        'w_k': (jax.random.normal(shared[4], (D_MODEL, HEAD_DIM), jnp.float32) * in_scale).astype(jnp.bfloat16),
        'w_v': (jax.random.normal(shared[5], (D_MODEL, HEAD_DIM), jnp.float32) * in_scale).astype(jnp.bfloat16),
        'w_o': (jax.random.normal(shared[6], (Q_WIDTH, D_MODEL), jnp.float32) * (2.0 * Q_WIDTH ** -0.5)).astype(jnp.bfloat16),
        'w_d': (jax.random.normal(shared[7], (D_FF, D_MODEL), jnp.float32) * D_FF ** -0.5).astype(jnp.bfloat16),
    }


def to_bf16(values):
    return values.astype(jnp.bfloat16).astype(jnp.float32)


def rope_tables(positions):
    half_dim = HEAD_DIM // 2
    inv_freq = ROPE_BASE ** (-2.0 * jnp.arange(half_dim, dtype=jnp.float32) / HEAD_DIM)
    angles = positions.astype(jnp.float32)[:, None] * inv_freq[None, :]
    return jnp.cos(angles), jnp.sin(angles)


def apply_rope(values, cos_t, sin_t):
    half_dim = values.shape[-1] // 2
    first = values[..., :half_dim]
    second = values[..., half_dim:]
    return jnp.concatenate([first * cos_t - second * sin_t, second * cos_t + first * sin_t], axis=-1)


def attend_seq(operands):
    q_seq, k_seq, v_seq = operands
    scores = jnp.einsum('ihe,je->ihj', q_seq, k_seq) * SCORE_SCALE
    seq_idx = jnp.arange(SEQ_LEN)
    causal = seq_idx[:, None, None] >= seq_idx[None, None, :]
    prob_mat = to_bf16(jax.nn.softmax(jnp.where(causal, scores, -1e30), axis=-1))
    return to_bf16(jnp.einsum('ihj,je->ihe', prob_mat, v_seq))


def forward(x_f, ln_gamma, w_q, w_g, w_u, w_k, w_v, w_o, w_d, cos_t=None, sin_t=None):
    x_flat = x_f.reshape(TOKENS, D_MODEL)
    tok_mean = jnp.mean(x_flat, axis=1, keepdims=True)
    tok_var = jnp.mean(x_flat * x_flat, axis=1, keepdims=True) - tok_mean * tok_mean
    x_hat = (x_flat - tok_mean) * lax.rsqrt(tok_var + EPS)
    normed = to_bf16(x_hat * ln_gamma)
    q_lin = jnp.dot(normed, w_q, preferred_element_type=jnp.float32).reshape(TOKENS, N_HEADS, HEAD_DIM)
    q_rot = to_bf16(apply_rope(q_lin, cos_t[:, None, :], sin_t[:, None, :]))
    k_rot = to_bf16(apply_rope(jnp.dot(normed, w_k, preferred_element_type=jnp.float32), cos_t, sin_t))
    v_val = to_bf16(jnp.dot(normed, w_v, preferred_element_type=jnp.float32))
    gate_proj = to_bf16(jnp.dot(normed, w_g, preferred_element_type=jnp.float32))
    up_proj = to_bf16(jnp.dot(normed, w_u, preferred_element_type=jnp.float32))
    attn_out = lax.map(jax.checkpoint(attend_seq), (q_rot.reshape(N_SEQS, SEQ_LEN, N_HEADS, HEAD_DIM), k_rot.reshape(N_SEQS, SEQ_LEN, HEAD_DIM), v_val.reshape(N_SEQS, SEQ_LEN, HEAD_DIM)))
    hidden_act = to_bf16(jax.nn.silu(gate_proj) * up_proj)
    branch = jnp.dot(attn_out.reshape(TOKENS, Q_WIDTH), w_o, preferred_element_type=jnp.float32) + jnp.dot(hidden_act, w_d, preferred_element_type=jnp.float32)
    return to_bf16(x_flat + branch).reshape(N_SEQS, SEQ_LEN, D_MODEL)


def reference(x_in, positions, d_y, ln_gamma, w_q, w_g, w_u, w_k, w_v, w_o, w_d):
    cos_t, sin_t = rope_tables(positions.reshape(TOKENS))
    primals = [operand.astype(jnp.float32) for operand in (x_in, ln_gamma, w_q, w_g, w_u, w_k, w_v, w_o, w_d)]
    y_f, pullback = jax.vjp(functools.partial(forward, cos_t=cos_t, sin_t=sin_t), *primals)
    grad_list = pullback(d_y.astype(jnp.float32))
    return (y_f.astype(jnp.bfloat16), grad_list[0].astype(jnp.bfloat16), grad_list[1], grad_list[2], grad_list[3], grad_list[4], grad_list[5], grad_list[6], grad_list[7], grad_list[8])
```

```python
import jax
import jax.numpy as jnp
from jax import lax
from jax.sharding import PartitionSpec as P

EPS = 1e-6
ROPE_BASE = 10000.0
F32 = jnp.float32
BF16 = jnp.bfloat16
N_CHUNKS = 4


CORE_PAIRS = [(0, 1), (1, 0), (2, 3), (3, 2)]
CHIP_PAIRS = [(0, 2), (2, 0), (1, 3), (3, 1)]
FAR_PAIRS = [(0, 3), (3, 0), (1, 2), (2, 1)]
TY_PAIRS = [(0, 1), (1, 0)]


def swap_core(v):
    return lax.ppermute(v, 'tx', CORE_PAIRS)


def swap_chip(v):
    return lax.ppermute(v, 'tx', CHIP_PAIRS)


def swap_ty(v):
    return lax.ppermute(v, 'ty', TY_PAIRS)


def sum_tx(v):
    near = lax.ppermute(v, 'tx', CORE_PAIRS)
    across = lax.ppermute(v, 'tx', CHIP_PAIRS)
    far = lax.ppermute(v, 'tx', FAR_PAIRS)
    return (v + near) + (across + far)


def dot(a, b, dims):
    return lax.dot_general(a, b, (dims, ((), ())), preferred_element_type=F32)


def mm(a, b):
    return dot(a, b, ((1,), (0,)))


def mm_bt(a, b):
    return dot(a, b, ((1,), (1,)))


def mm_at(a, b):
    return dot(a, b, ((0,), (0,)))


def rope_tables(positions, head_dim):
    half_dim = head_dim // 2
    inv_freq = ROPE_BASE ** (-2.0 * jnp.arange(half_dim, dtype=F32) / head_dim)
    angles = positions.astype(F32)[:, None] * inv_freq[None, :]
    return jnp.cos(angles), jnp.sin(angles)


def apply_rope(values, cos_t, sin_t):
    half_dim = values.shape[-1] // 2
    first = values[..., :half_dim]
    second = values[..., half_dim:]
    return jnp.concatenate([first * cos_t - second * sin_t, second * cos_t + first * sin_t], axis=-1)


def rope_grad(grad_out, cos_t, sin_t):
    half_dim = grad_out.shape[-1] // 2
    first = grad_out[..., :half_dim]
    second = grad_out[..., half_dim:]
    return jnp.concatenate([first * cos_t + second * sin_t, second * cos_t - first * sin_t], axis=-1)


def solution(mesh):
    tx_size = mesh.shape['tx']
    tok_spec = P('dp', None, 'tx')
    in_specs = (tok_spec, P('dp', None), tok_spec, P('tx'), P('tx', 'ty'), P('tx', 'ty'), P('tx', 'ty'),
                P('tx', None), P('tx', None), P('ty', 'tx'), P('ty', 'tx'))
    out_specs = (tok_spec, tok_spec, P(('dp', 'tx')), P(('dp', 'tx'), 'ty'), P(('dp', 'tx'), 'ty'), P(('dp', 'tx'), 'ty'),
                 P(('dp', 'tx'), None), P(('dp', 'tx'), None), P(('dp', 'ty'), 'tx'), P(('dp', 'ty'), 'tx'))

    def local_layer(x_in, positions, d_y, ln_gamma, w_q, w_g, w_u, w_k, w_v, w_o, w_d):
        _, n_tok, d_local = x_in.shape
        half = n_tok // 2
        d_model = d_local * tx_size
        head_dim = w_k.shape[1]
        q_width = w_q.shape[1]
        heads_local = q_width // head_dim
        d_ff = w_g.shape[1]
        chunk = d_ff // N_CHUNKS
        core = lax.axis_index('tx') % 2

        def roll(v):
            return lax.dynamic_slice_in_dim(jnp.concatenate([v, v[:half]], axis=0), core * half, n_tok, axis=0)

        x_b = roll(x_in.reshape(n_tok, d_local))
        dy = roll(d_y.reshape(n_tok, d_local))
        pos = roll(positions.reshape(n_tok))

        def scatter_core(a, weights, matmul):
            sent = jnp.concatenate([matmul(a[half:], w).astype(BF16) for w in weights], axis=1) if len(weights) > 1 else matmul(a[half:], weights[0]).astype(BF16)
            got = swap_core(sent)
            kept = []
            lo = 0
            for w in weights:
                part = matmul(a[:half], w)
                kept.append((part + got[:, lo:lo + part.shape[1]].astype(F32)).astype(BF16))
                lo += part.shape[1]
            return jnp.concatenate(kept, axis=1) if len(kept) > 1 else kept[0]

        def exchange(chip_sum):
            return chip_sum.astype(F32) + swap_chip(chip_sum).astype(F32)

        def gather_core(mine):
            return jnp.concatenate([mine, swap_core(mine)], axis=0)

        d_attn_half = exchange(scatter_core(dy, [w_o], mm_bt)).astype(BF16)
        d_act_halves = [exchange(scatter_core(dy, [w_d[i * chunk:(i + 1) * chunk]], mm_bt)).astype(BF16) for i in range(N_CHUNKS - 1)]

        x_nat = x_in.reshape(n_tok, d_local).astype(F32)
        tok_stats = roll(sum_tx(jnp.stack([jnp.sum(x_nat, axis=1), jnp.sum(x_nat * x_nat, axis=1)], axis=1)))
        x_f = x_b.astype(F32)
        tok_mean = tok_stats[:, 0:1] / d_model
        tok_var = tok_stats[:, 1:2] / d_model - tok_mean * tok_mean
        inv_std = lax.rsqrt(tok_var + EPS)
        x_hat = (x_f - tok_mean) * inv_std
        normed = (x_hat * ln_gamma).astype(BF16)

        qkv = exchange(scatter_core(normed, [w_q, w_k, w_v], mm))
        cos_t, sin_t = rope_tables(pos, head_dim)
        cos_h, sin_h = cos_t[:half], sin_t[:half]
        q_half = apply_rope(qkv[:, :q_width].reshape(half, heads_local, head_dim), cos_h[:, None, :], sin_h[:, None, :]).astype(BF16).reshape(half, q_width)
        k_half = apply_rope(qkv[:, q_width:q_width + head_dim], cos_h, sin_h).astype(BF16)
        v_half = qkv[:, q_width + head_dim:].astype(BF16)
        packed = gather_core(jnp.concatenate([q_half, k_half, v_half, d_attn_half], axis=1))
        q_rot = packed[:, :q_width]
        k_rot = packed[:, q_width:q_width + head_dim]
        v_val = packed[:, q_width + head_dim:q_width + 2 * head_dim]
        d_attn = packed[:, q_width + 2 * head_dim:]

        tok_idx = (jnp.arange(n_tok) + core * half) % n_tok
        causal = tok_idx[:, None] >= tok_idx[None, :]
        scale = head_dim ** -0.5
        attn_cols, dq_cols = [], []
        d_k_part = 0.0
        d_v_part = 0.0
        for head in range(heads_local):
            cols = slice(head * head_dim, (head + 1) * head_dim)
            q_h, da_h = q_rot[:, cols], d_attn[:, cols]
            scores = jnp.where(causal, mm_bt(q_h, k_rot) * scale, -1e30)
            probs_f = jax.nn.softmax(scores, axis=-1)
            probs = probs_f.astype(BF16)
            attn_cols.append(mm(probs, v_val).astype(BF16))
            d_v_part += mm_at(probs, da_h)
            d_probs = mm_bt(da_h, v_val).astype(BF16).astype(F32)
            d_scores = (probs_f * (d_probs - jnp.sum(d_probs * probs_f, axis=-1, keepdims=True)) * scale).astype(BF16)
            dq_h = mm(d_scores, k_rot).astype(BF16).astype(F32)
            dq_cols.append(rope_grad(dq_h, cos_t, sin_t).astype(BF16))
            d_k_part += mm_at(d_scores, q_h)
        attn_flat = jnp.concatenate(attn_cols, axis=1)
        d_q = jnp.concatenate(dq_cols, axis=1)
        d_kv_part = jnp.concatenate([d_k_part, d_v_part], axis=1).astype(BF16)
        d_kv = d_kv_part.astype(F32) + swap_ty(d_kv_part).astype(F32)
        d_k = rope_grad(d_kv[:, :head_dim].astype(BF16).astype(F32), cos_t, sin_t).astype(BF16)
        d_v = d_kv[:, head_dim:].astype(BF16)

        acts, d_gates, d_ups = [], [], []
        branch_part = mm(attn_flat, w_o)
        dh_part = mm_bt(d_q, w_q)
        for i in range(N_CHUNKS):
            cols = slice(i * chunk, (i + 1) * chunk)
            gu = exchange(scatter_core(normed, [w_g[:, cols], w_u[:, cols]], mm)).astype(BF16).astype(F32)
            gate_f, up_f = gu[:, :chunk], gu[:, chunk:]
            sig_gate = jax.nn.sigmoid(gate_f)
            silu_gate = gate_f * sig_gate
            act_half = (silu_gate * up_f).astype(BF16)
            if i == N_CHUNKS - 1:
                act = gather_core(act_half)
                d_act_f = exchange(scatter_core(dy, [w_d[cols]], mm_bt)).astype(BF16).astype(F32)
            else:
                d_act_f = d_act_halves[i].astype(F32)
            d_up_half = (d_act_f * silu_gate).astype(BF16)
            d_gate_half = (d_act_f * up_f * sig_gate * (1.0 + gate_f * (1.0 - sig_gate))).astype(BF16)
            if i == N_CHUNKS - 1:
                both = gather_core(jnp.concatenate([d_gate_half, d_up_half], axis=1))
                d_gate, d_up = both[:, :chunk], both[:, chunk:]
            else:
                both = gather_core(jnp.concatenate([d_gate_half, d_up_half, act_half], axis=1))
                d_gate, d_up, act = both[:, :chunk], both[:, chunk:2 * chunk], both[:, 2 * chunk:]
            branch_part += mm(act, w_d[cols])
            dh_part += mm_bt(d_gate, w_g[:, cols]) + mm_bt(d_up, w_u[:, cols])
            acts.append(act)
            d_gates.append(d_gate)
            d_ups.append(d_up)

        branch_b = branch_part.astype(BF16)
        branch = branch_b.astype(F32) + swap_ty(branch_b).astype(F32)
        y_out = roll((x_f + branch).astype(BF16))

        dh_b = dh_part.astype(BF16)
        d_normed = (dh_b.astype(F32) + swap_ty(dh_b).astype(F32)) + mm_bt(d_k, w_k) + mm_bt(d_v, w_v)
        d_hat = d_normed * ln_gamma
        d_gamma = jnp.sum(d_normed * x_hat, axis=0)
        back_part = roll(jnp.stack([jnp.sum(d_hat, axis=1), jnp.sum(d_hat * x_hat, axis=1)], axis=1))
        back_stats = roll(sum_tx(back_part))
        d_x = dy.astype(F32) + inv_std * (d_hat - back_stats[:, 0:1] / d_model - x_hat * back_stats[:, 1:2] / d_model)
        d_x = roll(d_x.astype(BF16))

        d_wo = mm_at(attn_flat, dy)
        d_wd = mm_at(jnp.concatenate(acts, axis=1), dy)
        d_wq, d_wk, d_wv = (mm_at(normed, g) for g in (d_q, d_k, d_v))
        d_wg = mm_at(normed, jnp.concatenate(d_gates, axis=1))
        d_wu = mm_at(normed, jnp.concatenate(d_ups, axis=1))
        return (y_out.reshape(x_in.shape), d_x.reshape(x_in.shape), d_gamma,
                d_wq, d_wg, d_wu, d_wk, d_wv, d_wo, d_wd)

    return jax.shard_map(local_layer, mesh=mesh, in_specs=in_specs, out_specs=out_specs, check_vma=False)
```

```python
import functools

import jax
import jax.numpy as jnp
import numpy as np
from jax import lax
from jax.experimental import pallas as pl
from jax.experimental.pallas import tpu as pltpu
from jax.sharding import PartitionSpec as P

EPS = 1e-6
ROPE_BASE = 10000.0
F32 = jnp.float32
BF16 = jnp.bfloat16
MESH = pl.DeviceIdType.MESH

BLK = 512
CHUNK = 1024
B_DATTN, B_DACT_LO, B_QKV, B_GU, B_DACT_HI, N_BLK = 0, 2, 6, 9, 25, 29
X_UNITS = ((0, 1), (1, 1), (2, 2), (4, 2), (6, 3), (9, 4), (13, 4), (17, 4), (21, 4), (25, 2), (27, 2))


def dot(a, b, dims):
    return lax.dot_general(a, b, (dims, ((), ())), preferred_element_type=F32)


def mm(a, b):
    return dot(a, b, ((1,), (0,)))


def mm_bt(a, b):
    return dot(a, b, ((1,), (1,)))


def mm_at(a, b):
    return dot(a, b, ((0,), (0,)))


def rope(first, second, cos_t, sin_t):
    return first * cos_t - second * sin_t, second * cos_t + first * sin_t


def layer_kernel(d_model, x_hbm, pos_ref, freq_ref, dy_hbm, gamma_ref, wq_hbm, wg_hbm, wu_hbm, wk_hbm, wv_hbm, wo_hbm, wd_hbm,
                 y_hbm, dx_hbm, dgamma_ref, nrm_hbm, attn_hbm, act_hbm, dq_hbm, dkv_hbm, dg_hbm, du_hbm,
                 x_v, dy_v, wqkv_v, wg_v, wu_v, wo_v, wd_v,
                 keep, send, rcore, chip, rx, md, packed, attn_v, dq_v, dkv_part, dkv_rx, dkv_v, kv_acc,
                 nrm_v, xhat_v, inv_v, cos_v, sin_v, br_v, dh_v, kvdh_v, y_snd, y_rx, dh_snd, dh_rx, y_o, dx_o,
                 st_snd, st_rx, bst_snd, bst_rx,
                 ld_sem, st_sem, cs, cr, xs, xr, gs, gr, ps, pr, ts, tr, ss, sr):
    tx = lax.axis_index('tx')
    ty = lax.axis_index('ty')
    core = lax.rem(tx, 2)
    near = {'tx': tx + 1 - 2 * core}
    across = {'tx': lax.rem(tx + 2, 4)}
    far = {'tx': lax.rem(tx + 1 - 2 * core + 2, 4)}
    other_ty = {'ty': 1 - ty}
    n_tok = x_v.shape[0]
    half = n_tok // 2
    mine = pl.multiple_of(core * half, half)
    other = pl.multiple_of((1 - core) * half, half)
    head_dim = 256
    q_width = wo_v.shape[0]
    heads = q_width // head_dim

    def load(i, src, dst):
        return pltpu.make_async_copy(src, dst, ld_sem.at[i])

    d_half = wd_v.shape[0] // 2
    loads = [
        load(0, dy_hbm.at[pl.ds(mine, half)], dy_v.at[0:half]),
        load(1, dy_hbm.at[pl.ds(other, half)], dy_v.at[half:n_tok]),
        load(2, wo_hbm, wo_v),
        load(3, x_hbm.at[pl.ds(mine, half)], x_v.at[0:half]),
        load(4, x_hbm.at[pl.ds(other, half)], x_v.at[half:n_tok]),
        load(5, wd_hbm.at[0:d_half], wd_v.at[0:d_half]),
        load(6, wq_hbm, wqkv_v.at[:, 0:q_width]),
        load(7, wk_hbm, wqkv_v.at[:, q_width:q_width + head_dim]),
        load(8, wv_hbm, wqkv_v.at[:, q_width + head_dim:q_width + 2 * head_dim]),
        load(9, wg_hbm, wg_v),
        load(10, wu_hbm, wu_v),
        load(11, wd_hbm.at[d_half:2 * d_half], wd_v.at[d_half:2 * d_half]),
    ]
    for ld in loads:
        ld.start()

    barrier = pltpu.get_barrier_semaphore()
    for peer in (near, across, far, other_ty):
        pl.semaphore_signal(barrier, inc=1, device_id=peer, device_id_type=MESH)
    pl.semaphore_wait(barrier, 4)

    def remote(src, dst, send_sem, recv_sem, peer):
        return pltpu.make_async_remote_copy(src_ref=src, dst_ref=dst, send_sem=send_sem, recv_sem=recv_sem,
                                            device_id=peer, device_id_type=MESH)

    def core_copy(b):
        return remote(send.at[b], rcore.at[b], cs.at[b], cr.at[b], near)

    def x_copy(u):
        start, count = X_UNITS[u]
        return remote(chip.at[pl.ds(start, count)], rx.at[pl.ds(start, count)], xs.at[u], xr.at[u], across)

    def put(b, part):
        keep[b] = part[:half]
        send[b] = part[half:].astype(BF16)
        core_copy(b).start()

    def issue_bwd(b, w_ref, row):
        put(b, mm_bt(dy_v[...], w_ref[pl.ds(row, BLK), :]))

    def issue_fwd(b, w_ref, col):
        put(b, mm(nrm_v[...], w_ref[:, pl.ds(col, BLK)]))

    def combine(b):
        core_copy(b).wait_recv()
        chip[b] = (keep[b] + rcore[b].astype(F32)).astype(BF16)

    def total(b):
        return chip[b].astype(F32) + rx[b].astype(F32)

    for i in range(3):
        loads[i].wait()
    issue_bwd(0, wo_v, 0)
    issue_bwd(1, wo_v, BLK)

    def rows_of(col_a, col_b):
        lane = lax.broadcasted_iota(jnp.int32, (half, 128), 1)
        return jnp.where(lane == 0, col_a, col_b).T[0:8]

    def stats_copy(snd, got, k, i):
        return remote(snd, got.at[i], ss.at[k * 3 + i], sr.at[k * 3 + i], (near, across, far)[i])

    def stats_start(snd, got, k, col_a, col_b):
        for lo, at in ((0, mine), (half, other)):
            snd[:, pl.ds(at, half)] = rows_of(col_a[lo:lo + half], col_b[lo:lo + half])
        for i in range(3):
            stats_copy(snd, got, k, i).start()

    def stats_finish(snd, got, k):
        for i in range(3):
            stats_copy(snd, got, k, i).wait_recv()
        rows = (snd[...] + got[0]) + (got[1] + got[2])
        snd_sum = got
        snd_sum[0] = rows
        cols = []
        for at in (mine, other):
            tile = jnp.broadcast_to(snd_sum[0, 0:1, pl.ds(at, half)], (128, half)).T
            tile_b = jnp.broadcast_to(snd_sum[0, 1:2, pl.ds(at, half)], (128, half)).T
            cols.append((tile[:, 0:1], tile_b[:, 0:1]))
        return (jnp.concatenate([cols[0][0], cols[1][0]], axis=0), jnp.concatenate([cols[0][1], cols[1][1]], axis=0))

    loads[3].wait()
    loads[4].wait()
    x_f = x_v[...].astype(F32)
    stats_start(st_snd, st_rx, 0, jnp.sum(x_f, axis=1, keepdims=True), jnp.sum(x_f * x_f, axis=1, keepdims=True))

    combine(0)
    x_copy(0).start()
    combine(1)
    x_copy(1).start()

    loads[5].wait()
    for i in range(4):
        issue_bwd(B_DACT_LO + i, wd_v, i * BLK)
        if i >= 1:
            combine(B_DACT_LO + i - 1)
        if i == 2:
            x_copy(2).start()
    combine(B_DACT_LO + 3)
    x_copy(3).start()

    sum_x, sum_xx = stats_finish(st_snd, st_rx, 0)
    tok_mean = sum_x / d_model
    inv_std = lax.rsqrt(sum_xx / d_model - tok_mean * tok_mean + EPS)
    inv_v[...] = jnp.broadcast_to(inv_std, (n_tok, 128))
    x_hat = (x_v[...].astype(F32) - tok_mean) * inv_std
    xhat_v[...] = x_hat
    nrm_v[...] = (x_hat * gamma_ref[...]).astype(BF16)

    for i in range(6, 9):
        loads[i].wait()
    for i in range(3):
        issue_fwd(B_QKV + i, wqkv_v, i * BLK)
    for i in range(3):
        combine(B_QKV + i)
    x_copy(4).start()

    loads[9].wait()
    loads[10].wait()
    for k in range(4):
        def gu_issue(j, carry, k=k):
            col = pl.multiple_of(k * CHUNK + j * BLK, BLK)
            issue_fwd(B_GU + 4 * k + j, wg_v, col)
            issue_fwd(B_GU + 4 * k + 2 + j, wu_v, col)
            return carry

        def gu_combine(j, carry, k=k):
            combine(B_GU + 4 * k + j)
            return carry

        lax.fori_loop(0, 2, gu_issue, 0)
        lax.fori_loop(0, 4, gu_combine, 0)
        x_copy(5 + k).start()

    loads[11].wait()

    def hi_issue(j, carry):
        issue_bwd(B_DACT_HI + j, wd_v, pl.multiple_of(d_half + j * BLK, BLK))
        return carry

    lax.fori_loop(0, 4, hi_issue, 0)
    for j in range(4):
        combine(B_DACT_HI + j)
        if j % 2 == 1:
            x_copy(9 + j // 2).start()

    freq = freq_ref[...]
    for lo, at in ((0, mine), (half, other)):
        pos_col = jnp.broadcast_to(pos_ref[0:1, pl.ds(at, half)].astype(F32), (128, half)).T
        angles = pos_col * freq
        cos_v[lo:lo + half] = jnp.cos(angles)
        sin_v[lo:lo + half] = jnp.sin(angles)

    def store(i, src, dst):
        return pltpu.make_async_copy(src, dst, st_sem.at[i])

    def store_rows(i, src, dst, cols):
        return [store(i, src.at[0:half], dst.at[pl.ds(mine, half), cols]),
                store(i + 1, src.at[half:n_tok], dst.at[pl.ds(other, half), cols])]

    stores = store_rows(0, nrm_v, nrm_hbm, pl.ds(0, x_v.shape[1]))
    for st in stores:
        st.start()

    packed_copy = remote(packed.at[0:half], packed.at[half:n_tok], ps.at[0], pr.at[0], near)
    x_copy(0).wait_recv()
    x_copy(1).wait_recv()
    for j in range(2):
        packed[0:half, q_width + 512 + j * BLK:q_width + 512 + (j + 1) * BLK] = total(B_DATTN + j).astype(BF16)
    x_copy(4).wait_recv()
    cos_h, sin_h = cos_v[0:half], sin_v[0:half]
    for j in range(2):
        blk = total(B_QKV + j)
        for h in range(2):
            lo = h * head_dim
            first, second = rope(blk[:, lo:lo + 128], blk[:, lo + 128:lo + 256], cos_h, sin_h)
            packed[0:half, j * BLK + lo:j * BLK + lo + 128] = first.astype(BF16)
            packed[0:half, j * BLK + lo + 128:j * BLK + lo + 256] = second.astype(BF16)
    blk = total(B_QKV + 2)
    first, second = rope(blk[:, 0:128], blk[:, 128:256], cos_h, sin_h)
    packed[0:half, q_width:q_width + 128] = first.astype(BF16)
    packed[0:half, q_width + 128:q_width + 256] = second.astype(BF16)
    packed[0:half, q_width + 256:q_width + 512] = blk[:, 256:512].astype(BF16)
    packed_copy.start()
    packed_copy.wait_recv()

    row_i = lax.rem(lax.broadcasted_iota(jnp.int32, (n_tok, n_tok), 0) + core * half, n_tok)
    col_i = lax.rem(lax.broadcasted_iota(jnp.int32, (n_tok, n_tok), 1) + core * half, n_tok)
    scale = head_dim ** -0.5
    kv_acc[...] = jnp.zeros_like(kv_acc)

    def head_step(h, carry):
        cols = pl.ds(pl.multiple_of(h * head_dim, head_dim), head_dim)
        q_h = packed[:, cols]
        da_h = packed[:, pl.ds(pl.multiple_of(q_width + 512 + h * head_dim, head_dim), head_dim)]
        k_rot = packed[:, q_width:q_width + 256]
        v_val = packed[:, q_width + 256:q_width + 512]
        scores = jnp.where(row_i >= col_i, mm_bt(q_h, k_rot) * scale, -1e30)
        exps = jnp.exp(scores - jnp.max(scores, axis=1, keepdims=True))
        probs_f = exps / jnp.sum(exps, axis=1, keepdims=True)
        probs = probs_f.astype(BF16)
        attn_v[:, cols] = mm(probs, v_val).astype(BF16)
        d_probs = mm_bt(da_h, v_val).astype(BF16).astype(F32)
        d_scores = (probs_f * (d_probs - jnp.sum(d_probs * probs_f, axis=1, keepdims=True)) * scale).astype(BF16)
        dq_h = mm(d_scores, k_rot).astype(BF16).astype(F32)
        first, second = rope(dq_h[:, 0:128], dq_h[:, 128:256], cos_v[...], -sin_v[...])
        dq_v[:, pl.ds(pl.multiple_of(h * head_dim, head_dim), 128)] = first.astype(BF16)
        dq_v[:, pl.ds(pl.multiple_of(h * head_dim + 128, 128), 128)] = second.astype(BF16)
        kv_acc[:, 0:256] += mm_at(d_scores, q_h)
        kv_acc[:, 256:512] += mm_at(probs, da_h)
        return carry

    lax.fori_loop(0, heads, head_step, 0)
    dkv_part[...] = kv_acc[...].astype(BF16)
    dkv_copy = remote(dkv_part, dkv_rx, ts.at[0], tr.at[0], other_ty)
    dkv_copy.start()
    for st in store_rows(2, attn_v, attn_hbm, pl.ds(0, q_width)) + store_rows(4, dq_v, dq_hbm, pl.ds(0, q_width)):
        st.start()
        stores.append(st)
    br_v[...] = mm(attn_v[...], wo_v[...])
    dh_v[...] = mm_bt(dq_v[...], wqkv_v[:, 0:q_width])

    def gather_copy(k, i):
        return remote(md.at[k, i, 0:half], md.at[k, i, half:n_tok], gs.at[3 * k + i], gr.at[3 * k + i], near)

    def dact_block(k, j):
        return B_DACT_LO + 2 * k + j if k < 2 else B_DACT_HI + 2 * (k - 2) + j

    def gated(k, want_act, want_grad):
        def step(r, carry):
            rows = pl.ds(pl.multiple_of(r * 16, 16), 16)
            for j in range(2):
                bg, bu, bd = B_GU + 4 * k + j, B_GU + 4 * k + 2 + j, dact_block(k, j)
                gate = (chip[bg, rows].astype(F32) + rx[bg, rows].astype(F32)).astype(BF16).astype(F32)
                up = (chip[bu, rows].astype(F32) + rx[bu, rows].astype(F32)).astype(BF16).astype(F32)
                sig = jax.nn.sigmoid(gate)
                silu = gate * sig
                cols = slice(j * BLK, (j + 1) * BLK)
                if want_act:
                    md[k, 0, rows, cols] = (silu * up).astype(BF16)
                if want_grad:
                    d_act = (chip[bd, rows].astype(F32) + rx[bd, rows].astype(F32)).astype(BF16).astype(F32)
                    md[k, 1, rows, cols] = (d_act * up * sig * (1.0 + gate * (1.0 - sig))).astype(BF16)
                    md[k, 2, rows, cols] = (d_act * silu).astype(BF16)
            return carry

        lax.fori_loop(0, half // 16, step, 0)
        for i in ((0,) if want_act else ()) + ((1, 2) if want_grad else ()):
            gather_copy(k, i).start()

    def md_store(k, i):
        for st in store_rows(8 + 6 * k + 2 * i, md.at[k, i], (act_hbm, dg_hbm, du_hbm)[i], pl.ds(k * CHUNK, CHUNK)):
            st.start()
            stores.append(st)

    def use_act(k):
        gather_copy(k, 0).wait_recv()
        md_store(k, 0)
        br_v[...] += mm(md[k, 0], wd_v[k * CHUNK:(k + 1) * CHUNK, :])

    def use_grad(k):
        for i in (1, 2):
            gather_copy(k, i).wait_recv()
            md_store(k, i)
        dh_v[...] += (mm_bt(md[k, 1], wg_v[:, k * CHUNK:(k + 1) * CHUNK])
                      + mm_bt(md[k, 2], wu_v[:, k * CHUNK:(k + 1) * CHUNK]))

    x_copy(2).wait_recv()
    x_copy(3).wait_recv()
    for k in range(2):
        x_copy(5 + k).wait_recv()
        gated(k, True, True)
        use_act(k)
        use_grad(k)
        if k == 0:
            dkv_copy.wait_recv()
            d_k = dkv_part[:, 0:256].astype(F32) + dkv_rx[:, 0:256].astype(F32)
            d_k = d_k.astype(BF16).astype(F32)
            first, second = rope(d_k[:, 0:128], d_k[:, 128:256], cos_v[...], -sin_v[...])
            dkv_v[:, 0:128] = first.astype(BF16)
            dkv_v[:, 128:256] = second.astype(BF16)
            dkv_v[:, 256:512] = (dkv_part[:, 256:512].astype(F32) + dkv_rx[:, 256:512].astype(F32)).astype(BF16)
            for st in store_rows(6, dkv_v, dkv_hbm, pl.ds(0, 512)):
                st.start()
                stores.append(st)
            kvdh_v[...] = mm_bt(dkv_v[...], wqkv_v[:, q_width:q_width + 512])
    for k in (2, 3):
        x_copy(5 + k).wait_recv()
        gated(k, True, False)
        use_act(k)
    y_snd[...] = br_v[...].astype(BF16)
    y_copy = remote(y_snd, y_rx, ts.at[1], tr.at[1], other_ty)
    y_copy.start()
    for k in (2, 3):
        x_copy(7 + k).wait_recv()
        gated(k, False, True)
        use_grad(k)
    dh_snd[...] = dh_v[...].astype(BF16)
    dh_copy = remote(dh_snd, dh_rx, ts.at[2], tr.at[2], other_ty)
    dh_copy.start()

    y_copy.wait_recv()
    y_o[...] = (x_v[...].astype(F32) + (y_snd[...].astype(F32) + y_rx[...].astype(F32))).astype(BF16)
    for st in store_rows(32, y_o, y_hbm, pl.ds(0, x_v.shape[1])):
        st.start()
        stores.append(st)

    dh_copy.wait_recv()
    d_nrm = (dh_snd[...].astype(F32) + dh_rx[...].astype(F32)) + kvdh_v[...]
    dh_v[...] = d_nrm
    d_hat = d_nrm * gamma_ref[...]
    x_hat = xhat_v[...]
    dgamma_ref[...] = jnp.sum(d_nrm * x_hat, axis=0, keepdims=True)
    stats_start(bst_snd, bst_rx, 1, jnp.sum(d_hat, axis=1, keepdims=True), jnp.sum(d_hat * x_hat, axis=1, keepdims=True))
    sum_d, sum_dx = stats_finish(bst_snd, bst_rx, 1)
    d_hat = dh_v[...] * gamma_ref[...]
    d_x = dy_v[...].astype(F32) + inv_v[:, 0:1] * (d_hat - sum_d / d_model - xhat_v[...] * (sum_dx / d_model))
    dx_o[...] = d_x.astype(BF16)
    for st in store_rows(34, dx_o, dx_hbm, pl.ds(0, x_v.shape[1])):
        st.start()
        stores.append(st)

    def drain(b, carry):
        core_copy(b).wait_send()
        return carry

    lax.fori_loop(0, N_BLK, drain, 0)
    for u in range(len(X_UNITS)):
        x_copy(u).wait_send()
    for k in range(4):
        for i in range(3):
            gather_copy(k, i).wait_send()
    for copy in (packed_copy, dkv_copy, y_copy, dh_copy):
        copy.wait_send()
    for i in range(3):
        stats_copy(st_snd, st_rx, 0, i).wait_send()
        stats_copy(bst_snd, bst_rx, 1, i).wait_send()
    for st in stores:
        st.wait()


def solution(mesh):
    tx_size = mesh.shape['tx']
    tok_spec = P('dp', None, 'tx')
    in_specs = (tok_spec, P('dp', None), tok_spec, P('tx'), P('tx', 'ty'), P('tx', 'ty'), P('tx', 'ty'),
                P('tx', None), P('tx', None), P('ty', 'tx'), P('ty', 'tx'))
    out_specs = (tok_spec, tok_spec, P(('dp', 'tx')), P(('dp', 'tx'), 'ty'), P(('dp', 'tx'), 'ty'), P(('dp', 'tx'), 'ty'),
                 P(('dp', 'tx'), None), P(('dp', 'tx'), None), P(('dp', 'ty'), 'tx'), P(('dp', 'ty'), 'tx'))

    def local_layer(x_in, positions, d_y, ln_gamma, w_q, w_g, w_u, w_k, w_v, w_o, w_d):
        _, n_tok, d_local = x_in.shape
        half = n_tok // 2
        d_model = d_local * tx_size
        head_dim = w_k.shape[1]
        q_width = w_q.shape[1]
        d_ff = w_g.shape[1]
        freq = jnp.asarray((ROPE_BASE ** (-2.0 * np.arange(head_dim // 2) / head_dim)).astype(np.float32)[None])
        any_spec = pl.BlockSpec(memory_space=pl.ANY)
        vmem_spec = pl.BlockSpec(memory_space=pltpu.VMEM)
        tok = (n_tok, d_local)
        sem = pltpu.SemaphoreType.DMA
        y_loc, dx_loc, d_gamma, normed, attn_flat, act, d_q, d_kv, d_gate, d_up = pl.pallas_call(
            functools.partial(layer_kernel, d_model),
            out_shape=[jax.ShapeDtypeStruct(tok, BF16), jax.ShapeDtypeStruct(tok, BF16), jax.ShapeDtypeStruct((1, d_local), F32),
                       jax.ShapeDtypeStruct(tok, BF16), jax.ShapeDtypeStruct((n_tok, q_width), BF16),
                       jax.ShapeDtypeStruct((n_tok, d_ff), BF16), jax.ShapeDtypeStruct((n_tok, q_width), BF16),
                       jax.ShapeDtypeStruct((n_tok, 2 * head_dim), BF16), jax.ShapeDtypeStruct((n_tok, d_ff), BF16),
                       jax.ShapeDtypeStruct((n_tok, d_ff), BF16)],
            in_specs=[any_spec, vmem_spec, vmem_spec, any_spec, vmem_spec] + [any_spec] * 7,
            out_specs=[any_spec, any_spec, vmem_spec] + [any_spec] * 7,
            scratch_shapes=[
                pltpu.VMEM(tok, BF16), pltpu.VMEM(tok, BF16), pltpu.VMEM((d_local, q_width + 2 * head_dim), BF16),
                pltpu.VMEM((d_local, d_ff), BF16), pltpu.VMEM((d_local, d_ff), BF16), pltpu.VMEM((q_width, d_local), BF16),
                pltpu.VMEM((d_ff, d_local), BF16),
                pltpu.VMEM((N_BLK, half, BLK), F32), pltpu.VMEM((N_BLK, half, BLK), BF16), pltpu.VMEM((N_BLK, half, BLK), BF16),
                pltpu.VMEM((N_BLK, half, BLK), BF16), pltpu.VMEM((N_BLK, half, BLK), BF16),
                pltpu.VMEM((4, 3, n_tok, CHUNK), BF16), pltpu.VMEM((n_tok, 2 * q_width + 2 * head_dim), BF16),
                pltpu.VMEM((n_tok, q_width), BF16), pltpu.VMEM((n_tok, q_width), BF16),
                pltpu.VMEM((n_tok, 512), BF16), pltpu.VMEM((n_tok, 512), BF16), pltpu.VMEM((n_tok, 512), BF16),
                pltpu.VMEM((n_tok, 512), F32),
                pltpu.VMEM(tok, BF16), pltpu.VMEM(tok, F32), pltpu.VMEM((n_tok, 128), F32), pltpu.VMEM((n_tok, 128), F32),
                pltpu.VMEM((n_tok, 128), F32), pltpu.VMEM(tok, F32), pltpu.VMEM(tok, F32), pltpu.VMEM(tok, F32),
                pltpu.VMEM(tok, BF16), pltpu.VMEM(tok, BF16), pltpu.VMEM(tok, BF16), pltpu.VMEM(tok, BF16),
                pltpu.VMEM(tok, BF16), pltpu.VMEM(tok, BF16),
                pltpu.VMEM((8, n_tok), F32), pltpu.VMEM((3, 8, n_tok), F32), pltpu.VMEM((8, n_tok), F32), pltpu.VMEM((3, 8, n_tok), F32),
                sem((12,)), sem((36,)), sem((N_BLK,)), sem((N_BLK,)), sem((len(X_UNITS),)), sem((len(X_UNITS),)),
                sem((12,)), sem((12,)), sem((1,)), sem((1,)), sem((3,)), sem((3,)), sem((6,)), sem((6,))],
            compiler_params=pltpu.CompilerParams(collective_id=0, has_side_effects=True, vmem_limit_bytes=67043328),
            name='layer',
        )(x_in.reshape(tok), positions, freq, d_y.reshape(tok), ln_gamma[None], w_q, w_g, w_u, w_k, w_v, w_o, w_d)

        dy = d_y.reshape(tok)
        d_wo = mm_at(attn_flat, dy)
        d_wd = mm_at(act, dy)
        d_wq = mm_at(normed, d_q)
        d_wk = mm_at(normed, d_kv[:, :head_dim])
        d_wv = mm_at(normed, d_kv[:, head_dim:])
        d_wg = mm_at(normed, d_gate)
        d_wu = mm_at(normed, d_up)
        return (y_loc.reshape(x_in.shape), dx_loc.reshape(x_in.shape), d_gamma.reshape(d_local),
                d_wq, d_wg, d_wu, d_wk, d_wv, d_wo, d_wd)

    return jax.shard_map(local_layer, mesh=mesh, in_specs=in_specs, out_specs=out_specs, check_vma=False)
```

```python
import functools

import jax
import jax.numpy as jnp
import numpy as np
from jax import lax
from jax.experimental import pallas as pl
from jax.experimental.pallas import tpu as pltpu
from jax.sharding import PartitionSpec as P

EPS = 1e-6
ROPE_BASE = 10000.0
F32 = jnp.float32
BF16 = jnp.bfloat16
MESH = pl.DeviceIdType.MESH

BLK = 512
CHUNK = 1024
B_DATTN, B_DACT_LO, B_QKV, B_GU, B_DACT_HI, N_BLK = 0, 2, 6, 9, 25, 29
X_UNITS = ((0, 1), (1, 1), (2, 2), (4, 2), (6, 3), (9, 4), (13, 4), (17, 4), (21, 4), (25, 2), (27, 2))


def dot(a, b, dims):
    return lax.dot_general(a, b, (dims, ((), ())), preferred_element_type=F32)


def mm(a, b):
    return dot(a, b, ((1,), (0,)))


def mm_bt(a, b):
    return dot(a, b, ((1,), (1,)))


def mm_at(a, b):
    return dot(a, b, ((0,), (0,)))


def rope(first, second, cos_t, sin_t):
    return first * cos_t - second * sin_t, second * cos_t + first * sin_t


def layer_kernel(d_model, x_hbm, pos_ref, freq_ref, dy_hbm, gamma_ref, wq_hbm, wg_hbm, wu_hbm, wk_hbm, wv_hbm, wo_hbm, wd_hbm,
                 y_hbm, dx_hbm, dgamma_ref, nrm_hbm, attn_hbm, act_hbm, dq_hbm, dkv_hbm, dg_hbm, du_hbm,
                 x_v, dy_v, wqkv_v, wg_v, wu_v, wo_v, wd_v,
                 keep, send, rcore, chip, rx, md, packed, attn_v, dq_v, dkv_part, dkv_rx, dkv_v, kv_acc,
                 nrm_v, xhat_v, inv_v, cos_v, sin_v, br_v, dh_v, kvdh_v, y_snd, y_rx, dh_snd, dh_rx, y_o, dx_o,
                 st_snd, st_rx, bst_snd, bst_rx,
                 ld_sem, st_sem, cs, cr, xs, xr, gs, gr, ps, pr, ts, tr, ss, sr):
    tx = lax.axis_index('tx')
    ty = lax.axis_index('ty')
    core = lax.rem(tx, 2)
    near = {'tx': tx + 1 - 2 * core}
    across = {'tx': lax.rem(tx + 2, 4)}
    far = {'tx': lax.rem(tx + 1 - 2 * core + 2, 4)}
    other_ty = {'ty': 1 - ty}
    n_tok = x_v.shape[0]
    half = n_tok // 2
    mine = pl.multiple_of(core * half, half)
    other = pl.multiple_of((1 - core) * half, half)
    head_dim = 256
    q_width = wo_v.shape[0]
    heads = q_width // head_dim

    def load(i, src, dst):
        return pltpu.make_async_copy(src, dst, ld_sem.at[i])

    d_half = wd_v.shape[0] // 2
    loads = [
        load(0, dy_hbm.at[pl.ds(mine, half)], dy_v.at[0:half]),
        load(1, dy_hbm.at[pl.ds(other, half)], dy_v.at[half:n_tok]),
        load(2, wo_hbm, wo_v),
        load(3, x_hbm.at[pl.ds(mine, half)], x_v.at[0:half]),
        load(4, x_hbm.at[pl.ds(other, half)], x_v.at[half:n_tok]),
        load(5, wd_hbm.at[0:d_half], wd_v.at[0:d_half]),
        load(6, wq_hbm, wqkv_v.at[:, 0:q_width]),
        load(7, wk_hbm, wqkv_v.at[:, q_width:q_width + head_dim]),
        load(8, wv_hbm, wqkv_v.at[:, q_width + head_dim:q_width + 2 * head_dim]),
        load(9, wg_hbm, wg_v),
        load(10, wu_hbm, wu_v),
        load(11, wd_hbm.at[d_half:2 * d_half], wd_v.at[d_half:2 * d_half]),
    ]
    for ld in loads:
        ld.start()

    barrier = pltpu.get_barrier_semaphore()
    for peer in (near, across, far, other_ty):
        pl.semaphore_signal(barrier, inc=1, device_id=peer, device_id_type=MESH)
    pl.semaphore_wait(barrier, 4)

    def remote(src, dst, send_sem, recv_sem, peer):
        return pltpu.make_async_remote_copy(src_ref=src, dst_ref=dst, send_sem=send_sem, recv_sem=recv_sem,
                                            device_id=peer, device_id_type=MESH)

    def core_copy(b):
        return remote(send.at[b], rcore.at[b], cs.at[b], cr.at[b], near)

    def x_copy(u):
        start, count = X_UNITS[u]
        return remote(chip.at[pl.ds(start, count)], rx.at[pl.ds(start, count)], xs.at[u], xr.at[u], across)

    def put(b, part):
        keep[b] = part[:half]
        send[b] = part[half:].astype(BF16)
        core_copy(b).start()

    def issue_bwd(b, w_ref, row):
        put(b, mm_bt(dy_v[...], w_ref[pl.ds(row, BLK), :]))

    def issue_fwd(b, w_ref, col):
        put(b, mm(nrm_v[...], w_ref[:, pl.ds(col, BLK)]))

    def combine(b):
        core_copy(b).wait_recv()
        chip[b] = (keep[b] + rcore[b].astype(F32)).astype(BF16)

    def total(b):
        return chip[b].astype(F32) + rx[b].astype(F32)

    for i in range(3):
        loads[i].wait()
    issue_bwd(0, wo_v, 0)
    issue_bwd(1, wo_v, BLK)

    def rows_of(col_a, col_b):
        lane = lax.broadcasted_iota(jnp.int32, (half, 128), 1)
        return jnp.where(lane == 0, col_a, col_b).T[0:8]

    def stats_copy(snd, got, k, i):
        return remote(snd, got.at[i], ss.at[k * 3 + i], sr.at[k * 3 + i], (near, across, far)[i])

    def stats_start(snd, got, k, col_a, col_b):
        for lo, at in ((0, mine), (half, other)):
            snd[:, pl.ds(at, half)] = rows_of(col_a[lo:lo + half], col_b[lo:lo + half])
        for i in range(3):
            stats_copy(snd, got, k, i).start()

    def stats_finish(snd, got, k):
        for i in range(3):
            stats_copy(snd, got, k, i).wait_recv()
        rows = (snd[...] + got[0]) + (got[1] + got[2])
        snd_sum = got
        snd_sum[0] = rows
        cols = []
        for at in (mine, other):
            tile = jnp.broadcast_to(snd_sum[0, 0:1, pl.ds(at, half)], (128, half)).T
            tile_b = jnp.broadcast_to(snd_sum[0, 1:2, pl.ds(at, half)], (128, half)).T
            cols.append((tile[:, 0:1], tile_b[:, 0:1]))
        return (jnp.concatenate([cols[0][0], cols[1][0]], axis=0), jnp.concatenate([cols[0][1], cols[1][1]], axis=0))

    loads[3].wait()
    loads[4].wait()
    x_f = x_v[...].astype(F32)
    stats_start(st_snd, st_rx, 0, jnp.sum(x_f, axis=1, keepdims=True), jnp.sum(x_f * x_f, axis=1, keepdims=True))

    combine(0)
    x_copy(0).start()
    combine(1)
    x_copy(1).start()

    loads[5].wait()
    for i in range(4):
        issue_bwd(B_DACT_LO + i, wd_v, i * BLK)
        if i >= 1:
            combine(B_DACT_LO + i - 1)
        if i == 2:
            x_copy(2).start()
    combine(B_DACT_LO + 3)
    x_copy(3).start()

    sum_x, sum_xx = stats_finish(st_snd, st_rx, 0)
    tok_mean = sum_x / d_model
    inv_std = lax.rsqrt(sum_xx / d_model - tok_mean * tok_mean + EPS)
    inv_v[...] = jnp.broadcast_to(inv_std, (n_tok, 128))
    x_hat = (x_v[...].astype(F32) - tok_mean) * inv_std
    xhat_v[...] = x_hat
    nrm_v[...] = (x_hat * gamma_ref[...]).astype(BF16)

    for i in range(6, 9):
        loads[i].wait()
    for i in range(3):
        issue_fwd(B_QKV + i, wqkv_v, i * BLK)
    for i in range(3):
        combine(B_QKV + i)
    x_copy(4).start()

    loads[9].wait()
    loads[10].wait()
    for k in range(4):
        def gu_issue(j, carry, k=k):
            col = pl.multiple_of(k * CHUNK + j * BLK, BLK)
            issue_fwd(B_GU + 4 * k + j, wg_v, col)
            issue_fwd(B_GU + 4 * k + 2 + j, wu_v, col)
            return carry

        def gu_combine(j, carry, k=k):
            combine(B_GU + 4 * k + j)
            return carry

        lax.fori_loop(0, 2, gu_issue, 0)
        lax.fori_loop(0, 4, gu_combine, 0)
        x_copy(5 + k).start()

    loads[11].wait()

    def hi_issue(j, carry):
        issue_bwd(B_DACT_HI + j, wd_v, pl.multiple_of(d_half + j * BLK, BLK))
        return carry

    lax.fori_loop(0, 4, hi_issue, 0)
    for j in range(4):
        combine(B_DACT_HI + j)
        if j % 2 == 1:
            x_copy(9 + j // 2).start()

    freq = freq_ref[...]
    for lo, at in ((0, mine), (half, other)):
        pos_col = jnp.broadcast_to(pos_ref[0:1, pl.ds(at, half)].astype(F32), (128, half)).T
        angles = pos_col * freq
        cos_v[lo:lo + half] = jnp.cos(angles)
        sin_v[lo:lo + half] = jnp.sin(angles)

    def store(i, src, dst):
        return pltpu.make_async_copy(src, dst, st_sem.at[i])

    def store_rows(i, src, dst, cols):
        return [store(i, src.at[0:half], dst.at[pl.ds(mine, half), cols]),
                store(i + 1, src.at[half:n_tok], dst.at[pl.ds(other, half), cols])]

    stores = store_rows(0, nrm_v, nrm_hbm, pl.ds(0, x_v.shape[1]))
    for st in stores:
        st.start()

    packed_copy = remote(packed.at[0:half], packed.at[half:n_tok], ps.at[0], pr.at[0], near)
    x_copy(0).wait_recv()
    x_copy(1).wait_recv()
    for j in range(2):
        packed[0:half, q_width + 512 + j * BLK:q_width + 512 + (j + 1) * BLK] = total(B_DATTN + j).astype(BF16)
    x_copy(4).wait_recv()
    cos_h, sin_h = cos_v[0:half], sin_v[0:half]
    for j in range(2):
        blk = total(B_QKV + j)
        for h in range(2):
            lo = h * head_dim
            first, second = rope(blk[:, lo:lo + 128], blk[:, lo + 128:lo + 256], cos_h, sin_h)
            packed[0:half, j * BLK + lo:j * BLK + lo + 128] = first.astype(BF16)
            packed[0:half, j * BLK + lo + 128:j * BLK + lo + 256] = second.astype(BF16)
    blk = total(B_QKV + 2)
    first, second = rope(blk[:, 0:128], blk[:, 128:256], cos_h, sin_h)
    packed[0:half, q_width:q_width + 128] = first.astype(BF16)
    packed[0:half, q_width + 128:q_width + 256] = second.astype(BF16)
    packed[0:half, q_width + 256:q_width + 512] = blk[:, 256:512].astype(BF16)
    packed_copy.start()
    packed_copy.wait_recv()

    row_i = lax.rem(lax.broadcasted_iota(jnp.int32, (n_tok, n_tok), 0) + core * half, n_tok)
    col_i = lax.rem(lax.broadcasted_iota(jnp.int32, (n_tok, n_tok), 1) + core * half, n_tok)
    scale = head_dim ** -0.5
    kv_acc[...] = jnp.zeros_like(kv_acc)

    def head_step(h, carry):
        cols = pl.ds(pl.multiple_of(h * head_dim, head_dim), head_dim)
        q_h = packed[:, cols]
        da_h = packed[:, pl.ds(pl.multiple_of(q_width + 512 + h * head_dim, head_dim), head_dim)]
        k_rot = packed[:, q_width:q_width + 256]
        v_val = packed[:, q_width + 256:q_width + 512]
        scores = jnp.where(row_i >= col_i, mm_bt(q_h, k_rot) * scale, -1e30)
        exps = jnp.exp(scores - jnp.max(scores, axis=1, keepdims=True))
        probs_f = exps / jnp.sum(exps, axis=1, keepdims=True)
        probs = probs_f.astype(BF16)
        attn_v[:, cols] = mm(probs, v_val).astype(BF16)
        d_probs = mm_bt(da_h, v_val).astype(BF16).astype(F32)
        d_scores = (probs_f * (d_probs - jnp.sum(d_probs * probs_f, axis=1, keepdims=True)) * scale).astype(BF16)
        dq_h = mm(d_scores, k_rot).astype(BF16).astype(F32)
        first, second = rope(dq_h[:, 0:128], dq_h[:, 128:256], cos_v[...], -sin_v[...])
        dq_v[:, pl.ds(pl.multiple_of(h * head_dim, head_dim), 128)] = first.astype(BF16)
        dq_v[:, pl.ds(pl.multiple_of(h * head_dim + 128, 128), 128)] = second.astype(BF16)
        kv_acc[:, 0:256] += mm_at(d_scores, q_h)
        kv_acc[:, 256:512] += mm_at(probs, da_h)
        return carry

    lax.fori_loop(0, heads, head_step, 0)
    dkv_part[...] = kv_acc[...].astype(BF16)
    dkv_copy = remote(dkv_part, dkv_rx, ts.at[0], tr.at[0], other_ty)
    dkv_copy.start()
    for st in store_rows(2, attn_v, attn_hbm, pl.ds(0, q_width)) + store_rows(4, dq_v, dq_hbm, pl.ds(0, q_width)):
        st.start()
        stores.append(st)
    br_v[...] = mm(attn_v[...], wo_v[...])
    dh_v[...] = mm_bt(dq_v[...], wqkv_v[:, 0:q_width])

    def gather_copy(k, i):
        return remote(md.at[k, i, 0:half], md.at[k, i, half:n_tok], gs.at[3 * k + i], gr.at[3 * k + i], near)

    def dact_block(k, j):
        return B_DACT_LO + 2 * k + j if k < 2 else B_DACT_HI + 2 * (k - 2) + j

    def gated(k, want_act, want_grad):
        def step(r, carry):
            rows = pl.ds(pl.multiple_of(r * 16, 16), 16)
            for j in range(2):
                bg, bu, bd = B_GU + 4 * k + j, B_GU + 4 * k + 2 + j, dact_block(k, j)
                gate = (chip[bg, rows].astype(F32) + rx[bg, rows].astype(F32)).astype(BF16).astype(F32)
                up = (chip[bu, rows].astype(F32) + rx[bu, rows].astype(F32)).astype(BF16).astype(F32)
                sig = jax.nn.sigmoid(gate)
                silu = gate * sig
                cols = slice(j * BLK, (j + 1) * BLK)
                if want_act:
                    md[k, 0, rows, cols] = (silu * up).astype(BF16)
                if want_grad:
                    d_act = (chip[bd, rows].astype(F32) + rx[bd, rows].astype(F32)).astype(BF16).astype(F32)
                    md[k, 1, rows, cols] = (d_act * up * sig * (1.0 + gate * (1.0 - sig))).astype(BF16)
                    md[k, 2, rows, cols] = (d_act * silu).astype(BF16)
            return carry

        lax.fori_loop(0, half // 16, step, 0)
        for i in ((0,) if want_act else ()) + ((1, 2) if want_grad else ()):
            gather_copy(k, i).start()

    def md_store(k, i):
        for st in store_rows(8 + 6 * k + 2 * i, md.at[k, i], (act_hbm, dg_hbm, du_hbm)[i], pl.ds(k * CHUNK, CHUNK)):
            st.start()
            stores.append(st)

    def use_act(k):
        gather_copy(k, 0).wait_recv()
        md_store(k, 0)
        br_v[...] += mm(md[k, 0], wd_v[k * CHUNK:(k + 1) * CHUNK, :])

    def use_grad(k):
        for i in (1, 2):
            gather_copy(k, i).wait_recv()
            md_store(k, i)
        dh_v[...] += (mm_bt(md[k, 1], wg_v[:, k * CHUNK:(k + 1) * CHUNK])
                      + mm_bt(md[k, 2], wu_v[:, k * CHUNK:(k + 1) * CHUNK]))

    x_copy(2).wait_recv()
    x_copy(3).wait_recv()
    for k in range(2):
        x_copy(5 + k).wait_recv()
        gated(k, True, True)
        use_act(k)
        use_grad(k)
        if k == 0:
            dkv_copy.wait_recv()
            d_k = dkv_part[:, 0:256].astype(F32) + dkv_rx[:, 0:256].astype(F32)
            d_k = d_k.astype(BF16).astype(F32)
            first, second = rope(d_k[:, 0:128], d_k[:, 128:256], cos_v[...], -sin_v[...])
            dkv_v[:, 0:128] = first.astype(BF16)
            dkv_v[:, 128:256] = second.astype(BF16)
            dkv_v[:, 256:512] = (dkv_part[:, 256:512].astype(F32) + dkv_rx[:, 256:512].astype(F32)).astype(BF16)
            for st in store_rows(6, dkv_v, dkv_hbm, pl.ds(0, 512)):
                st.start()
                stores.append(st)
            kvdh_v[...] = mm_bt(dkv_v[...], wqkv_v[:, q_width:q_width + 512])
    for k in (2, 3):
        x_copy(5 + k).wait_recv()
        gated(k, True, False)
        use_act(k)
    y_snd[...] = br_v[...].astype(BF16)
    y_copy = remote(y_snd, y_rx, ts.at[1], tr.at[1], other_ty)
    y_copy.start()
    for k in (2, 3):
        x_copy(7 + k).wait_recv()
        gated(k, False, True)
        use_grad(k)
    dh_snd[...] = dh_v[...].astype(BF16)
    dh_copy = remote(dh_snd, dh_rx, ts.at[2], tr.at[2], other_ty)
    dh_copy.start()

    y_copy.wait_recv()
    y_o[...] = (x_v[...].astype(F32) + (y_snd[...].astype(F32) + y_rx[...].astype(F32))).astype(BF16)
    for st in store_rows(32, y_o, y_hbm, pl.ds(0, x_v.shape[1])):
        st.start()
        stores.append(st)

    dh_copy.wait_recv()
    d_nrm = (dh_snd[...].astype(F32) + dh_rx[...].astype(F32)) + kvdh_v[...]
    dh_v[...] = d_nrm
    d_hat = d_nrm * gamma_ref[...]
    x_hat = xhat_v[...]
    dgamma_ref[...] = jnp.sum(d_nrm * x_hat, axis=0, keepdims=True)
    stats_start(bst_snd, bst_rx, 1, jnp.sum(d_hat, axis=1, keepdims=True), jnp.sum(d_hat * x_hat, axis=1, keepdims=True))
    sum_d, sum_dx = stats_finish(bst_snd, bst_rx, 1)
    d_hat = dh_v[...] * gamma_ref[...]
    d_x = dy_v[...].astype(F32) + inv_v[:, 0:1] * (d_hat - sum_d / d_model - xhat_v[...] * (sum_dx / d_model))
    dx_o[...] = d_x.astype(BF16)
    for st in store_rows(34, dx_o, dx_hbm, pl.ds(0, x_v.shape[1])):
        st.start()
        stores.append(st)

    def drain(b, carry):
        core_copy(b).wait_send()
        return carry

    lax.fori_loop(0, N_BLK, drain, 0)
    for u in range(len(X_UNITS)):
        x_copy(u).wait_send()
    for k in range(4):
        for i in range(3):
            gather_copy(k, i).wait_send()
    for copy in (packed_copy, dkv_copy, y_copy, dh_copy):
        copy.wait_send()
    for i in range(3):
        stats_copy(st_snd, st_rx, 0, i).wait_send()
        stats_copy(bst_snd, bst_rx, 1, i).wait_send()
    for st in stores:
        st.wait()


def grad_kernel(nrm_hbm, attn_hbm, act_hbm, dq_hbm, dkv_hbm, dg_hbm, du_hbm, dy_hbm, y_in, dx_in, dgamma_in,
                y_hbm, dx_hbm, dgamma_ref, dwq_hbm, dwg_hbm, dwu_hbm, dwk_hbm, dwv_hbm, dwo_hbm, dwd_hbm,
                nrm_v, nrm_t, attn_v, act_v, dq_v, dkv_v, dg_v, du_v, dy_v, y_v, dx_v, ring, ld_sem, out_sem, cp_sem):
    width = nrm_v.shape[1]
    n_ring = ring.shape[0]

    def load(i, src, dst):
        return pltpu.make_async_copy(src, dst, ld_sem.at[i])

    pairs = [(nrm_hbm, nrm_v), (dq_hbm, dq_v), (dkv_hbm, dkv_v), (dg_hbm, dg_v), (du_hbm, du_v), (dy_hbm, dy_v), (attn_hbm, attn_v), (act_hbm, act_v)]
    loads = [load(i, src, dst) for i, (src, dst) in enumerate(pairs)]
    for ld in loads:
        ld.start()
    hand_in = [load(8, y_in, y_v), load(9, dx_in, dx_v)]
    for ld in hand_in:
        ld.start()
    dgamma_ref[...] = dgamma_in[...]

    def tile_copy(slot, dst):
        return pltpu.make_async_copy(ring.at[slot], dst, out_sem.at[slot])

    def emit(t, value, dst):
        slot = lax.rem(t, n_ring)

        @pl.when(t >= n_ring)
        def _():
            tile_copy(slot, dwq_hbm.at[:, 0:BLK]).wait()

        ring[slot] = value
        tile_copy(slot, dst).start()

    loads[0].wait()
    nrm_t[...] = nrm_v[...].T

    def columns(base, count, grads, out):
        def step(j, carry):
            cols = pl.ds(pl.multiple_of(j * BLK, BLK), BLK)
            emit(base + j, mm(nrm_t[...], grads[:, cols]), out.at[:, cols])
            return carry

        lax.fori_loop(0, count, step, 0)

    def rows(base, count, acts, out):
        def step(j, carry):
            at = pl.ds(pl.multiple_of(j * width, width), width)
            emit(base + j, mm_at(acts[:, at], dy_v[...]), out.at[at, :])
            return carry

        lax.fori_loop(0, count, step, 0)

    t = 0
    n_q, n_f = dq_v.shape[1] // BLK, dg_v.shape[1] // BLK
    loads[1].wait()
    columns(t, n_q, dq_v, dwq_hbm)
    t += n_q
    loads[3].wait()
    columns(t, n_f, dg_v, dwg_hbm)
    t += n_f
    loads[4].wait()
    columns(t, n_f, du_v, dwu_hbm)
    t += n_f
    loads[5].wait()
    loads[6].wait()
    rows(t, n_q, attn_v, dwo_hbm)
    t += n_q
    loads[7].wait()
    rows(t, n_f, act_v, dwd_hbm)
    t += n_f
    loads[2].wait()
    for ld in hand_in:
        ld.wait()
    hand_out = [pltpu.make_async_copy(y_v, y_hbm, cp_sem.at[0]), pltpu.make_async_copy(dx_v, dx_hbm, cp_sem.at[1])]
    for cp in hand_out:
        cp.start()
    slot = t % n_ring
    tile_copy(slot, dwq_hbm.at[:, 0:BLK]).wait()
    ring[slot] = mm(nrm_t[...], dkv_v[...])
    kv_out = [pltpu.make_async_copy(ring.at[slot, :, 0:256], dwk_hbm, cp_sem.at[2]),
              pltpu.make_async_copy(ring.at[slot, :, 256:512], dwv_hbm, cp_sem.at[3])]
    for cp in kv_out:
        cp.start()
    for i in range(1, n_ring):
        tile_copy((t + i) % n_ring, dwq_hbm.at[:, 0:BLK]).wait()
    for cp in hand_out + kv_out:
        cp.wait()


def solution(mesh):
    tx_size = mesh.shape['tx']
    tok_spec = P('dp', None, 'tx')
    in_specs = (tok_spec, P('dp', None), tok_spec, P('tx'), P('tx', 'ty'), P('tx', 'ty'), P('tx', 'ty'),
                P('tx', None), P('tx', None), P('ty', 'tx'), P('ty', 'tx'))
    out_specs = (tok_spec, tok_spec, P(('dp', 'tx')), P(('dp', 'tx'), 'ty'), P(('dp', 'tx'), 'ty'), P(('dp', 'tx'), 'ty'),
                 P(('dp', 'tx'), None), P(('dp', 'tx'), None), P(('dp', 'ty'), 'tx'), P(('dp', 'ty'), 'tx'))

    def local_layer(x_in, positions, d_y, ln_gamma, w_q, w_g, w_u, w_k, w_v, w_o, w_d):
        _, n_tok, d_local = x_in.shape
        half = n_tok // 2
        d_model = d_local * tx_size
        head_dim = w_k.shape[1]
        q_width = w_q.shape[1]
        d_ff = w_g.shape[1]
        freq = jnp.asarray((ROPE_BASE ** (-2.0 * np.arange(head_dim // 2) / head_dim)).astype(np.float32)[None])
        any_spec = pl.BlockSpec(memory_space=pl.ANY)
        vmem_spec = pl.BlockSpec(memory_space=pltpu.VMEM)
        tok = (n_tok, d_local)
        sem = pltpu.SemaphoreType.DMA
        y_loc, dx_loc, d_gamma, normed, attn_flat, act, d_q, d_kv, d_gate, d_up = pl.pallas_call(
            functools.partial(layer_kernel, d_model),
            out_shape=[jax.ShapeDtypeStruct(tok, BF16), jax.ShapeDtypeStruct(tok, BF16), jax.ShapeDtypeStruct((1, d_local), F32),
                       jax.ShapeDtypeStruct(tok, BF16), jax.ShapeDtypeStruct((n_tok, q_width), BF16),
                       jax.ShapeDtypeStruct((n_tok, d_ff), BF16), jax.ShapeDtypeStruct((n_tok, q_width), BF16),
                       jax.ShapeDtypeStruct((n_tok, 2 * head_dim), BF16), jax.ShapeDtypeStruct((n_tok, d_ff), BF16),
                       jax.ShapeDtypeStruct((n_tok, d_ff), BF16)],
            in_specs=[any_spec, vmem_spec, vmem_spec, any_spec, vmem_spec] + [any_spec] * 7,
            out_specs=[any_spec, any_spec, vmem_spec] + [any_spec] * 7,
            scratch_shapes=[
                pltpu.VMEM(tok, BF16), pltpu.VMEM(tok, BF16), pltpu.VMEM((d_local, q_width + 2 * head_dim), BF16),
                pltpu.VMEM((d_local, d_ff), BF16), pltpu.VMEM((d_local, d_ff), BF16), pltpu.VMEM((q_width, d_local), BF16),
                pltpu.VMEM((d_ff, d_local), BF16),
                pltpu.VMEM((N_BLK, half, BLK), F32), pltpu.VMEM((N_BLK, half, BLK), BF16), pltpu.VMEM((N_BLK, half, BLK), BF16),
                pltpu.VMEM((N_BLK, half, BLK), BF16), pltpu.VMEM((N_BLK, half, BLK), BF16),
                pltpu.VMEM((4, 3, n_tok, CHUNK), BF16), pltpu.VMEM((n_tok, 2 * q_width + 2 * head_dim), BF16),
                pltpu.VMEM((n_tok, q_width), BF16), pltpu.VMEM((n_tok, q_width), BF16),
                pltpu.VMEM((n_tok, 512), BF16), pltpu.VMEM((n_tok, 512), BF16), pltpu.VMEM((n_tok, 512), BF16),
                pltpu.VMEM((n_tok, 512), F32),
                pltpu.VMEM(tok, BF16), pltpu.VMEM(tok, F32), pltpu.VMEM((n_tok, 128), F32), pltpu.VMEM((n_tok, 128), F32),
                pltpu.VMEM((n_tok, 128), F32), pltpu.VMEM(tok, F32), pltpu.VMEM(tok, F32), pltpu.VMEM(tok, F32),
                pltpu.VMEM(tok, BF16), pltpu.VMEM(tok, BF16), pltpu.VMEM(tok, BF16), pltpu.VMEM(tok, BF16),
                pltpu.VMEM(tok, BF16), pltpu.VMEM(tok, BF16),
                pltpu.VMEM((8, n_tok), F32), pltpu.VMEM((3, 8, n_tok), F32), pltpu.VMEM((8, n_tok), F32), pltpu.VMEM((3, 8, n_tok), F32),
                sem((12,)), sem((36,)), sem((N_BLK,)), sem((N_BLK,)), sem((len(X_UNITS),)), sem((len(X_UNITS),)),
                sem((12,)), sem((12,)), sem((1,)), sem((1,)), sem((3,)), sem((3,)), sem((6,)), sem((6,))],
            compiler_params=pltpu.CompilerParams(collective_id=0, has_side_effects=True, vmem_limit_bytes=67043328),
            name='layer',
        )(x_in.reshape(tok), positions, freq, d_y.reshape(tok), ln_gamma[None], w_q, w_g, w_u, w_k, w_v, w_o, w_d)

        vm = pltpu.VMEM
        y_out, d_x, d_gamma, d_wq, d_wg, d_wu, d_wk, d_wv, d_wo, d_wd = pl.pallas_call(
            grad_kernel,
            out_shape=[jax.ShapeDtypeStruct(tok, BF16), jax.ShapeDtypeStruct(tok, BF16), jax.ShapeDtypeStruct((1, d_local), F32)]
            + [jax.ShapeDtypeStruct(w.shape, F32) for w in (w_q, w_g, w_u, w_k, w_v, w_o, w_d)],
            in_specs=[any_spec] * 10 + [vmem_spec],
            out_specs=[any_spec, any_spec, vmem_spec] + [any_spec] * 7,
            scratch_shapes=[vm(tok, BF16), vm((d_local, n_tok), BF16), vm((n_tok, q_width), BF16), vm((n_tok, d_ff), BF16),
                            vm((n_tok, q_width), BF16), vm((n_tok, 2 * head_dim), BF16), vm((n_tok, d_ff), BF16), vm((n_tok, d_ff), BF16),
                            vm(tok, BF16), vm(tok, BF16), vm(tok, BF16), vm((8, d_local, BLK), F32), sem((10,)), sem((8,)), sem((4,))],
            compiler_params=pltpu.CompilerParams(vmem_limit_bytes=60 * 1024 * 1024),
            name='weight_grads',
        )(normed, attn_flat, act, d_q, d_kv, d_gate, d_up, d_y.reshape(tok), y_loc, dx_loc, d_gamma)
        return (y_out.reshape(x_in.shape), d_x.reshape(x_in.shape), d_gamma.reshape(d_local),
                d_wq, d_wg, d_wu, d_wk, d_wv, d_wo, d_wd)

    return jax.shard_map(local_layer, mesh=mesh, in_specs=in_specs, out_specs=out_specs, check_vma=False)
```

```python
import functools

import jax
import jax.numpy as jnp
import numpy as np
from jax import lax
from jax.experimental import pallas as pl
from jax.experimental.pallas import tpu as pltpu
from jax.sharding import PartitionSpec as P

EPS = 1e-6
ROPE_BASE = 10000.0
F32 = jnp.float32
BF16 = jnp.bfloat16
MESH = pl.DeviceIdType.MESH

BLK = 512
CHUNK = 1024
B_DATTN, B_DACT_LO, B_QKV, B_GU, B_DACT_HI, N_BLK = 0, 2, 6, 9, 25, 29
X_UNITS = ((0, 1), (1, 1), (2, 2), (4, 2), (6, 2), (9, 4), (13, 4), (17, 4), (21, 4), (25, 2))
SPLITS = 4
X_KV = len(X_UNITS)
X_LAST = X_KV + 1
N_X = X_LAST + SPLITS


def dot(a, b, dims):
    return lax.dot_general(a, b, (dims, ((), ())), preferred_element_type=F32)


def mm(a, b):
    return dot(a, b, ((1,), (0,)))


def mm_bt(a, b):
    return dot(a, b, ((1,), (1,)))


def mm_at(a, b):
    return dot(a, b, ((0,), (0,)))


def rope(first, second, cos_t, sin_t):
    return first * cos_t - second * sin_t, second * cos_t + first * sin_t


def layer_kernel(d_model, x_hbm, pos_ref, freq_ref, dy_hbm, gamma_ref, wq_hbm, wg_hbm, wu_hbm, wk_hbm, wv_hbm, wo_hbm, wd_hbm,
                 y_hbm, dx_hbm, dgamma_ref, nrm_hbm, attn_hbm, act_hbm, dq_hbm, dkv_hbm, dg_hbm, du_hbm,
                 x_v, dy_v, wqkv_v, wg_v, wu_v, wo_v, wd_v,
                 keep, send, rcore, chip, rx, md, packed, attn_v, dq_v, dkv_part, dkv_rx, dkv_v, kv_acc,
                 nrm_v, xhat_v, inv_v, cos_v, sin_v, br_v, dh_v, y_snd, y_rx, dh_snd, dh_rx, y_o, dx_o,
                 st_snd, st_rx, st_sum, bst_snd, bst_rx,
                 ld_sem, st_sem, cs, cr, xs, xr, gs, gr, ps, pr, ts, tr, ss, sr, ds, dr):
    tx = lax.axis_index('tx')
    ty = lax.axis_index('ty')
    core = lax.rem(tx, 2)
    near = {'tx': tx + 1 - 2 * core}
    across = {'tx': lax.rem(tx + 2, 4)}
    far = {'tx': lax.rem(tx + 1 - 2 * core + 2, 4)}
    other_ty = {'ty': 1 - ty}
    peers = [near, across, far, other_ty] + [{'tx': p['tx'], 'ty': 1 - ty} for p in (near, across, far)]
    n_tok = x_v.shape[0]
    half = n_tok // 2
    mine = pl.multiple_of(core * half, half)
    other = pl.multiple_of((1 - core) * half, half)
    head_dim = 256
    q_width = wo_v.shape[0]
    heads = q_width // head_dim
    piece = half // SPLITS

    def load(i, src, dst):
        return pltpu.make_async_copy(src, dst, ld_sem.at[i])

    d_half = wd_v.shape[0] // 2
    loads = [
        load(0, dy_hbm.at[pl.ds(mine, half)], dy_v.at[0:half]),
        load(1, dy_hbm.at[pl.ds(other, half)], dy_v.at[half:n_tok]),
        load(2, wo_hbm, wo_v),
        load(3, x_hbm.at[pl.ds(mine, half)], x_v.at[0:half]),
        load(4, x_hbm.at[pl.ds(other, half)], x_v.at[half:n_tok]),
        load(5, wd_hbm.at[0:d_half], wd_v.at[0:d_half]),
        load(6, wq_hbm, wqkv_v.at[:, 0:q_width]),
        load(7, wk_hbm, wqkv_v.at[:, q_width:q_width + head_dim]),
        load(8, wv_hbm, wqkv_v.at[:, q_width + head_dim:q_width + 2 * head_dim]),
        load(9, wg_hbm, wg_v),
        load(10, wu_hbm, wu_v),
        load(11, wd_hbm.at[d_half:2 * d_half], wd_v.at[d_half:2 * d_half]),
    ]
    for ld in loads[:5]:
        ld.start()

    barrier = pltpu.get_barrier_semaphore()
    for peer in peers:
        pl.semaphore_signal(barrier, inc=1, device_id=peer, device_id_type=MESH)
    for ld in loads[:3]:
        ld.wait()
    for ld in loads[5:]:
        ld.start()
    pl.semaphore_wait(barrier, len(peers))

    def remote(src, dst, send_sem, recv_sem, peer):
        return pltpu.make_async_remote_copy(src_ref=src, dst_ref=dst, send_sem=send_sem, recv_sem=recv_sem,
                                            device_id=peer, device_id_type=MESH)

    def core_copy(b):
        return remote(send.at[b], rcore.at[b], cs.at[b], cr.at[b], near)

    def x_copy(u):
        if u >= X_LAST:
            rows = pl.ds((u - X_LAST) * piece, piece)
            return remote(chip.at[pl.ds(N_BLK - 2, 2), rows], rx.at[pl.ds(N_BLK - 2, 2), rows], xs.at[u], xr.at[u], across)
        if u == X_KV:
            cols = pl.ds(pl.multiple_of(ty * head_dim, head_dim), head_dim)
            return remote(chip.at[B_QKV + 2, :, cols], rx.at[B_QKV + 2, :, cols], xs.at[u], xr.at[u], across)
        start, count = X_UNITS[u]
        return remote(chip.at[pl.ds(start, count)], rx.at[pl.ds(start, count)], xs.at[u], xr.at[u], across)

    def put(b, part):
        keep[b] = part[:half]
        send[b] = part[half:].astype(BF16)
        core_copy(b).start()

    def issue_bwd(b, w_ref, row):
        put(b, mm_bt(dy_v[...], w_ref[pl.ds(row, BLK), :]))

    def issue_fwd(b, w_ref, col):
        put(b, mm(nrm_v[...], w_ref[:, pl.ds(col, BLK)]))

    def combine(b):
        core_copy(b).wait_recv()
        chip[b] = (keep[b] + rcore[b].astype(F32)).astype(BF16)

    def total(b):
        return chip[b].astype(F32) + rx[b].astype(F32)

    issue_bwd(0, wo_v, 0)
    issue_bwd(1, wo_v, BLK)

    def rows_of(col_a, col_b):
        lane = lax.broadcasted_iota(jnp.int32, (half, 128), 1)
        return jnp.where(lane == 0, col_a, col_b).T[0:8]

    def stats_copies(snd, got, base, to):
        return [remote(snd, got.at[i], ss.at[base + i], sr.at[base + i], peer) for i, peer in enumerate(to)]

    def stats_put(snd, col_a, col_b):
        for lo, at in ((0, mine), (half, other)):
            snd[:, pl.ds(at, half)] = rows_of(col_a[lo:lo + half], col_b[lo:lo + half])

    def stats_columns(rows_ref):
        cols = []
        for i in range(2):
            parts = [jnp.broadcast_to(rows_ref[i:i + 1, pl.ds(at, half)], (128, half)).T[:, 0:1] for at in (mine, other)]
            cols.append(jnp.concatenate(parts, axis=0))
        return cols

    loads[3].wait()
    loads[4].wait()
    x_f = x_v[...].astype(F32)
    stats_put(st_snd, jnp.sum(x_f, axis=1, keepdims=True), jnp.sum(x_f * x_f, axis=1, keepdims=True))
    fwd_stats = stats_copies(st_snd, st_rx, 0, (near, across, far))
    for copy in fwd_stats:
        copy.start()

    combine(0)
    x_copy(0).start()
    combine(1)
    x_copy(1).start()

    loads[5].wait()
    for i in range(4):
        issue_bwd(B_DACT_LO + i, wd_v, i * BLK)
        if i >= 1:
            combine(B_DACT_LO + i - 1)
        if i == 2:
            x_copy(2).start()
    combine(B_DACT_LO + 3)
    x_copy(3).start()

    for copy in fwd_stats:
        copy.wait_recv()
    st_sum[...] = (st_snd[...] + st_rx[0]) + (st_rx[1] + st_rx[2])
    sum_x, sum_xx = stats_columns(st_sum)
    tok_mean = sum_x / d_model
    inv_std = lax.rsqrt(sum_xx / d_model - tok_mean * tok_mean + EPS)
    inv_v[...] = jnp.broadcast_to(inv_std, (n_tok, 128))
    x_hat = (x_v[...].astype(F32) - tok_mean) * inv_std
    xhat_v[...] = x_hat
    nrm_v[...] = (x_hat * gamma_ref[...]).astype(BF16)

    for i in range(6, 9):
        loads[i].wait()
    for i in range(3):
        issue_fwd(B_QKV + i, wqkv_v, i * BLK)
    for i in (2, 0, 1):
        combine(B_QKV + i)
        if i == 2:
            x_copy(X_KV).start()
    x_copy(4).start()

    loads[9].wait()
    loads[10].wait()
    for k in range(4):
        def gu_issue(j, carry, k=k):
            col = pl.multiple_of(k * CHUNK + j * BLK, BLK)
            issue_fwd(B_GU + 4 * k + j, wg_v, col)
            issue_fwd(B_GU + 4 * k + 2 + j, wu_v, col)
            return carry

        def gu_combine(j, carry, k=k):
            combine(B_GU + 4 * k + j)
            return carry

        lax.fori_loop(0, 2, gu_issue, 0)
        lax.fori_loop(0, 4, gu_combine, 0)
        x_copy(5 + k).start()

    loads[11].wait()

    def hi_issue(j, carry):
        issue_bwd(B_DACT_HI + j, wd_v, pl.multiple_of(d_half + j * BLK, BLK))
        return carry

    lax.fori_loop(0, 4, hi_issue, 0)
    for j in range(4):
        combine(B_DACT_HI + j)
        if j == 1:
            x_copy(9).start()
    for r in range(SPLITS):
        x_copy(X_LAST + r).start()

    freq = freq_ref[...]
    for lo, at in ((0, mine), (half, other)):
        pos_col = jnp.broadcast_to(pos_ref[0:1, pl.ds(at, half)].astype(F32), (128, half)).T
        angles = pos_col * freq
        cos_v[lo:lo + half] = jnp.cos(angles)
        sin_v[lo:lo + half] = jnp.sin(angles)

    def store(i, src, dst):
        return pltpu.make_async_copy(src, dst, st_sem.at[i])

    def store_rows(i, src, dst, cols):
        return [store(i, src.at[0:half], dst.at[pl.ds(mine, half), cols]),
                store(i + 1, src.at[half:n_tok], dst.at[pl.ds(other, half), cols])]

    stores = store_rows(0, nrm_v, nrm_hbm, pl.ds(0, x_v.shape[1]))
    for st in stores:
        st.start()

    packed_copy = remote(packed.at[0:half], packed.at[half:n_tok], ps.at[0], pr.at[0], near)
    x_copy(0).wait_recv()
    x_copy(1).wait_recv()
    for j in range(2):
        packed[0:half, q_width + 512 + j * BLK:q_width + 512 + (j + 1) * BLK] = total(B_DATTN + j).astype(BF16)
    x_copy(4).wait_recv()
    cos_h, sin_h = cos_v[0:half], sin_v[0:half]
    for j in range(2):
        blk = total(B_QKV + j)
        for h in range(2):
            lo = h * head_dim
            first, second = rope(blk[:, lo:lo + 128], blk[:, lo + 128:lo + 256], cos_h, sin_h)
            packed[0:half, j * BLK + lo:j * BLK + lo + 128] = first.astype(BF16)
            packed[0:half, j * BLK + lo + 128:j * BLK + lo + 256] = second.astype(BF16)
    x_copy(X_KV).wait_recv()
    kv_cols = pl.ds(pl.multiple_of(ty * head_dim, head_dim), head_dim)
    blk = chip[B_QKV + 2, :, kv_cols].astype(F32) + rx[B_QKV + 2, :, kv_cols].astype(F32)
    first, second = rope(blk[:, 0:128], blk[:, 128:256], cos_h, sin_h)
    kv_mine = jnp.where(ty == 0, jnp.concatenate([first, second], axis=1), blk).astype(BF16)
    kv_dst = packed.at[0:half, pl.ds(pl.multiple_of(q_width + ty * head_dim, head_dim), head_dim)]
    kv_dst[...] = kv_mine
    kv_copy = remote(kv_dst, kv_dst, ts.at[3], tr.at[3], other_ty)
    kv_copy.start()
    kv_copy.wait_recv()
    packed_copy.start()
    packed_copy.wait_recv()

    row_i = lax.rem(lax.broadcasted_iota(jnp.int32, (n_tok, n_tok), 0) + core * half, n_tok)
    col_i = lax.rem(lax.broadcasted_iota(jnp.int32, (n_tok, n_tok), 1) + core * half, n_tok)
    scale = head_dim ** -0.5
    kv_acc[...] = jnp.zeros_like(kv_acc)

    def head_step(h, carry):
        cols = pl.ds(pl.multiple_of(h * head_dim, head_dim), head_dim)
        q_h = packed[:, cols]
        da_h = packed[:, pl.ds(pl.multiple_of(q_width + 512 + h * head_dim, head_dim), head_dim)]
        k_rot = packed[:, q_width:q_width + 256]
        v_val = packed[:, q_width + 256:q_width + 512]
        scores = jnp.where(row_i >= col_i, mm_bt(q_h, k_rot) * scale, -1e30)
        exps = jnp.exp(scores - jnp.max(scores, axis=1, keepdims=True))
        probs_f = exps / jnp.sum(exps, axis=1, keepdims=True)
        probs = probs_f.astype(BF16)
        attn_v[:, cols] = mm(probs, v_val).astype(BF16)
        d_probs = mm_bt(da_h, v_val).astype(BF16).astype(F32)
        d_scores = (probs_f * (d_probs - jnp.sum(d_probs * probs_f, axis=1, keepdims=True)) * scale).astype(BF16)
        dq_h = mm(d_scores, k_rot).astype(BF16).astype(F32)
        first, second = rope(dq_h[:, 0:128], dq_h[:, 128:256], cos_v[...], -sin_v[...])
        dq_v[:, pl.ds(pl.multiple_of(h * head_dim, head_dim), 128)] = first.astype(BF16)
        dq_v[:, pl.ds(pl.multiple_of(h * head_dim + 128, 128), 128)] = second.astype(BF16)
        kv_acc[:, 0:256] += mm_at(d_scores, q_h)
        kv_acc[:, 256:512] += mm_at(probs, da_h)
        return carry

    lax.fori_loop(0, heads, head_step, 0)
    dkv_part[...] = kv_acc[...].astype(BF16)
    dkv_copy = remote(dkv_part, dkv_rx, ts.at[0], tr.at[0], other_ty)
    dkv_copy.start()
    for st in store_rows(2, attn_v, attn_hbm, pl.ds(0, q_width)) + store_rows(4, dq_v, dq_hbm, pl.ds(0, q_width)):
        st.start()
        stores.append(st)
    br_v[...] = mm(attn_v[...], wo_v[...])
    dh_v[...] = mm_bt(dq_v[...], wqkv_v[:, 0:q_width])

    def piece_copy(r, i):
        at = 12 + 2 * r + i - 1
        return remote(md.at[3, i, r * piece:(r + 1) * piece], md.at[3, i, half + r * piece:half + (r + 1) * piece], gs.at[at], gr.at[at], near)

    def gather_copy(k, i):
        return remote(md.at[k, i, 0:half], md.at[k, i, half:n_tok], gs.at[3 * k + i], gr.at[3 * k + i], near)

    def dact_block(k, j):
        return B_DACT_LO + 2 * k + j if k < 2 else B_DACT_HI + 2 * (k - 2) + j

    def gated(k, want_act, want_grad, lo=0, hi=None):
        def step(r, carry):
            rows = pl.ds(pl.multiple_of(r * 16, 16), 16)
            for j in range(2):
                bg, bu, bd = B_GU + 4 * k + j, B_GU + 4 * k + 2 + j, dact_block(k, j)
                gate = (chip[bg, rows].astype(F32) + rx[bg, rows].astype(F32)).astype(BF16).astype(F32)
                up = (chip[bu, rows].astype(F32) + rx[bu, rows].astype(F32)).astype(BF16).astype(F32)
                sig = jax.nn.sigmoid(gate)
                silu = gate * sig
                cols = slice(j * BLK, (j + 1) * BLK)
                if want_act:
                    md[k, 0, rows, cols] = (silu * up).astype(BF16)
                if want_grad:
                    d_act = (chip[bd, rows].astype(F32) + rx[bd, rows].astype(F32)).astype(BF16).astype(F32)
                    md[k, 1, rows, cols] = (d_act * up * sig * (1.0 + gate * (1.0 - sig))).astype(BF16)
                    md[k, 2, rows, cols] = (d_act * silu).astype(BF16)
            return carry

        lax.fori_loop(lo // 16, (half if hi is None else hi) // 16, step, 0)
        if hi is None:
            for i in ((0,) if want_act else ()) + ((1, 2) if want_grad else ()):
                gather_copy(k, i).start()

    def md_store(k, i):
        for st in store_rows(8 + 6 * k + 2 * i, md.at[k, i], (act_hbm, dg_hbm, du_hbm)[i], pl.ds(k * CHUNK, CHUNK)):
            st.start()
            stores.append(st)

    def use_act(k):
        gather_copy(k, 0).wait_recv()
        md_store(k, 0)
        br_v[...] += mm(md[k, 0], wd_v[k * CHUNK:(k + 1) * CHUNK, :])

    def use_grad(k):
        for i in (1, 2):
            gather_copy(k, i).wait_recv()
            md_store(k, i)
        dh_v[...] += (mm_bt(md[k, 1], wg_v[:, k * CHUNK:(k + 1) * CHUNK])
                      + mm_bt(md[k, 2], wu_v[:, k * CHUNK:(k + 1) * CHUNK]))

    x_copy(2).wait_recv()
    x_copy(3).wait_recv()
    for k in range(2):
        x_copy(5 + k).wait_recv()
        gated(k, True, True)
        use_act(k)
        use_grad(k)
        if k == 0:
            dkv_copy.wait_recv()
            d_k = dkv_part[:, 0:256].astype(F32) + dkv_rx[:, 0:256].astype(F32)
            d_k = d_k.astype(BF16).astype(F32)
            first, second = rope(d_k[:, 0:128], d_k[:, 128:256], cos_v[...], -sin_v[...])
            dkv_v[:, 0:128] = first.astype(BF16)
            dkv_v[:, 128:256] = second.astype(BF16)
            dkv_v[:, 256:512] = (dkv_part[:, 256:512].astype(F32) + dkv_rx[:, 256:512].astype(F32)).astype(BF16)
            for st in store_rows(6, dkv_v, dkv_hbm, pl.ds(0, 512)):
                st.start()
                stores.append(st)
            dh_v[...] += 0.5 * mm_bt(dkv_v[...], wqkv_v[:, q_width:q_width + 512])
    for k in (2, 3):
        x_copy(5 + k).wait_recv()
        gated(k, True, False)
        use_act(k)
    y_snd[...] = br_v[...].astype(BF16)
    y_copy = remote(y_snd, y_rx, ts.at[1], tr.at[1], other_ty)
    y_copy.start()
    x_copy(9).wait_recv()
    gated(2, False, True)
    use_grad(2)

    def dh_copy(r):
        return remote(dh_snd.at[r], dh_rx.at[r], ds.at[r], dr.at[r], other_ty)

    def both(ref, r):
        return jnp.concatenate([ref[r * piece:(r + 1) * piece], ref[half + r * piece:half + (r + 1) * piece]], axis=0)

    sums = []

    def piece_grad(r):
        x_copy(X_LAST + r).wait_recv()
        gated(3, False, True, r * piece, (r + 1) * piece)
        for i in (1, 2):
            piece_copy(r, i).start()

    def piece_dh(r):
        for i in (1, 2):
            piece_copy(r, i).wait_recv()
        part = both(dh_v, r) + mm_bt(both(md.at[3, 1], r), wg_v[:, 3 * CHUNK:4 * CHUNK]) + mm_bt(both(md.at[3, 2], r), wu_v[:, 3 * CHUNK:4 * CHUNK])
        part_b = part.astype(BF16)
        dh_snd[r] = part_b
        dh_copy(r).start()
        d_hat = part_b.astype(F32) * gamma_ref[...]
        sums.append((jnp.sum(d_hat, axis=1, keepdims=True), jnp.sum(d_hat * both(xhat_v, r), axis=1, keepdims=True)))

    for r in range(SPLITS):
        piece_grad(r)
        piece_dh(r)
    cols = [jnp.concatenate([sums[r][i][:piece] for r in range(SPLITS)] + [sums[r][i][piece:] for r in range(SPLITS)], axis=0) for i in range(2)]
    stats_put(bst_snd, cols[0], cols[1])
    bwd_stats = stats_copies(bst_snd, bst_rx, 3, peers)
    for copy in bwd_stats:
        copy.start()
    md_store(3, 1)
    md_store(3, 2)

    y_copy.wait_recv()
    y_o[...] = (x_v[...].astype(F32) + (y_snd[...].astype(F32) + y_rx[...].astype(F32))).astype(BF16)
    for st in store_rows(32, y_o, y_hbm, pl.ds(0, x_v.shape[1])):
        st.start()
        stores.append(st)

    d_gamma = jnp.zeros_like(dgamma_ref)
    for r in range(SPLITS):
        dh_copy(r).wait_recv()
        d_nrm = dh_snd[r].astype(F32) + dh_rx[r].astype(F32)
        d_gamma = d_gamma + jnp.sum(d_nrm * both(xhat_v, r), axis=0, keepdims=True)
        dh_v[r * piece:(r + 1) * piece] = d_nrm[:piece]
        dh_v[half + r * piece:half + (r + 1) * piece] = d_nrm[piece:]
    dgamma_ref[...] = d_gamma
    for copy in bwd_stats:
        copy.wait_recv()
    st_sum[...] = ((bst_snd[...] + bst_rx[0]) + (bst_rx[1] + bst_rx[2])) + ((bst_rx[3] + bst_rx[4]) + (bst_rx[5] + bst_rx[6]))
    sum_d, sum_dx = stats_columns(st_sum)
    d_hat = dh_v[...] * gamma_ref[...]
    d_x = dy_v[...].astype(F32) + inv_v[:, 0:1] * (d_hat - sum_d / d_model - xhat_v[...] * (sum_dx / d_model))
    dx_o[...] = d_x.astype(BF16)
    for st in store_rows(34, dx_o, dx_hbm, pl.ds(0, x_v.shape[1])):
        st.start()
        stores.append(st)

    def drain(b, carry):
        core_copy(b).wait_send()
        return carry

    lax.fori_loop(0, N_BLK, drain, 0)
    for u in range(N_X):
        x_copy(u).wait_send()
    for k in range(4):
        for i in range(3 if k < 3 else 1):
            gather_copy(k, i).wait_send()
    for r in range(SPLITS):
        for i in (1, 2):
            piece_copy(r, i).wait_send()
        dh_copy(r).wait_send()
    for copy in [packed_copy, dkv_copy, y_copy, kv_copy] + fwd_stats + bwd_stats:
        copy.wait_send()
    for st in stores:
        st.wait()


def grad_kernel(nrm_hbm, attn_hbm, act_hbm, dq_hbm, dkv_hbm, dg_hbm, du_hbm, dy_hbm, y_in, dx_in, dgamma_in,
                y_hbm, dx_hbm, dgamma_ref, dwq_hbm, dwg_hbm, dwu_hbm, dwk_hbm, dwv_hbm, dwo_hbm, dwd_hbm,
                nrm_v, nrm_t, attn_v, act_v, dq_v, dkv_v, dg_v, du_v, dy_v, y_v, dx_v, ring, ld_sem, out_sem, cp_sem):
    width = nrm_v.shape[1]
    n_ring = ring.shape[0]

    def load(i, src, dst):
        return pltpu.make_async_copy(src, dst, ld_sem.at[i])

    pairs = [(nrm_hbm, nrm_v), (dq_hbm, dq_v), (dkv_hbm, dkv_v), (dg_hbm, dg_v), (du_hbm, du_v), (dy_hbm, dy_v), (attn_hbm, attn_v), (act_hbm, act_v)]
    loads = [load(i, src, dst) for i, (src, dst) in enumerate(pairs)]
    for ld in loads:
        ld.start()
    hand_in = [load(8, y_in, y_v), load(9, dx_in, dx_v)]
    for ld in hand_in:
        ld.start()
    dgamma_ref[...] = dgamma_in[...]

    def tile_copy(slot, dst):
        return pltpu.make_async_copy(ring.at[slot], dst, out_sem.at[slot])

    def emit(t, value, dst):
        slot = lax.rem(t, n_ring)

        @pl.when(t >= n_ring)
        def _():
            tile_copy(slot, dwq_hbm.at[:, 0:BLK]).wait()

        ring[slot] = value
        tile_copy(slot, dst).start()

    loads[0].wait()
    nrm_t[...] = nrm_v[...].T

    def columns(base, count, grads, out):
        def step(j, carry):
            cols = pl.ds(pl.multiple_of(j * BLK, BLK), BLK)
            emit(base + j, mm(nrm_t[...], grads[:, cols]), out.at[:, cols])
            return carry

        lax.fori_loop(0, count, step, 0)

    def rows(base, count, acts, out):
        def step(j, carry):
            at = pl.ds(pl.multiple_of(j * width, width), width)
            emit(base + j, mm_at(acts[:, at], dy_v[...]), out.at[at, :])
            return carry

        lax.fori_loop(0, count, step, 0)

    t = 0
    n_q, n_f = dq_v.shape[1] // BLK, dg_v.shape[1] // BLK
    loads[1].wait()
    columns(t, n_q, dq_v, dwq_hbm)
    t += n_q
    loads[3].wait()
    columns(t, n_f, dg_v, dwg_hbm)
    t += n_f
    loads[4].wait()
    columns(t, n_f, du_v, dwu_hbm)
    t += n_f
    loads[5].wait()
    loads[6].wait()
    rows(t, n_q, attn_v, dwo_hbm)
    t += n_q
    loads[7].wait()
    rows(t, n_f, act_v, dwd_hbm)
    t += n_f
    loads[2].wait()
    for ld in hand_in:
        ld.wait()
    hand_out = [pltpu.make_async_copy(y_v, y_hbm, cp_sem.at[0]), pltpu.make_async_copy(dx_v, dx_hbm, cp_sem.at[1])]
    for cp in hand_out:
        cp.start()
    slot = t % n_ring
    tile_copy(slot, dwq_hbm.at[:, 0:BLK]).wait()
    ring[slot] = mm(nrm_t[...], dkv_v[...])
    kv_out = [pltpu.make_async_copy(ring.at[slot, :, 0:256], dwk_hbm, cp_sem.at[2]),
              pltpu.make_async_copy(ring.at[slot, :, 256:512], dwv_hbm, cp_sem.at[3])]
    for cp in kv_out:
        cp.start()
    for i in range(1, n_ring):
        tile_copy((t + i) % n_ring, dwq_hbm.at[:, 0:BLK]).wait()
    for cp in hand_out + kv_out:
        cp.wait()


def solution(mesh):
    tx_size = mesh.shape['tx']
    tok_spec = P('dp', None, 'tx')
    in_specs = (tok_spec, P('dp', None), tok_spec, P('tx'), P('tx', 'ty'), P('tx', 'ty'), P('tx', 'ty'),
                P('tx', None), P('tx', None), P('ty', 'tx'), P('ty', 'tx'))
    out_specs = (tok_spec, tok_spec, P(('dp', 'tx')), P(('dp', 'tx'), 'ty'), P(('dp', 'tx'), 'ty'), P(('dp', 'tx'), 'ty'),
                 P(('dp', 'tx'), None), P(('dp', 'tx'), None), P(('dp', 'ty'), 'tx'), P(('dp', 'ty'), 'tx'))

    def local_layer(x_in, positions, d_y, ln_gamma, w_q, w_g, w_u, w_k, w_v, w_o, w_d):
        _, n_tok, d_local = x_in.shape
        half = n_tok // 2
        d_model = d_local * tx_size
        head_dim = w_k.shape[1]
        q_width = w_q.shape[1]
        d_ff = w_g.shape[1]
        freq = jnp.asarray((ROPE_BASE ** (-2.0 * np.arange(head_dim // 2) / head_dim)).astype(np.float32)[None])
        any_spec = pl.BlockSpec(memory_space=pl.ANY)
        vmem_spec = pl.BlockSpec(memory_space=pltpu.VMEM)
        tok = (n_tok, d_local)
        sem = pltpu.SemaphoreType.DMA
        y_loc, dx_loc, d_gamma, normed, attn_flat, act, d_q, d_kv, d_gate, d_up = pl.pallas_call(
            functools.partial(layer_kernel, d_model),
            out_shape=[jax.ShapeDtypeStruct(tok, BF16), jax.ShapeDtypeStruct(tok, BF16), jax.ShapeDtypeStruct((1, d_local), F32),
                       jax.ShapeDtypeStruct(tok, BF16), jax.ShapeDtypeStruct((n_tok, q_width), BF16),
                       jax.ShapeDtypeStruct((n_tok, d_ff), BF16), jax.ShapeDtypeStruct((n_tok, q_width), BF16),
                       jax.ShapeDtypeStruct((n_tok, 2 * head_dim), BF16), jax.ShapeDtypeStruct((n_tok, d_ff), BF16),
                       jax.ShapeDtypeStruct((n_tok, d_ff), BF16)],
            in_specs=[any_spec, vmem_spec, vmem_spec, any_spec, vmem_spec] + [any_spec] * 7,
            out_specs=[any_spec, any_spec, vmem_spec] + [any_spec] * 7,
            scratch_shapes=[
                pltpu.VMEM(tok, BF16), pltpu.VMEM(tok, BF16), pltpu.VMEM((d_local, q_width + 2 * head_dim), BF16),
                pltpu.VMEM((d_local, d_ff), BF16), pltpu.VMEM((d_local, d_ff), BF16), pltpu.VMEM((q_width, d_local), BF16),
                pltpu.VMEM((d_ff, d_local), BF16),
                pltpu.VMEM((N_BLK, half, BLK), F32), pltpu.VMEM((N_BLK, half, BLK), BF16), pltpu.VMEM((N_BLK, half, BLK), BF16),
                pltpu.VMEM((N_BLK, half, BLK), BF16), pltpu.VMEM((N_BLK, half, BLK), BF16),
                pltpu.VMEM((4, 3, n_tok, CHUNK), BF16), pltpu.VMEM((n_tok, 2 * q_width + 2 * head_dim), BF16),
                pltpu.VMEM((n_tok, q_width), BF16), pltpu.VMEM((n_tok, q_width), BF16),
                pltpu.VMEM((n_tok, 512), BF16), pltpu.VMEM((n_tok, 512), BF16), pltpu.VMEM((n_tok, 512), BF16),
                pltpu.VMEM((n_tok, 512), F32),
                pltpu.VMEM(tok, BF16), pltpu.VMEM(tok, F32), pltpu.VMEM((n_tok, 128), F32), pltpu.VMEM((n_tok, 128), F32),
                pltpu.VMEM((n_tok, 128), F32), pltpu.VMEM(tok, F32), pltpu.VMEM(tok, F32),
                pltpu.VMEM(tok, BF16), pltpu.VMEM(tok, BF16), pltpu.VMEM((SPLITS, n_tok // SPLITS, d_local), BF16), pltpu.VMEM((SPLITS, n_tok // SPLITS, d_local), BF16),
                pltpu.VMEM(tok, BF16), pltpu.VMEM(tok, BF16),
                pltpu.VMEM((8, n_tok), F32), pltpu.VMEM((3, 8, n_tok), F32), pltpu.VMEM((8, n_tok), F32), pltpu.VMEM((8, n_tok), F32), pltpu.VMEM((7, 8, n_tok), F32),
                sem((12,)), sem((36,)), sem((N_BLK,)), sem((N_BLK,)), sem((N_X,)), sem((N_X,)),
                sem((12 + 2 * SPLITS,)), sem((12 + 2 * SPLITS,)), sem((1,)), sem((1,)), sem((4,)), sem((4,)), sem((10,)), sem((10,)),
                sem((SPLITS,)), sem((SPLITS,))],
            compiler_params=pltpu.CompilerParams(collective_id=0, has_side_effects=True, vmem_limit_bytes=67043328),
            name='layer',
        )(x_in.reshape(tok), positions, freq, d_y.reshape(tok), ln_gamma[None], w_q, w_g, w_u, w_k, w_v, w_o, w_d)

        vm = pltpu.VMEM
        y_out, d_x, d_gamma, d_wq, d_wg, d_wu, d_wk, d_wv, d_wo, d_wd = pl.pallas_call(
            grad_kernel,
            out_shape=[jax.ShapeDtypeStruct(tok, BF16), jax.ShapeDtypeStruct(tok, BF16), jax.ShapeDtypeStruct((1, d_local), F32)]
            + [jax.ShapeDtypeStruct(w.shape, F32) for w in (w_q, w_g, w_u, w_k, w_v, w_o, w_d)],
            in_specs=[any_spec] * 10 + [vmem_spec],
            out_specs=[any_spec, any_spec, vmem_spec] + [any_spec] * 7,
            scratch_shapes=[vm(tok, BF16), vm((d_local, n_tok), BF16), vm((n_tok, q_width), BF16), vm((n_tok, d_ff), BF16),
                            vm((n_tok, q_width), BF16), vm((n_tok, 2 * head_dim), BF16), vm((n_tok, d_ff), BF16), vm((n_tok, d_ff), BF16),
                            vm(tok, BF16), vm(tok, BF16), vm(tok, BF16), vm((8, d_local, BLK), F32), sem((10,)), sem((8,)), sem((4,))],
            compiler_params=pltpu.CompilerParams(vmem_limit_bytes=60 * 1024 * 1024),
            name='weight_grads',
        )(normed, attn_flat, act, d_q, d_kv, d_gate, d_up, d_y.reshape(tok), y_loc, dx_loc, d_gamma)
        return (y_out.reshape(x_in.shape), d_x.reshape(x_in.shape), d_gamma.reshape(d_local),
                d_wq, d_wg, d_wu, d_wk, d_wv, d_wo, d_wd)

    return jax.shard_map(local_layer, mesh=mesh, in_specs=in_specs, out_specs=out_specs, check_vma=False)
```

```python
import functools

import jax
import jax.numpy as jnp
import numpy as np
from jax import lax
from jax.experimental import pallas as pl
from jax.experimental.pallas import tpu as pltpu
from jax.sharding import PartitionSpec as P

EPS = 1e-6
ROPE_BASE = 10000.0
F32 = jnp.float32
BF16 = jnp.bfloat16
MESH = pl.DeviceIdType.MESH

BLK = 512
CHUNK = 1024
B_DATTN, B_DACT_LO, B_QKV, B_GU, B_DACT_HI, N_BLK = 0, 2, 6, 9, 25, 29
X_UNITS = ((0, 1), (1, 1), (2, 2), (4, 2), (6, 2), (9, 4), (13, 4), (17, 4), (21, 4), (25, 2))
SPLITS = 4
X_KV = len(X_UNITS)
X_LAST = X_KV + 1
N_X = X_LAST + SPLITS


def dot(a, b, dims):
    return lax.dot_general(a, b, (dims, ((), ())), preferred_element_type=F32)


def mm(a, b):
    return dot(a, b, ((1,), (0,)))


def mm_bt(a, b):
    return dot(a, b, ((1,), (1,)))


def mm_at(a, b):
    return dot(a, b, ((0,), (0,)))


def rope(first, second, cos_t, sin_t):
    return first * cos_t - second * sin_t, second * cos_t + first * sin_t


def layer_kernel(d_model, x_hbm, pos_ref, freq_ref, dy_hbm, gamma_ref, wq_hbm, wg_hbm, wu_hbm, wk_hbm, wv_hbm, wo_hbm, wd_hbm,
                 y_o, dx_o, dgamma_ref, nrm_v, attn_v, md, dq_v, dkv_v, dy_v,
                 x_v, wqkv_v, wg_v, wu_v, wo_v, wd_v,
                 keep, send, rcore, chip, rx, packed, dkv_part, dkv_rx, kv_acc,
                 xhat_v, inv_v, cos_v, sin_v, br_v, dh_v, y_snd, y_rx, dh_snd, dh_rx,
                 st_snd, st_rx, st_sum, bst_snd, bst_rx,
                 ld_sem, cs, cr, xs, xr, gs, gr, ps, pr, ts, tr, ss, sr, ds, dr):
    tx = lax.axis_index('tx')
    ty = lax.axis_index('ty')
    core = lax.rem(tx, 2)
    near = {'tx': tx + 1 - 2 * core}
    across = {'tx': lax.rem(tx + 2, 4)}
    far = {'tx': lax.rem(tx + 1 - 2 * core + 2, 4)}
    other_ty = {'ty': 1 - ty}
    peers = [near, across, far, other_ty] + [{'tx': p['tx'], 'ty': 1 - ty} for p in (near, across, far)]
    n_tok = x_v.shape[0]
    half = n_tok // 2
    mine = pl.multiple_of(core * half, half)
    other = pl.multiple_of((1 - core) * half, half)
    head_dim = 256
    q_width = wo_v.shape[0]
    heads = q_width // head_dim
    piece = half // SPLITS

    def load(i, src, dst):
        return pltpu.make_async_copy(src, dst, ld_sem.at[i])

    d_half = wd_v.shape[0] // 2
    loads = [
        load(0, dy_hbm.at[pl.ds(mine, half)], dy_v.at[0:half]),
        load(1, dy_hbm.at[pl.ds(other, half)], dy_v.at[half:n_tok]),
        load(2, wo_hbm, wo_v),
        load(3, x_hbm.at[pl.ds(mine, half)], x_v.at[0:half]),
        load(4, x_hbm.at[pl.ds(other, half)], x_v.at[half:n_tok]),
        load(5, wd_hbm.at[0:d_half], wd_v.at[0:d_half]),
        load(6, wq_hbm, wqkv_v.at[:, 0:q_width]),
        load(7, wk_hbm, wqkv_v.at[:, q_width:q_width + head_dim]),
        load(8, wv_hbm, wqkv_v.at[:, q_width + head_dim:q_width + 2 * head_dim]),
        load(9, wg_hbm, wg_v),
        load(10, wu_hbm, wu_v),
        load(11, wd_hbm.at[d_half:2 * d_half], wd_v.at[d_half:2 * d_half]),
    ]
    for ld in loads[:5]:
        ld.start()

    barrier = pltpu.get_barrier_semaphore()
    for peer in peers:
        pl.semaphore_signal(barrier, inc=1, device_id=peer, device_id_type=MESH)
    for ld in loads[:3]:
        ld.wait()
    for ld in loads[5:]:
        ld.start()
    pl.semaphore_wait(barrier, len(peers))

    def remote(src, dst, send_sem, recv_sem, peer):
        return pltpu.make_async_remote_copy(src_ref=src, dst_ref=dst, send_sem=send_sem, recv_sem=recv_sem,
                                            device_id=peer, device_id_type=MESH)

    def core_copy(b):
        return remote(send.at[b], rcore.at[b], cs.at[b], cr.at[b], near)

    def x_copy(u):
        if u >= X_LAST:
            rows = pl.ds((u - X_LAST) * piece, piece)
            return remote(chip.at[pl.ds(N_BLK - 2, 2), rows], rx.at[pl.ds(N_BLK - 2, 2), rows], xs.at[u], xr.at[u], across)
        if u == X_KV:
            cols = pl.ds(pl.multiple_of(ty * head_dim, head_dim), head_dim)
            return remote(chip.at[B_QKV + 2, :, cols], rx.at[B_QKV + 2, :, cols], xs.at[u], xr.at[u], across)
        start, count = X_UNITS[u]
        return remote(chip.at[pl.ds(start, count)], rx.at[pl.ds(start, count)], xs.at[u], xr.at[u], across)

    def put(b, part):
        keep[b] = part[:half]
        send[b] = part[half:].astype(BF16)
        core_copy(b).start()

    def issue_bwd(b, w_ref, row):
        put(b, mm_bt(dy_v[...], w_ref[pl.ds(row, BLK), :]))

    def issue_fwd(b, w_ref, col):
        put(b, mm(nrm_v[...], w_ref[:, pl.ds(col, BLK)]))

    def combine(b):
        core_copy(b).wait_recv()
        chip[b] = (keep[b] + rcore[b].astype(F32)).astype(BF16)

    def total(b):
        return chip[b].astype(F32) + rx[b].astype(F32)

    issue_bwd(0, wo_v, 0)
    issue_bwd(1, wo_v, BLK)

    def rows_of(col_a, col_b):
        lane = lax.broadcasted_iota(jnp.int32, (half, 128), 1)
        return jnp.where(lane == 0, col_a, col_b).T[0:8]

    def stats_copies(snd, got, base, to):
        return [remote(snd, got.at[i], ss.at[base + i], sr.at[base + i], peer) for i, peer in enumerate(to)]

    def stats_put(snd, col_a, col_b):
        for lo, at in ((0, mine), (half, other)):
            snd[:, pl.ds(at, half)] = rows_of(col_a[lo:lo + half], col_b[lo:lo + half])

    def stats_columns(rows_ref):
        cols = []
        for i in range(2):
            parts = [jnp.broadcast_to(rows_ref[i:i + 1, pl.ds(at, half)], (128, half)).T[:, 0:1] for at in (mine, other)]
            cols.append(jnp.concatenate(parts, axis=0))
        return cols

    loads[3].wait()
    loads[4].wait()
    x_f = x_v[...].astype(F32)
    stats_put(st_snd, jnp.sum(x_f, axis=1, keepdims=True), jnp.sum(x_f * x_f, axis=1, keepdims=True))
    fwd_stats = stats_copies(st_snd, st_rx, 0, (near, across, far))
    for copy in fwd_stats:
        copy.start()

    combine(0)
    x_copy(0).start()
    combine(1)
    x_copy(1).start()

    loads[5].wait()
    for i in range(4):
        issue_bwd(B_DACT_LO + i, wd_v, i * BLK)
        if i >= 1:
            combine(B_DACT_LO + i - 1)
        if i == 2:
            x_copy(2).start()
    combine(B_DACT_LO + 3)
    x_copy(3).start()

    for copy in fwd_stats:
        copy.wait_recv()
    st_sum[...] = (st_snd[...] + st_rx[0]) + (st_rx[1] + st_rx[2])
    sum_x, sum_xx = stats_columns(st_sum)
    tok_mean = sum_x / d_model
    inv_std = lax.rsqrt(sum_xx / d_model - tok_mean * tok_mean + EPS)
    inv_v[...] = jnp.broadcast_to(inv_std, (n_tok, 128))
    x_hat = (x_v[...].astype(F32) - tok_mean) * inv_std
    xhat_v[...] = x_hat
    nrm_v[...] = (x_hat * gamma_ref[...]).astype(BF16)

    for i in range(6, 9):
        loads[i].wait()
    for i in range(3):
        issue_fwd(B_QKV + i, wqkv_v, i * BLK)
    for i in (2, 0, 1):
        combine(B_QKV + i)
        if i == 2:
            x_copy(X_KV).start()
    x_copy(4).start()

    loads[9].wait()
    loads[10].wait()
    for k in range(4):
        def gu_issue(j, carry, k=k):
            col = pl.multiple_of(k * CHUNK + j * BLK, BLK)
            issue_fwd(B_GU + 4 * k + j, wg_v, col)
            issue_fwd(B_GU + 4 * k + 2 + j, wu_v, col)
            return carry

        def gu_combine(j, carry, k=k):
            combine(B_GU + 4 * k + j)
            return carry

        lax.fori_loop(0, 2, gu_issue, 0)
        lax.fori_loop(0, 4, gu_combine, 0)
        x_copy(5 + k).start()

    loads[11].wait()

    def hi_issue(j, carry):
        issue_bwd(B_DACT_HI + j, wd_v, pl.multiple_of(d_half + j * BLK, BLK))
        return carry

    lax.fori_loop(0, 4, hi_issue, 0)
    for j in range(4):
        combine(B_DACT_HI + j)
        if j == 1:
            x_copy(9).start()
    for r in range(SPLITS):
        x_copy(X_LAST + r).start()

    freq = freq_ref[...]
    for lo, at in ((0, mine), (half, other)):
        pos_col = jnp.broadcast_to(pos_ref[0:1, pl.ds(at, half)].astype(F32), (128, half)).T
        angles = pos_col * freq
        cos_v[lo:lo + half] = jnp.cos(angles)
        sin_v[lo:lo + half] = jnp.sin(angles)

    packed_copy = remote(packed.at[0:half], packed.at[half:n_tok], ps.at[0], pr.at[0], near)
    x_copy(0).wait_recv()
    x_copy(1).wait_recv()
    for j in range(2):
        packed[0:half, q_width + 512 + j * BLK:q_width + 512 + (j + 1) * BLK] = total(B_DATTN + j).astype(BF16)
    x_copy(4).wait_recv()
    cos_h, sin_h = cos_v[0:half], sin_v[0:half]
    for j in range(2):
        blk = total(B_QKV + j)
        for h in range(2):
            lo = h * head_dim
            first, second = rope(blk[:, lo:lo + 128], blk[:, lo + 128:lo + 256], cos_h, sin_h)
            packed[0:half, j * BLK + lo:j * BLK + lo + 128] = first.astype(BF16)
            packed[0:half, j * BLK + lo + 128:j * BLK + lo + 256] = second.astype(BF16)
    x_copy(X_KV).wait_recv()
    kv_cols = pl.ds(pl.multiple_of(ty * head_dim, head_dim), head_dim)
    blk = chip[B_QKV + 2, :, kv_cols].astype(F32) + rx[B_QKV + 2, :, kv_cols].astype(F32)
    first, second = rope(blk[:, 0:128], blk[:, 128:256], cos_h, sin_h)
    kv_mine = jnp.where(ty == 0, jnp.concatenate([first, second], axis=1), blk).astype(BF16)
    kv_dst = packed.at[0:half, pl.ds(pl.multiple_of(q_width + ty * head_dim, head_dim), head_dim)]
    kv_dst[...] = kv_mine
    kv_copy = remote(kv_dst, kv_dst, ts.at[3], tr.at[3], other_ty)
    kv_copy.start()
    kv_copy.wait_recv()
    packed_copy.start()
    packed_copy.wait_recv()

    row_i = lax.rem(lax.broadcasted_iota(jnp.int32, (n_tok, n_tok), 0) + core * half, n_tok)
    col_i = lax.rem(lax.broadcasted_iota(jnp.int32, (n_tok, n_tok), 1) + core * half, n_tok)
    scale = head_dim ** -0.5
    kv_acc[...] = jnp.zeros_like(kv_acc)

    def head_step(h, carry):
        cols = pl.ds(pl.multiple_of(h * head_dim, head_dim), head_dim)
        q_h = packed[:, cols]
        da_h = packed[:, pl.ds(pl.multiple_of(q_width + 512 + h * head_dim, head_dim), head_dim)]
        k_rot = packed[:, q_width:q_width + 256]
        v_val = packed[:, q_width + 256:q_width + 512]
        scores = jnp.where(row_i >= col_i, mm_bt(q_h, k_rot) * scale, -1e30)
        exps = jnp.exp(scores - jnp.max(scores, axis=1, keepdims=True))
        probs_f = exps / jnp.sum(exps, axis=1, keepdims=True)
        probs = probs_f.astype(BF16)
        attn_v[:, cols] = mm(probs, v_val).astype(BF16)
        d_probs = mm_bt(da_h, v_val).astype(BF16).astype(F32)
        d_scores = (probs_f * (d_probs - jnp.sum(d_probs * probs_f, axis=1, keepdims=True)) * scale).astype(BF16)
        dq_h = mm(d_scores, k_rot).astype(BF16).astype(F32)
        first, second = rope(dq_h[:, 0:128], dq_h[:, 128:256], cos_v[...], -sin_v[...])
        dq_v[:, pl.ds(pl.multiple_of(h * head_dim, head_dim), 128)] = first.astype(BF16)
        dq_v[:, pl.ds(pl.multiple_of(h * head_dim + 128, 128), 128)] = second.astype(BF16)
        kv_acc[:, 0:256] += mm_at(d_scores, q_h)
        kv_acc[:, 256:512] += mm_at(probs, da_h)
        return carry

    lax.fori_loop(0, heads, head_step, 0)
    dkv_part[...] = kv_acc[...].astype(BF16)
    dkv_copy = remote(dkv_part, dkv_rx, ts.at[0], tr.at[0], other_ty)
    dkv_copy.start()
    br_v[...] = mm(attn_v[...], wo_v[...])
    dh_v[...] = mm_bt(dq_v[...], wqkv_v[:, 0:q_width])

    def piece_copy(r, i):
        at = 12 + 2 * r + i - 1
        return remote(md.at[3, i, r * piece:(r + 1) * piece], md.at[3, i, half + r * piece:half + (r + 1) * piece], gs.at[at], gr.at[at], near)

    def gather_copy(k, i):
        return remote(md.at[k, i, 0:half], md.at[k, i, half:n_tok], gs.at[3 * k + i], gr.at[3 * k + i], near)

    def dact_block(k, j):
        return B_DACT_LO + 2 * k + j if k < 2 else B_DACT_HI + 2 * (k - 2) + j

    def gated(k, want_act, want_grad, lo=0, hi=None):
        def step(r, carry):
            rows = pl.ds(pl.multiple_of(r * 16, 16), 16)
            for j in range(2):
                bg, bu, bd = B_GU + 4 * k + j, B_GU + 4 * k + 2 + j, dact_block(k, j)
                gate = (chip[bg, rows].astype(F32) + rx[bg, rows].astype(F32)).astype(BF16).astype(F32)
                up = (chip[bu, rows].astype(F32) + rx[bu, rows].astype(F32)).astype(BF16).astype(F32)
                sig = jax.nn.sigmoid(gate)
                silu = gate * sig
                cols = slice(j * BLK, (j + 1) * BLK)
                if want_act:
                    md[k, 0, rows, cols] = (silu * up).astype(BF16)
                if want_grad:
                    d_act = (chip[bd, rows].astype(F32) + rx[bd, rows].astype(F32)).astype(BF16).astype(F32)
                    md[k, 1, rows, cols] = (d_act * up * sig * (1.0 + gate * (1.0 - sig))).astype(BF16)
                    md[k, 2, rows, cols] = (d_act * silu).astype(BF16)
            return carry

        lax.fori_loop(lo // 16, (half if hi is None else hi) // 16, step, 0)
        if hi is None:
            for i in ((0,) if want_act else ()) + ((1, 2) if want_grad else ()):
                gather_copy(k, i).start()

    def use_act(k):
        gather_copy(k, 0).wait_recv()
        br_v[...] += mm(md[k, 0], wd_v[k * CHUNK:(k + 1) * CHUNK, :])

    def use_grad(k):
        for i in (1, 2):
            gather_copy(k, i).wait_recv()
        dh_v[...] += (mm_bt(md[k, 1], wg_v[:, k * CHUNK:(k + 1) * CHUNK])
                      + mm_bt(md[k, 2], wu_v[:, k * CHUNK:(k + 1) * CHUNK]))

    x_copy(2).wait_recv()
    x_copy(3).wait_recv()
    for k in range(2):
        x_copy(5 + k).wait_recv()
        gated(k, True, True)
        use_act(k)
        use_grad(k)
        if k == 0:
            dkv_copy.wait_recv()
            d_k = dkv_part[:, 0:256].astype(F32) + dkv_rx[:, 0:256].astype(F32)
            d_k = d_k.astype(BF16).astype(F32)
            first, second = rope(d_k[:, 0:128], d_k[:, 128:256], cos_v[...], -sin_v[...])
            dkv_v[:, 0:128] = first.astype(BF16)
            dkv_v[:, 128:256] = second.astype(BF16)
            dkv_v[:, 256:512] = (dkv_part[:, 256:512].astype(F32) + dkv_rx[:, 256:512].astype(F32)).astype(BF16)
            dh_v[...] += 0.5 * mm_bt(dkv_v[...], wqkv_v[:, q_width:q_width + 512])
    for k in (2, 3):
        x_copy(5 + k).wait_recv()
        gated(k, True, False)
        use_act(k)
    y_snd[...] = br_v[...].astype(BF16)
    y_copy = remote(y_snd, y_rx, ts.at[1], tr.at[1], other_ty)
    y_copy.start()
    x_copy(9).wait_recv()
    gated(2, False, True)
    use_grad(2)

    def dh_copy(r):
        return remote(dh_snd.at[r], dh_rx.at[r], ds.at[r], dr.at[r], other_ty)

    def both(ref, r):
        return jnp.concatenate([ref[r * piece:(r + 1) * piece], ref[half + r * piece:half + (r + 1) * piece]], axis=0)

    sums = []

    def piece_grad(r):
        x_copy(X_LAST + r).wait_recv()
        gated(3, False, True, r * piece, (r + 1) * piece)
        for i in (1, 2):
            piece_copy(r, i).start()

    def piece_dh(r):
        for i in (1, 2):
            piece_copy(r, i).wait_recv()
        part = both(dh_v, r) + mm_bt(both(md.at[3, 1], r), wg_v[:, 3 * CHUNK:4 * CHUNK]) + mm_bt(both(md.at[3, 2], r), wu_v[:, 3 * CHUNK:4 * CHUNK])
        part_b = part.astype(BF16)
        dh_snd[r] = part_b
        dh_copy(r).start()
        d_hat = part_b.astype(F32) * gamma_ref[...]
        sums.append((jnp.sum(d_hat, axis=1, keepdims=True), jnp.sum(d_hat * both(xhat_v, r), axis=1, keepdims=True)))

    for r in range(SPLITS):
        piece_grad(r)
        piece_dh(r)
    cols = [jnp.concatenate([sums[r][i][:piece] for r in range(SPLITS)] + [sums[r][i][piece:] for r in range(SPLITS)], axis=0) for i in range(2)]
    stats_put(bst_snd, cols[0], cols[1])
    bwd_stats = stats_copies(bst_snd, bst_rx, 3, peers)
    for copy in bwd_stats:
        copy.start()

    y_copy.wait_recv()
    y_o[...] = (x_v[...].astype(F32) + (y_snd[...].astype(F32) + y_rx[...].astype(F32))).astype(BF16)

    d_gamma = jnp.zeros_like(dgamma_ref)
    for r in range(SPLITS):
        dh_copy(r).wait_recv()
        d_nrm = dh_snd[r].astype(F32) + dh_rx[r].astype(F32)
        d_gamma = d_gamma + jnp.sum(d_nrm * both(xhat_v, r), axis=0, keepdims=True)
        dh_v[r * piece:(r + 1) * piece] = d_nrm[:piece]
        dh_v[half + r * piece:half + (r + 1) * piece] = d_nrm[piece:]
    dgamma_ref[...] = d_gamma
    for copy in bwd_stats:
        copy.wait_recv()
    st_sum[...] = ((bst_snd[...] + bst_rx[0]) + (bst_rx[1] + bst_rx[2])) + ((bst_rx[3] + bst_rx[4]) + (bst_rx[5] + bst_rx[6]))
    sum_d, sum_dx = stats_columns(st_sum)
    d_hat = dh_v[...] * gamma_ref[...]
    d_x = dy_v[...].astype(F32) + inv_v[:, 0:1] * (d_hat - sum_d / d_model - xhat_v[...] * (sum_dx / d_model))
    dx_o[...] = d_x.astype(BF16)

    def drain(b, carry):
        core_copy(b).wait_send()
        return carry

    lax.fori_loop(0, N_BLK, drain, 0)
    for u in range(N_X):
        x_copy(u).wait_send()
    for k in range(4):
        for i in range(3 if k < 3 else 1):
            gather_copy(k, i).wait_send()
    for r in range(SPLITS):
        for i in (1, 2):
            piece_copy(r, i).wait_send()
        dh_copy(r).wait_send()
    for copy in [packed_copy, dkv_copy, y_copy, kv_copy] + fwd_stats + bwd_stats:
        copy.wait_send()


def grad_kernel(y_v, dx_v, dgamma_in, nrm_v, attn_v, md, dq_v, dkv_v, dy_v,
                y_hbm, dx_hbm, dgamma_ref, dwq_hbm, dwg_hbm, dwu_hbm, dwk_hbm, dwv_hbm, dwo_hbm, dwd_hbm,
                nrm_t, ring, out_sem, cp_sem):
    n_tok, width = nrm_v.shape
    half = n_tok // 2
    n_ring = ring.shape[0]
    core = lax.rem(lax.axis_index('tx'), 2)
    mine = pl.multiple_of(core * half, half)
    other = pl.multiple_of((1 - core) * half, half)
    hand_out = [pltpu.make_async_copy(src.at[lo:lo + half], dst.at[pl.ds(at, half)], cp_sem.at[i])
                for i, (src, dst, lo, at) in enumerate(((y_v, y_hbm, 0, mine), (y_v, y_hbm, half, other), (dx_v, dx_hbm, 0, mine), (dx_v, dx_hbm, half, other)))]
    for cp in hand_out:
        cp.start()
    dgamma_ref[...] = dgamma_in[...]

    def tile_copy(slot, dst):
        return pltpu.make_async_copy(ring.at[slot], dst, out_sem.at[slot])

    def emit(t, value, dst):
        slot = lax.rem(t, n_ring)

        @pl.when(t >= n_ring)
        def _():
            tile_copy(slot, dwq_hbm.at[:, 0:BLK]).wait()

        ring[slot] = value
        tile_copy(slot, dst).start()

    nrm_t[...] = nrm_v[...].T

    def columns(base, count, grads, out, col0=0):
        def step(j, carry):
            cols = pl.ds(pl.multiple_of(j * BLK, BLK), BLK)
            emit(base + j, mm(nrm_t[...], grads[:, cols]), out.at[:, pl.ds(pl.multiple_of(col0 + j * BLK, BLK), BLK)])
            return carry

        lax.fori_loop(0, count, step, 0)

    def rows(base, count, acts, out, row0=0):
        def step(j, carry):
            at = pl.ds(pl.multiple_of(j * width, width), width)
            emit(base + j, mm_at(acts[:, at], dy_v[...]), out.at[pl.ds(pl.multiple_of(row0 + j * width, width), width), :])
            return carry

        lax.fori_loop(0, count, step, 0)

    columns(0, 2, dq_v, dwq_hbm)

    def chunk_step(k, carry):
        columns(2 + 6 * k, 2, md.at[k, 1], dwg_hbm, k * CHUNK)
        columns(4 + 6 * k, 2, md.at[k, 2], dwu_hbm, k * CHUNK)
        rows(6 + 6 * k, 2, md.at[k, 0], dwd_hbm, k * CHUNK)
        return carry

    lax.fori_loop(0, 4, chunk_step, 0)
    rows(26, 2, attn_v, dwo_hbm)
    t = 28
    slot = t % n_ring
    tile_copy(slot, dwq_hbm.at[:, 0:BLK]).wait()
    ring[slot] = mm(nrm_t[...], dkv_v[...])
    kv_out = [pltpu.make_async_copy(ring.at[slot, :, 0:256], dwk_hbm, cp_sem.at[4]),
              pltpu.make_async_copy(ring.at[slot, :, 256:512], dwv_hbm, cp_sem.at[5])]
    for cp in kv_out:
        cp.start()
    for i in range(1, n_ring):
        tile_copy((t + i) % n_ring, dwq_hbm.at[:, 0:BLK]).wait()
    for cp in hand_out + kv_out:
        cp.wait()


def solution(mesh):
    tx_size = mesh.shape['tx']
    tok_spec = P('dp', None, 'tx')
    in_specs = (tok_spec, P('dp', None), tok_spec, P('tx'), P('tx', 'ty'), P('tx', 'ty'), P('tx', 'ty'),
                P('tx', None), P('tx', None), P('ty', 'tx'), P('ty', 'tx'))
    out_specs = (tok_spec, tok_spec, P(('dp', 'tx')), P(('dp', 'tx'), 'ty'), P(('dp', 'tx'), 'ty'), P(('dp', 'tx'), 'ty'),
                 P(('dp', 'tx'), None), P(('dp', 'tx'), None), P(('dp', 'ty'), 'tx'), P(('dp', 'ty'), 'tx'))

    def local_layer(x_in, positions, d_y, ln_gamma, w_q, w_g, w_u, w_k, w_v, w_o, w_d):
        _, n_tok, d_local = x_in.shape
        half = n_tok // 2
        d_model = d_local * tx_size
        head_dim = w_k.shape[1]
        q_width = w_q.shape[1]
        d_ff = w_g.shape[1]
        freq = jnp.asarray((ROPE_BASE ** (-2.0 * np.arange(head_dim // 2) / head_dim)).astype(np.float32)[None])
        any_spec = pl.BlockSpec(memory_space=pl.ANY)
        vmem_spec = pl.BlockSpec(memory_space=pltpu.VMEM)
        tok = (n_tok, d_local)
        sem = pltpu.SemaphoreType.DMA
        vm = pltpu.VMEM
        kept = pl.pallas_call(
            functools.partial(layer_kernel, d_model),
            out_shape=[vm(tok, BF16), vm(tok, BF16), vm((1, d_local), F32), vm(tok, BF16), vm((n_tok, q_width), BF16),
                       vm((4, 3, n_tok, CHUNK), BF16), vm((n_tok, q_width), BF16), vm((n_tok, 2 * head_dim), BF16), vm(tok, BF16)],
            in_specs=[any_spec, vmem_spec, vmem_spec, any_spec, vmem_spec] + [any_spec] * 7,
            out_specs=[vmem_spec] * 9,
            scratch_shapes=[
                vm(tok, BF16), vm((d_local, q_width + 2 * head_dim), BF16), vm((d_local, d_ff), BF16), vm((d_local, d_ff), BF16),
                vm((q_width, d_local), BF16), vm((d_ff, d_local), BF16),
                vm((N_BLK, half, BLK), F32), vm((N_BLK, half, BLK), BF16), vm((N_BLK, half, BLK), BF16),
                vm((N_BLK, half, BLK), BF16), vm((N_BLK, half, BLK), BF16), vm((n_tok, 2 * q_width + 2 * head_dim), BF16),
                vm((n_tok, 512), BF16), vm((n_tok, 512), BF16), vm((n_tok, 512), F32),
                vm(tok, F32), vm((n_tok, 128), F32), vm((n_tok, 128), F32), vm((n_tok, 128), F32), vm(tok, F32), vm(tok, F32),
                vm(tok, BF16), vm(tok, BF16), vm((SPLITS, n_tok // SPLITS, d_local), BF16), vm((SPLITS, n_tok // SPLITS, d_local), BF16),
                vm((8, n_tok), F32), vm((3, 8, n_tok), F32), vm((8, n_tok), F32), vm((8, n_tok), F32), vm((7, 8, n_tok), F32),
                sem((12,)), sem((N_BLK,)), sem((N_BLK,)), sem((N_X,)), sem((N_X,)),
                sem((12 + 2 * SPLITS,)), sem((12 + 2 * SPLITS,)), sem((1,)), sem((1,)), sem((4,)), sem((4,)), sem((10,)), sem((10,)),
                sem((SPLITS,)), sem((SPLITS,))],
            compiler_params=pltpu.CompilerParams(collective_id=0, has_side_effects=True, vmem_limit_bytes=50 * 1024 * 1024),
            name='layer',
        )(x_in.reshape(tok), positions, freq, d_y.reshape(tok), ln_gamma[None], w_q, w_g, w_u, w_k, w_v, w_o, w_d)

        y_out, d_x, d_gamma, d_wq, d_wg, d_wu, d_wk, d_wv, d_wo, d_wd = pl.pallas_call(
            grad_kernel,
            out_shape=[jax.ShapeDtypeStruct(tok, BF16), jax.ShapeDtypeStruct(tok, BF16), jax.ShapeDtypeStruct((1, d_local), F32)]
            + [jax.ShapeDtypeStruct(w.shape, F32) for w in (w_q, w_g, w_u, w_k, w_v, w_o, w_d)],
            in_specs=[vmem_spec] * 9,
            out_specs=[any_spec, any_spec, vmem_spec] + [any_spec] * 7,
            scratch_shapes=[vm((d_local, n_tok), BF16), vm((8, d_local, BLK), F32), sem((8,)), sem((6,))],
            compiler_params=pltpu.CompilerParams(vmem_limit_bytes=40 * 1024 * 1024),
            name='weight_grads',
        )(*kept)
        return (y_out.reshape(x_in.shape), d_x.reshape(x_in.shape), d_gamma.reshape(d_local),
                d_wq, d_wg, d_wu, d_wk, d_wv, d_wo, d_wd)

    return jax.shard_map(local_layer, mesh=mesh, in_specs=in_specs, out_specs=out_specs, check_vma=False)
```

```python
import functools

import jax
import jax.numpy as jnp
import numpy as np
from jax import lax
from jax.experimental import pallas as pl
from jax.experimental.pallas import tpu as pltpu
from jax.sharding import PartitionSpec as P

EPS = 1e-6
ROPE_BASE = 10000.0
F32 = jnp.float32
BF16 = jnp.bfloat16
MESH = pl.DeviceIdType.MESH

BLK = 512
CHUNK = 1024
B_DATTN, B_DACT_LO, B_QKV, B_GU, B_DACT_HI, N_BLK = 0, 2, 6, 9, 25, 29
X_UNITS = ((0, 1), (1, 1), (2, 2), (4, 2), (6, 2), (9, 4), (13, 4), (17, 4), (21, 4), (25, 2))
SPLITS = 4
X_KV = len(X_UNITS)
X_LAST = X_KV + 1
N_X = X_LAST + SPLITS


def dot(a, b, dims):
    return lax.dot_general(a, b, (dims, ((), ())), preferred_element_type=F32)


def mm(a, b):
    return dot(a, b, ((1,), (0,)))


def mm_bt(a, b):
    return dot(a, b, ((1,), (1,)))


def mm_at(a, b):
    return dot(a, b, ((0,), (0,)))


def rope(first, second, cos_t, sin_t):
    return first * cos_t - second * sin_t, second * cos_t + first * sin_t


def layer_kernel(d_model, x_hbm, pos_ref, freq_ref, dy_hbm, gamma_ref, wq_hbm, wg_hbm, wu_hbm, wk_hbm, wv_hbm, wo_hbm, wd_hbm,
                 y_o, dx_o, dgamma_ref, nrm_v, attn_v, md, dq_v, dkv_v, dy_v,
                 x_v, wqkv_v, wg_v, wu_v, wo_v, wd_v,
                 keep, send, rcore, chip, rx, packed, dkv_part, dkv_rx, kv_acc,
                 xhat_v, inv_v, cos_v, sin_v, br_v, dh_v, y_snd, y_rx, dh_snd, dh_rx,
                 st_snd, st_rx, st_sum, bst_snd, bst_rx,
                 ld_sem, cs, cr, xs, xr, gs, gr, ps, pr, ts, tr, ss, sr, ds, dr):
    tx = lax.axis_index('tx')
    ty = lax.axis_index('ty')
    core = lax.rem(tx, 2)
    near = {'tx': tx + 1 - 2 * core}
    across = {'tx': lax.rem(tx + 2, 4)}
    far = {'tx': lax.rem(tx + 1 - 2 * core + 2, 4)}
    other_ty = {'ty': 1 - ty}
    peers = [near, across, far, other_ty] + [{'tx': p['tx'], 'ty': 1 - ty} for p in (near, across, far)]
    n_tok = x_v.shape[0]
    half = n_tok // 2
    mine = pl.multiple_of(core * half, half)
    other = pl.multiple_of((1 - core) * half, half)
    head_dim = 256
    q_width = wo_v.shape[0]
    heads = q_width // head_dim
    piece = half // SPLITS

    def load(i, src, dst):
        return pltpu.make_async_copy(src, dst, ld_sem.at[i])

    d_half = wd_v.shape[0] // 2
    loads = [
        load(0, dy_hbm.at[pl.ds(mine, half)], dy_v.at[0:half]),
        load(1, dy_hbm.at[pl.ds(other, half)], dy_v.at[half:n_tok]),
        load(2, wo_hbm, wo_v),
        load(3, x_hbm.at[pl.ds(mine, half)], x_v.at[0:half]),
        load(4, x_hbm.at[pl.ds(other, half)], x_v.at[half:n_tok]),
        load(5, wd_hbm.at[0:d_half], wd_v.at[0:d_half]),
        load(6, wq_hbm, wqkv_v.at[:, 0:q_width]),
        load(7, wk_hbm, wqkv_v.at[:, q_width:q_width + head_dim]),
        load(8, wv_hbm, wqkv_v.at[:, q_width + head_dim:q_width + 2 * head_dim]),
        load(9, wg_hbm, wg_v),
        load(10, wu_hbm, wu_v),
        load(11, wd_hbm.at[d_half:2 * d_half], wd_v.at[d_half:2 * d_half]),
    ]
    for ld in loads[:5]:
        ld.start()

    barrier = pltpu.get_barrier_semaphore()
    for peer in peers:
        pl.semaphore_signal(barrier, inc=1, device_id=peer, device_id_type=MESH)
    for ld in loads[:3]:
        ld.wait()
    for ld in loads[5:]:
        ld.start()
    pl.semaphore_wait(barrier, len(peers))

    def remote(src, dst, send_sem, recv_sem, peer):
        return pltpu.make_async_remote_copy(src_ref=src, dst_ref=dst, send_sem=send_sem, recv_sem=recv_sem,
                                            device_id=peer, device_id_type=MESH)

    def core_copy(b):
        return remote(send.at[b], rcore.at[b], cs.at[b], cr.at[b], near)

    def x_copy(u):
        if u >= X_LAST:
            rows = pl.ds((u - X_LAST) * piece, piece)
            return remote(chip.at[pl.ds(N_BLK - 2, 2), rows], rx.at[pl.ds(N_BLK - 2, 2), rows], xs.at[u], xr.at[u], across)
        if u == X_KV:
            cols = pl.ds(pl.multiple_of(ty * head_dim, head_dim), head_dim)
            return remote(chip.at[B_QKV + 2, :, cols], rx.at[B_QKV + 2, :, cols], xs.at[u], xr.at[u], across)
        start, count = X_UNITS[u]
        return remote(chip.at[pl.ds(start, count)], rx.at[pl.ds(start, count)], xs.at[u], xr.at[u], across)

    def put(b, part):
        keep[b] = part[:half]
        send[b] = part[half:].astype(BF16)
        core_copy(b).start()

    def issue_bwd(b, w_ref, row):
        put(b, mm_bt(dy_v[...], w_ref[pl.ds(row, BLK), :]))

    def issue_fwd(b, w_ref, col):
        put(b, mm(nrm_v[...], w_ref[:, pl.ds(col, BLK)]))

    def combine(b):
        core_copy(b).wait_recv()
        chip[b] = (keep[b] + rcore[b].astype(F32)).astype(BF16)

    def total(b):
        return chip[b].astype(F32) + rx[b].astype(F32)

    issue_bwd(0, wo_v, 0)
    issue_bwd(1, wo_v, BLK)

    def rows_of(col_a, col_b):
        lane = lax.broadcasted_iota(jnp.int32, (half, 128), 1)
        return jnp.where(lane == 0, col_a, col_b).T[0:8]

    def stats_copies(snd, got, base, to):
        return [remote(snd, got.at[i], ss.at[base + i], sr.at[base + i], peer) for i, peer in enumerate(to)]

    def stats_put(snd, col_a, col_b):
        for lo, at in ((0, mine), (half, other)):
            snd[:, pl.ds(at, half)] = rows_of(col_a[lo:lo + half], col_b[lo:lo + half])

    def stats_columns(rows_ref):
        cols = []
        for i in range(2):
            parts = [jnp.broadcast_to(rows_ref[i:i + 1, pl.ds(at, half)], (128, half)).T[:, 0:1] for at in (mine, other)]
            cols.append(jnp.concatenate(parts, axis=0))
        return cols

    loads[3].wait()
    loads[4].wait()
    x_f = x_v[...].astype(F32)
    stats_put(st_snd, jnp.sum(x_f, axis=1, keepdims=True), jnp.sum(x_f * x_f, axis=1, keepdims=True))
    fwd_stats = stats_copies(st_snd, st_rx, 0, (near, across, far))
    for copy in fwd_stats:
        copy.start()

    combine(0)
    x_copy(0).start()
    combine(1)
    x_copy(1).start()

    loads[5].wait()
    for i in range(4):
        issue_bwd(B_DACT_LO + i, wd_v, i * BLK)
        if i >= 1:
            combine(B_DACT_LO + i - 1)
        if i == 2:
            x_copy(2).start()
    combine(B_DACT_LO + 3)
    x_copy(3).start()

    for copy in fwd_stats:
        copy.wait_recv()
    st_sum[...] = (st_snd[...] + st_rx[0]) + (st_rx[1] + st_rx[2])
    sum_x, sum_xx = stats_columns(st_sum)
    tok_mean = sum_x / d_model
    inv_std = lax.rsqrt(sum_xx / d_model - tok_mean * tok_mean + EPS)
    inv_v[...] = jnp.broadcast_to(inv_std, (n_tok, 128))
    x_hat = (x_v[...].astype(F32) - tok_mean) * inv_std
    xhat_v[...] = x_hat
    nrm_v[...] = (x_hat * gamma_ref[...]).astype(BF16)

    for i in range(6, 9):
        loads[i].wait()
    for i in range(3):
        issue_fwd(B_QKV + i, wqkv_v, i * BLK)
    for i in (2, 0, 1):
        combine(B_QKV + i)
        if i == 2:
            x_copy(X_KV).start()
    x_copy(4).start()

    loads[9].wait()
    loads[10].wait()
    for k in range(4):
        def gu_issue(j, carry, k=k):
            col = pl.multiple_of(k * CHUNK + j * BLK, BLK)
            issue_fwd(B_GU + 4 * k + j, wg_v, col)
            issue_fwd(B_GU + 4 * k + 2 + j, wu_v, col)
            return carry

        def gu_combine(j, carry, k=k):
            combine(B_GU + 4 * k + j)
            return carry

        lax.fori_loop(0, 2, gu_issue, 0)
        lax.fori_loop(0, 4, gu_combine, 0)
        x_copy(5 + k).start()

    loads[11].wait()

    def hi_issue(j, carry):
        issue_bwd(B_DACT_HI + j, wd_v, pl.multiple_of(d_half + j * BLK, BLK))
        return carry

    lax.fori_loop(0, 4, hi_issue, 0)
    for j in range(4):
        combine(B_DACT_HI + j)
        if j == 1:
            x_copy(9).start()
    for r in range(SPLITS):
        x_copy(X_LAST + r).start()

    freq = freq_ref[...]
    for lo, at in ((0, mine), (half, other)):
        pos_col = jnp.broadcast_to(pos_ref[0:1, pl.ds(at, half)].astype(F32), (128, half)).T
        angles = pos_col * freq
        cos_v[lo:lo + half] = jnp.cos(angles)
        sin_v[lo:lo + half] = jnp.sin(angles)

    packed_copy = remote(packed.at[0:half], packed.at[half:n_tok], ps.at[0], pr.at[0], near)
    x_copy(0).wait_recv()
    x_copy(1).wait_recv()
    for j in range(2):
        packed[0:half, q_width + 512 + j * BLK:q_width + 512 + (j + 1) * BLK] = total(B_DATTN + j).astype(BF16)
    x_copy(4).wait_recv()
    cos_h, sin_h = cos_v[0:half], sin_v[0:half]
    for j in range(2):
        blk = total(B_QKV + j)
        for h in range(2):
            lo = h * head_dim
            first, second = rope(blk[:, lo:lo + 128], blk[:, lo + 128:lo + 256], cos_h, sin_h)
            packed[0:half, j * BLK + lo:j * BLK + lo + 128] = first.astype(BF16)
            packed[0:half, j * BLK + lo + 128:j * BLK + lo + 256] = second.astype(BF16)
    x_copy(X_KV).wait_recv()
    kv_cols = pl.ds(pl.multiple_of(ty * head_dim, head_dim), head_dim)
    blk = chip[B_QKV + 2, :, kv_cols].astype(F32) + rx[B_QKV + 2, :, kv_cols].astype(F32)
    first, second = rope(blk[:, 0:128], blk[:, 128:256], cos_h, sin_h)
    kv_mine = jnp.where(ty == 0, jnp.concatenate([first, second], axis=1), blk).astype(BF16)
    kv_dst = packed.at[0:half, pl.ds(pl.multiple_of(q_width + ty * head_dim, head_dim), head_dim)]
    kv_dst[...] = kv_mine
    kv_copy = remote(kv_dst, kv_dst, ts.at[3], tr.at[3], other_ty)
    kv_copy.start()
    kv_copy.wait_recv()
    packed_copy.start()
    packed_copy.wait_recv()

    row_i = lax.rem(lax.broadcasted_iota(jnp.int32, (n_tok, n_tok), 0) + core * half, n_tok)
    col_i = lax.rem(lax.broadcasted_iota(jnp.int32, (n_tok, n_tok), 1) + core * half, n_tok)
    scale = head_dim ** -0.5
    kv_acc[...] = jnp.zeros_like(kv_acc)

    def head_step(h, carry):
        cols = pl.ds(pl.multiple_of(h * head_dim, head_dim), head_dim)
        q_h = packed[:, cols]
        da_h = packed[:, pl.ds(pl.multiple_of(q_width + 512 + h * head_dim, head_dim), head_dim)]
        k_rot = packed[:, q_width:q_width + 256]
        v_val = packed[:, q_width + 256:q_width + 512]
        scores = jnp.where(row_i >= col_i, mm_bt(q_h, k_rot) * scale, -1e30)
        exps = jnp.exp(scores - jnp.max(scores, axis=1, keepdims=True))
        probs_f = exps / jnp.sum(exps, axis=1, keepdims=True)
        probs = probs_f.astype(BF16)
        attn_v[:, cols] = mm(probs, v_val).astype(BF16)
        d_probs = mm_bt(da_h, v_val).astype(BF16).astype(F32)
        d_scores = (probs_f * (d_probs - jnp.sum(d_probs * probs_f, axis=1, keepdims=True)) * scale).astype(BF16)
        dq_h = mm(d_scores, k_rot).astype(BF16).astype(F32)
        first, second = rope(dq_h[:, 0:128], dq_h[:, 128:256], cos_v[...], -sin_v[...])
        dq_v[:, pl.ds(pl.multiple_of(h * head_dim, head_dim), 128)] = first.astype(BF16)
        dq_v[:, pl.ds(pl.multiple_of(h * head_dim + 128, 128), 128)] = second.astype(BF16)
        kv_acc[:, 0:256] += mm_at(d_scores, q_h)
        kv_acc[:, 256:512] += mm_at(probs, da_h)
        return carry

    lax.fori_loop(0, heads, head_step, 0)
    dkv_part[...] = kv_acc[...].astype(BF16)
    dkv_copy = remote(dkv_part, dkv_rx, ts.at[0], tr.at[0], other_ty)
    dkv_copy.start()
    br_v[...] = mm(attn_v[...], wo_v[...])
    dh_v[...] = mm_bt(dq_v[...], wqkv_v[:, 0:q_width])

    def piece_copy(r, i):
        at = 12 + 2 * r + i - 1
        return remote(md.at[3, i, r * piece:(r + 1) * piece], md.at[3, i, half + r * piece:half + (r + 1) * piece], gs.at[at], gr.at[at], near)

    def gather_copy(k, i):
        return remote(md.at[k, i, 0:half], md.at[k, i, half:n_tok], gs.at[3 * k + i], gr.at[3 * k + i], near)

    def dact_block(k, j):
        return B_DACT_LO + 2 * k + j if k < 2 else B_DACT_HI + 2 * (k - 2) + j

    def gated(k, want_act, want_grad, lo=0, hi=None):
        def step(r, carry):
            rows = pl.ds(pl.multiple_of(r * 16, 16), 16)
            for j in range(2):
                bg, bu, bd = B_GU + 4 * k + j, B_GU + 4 * k + 2 + j, dact_block(k, j)
                gate = (chip[bg, rows].astype(F32) + rx[bg, rows].astype(F32)).astype(BF16).astype(F32)
                up = (chip[bu, rows].astype(F32) + rx[bu, rows].astype(F32)).astype(BF16).astype(F32)
                sig = jax.nn.sigmoid(gate)
                silu = gate * sig
                cols = slice(j * BLK, (j + 1) * BLK)
                if want_act:
                    md[k, 0, rows, cols] = (silu * up).astype(BF16)
                if want_grad:
                    d_act = (chip[bd, rows].astype(F32) + rx[bd, rows].astype(F32)).astype(BF16).astype(F32)
                    md[k, 1, rows, cols] = (d_act * up * sig * (1.0 + gate * (1.0 - sig))).astype(BF16)
                    md[k, 2, rows, cols] = (d_act * silu).astype(BF16)
            return carry

        lax.fori_loop(lo // 16, (half if hi is None else hi) // 16, step, 0)
        if hi is None:
            for i in ((0,) if want_act else ()) + ((1, 2) if want_grad else ()):
                gather_copy(k, i).start()

    def use_act(k):
        gather_copy(k, 0).wait_recv()
        br_v[...] += mm(md[k, 0], wd_v[k * CHUNK:(k + 1) * CHUNK, :])

    def use_grad(k):
        for i in (1, 2):
            gather_copy(k, i).wait_recv()
        dh_v[...] += (mm_bt(md[k, 1], wg_v[:, k * CHUNK:(k + 1) * CHUNK])
                      + mm_bt(md[k, 2], wu_v[:, k * CHUNK:(k + 1) * CHUNK]))

    x_copy(2).wait_recv()
    x_copy(3).wait_recv()
    for k in range(2):
        x_copy(5 + k).wait_recv()
        gated(k, True, True)
        use_act(k)
        use_grad(k)
        if k == 0:
            dkv_copy.wait_recv()
            d_k = dkv_part[:, 0:256].astype(F32) + dkv_rx[:, 0:256].astype(F32)
            d_k = d_k.astype(BF16).astype(F32)
            first, second = rope(d_k[:, 0:128], d_k[:, 128:256], cos_v[...], -sin_v[...])
            dkv_v[:, 0:128] = first.astype(BF16)
            dkv_v[:, 128:256] = second.astype(BF16)
            dkv_v[:, 256:512] = (dkv_part[:, 256:512].astype(F32) + dkv_rx[:, 256:512].astype(F32)).astype(BF16)
            dh_v[...] += 0.5 * mm_bt(dkv_v[...], wqkv_v[:, q_width:q_width + 512])
    for k in (2, 3):
        x_copy(5 + k).wait_recv()
        gated(k, True, False)
        use_act(k)
    y_snd[...] = br_v[...].astype(BF16)
    y_copy = remote(y_snd, y_rx, ts.at[1], tr.at[1], other_ty)
    y_copy.start()
    x_copy(9).wait_recv()
    gated(2, False, True)
    use_grad(2)

    def dh_copy(r):
        return remote(dh_snd.at[r], dh_rx.at[r], ds.at[r], dr.at[r], other_ty)

    def both(ref, r):
        return jnp.concatenate([ref[r * piece:(r + 1) * piece], ref[half + r * piece:half + (r + 1) * piece]], axis=0)

    sums = []

    def piece_grad(r):
        x_copy(X_LAST + r).wait_recv()
        gated(3, False, True, r * piece, (r + 1) * piece)
        for i in (1, 2):
            piece_copy(r, i).start()

    def piece_dh(r):
        for i in (1, 2):
            piece_copy(r, i).wait_recv()
        part = both(dh_v, r) + mm_bt(both(md.at[3, 1], r), wg_v[:, 3 * CHUNK:4 * CHUNK]) + mm_bt(both(md.at[3, 2], r), wu_v[:, 3 * CHUNK:4 * CHUNK])
        part_b = part.astype(BF16)
        dh_snd[r] = part_b
        dh_copy(r).start()
        d_hat = part_b.astype(F32) * gamma_ref[...]
        sums.append((jnp.sum(d_hat, axis=1, keepdims=True), jnp.sum(d_hat * both(xhat_v, r), axis=1, keepdims=True)))

    for r in range(SPLITS):
        piece_grad(r)
        piece_dh(r)
    cols = [jnp.concatenate([sums[r][i][:piece] for r in range(SPLITS)] + [sums[r][i][piece:] for r in range(SPLITS)], axis=0) for i in range(2)]
    stats_put(bst_snd, cols[0], cols[1])
    bwd_stats = stats_copies(bst_snd, bst_rx, 3, peers)
    for copy in bwd_stats:
        copy.start()

    y_copy.wait_recv()
    y_o[...] = (x_v[...].astype(F32) + (y_snd[...].astype(F32) + y_rx[...].astype(F32))).astype(BF16)

    d_gamma = jnp.zeros_like(dgamma_ref)
    for r in range(SPLITS):
        dh_copy(r).wait_recv()
        d_nrm = dh_snd[r].astype(F32) + dh_rx[r].astype(F32)
        d_gamma = d_gamma + jnp.sum(d_nrm * both(xhat_v, r), axis=0, keepdims=True)
        dh_v[r * piece:(r + 1) * piece] = d_nrm[:piece]
        dh_v[half + r * piece:half + (r + 1) * piece] = d_nrm[piece:]
    dgamma_ref[...] = d_gamma
    for copy in bwd_stats:
        copy.wait_recv()
    st_sum[...] = ((bst_snd[...] + bst_rx[0]) + (bst_rx[1] + bst_rx[2])) + ((bst_rx[3] + bst_rx[4]) + (bst_rx[5] + bst_rx[6]))
    sum_d, sum_dx = stats_columns(st_sum)
    d_hat = dh_v[...] * gamma_ref[...]
    d_x = dy_v[...].astype(F32) + inv_v[:, 0:1] * (d_hat - sum_d / d_model - xhat_v[...] * (sum_dx / d_model))
    dx_o[...] = d_x.astype(BF16)

    def drain(b, carry):
        core_copy(b).wait_send()
        return carry

    lax.fori_loop(0, N_BLK, drain, 0)
    for u in range(N_X):
        x_copy(u).wait_send()
    for k in range(4):
        for i in range(3 if k < 3 else 1):
            gather_copy(k, i).wait_send()
    for r in range(SPLITS):
        for i in (1, 2):
            piece_copy(r, i).wait_send()
        dh_copy(r).wait_send()
    for copy in [packed_copy, dkv_copy, y_copy, kv_copy] + fwd_stats + bwd_stats:
        copy.wait_send()


def grad_kernel(y_v, dx_v, dgamma_in, nrm_v, attn_v, md, dq_v, dkv_v, dy_v,
                y_hbm, dx_hbm, dgamma_ref, dwq_hbm, dwg_hbm, dwu_hbm, dwk_hbm, dwv_hbm, dwo_hbm, dwd_hbm,
                nrm_t, ring, out_sem, cp_sem):
    n_tok, width = nrm_v.shape
    half = n_tok // 2
    n_ring = ring.shape[0]
    core = lax.rem(lax.axis_index('tx'), 2)
    mine = pl.multiple_of(core * half, half)
    other = pl.multiple_of((1 - core) * half, half)
    hand_out = [pltpu.make_async_copy(src.at[lo:lo + half], dst.at[pl.ds(at, half)], cp_sem.at[i])
                for i, (src, dst, lo, at) in enumerate(((y_v, y_hbm, 0, mine), (y_v, y_hbm, half, other), (dx_v, dx_hbm, 0, mine), (dx_v, dx_hbm, half, other)))]
    for cp in hand_out:
        cp.start()
    dgamma_ref[...] = dgamma_in[...]

    flight = []

    def emit(value, dsts):
        t = len(flight)
        slot = t % n_ring
        if t >= n_ring:
            for cp in flight[t - n_ring]:
                cp.wait()
        ring[slot] = value
        copies = [pltpu.make_async_copy(ring.at[slot, :, lo:hi], dst, out_sem.at[slot, i]) for i, (lo, hi, dst) in enumerate(dsts)]
        for cp in copies:
            cp.start()
        flight.append(copies)

    nrm_t[...] = nrm_v[...].T

    def columns(grads, col, out, to):
        emit(mm(nrm_t[...], grads[:, col:col + BLK]), [(0, BLK, out.at[:, to:to + BLK])])

    def rows(acts, col, out, to):
        emit(mm_at(acts[:, col:col + width], dy_v[...]), [(0, BLK, out.at[to:to + width, :])])

    for j in range(2):
        columns(dq_v, j * BLK, dwq_hbm, j * BLK)
    for k in range(4):
        for j in range(2):
            columns(md.at[k, 1], j * BLK, dwg_hbm, k * CHUNK + j * BLK)
        for j in range(2):
            columns(md.at[k, 2], j * BLK, dwu_hbm, k * CHUNK + j * BLK)
        for j in range(2):
            rows(md.at[k, 0], j * BLK, dwd_hbm, k * CHUNK + j * BLK)
    for j in range(2):
        rows(attn_v, j * BLK, dwo_hbm, j * BLK)
    emit(mm(nrm_t[...], dkv_v[...]), [(0, 256, dwk_hbm), (256, 512, dwv_hbm)])
    for copies in flight[-n_ring:]:
        for cp in copies:
            cp.wait()
    for cp in hand_out:
        cp.wait()


def solution(mesh):
    tx_size = mesh.shape['tx']
    tok_spec = P('dp', None, 'tx')
    in_specs = (tok_spec, P('dp', None), tok_spec, P('tx'), P('tx', 'ty'), P('tx', 'ty'), P('tx', 'ty'),
                P('tx', None), P('tx', None), P('ty', 'tx'), P('ty', 'tx'))
    out_specs = (tok_spec, tok_spec, P(('dp', 'tx')), P(('dp', 'tx'), 'ty'), P(('dp', 'tx'), 'ty'), P(('dp', 'tx'), 'ty'),
                 P(('dp', 'tx'), None), P(('dp', 'tx'), None), P(('dp', 'ty'), 'tx'), P(('dp', 'ty'), 'tx'))

    def local_layer(x_in, positions, d_y, ln_gamma, w_q, w_g, w_u, w_k, w_v, w_o, w_d):
        _, n_tok, d_local = x_in.shape
        half = n_tok // 2
        d_model = d_local * tx_size
        head_dim = w_k.shape[1]
        q_width = w_q.shape[1]
        d_ff = w_g.shape[1]
        freq = jnp.asarray((ROPE_BASE ** (-2.0 * np.arange(head_dim // 2) / head_dim)).astype(np.float32)[None])
        any_spec = pl.BlockSpec(memory_space=pl.ANY)
        vmem_spec = pl.BlockSpec(memory_space=pltpu.VMEM)
        tok = (n_tok, d_local)
        sem = pltpu.SemaphoreType.DMA
        vm = pltpu.VMEM
        kept = pl.pallas_call(
            functools.partial(layer_kernel, d_model),
            out_shape=[vm(tok, BF16), vm(tok, BF16), vm((1, d_local), F32), vm(tok, BF16), vm((n_tok, q_width), BF16),
                       vm((4, 3, n_tok, CHUNK), BF16), vm((n_tok, q_width), BF16), vm((n_tok, 2 * head_dim), BF16), vm(tok, BF16)],
            in_specs=[any_spec, vmem_spec, vmem_spec, any_spec, vmem_spec] + [any_spec] * 7,
            out_specs=[vmem_spec] * 9,
            scratch_shapes=[
                vm(tok, BF16), vm((d_local, q_width + 2 * head_dim), BF16), vm((d_local, d_ff), BF16), vm((d_local, d_ff), BF16),
                vm((q_width, d_local), BF16), vm((d_ff, d_local), BF16),
                vm((N_BLK, half, BLK), F32), vm((N_BLK, half, BLK), BF16), vm((N_BLK, half, BLK), BF16),
                vm((N_BLK, half, BLK), BF16), vm((N_BLK, half, BLK), BF16), vm((n_tok, 2 * q_width + 2 * head_dim), BF16),
                vm((n_tok, 512), BF16), vm((n_tok, 512), BF16), vm((n_tok, 512), F32),
                vm(tok, F32), vm((n_tok, 128), F32), vm((n_tok, 128), F32), vm((n_tok, 128), F32), vm(tok, F32), vm(tok, F32),
                vm(tok, BF16), vm(tok, BF16), vm((SPLITS, n_tok // SPLITS, d_local), BF16), vm((SPLITS, n_tok // SPLITS, d_local), BF16),
                vm((8, n_tok), F32), vm((3, 8, n_tok), F32), vm((8, n_tok), F32), vm((8, n_tok), F32), vm((7, 8, n_tok), F32),
                sem((12,)), sem((N_BLK,)), sem((N_BLK,)), sem((N_X,)), sem((N_X,)),
                sem((12 + 2 * SPLITS,)), sem((12 + 2 * SPLITS,)), sem((1,)), sem((1,)), sem((4,)), sem((4,)), sem((10,)), sem((10,)),
                sem((SPLITS,)), sem((SPLITS,))],
            compiler_params=pltpu.CompilerParams(collective_id=0, has_side_effects=True, vmem_limit_bytes=50 * 1024 * 1024),
            name='layer',
        )(x_in.reshape(tok), positions, freq, d_y.reshape(tok), ln_gamma[None], w_q, w_g, w_u, w_k, w_v, w_o, w_d)

        y_out, d_x, d_gamma, d_wq, d_wg, d_wu, d_wk, d_wv, d_wo, d_wd = pl.pallas_call(
            grad_kernel,
            out_shape=[jax.ShapeDtypeStruct(tok, BF16), jax.ShapeDtypeStruct(tok, BF16), jax.ShapeDtypeStruct((1, d_local), F32)]
            + [jax.ShapeDtypeStruct(w.shape, F32) for w in (w_q, w_g, w_u, w_k, w_v, w_o, w_d)],
            in_specs=[vmem_spec] * 9,
            out_specs=[any_spec, any_spec, vmem_spec] + [any_spec] * 7,
            scratch_shapes=[vm((d_local, n_tok), BF16), vm((12, d_local, BLK), F32), sem((12, 2)), sem((4,))],
            compiler_params=pltpu.CompilerParams(vmem_limit_bytes=40 * 1024 * 1024),
            name='weight_grads',
        )(*kept)
        return (y_out.reshape(x_in.shape), d_x.reshape(x_in.shape), d_gamma.reshape(d_local),
                d_wq, d_wg, d_wu, d_wk, d_wv, d_wo, d_wd)

    return jax.shard_map(local_layer, mesh=mesh, in_specs=in_specs, out_specs=out_specs, check_vma=False)
```

```python
import functools

import jax
import jax.numpy as jnp
import numpy as np
from jax import lax
from jax.experimental import pallas as pl
from jax.experimental.pallas import tpu as pltpu
from jax.sharding import PartitionSpec as P

EPS = 1e-6
ROPE_BASE = 10000.0
F32 = jnp.float32
BF16 = jnp.bfloat16
MESH = pl.DeviceIdType.MESH

BLK = 512
CHUNK = 1024
B_DATTN, B_DACT_LO, B_QKV, B_GU, B_DACT_HI, N_BLK = 0, 2, 6, 9, 25, 29
X_UNITS = ((0, 1), (1, 1), (2, 2), (4, 2), (6, 2), (9, 4), (13, 4), (17, 4), (21, 4), (25, 2))
SPLITS = 4
X_KV = len(X_UNITS)
X_LAST = X_KV + 1
N_X = X_LAST + SPLITS


def dot(a, b, dims):
    return lax.dot_general(a, b, (dims, ((), ())), preferred_element_type=F32)


def mm(a, b):
    return dot(a, b, ((1,), (0,)))


def mm_bt(a, b):
    return dot(a, b, ((1,), (1,)))


def mm_at(a, b):
    return dot(a, b, ((0,), (0,)))


def rope(first, second, cos_t, sin_t):
    return first * cos_t - second * sin_t, second * cos_t + first * sin_t


def layer_kernel(d_model, x_hbm, pos_ref, freq_ref, dy_hbm, gamma_ref, wq_hbm, wg_hbm, wu_hbm, wk_hbm, wv_hbm, wo_hbm, wd_hbm,
                 y_o, dx_o, dgamma_ref, nrm_v, attn_v, md, dq_v, dkv_v, dy_v,
                 x_v, wqkv_v, wg_v, wu_v, wo_v, wd_v,
                 keep, send, rcore, chip, rx, packed, dkv_part, dkv_rx, kv_acc,
                 xhat_v, inv_v, cos_v, sin_v, br_v, dh_v, y_snd, y_rx, dh_snd, dh_rx,
                 st_snd, st_rx, st_sum, bst_snd, bst_rx, factors,
                 ld_sem, cs, cr, xs, xr, gs, gr, ps, pr, ts, tr, ss, sr, ds, dr):
    tx = lax.axis_index('tx')
    ty = lax.axis_index('ty')
    core = lax.rem(tx, 2)
    near = {'tx': tx + 1 - 2 * core}
    across = {'tx': lax.rem(tx + 2, 4)}
    far = {'tx': lax.rem(tx + 1 - 2 * core + 2, 4)}
    other_ty = {'ty': 1 - ty}
    peers = [near, across, far, other_ty] + [{'tx': p['tx'], 'ty': 1 - ty} for p in (near, across, far)]
    n_tok = x_v.shape[0]
    half = n_tok // 2
    mine = pl.multiple_of(core * half, half)
    other = pl.multiple_of((1 - core) * half, half)
    head_dim = 256
    q_width = wo_v.shape[0]
    heads = q_width // head_dim
    piece = half // SPLITS

    def load(i, src, dst):
        return pltpu.make_async_copy(src, dst, ld_sem.at[i])

    d_half = wd_v.shape[0] // 2
    loads = [
        load(0, dy_hbm.at[pl.ds(mine, half)], dy_v.at[0:half]),
        load(1, dy_hbm.at[pl.ds(other, half)], dy_v.at[half:n_tok]),
        load(2, wo_hbm, wo_v),
        load(3, x_hbm.at[pl.ds(mine, half)], x_v.at[0:half]),
        load(4, x_hbm.at[pl.ds(other, half)], x_v.at[half:n_tok]),
        load(5, wd_hbm.at[0:d_half], wd_v.at[0:d_half]),
        load(6, wq_hbm, wqkv_v.at[:, 0:q_width]),
        load(7, wk_hbm, wqkv_v.at[:, q_width:q_width + head_dim]),
        load(8, wv_hbm, wqkv_v.at[:, q_width + head_dim:q_width + 2 * head_dim]),
        load(9, wg_hbm, wg_v),
        load(10, wu_hbm, wu_v),
        load(11, wd_hbm.at[d_half:2 * d_half], wd_v.at[d_half:2 * d_half]),
    ]
    for ld in loads[:5]:
        ld.start()

    barrier = pltpu.get_barrier_semaphore()
    for peer in peers:
        pl.semaphore_signal(barrier, inc=1, device_id=peer, device_id_type=MESH)
    for ld in loads[:3]:
        ld.wait()
    for ld in loads[5:]:
        ld.start()
    pl.semaphore_wait(barrier, len(peers))

    def remote(src, dst, send_sem, recv_sem, peer):
        return pltpu.make_async_remote_copy(src_ref=src, dst_ref=dst, send_sem=send_sem, recv_sem=recv_sem,
                                            device_id=peer, device_id_type=MESH)

    def core_copy(b):
        return remote(send.at[b], rcore.at[b], cs.at[b], cr.at[b], near)

    def x_copy(u):
        if u >= X_LAST:
            rows = pl.ds((u - X_LAST) * piece, piece)
            return remote(chip.at[pl.ds(N_BLK - 2, 2), rows], rx.at[pl.ds(N_BLK - 2, 2), rows], xs.at[u], xr.at[u], across)
        if u == X_KV:
            cols = pl.ds(pl.multiple_of(ty * head_dim, head_dim), head_dim)
            return remote(chip.at[B_QKV + 2, :, cols], rx.at[B_QKV + 2, :, cols], xs.at[u], xr.at[u], across)
        start, count = X_UNITS[u]
        return remote(chip.at[pl.ds(start, count)], rx.at[pl.ds(start, count)], xs.at[u], xr.at[u], across)

    def put(b, part):
        keep[b] = part[:half]
        send[b] = part[half:].astype(BF16)
        core_copy(b).start()

    def issue_bwd(b, w_ref, row):
        put(b, mm_bt(dy_v[...], w_ref[pl.ds(row, BLK), :]))

    def issue_fwd(b, w_ref, col):
        put(b, mm(nrm_v[...], w_ref[:, pl.ds(col, BLK)]))

    def combine(b):
        core_copy(b).wait_recv()
        chip[b] = (keep[b] + rcore[b].astype(F32)).astype(BF16)

    def total(b):
        return chip[b].astype(F32) + rx[b].astype(F32)

    issue_bwd(0, wo_v, 0)
    issue_bwd(1, wo_v, BLK)

    def rows_of(col_a, col_b):
        lane = lax.broadcasted_iota(jnp.int32, (half, 128), 1)
        return jnp.where(lane == 0, col_a, col_b).T[0:8]

    def stats_copies(snd, got, base, to):
        return [remote(snd, got.at[i], ss.at[base + i], sr.at[base + i], peer) for i, peer in enumerate(to)]

    def stats_put(snd, col_a, col_b):
        for lo, at in ((0, mine), (half, other)):
            snd[:, pl.ds(at, half)] = rows_of(col_a[lo:lo + half], col_b[lo:lo + half])

    def stats_columns(rows_ref):
        cols = []
        for i in range(2):
            parts = [jnp.broadcast_to(rows_ref[i:i + 1, pl.ds(at, half)], (128, half)).T[:, 0:1] for at in (mine, other)]
            cols.append(jnp.concatenate(parts, axis=0))
        return cols

    loads[3].wait()
    loads[4].wait()
    x_f = x_v[...].astype(F32)
    stats_put(st_snd, jnp.sum(x_f, axis=1, keepdims=True), jnp.sum(x_f * x_f, axis=1, keepdims=True))
    fwd_stats = stats_copies(st_snd, st_rx, 0, (near, across, far))
    for copy in fwd_stats:
        copy.start()

    combine(0)
    x_copy(0).start()
    combine(1)
    x_copy(1).start()

    loads[5].wait()
    for i in range(4):
        issue_bwd(B_DACT_LO + i, wd_v, i * BLK)
        if i >= 1:
            combine(B_DACT_LO + i - 1)
        if i == 2:
            x_copy(2).start()
    combine(B_DACT_LO + 3)
    x_copy(3).start()

    for copy in fwd_stats:
        copy.wait_recv()
    st_sum[...] = (st_snd[...] + st_rx[0]) + (st_rx[1] + st_rx[2])
    sum_x, sum_xx = stats_columns(st_sum)
    tok_mean = sum_x / d_model
    inv_std = lax.rsqrt(sum_xx / d_model - tok_mean * tok_mean + EPS)
    inv_v[...] = jnp.broadcast_to(inv_std, (n_tok, 128))
    x_hat = (x_v[...].astype(F32) - tok_mean) * inv_std
    xhat_v[...] = x_hat
    nrm_v[...] = (x_hat * gamma_ref[...]).astype(BF16)

    for i in range(6, 9):
        loads[i].wait()
    for i in range(3):
        issue_fwd(B_QKV + i, wqkv_v, i * BLK)
    for i in (2, 0, 1):
        combine(B_QKV + i)
        if i == 2:
            x_copy(X_KV).start()
    x_copy(4).start()

    loads[9].wait()
    loads[10].wait()
    for k in range(4):
        def gu_issue(j, carry, k=k):
            col = pl.multiple_of(k * CHUNK + j * BLK, BLK)
            issue_fwd(B_GU + 4 * k + j, wg_v, col)
            issue_fwd(B_GU + 4 * k + 2 + j, wu_v, col)
            return carry

        def gu_combine(j, carry, k=k):
            combine(B_GU + 4 * k + j)
            return carry

        lax.fori_loop(0, 2, gu_issue, 0)
        lax.fori_loop(0, 4, gu_combine, 0)
        x_copy(5 + k).start()

    loads[11].wait()

    def hi_issue(j, carry):
        issue_bwd(B_DACT_HI + j, wd_v, pl.multiple_of(d_half + j * BLK, BLK))
        return carry

    lax.fori_loop(0, 4, hi_issue, 0)
    for j in range(4):
        combine(B_DACT_HI + j)
        if j == 1:
            x_copy(9).start()
    for r in range(SPLITS):
        x_copy(X_LAST + r).start()

    freq = freq_ref[...]
    for lo, at in ((0, mine), (half, other)):
        pos_col = jnp.broadcast_to(pos_ref[0:1, pl.ds(at, half)].astype(F32), (128, half)).T
        angles = pos_col * freq
        cos_v[lo:lo + half] = jnp.cos(angles)
        sin_v[lo:lo + half] = jnp.sin(angles)

    packed_copy = remote(packed.at[0:half], packed.at[half:n_tok], ps.at[0], pr.at[0], near)
    x_copy(0).wait_recv()
    x_copy(1).wait_recv()
    for j in range(2):
        packed[0:half, q_width + 512 + j * BLK:q_width + 512 + (j + 1) * BLK] = total(B_DATTN + j).astype(BF16)
    x_copy(4).wait_recv()
    cos_h, sin_h = cos_v[0:half], sin_v[0:half]
    for j in range(2):
        blk = total(B_QKV + j)
        for h in range(2):
            lo = h * head_dim
            first, second = rope(blk[:, lo:lo + 128], blk[:, lo + 128:lo + 256], cos_h, sin_h)
            packed[0:half, j * BLK + lo:j * BLK + lo + 128] = first.astype(BF16)
            packed[0:half, j * BLK + lo + 128:j * BLK + lo + 256] = second.astype(BF16)
    x_copy(X_KV).wait_recv()
    kv_cols = pl.ds(pl.multiple_of(ty * head_dim, head_dim), head_dim)
    blk = chip[B_QKV + 2, :, kv_cols].astype(F32) + rx[B_QKV + 2, :, kv_cols].astype(F32)
    first, second = rope(blk[:, 0:128], blk[:, 128:256], cos_h, sin_h)
    kv_mine = jnp.where(ty == 0, jnp.concatenate([first, second], axis=1), blk).astype(BF16)
    kv_dst = packed.at[0:half, pl.ds(pl.multiple_of(q_width + ty * head_dim, head_dim), head_dim)]
    kv_dst[...] = kv_mine
    kv_copy = remote(kv_dst, kv_dst, ts.at[3], tr.at[3], other_ty)
    kv_copy.start()
    kv_copy.wait_recv()
    packed_copy.start()
    packed_copy.wait_recv()

    row_i = lax.rem(lax.broadcasted_iota(jnp.int32, (n_tok, n_tok), 0) + core * half, n_tok)
    col_i = lax.rem(lax.broadcasted_iota(jnp.int32, (n_tok, n_tok), 1) + core * half, n_tok)
    scale = head_dim ** -0.5
    kv_acc[...] = jnp.zeros_like(kv_acc)

    def head_step(h, carry):
        cols = pl.ds(pl.multiple_of(h * head_dim, head_dim), head_dim)
        q_h = packed[:, cols]
        da_h = packed[:, pl.ds(pl.multiple_of(q_width + 512 + h * head_dim, head_dim), head_dim)]
        k_rot = packed[:, q_width:q_width + 256]
        v_val = packed[:, q_width + 256:q_width + 512]
        scores = jnp.where(row_i >= col_i, mm_bt(q_h, k_rot) * scale, -1e30)
        exps = jnp.exp(scores - jnp.max(scores, axis=1, keepdims=True))
        probs_f = exps / jnp.sum(exps, axis=1, keepdims=True)
        probs = probs_f.astype(BF16)
        attn_v[:, cols] = mm(probs, v_val).astype(BF16)
        d_probs = mm_bt(da_h, v_val).astype(BF16).astype(F32)
        d_scores = (probs_f * (d_probs - jnp.sum(d_probs * probs_f, axis=1, keepdims=True)) * scale).astype(BF16)
        dq_h = mm(d_scores, k_rot).astype(BF16).astype(F32)
        first, second = rope(dq_h[:, 0:128], dq_h[:, 128:256], cos_v[...], -sin_v[...])
        dq_v[:, pl.ds(pl.multiple_of(h * head_dim, head_dim), 128)] = first.astype(BF16)
        dq_v[:, pl.ds(pl.multiple_of(h * head_dim + 128, 128), 128)] = second.astype(BF16)
        kv_acc[:, 0:256] += mm_at(d_scores, q_h)
        kv_acc[:, 256:512] += mm_at(probs, da_h)
        return carry

    lax.fori_loop(0, heads, head_step, 0)
    dkv_part[...] = kv_acc[...].astype(BF16)
    dkv_copy = remote(dkv_part, dkv_rx, ts.at[0], tr.at[0], other_ty)
    dkv_copy.start()
    br_v[...] = mm(attn_v[...], wo_v[...])
    dh_v[...] = mm_bt(dq_v[...], wqkv_v[:, 0:q_width])

    def piece_copy(r):
        return remote(md.at[3, 1:3, r * piece:(r + 1) * piece], md.at[3, 1:3, half + r * piece:half + (r + 1) * piece],
                      gs.at[12 + r], gr.at[12 + r], near)

    def gather_copy(k, i):
        return remote(md.at[k, i, 0:half], md.at[k, i, half:n_tok], gs.at[3 * k + i], gr.at[3 * k + i], near)

    def dact_block(k, j):
        return B_DACT_LO + 2 * k + j if k < 2 else B_DACT_HI + 2 * (k - 2) + j

    def gated(k, want_act, want_grad):
        def step(r, carry):
            rows = pl.ds(pl.multiple_of(r * 16, 16), 16)
            for j in range(2):
                bg, bu, bd = B_GU + 4 * k + j, B_GU + 4 * k + 2 + j, dact_block(k, j)
                gate = (chip[bg, rows].astype(F32) + rx[bg, rows].astype(F32)).astype(BF16).astype(F32)
                up = (chip[bu, rows].astype(F32) + rx[bu, rows].astype(F32)).astype(BF16).astype(F32)
                sig = jax.nn.sigmoid(gate)
                silu = gate * sig
                cols = slice(j * BLK, (j + 1) * BLK)
                if want_act:
                    md[k, 0, rows, cols] = (silu * up).astype(BF16)
                if k == 3:
                    factors[0, rows, cols] = up * sig * (1.0 + gate * (1.0 - sig))
                    factors[1, rows, cols] = silu
                if want_grad:
                    d_act = (chip[bd, rows].astype(F32) + rx[bd, rows].astype(F32)).astype(BF16).astype(F32)
                    md[k, 1, rows, cols] = (d_act * up * sig * (1.0 + gate * (1.0 - sig))).astype(BF16)
                    md[k, 2, rows, cols] = (d_act * silu).astype(BF16)
            return carry

        lax.fori_loop(0, half // 16, step, 0)
        for i in ((0,) if want_act else ()) + ((1, 2) if want_grad else ()):
            gather_copy(k, i).start()

    def use_act(k):
        gather_copy(k, 0).wait_recv()
        br_v[...] += mm(md[k, 0], wd_v[k * CHUNK:(k + 1) * CHUNK, :])

    def use_grad(k):
        for i in (1, 2):
            gather_copy(k, i).wait_recv()
        dh_v[...] += (mm_bt(md[k, 1], wg_v[:, k * CHUNK:(k + 1) * CHUNK])
                      + mm_bt(md[k, 2], wu_v[:, k * CHUNK:(k + 1) * CHUNK]))

    x_copy(2).wait_recv()
    x_copy(3).wait_recv()
    for k in range(2):
        x_copy(5 + k).wait_recv()
        gated(k, True, True)
        use_act(k)
        use_grad(k)
        if k == 0:
            dkv_copy.wait_recv()
            d_k = dkv_part[:, 0:256].astype(F32) + dkv_rx[:, 0:256].astype(F32)
            d_k = d_k.astype(BF16).astype(F32)
            first, second = rope(d_k[:, 0:128], d_k[:, 128:256], cos_v[...], -sin_v[...])
            dkv_v[:, 0:128] = first.astype(BF16)
            dkv_v[:, 128:256] = second.astype(BF16)
            dkv_v[:, 256:512] = (dkv_part[:, 256:512].astype(F32) + dkv_rx[:, 256:512].astype(F32)).astype(BF16)
            dh_v[...] += 0.5 * mm_bt(dkv_v[...], wqkv_v[:, q_width:q_width + 512])
    for k in (2, 3):
        x_copy(5 + k).wait_recv()
        gated(k, True, False)
        use_act(k)
    y_snd[...] = br_v[...].astype(BF16)
    y_copy = remote(y_snd, y_rx, ts.at[1], tr.at[1], other_ty)
    y_copy.start()
    x_copy(9).wait_recv()
    gated(2, False, True)

    def dh_copy(r):
        return remote(dh_snd.at[r], dh_rx.at[r], ds.at[r], dr.at[r], other_ty)

    def both(ref, r):
        return jnp.concatenate([ref[r * piece:(r + 1) * piece], ref[half + r * piece:half + (r + 1) * piece]], axis=0)

    sums = []

    def piece_grad(r):
        x_copy(X_LAST + r).wait_recv()
        rows = slice(r * piece, (r + 1) * piece)
        for j in range(2):
            cols = slice(j * BLK, (j + 1) * BLK)
            b = dact_block(3, j)
            d_act = (chip[b, rows].astype(F32) + rx[b, rows].astype(F32)).astype(BF16).astype(F32)
            for i in range(2):
                md[3, 1 + i, rows, cols] = (d_act * factors[i, rows, cols]).astype(BF16)
        piece_copy(r).start()

    def piece_dh(r):
        piece_copy(r).wait_recv()
        part = both(dh_v, r) + mm_bt(both(md.at[3, 1], r), wg_v[:, 3 * CHUNK:4 * CHUNK]) + mm_bt(both(md.at[3, 2], r), wu_v[:, 3 * CHUNK:4 * CHUNK])
        part_b = part.astype(BF16)
        dh_snd[r] = part_b
        dh_copy(r).start()
        d_hat = part_b.astype(F32) * gamma_ref[...]
        sums.append((jnp.sum(d_hat, axis=1, keepdims=True), jnp.sum(d_hat * both(xhat_v, r), axis=1, keepdims=True)))

    piece_grad(0)
    use_grad(2)
    for r in range(1, SPLITS):
        piece_grad(r)
        piece_dh(r - 1)
    piece_dh(SPLITS - 1)
    cols = [jnp.concatenate([sums[r][i][:piece] for r in range(SPLITS)] + [sums[r][i][piece:] for r in range(SPLITS)], axis=0) for i in range(2)]
    stats_put(bst_snd, cols[0], cols[1])
    bwd_stats = stats_copies(bst_snd, bst_rx, 3, peers)
    for copy in bwd_stats:
        copy.start()

    y_copy.wait_recv()
    y_o[...] = (x_v[...].astype(F32) + (y_snd[...].astype(F32) + y_rx[...].astype(F32))).astype(BF16)

    d_gamma = jnp.zeros_like(dgamma_ref)
    for r in range(SPLITS):
        dh_copy(r).wait_recv()
        d_nrm = dh_snd[r].astype(F32) + dh_rx[r].astype(F32)
        d_gamma = d_gamma + jnp.sum(d_nrm * both(xhat_v, r), axis=0, keepdims=True)
        dh_v[r * piece:(r + 1) * piece] = d_nrm[:piece]
        dh_v[half + r * piece:half + (r + 1) * piece] = d_nrm[piece:]
    dgamma_ref[...] = d_gamma
    for copy in bwd_stats:
        copy.wait_recv()
    st_sum[...] = ((bst_snd[...] + bst_rx[0]) + (bst_rx[1] + bst_rx[2])) + ((bst_rx[3] + bst_rx[4]) + (bst_rx[5] + bst_rx[6]))
    sum_d, sum_dx = stats_columns(st_sum)
    d_hat = dh_v[...] * gamma_ref[...]
    d_x = dy_v[...].astype(F32) + inv_v[:, 0:1] * (d_hat - sum_d / d_model - xhat_v[...] * (sum_dx / d_model))
    dx_o[...] = d_x.astype(BF16)

    def drain(b, carry):
        core_copy(b).wait_send()
        return carry

    lax.fori_loop(0, N_BLK, drain, 0)
    for u in range(N_X):
        x_copy(u).wait_send()
    for k in range(4):
        for i in range(3 if k < 3 else 1):
            gather_copy(k, i).wait_send()
    for r in range(SPLITS):
        piece_copy(r).wait_send()
        dh_copy(r).wait_send()
    for copy in [packed_copy, dkv_copy, y_copy, kv_copy] + fwd_stats + bwd_stats:
        copy.wait_send()


def grad_kernel(y_v, dx_v, dgamma_in, nrm_v, attn_v, md, dq_v, dkv_v, dy_v,
                y_hbm, dx_hbm, dgamma_ref, dwq_hbm, dwg_hbm, dwu_hbm, dwk_hbm, dwv_hbm, dwo_hbm, dwd_hbm,
                nrm_t, ring, out_sem, cp_sem):
    n_tok, width = nrm_v.shape
    half = n_tok // 2
    n_ring = ring.shape[0]
    core = lax.rem(lax.axis_index('tx'), 2)
    mine = pl.multiple_of(core * half, half)
    other = pl.multiple_of((1 - core) * half, half)
    hand_out = [pltpu.make_async_copy(src.at[lo:lo + half], dst.at[pl.ds(at, half)], cp_sem.at[i])
                for i, (src, dst, lo, at) in enumerate(((y_v, y_hbm, 0, mine), (y_v, y_hbm, half, other), (dx_v, dx_hbm, 0, mine), (dx_v, dx_hbm, half, other)))]
    for cp in hand_out:
        cp.start()
    dgamma_ref[...] = dgamma_in[...]

    flight = []

    def emit(value, dsts):
        t = len(flight)
        slot = t % n_ring
        if t >= n_ring:
            for cp in flight[t - n_ring]:
                cp.wait()
        ring[slot] = value
        copies = [pltpu.make_async_copy(ring.at[slot, :, lo:hi], dst, out_sem.at[slot, i]) for i, (lo, hi, dst) in enumerate(dsts)]
        for cp in copies:
            cp.start()
        flight.append(copies)

    nrm_t[...] = nrm_v[...].T

    def columns(grads, col, out, to):
        emit(mm(nrm_t[...], grads[:, col:col + BLK]), [(0, BLK, out.at[:, to:to + BLK])])

    def rows(acts, col, out, to):
        emit(mm_at(acts[:, col:col + width], dy_v[...]), [(0, BLK, out.at[to:to + width, :])])

    for j in range(2):
        columns(dq_v, j * BLK, dwq_hbm, j * BLK)
    for k in range(4):
        for j in range(2):
            columns(md.at[k, 1], j * BLK, dwg_hbm, k * CHUNK + j * BLK)
        for j in range(2):
            columns(md.at[k, 2], j * BLK, dwu_hbm, k * CHUNK + j * BLK)
        for j in range(2):
            rows(md.at[k, 0], j * BLK, dwd_hbm, k * CHUNK + j * BLK)
    for j in range(2):
        rows(attn_v, j * BLK, dwo_hbm, j * BLK)
    emit(mm(nrm_t[...], dkv_v[...]), [(0, 256, dwk_hbm), (256, 512, dwv_hbm)])
    for copies in flight[-n_ring:]:
        for cp in copies:
            cp.wait()
    for cp in hand_out:
        cp.wait()


def solution(mesh):
    tx_size = mesh.shape['tx']
    tok_spec = P('dp', None, 'tx')
    in_specs = (tok_spec, P('dp', None), tok_spec, P('tx'), P('tx', 'ty'), P('tx', 'ty'), P('tx', 'ty'),
                P('tx', None), P('tx', None), P('ty', 'tx'), P('ty', 'tx'))
    out_specs = (tok_spec, tok_spec, P(('dp', 'tx')), P(('dp', 'tx'), 'ty'), P(('dp', 'tx'), 'ty'), P(('dp', 'tx'), 'ty'),
                 P(('dp', 'tx'), None), P(('dp', 'tx'), None), P(('dp', 'ty'), 'tx'), P(('dp', 'ty'), 'tx'))

    def local_layer(x_in, positions, d_y, ln_gamma, w_q, w_g, w_u, w_k, w_v, w_o, w_d):
        _, n_tok, d_local = x_in.shape
        half = n_tok // 2
        d_model = d_local * tx_size
        head_dim = w_k.shape[1]
        q_width = w_q.shape[1]
        d_ff = w_g.shape[1]
        freq = jnp.asarray((ROPE_BASE ** (-2.0 * np.arange(head_dim // 2) / head_dim)).astype(np.float32)[None])
        any_spec = pl.BlockSpec(memory_space=pl.ANY)
        vmem_spec = pl.BlockSpec(memory_space=pltpu.VMEM)
        tok = (n_tok, d_local)
        sem = pltpu.SemaphoreType.DMA
        vm = pltpu.VMEM
        kept = pl.pallas_call(
            functools.partial(layer_kernel, d_model),
            out_shape=[vm(tok, BF16), vm(tok, BF16), vm((1, d_local), F32), vm(tok, BF16), vm((n_tok, q_width), BF16),
                       vm((4, 3, n_tok, CHUNK), BF16), vm((n_tok, q_width), BF16), vm((n_tok, 2 * head_dim), BF16), vm(tok, BF16)],
            in_specs=[any_spec, vmem_spec, vmem_spec, any_spec, vmem_spec] + [any_spec] * 7,
            out_specs=[vmem_spec] * 9,
            scratch_shapes=[
                vm(tok, BF16), vm((d_local, q_width + 2 * head_dim), BF16), vm((d_local, d_ff), BF16), vm((d_local, d_ff), BF16),
                vm((q_width, d_local), BF16), vm((d_ff, d_local), BF16),
                vm((N_BLK, half, BLK), F32), vm((N_BLK, half, BLK), BF16), vm((N_BLK, half, BLK), BF16),
                vm((N_BLK, half, BLK), BF16), vm((N_BLK, half, BLK), BF16), vm((n_tok, 2 * q_width + 2 * head_dim), BF16),
                vm((n_tok, 512), BF16), vm((n_tok, 512), BF16), vm((n_tok, 512), F32),
                vm(tok, F32), vm((n_tok, 128), F32), vm((n_tok, 128), F32), vm((n_tok, 128), F32), vm(tok, F32), vm(tok, F32),
                vm(tok, BF16), vm(tok, BF16), vm((SPLITS, n_tok // SPLITS, d_local), BF16), vm((SPLITS, n_tok // SPLITS, d_local), BF16),
                vm((8, n_tok), F32), vm((3, 8, n_tok), F32), vm((8, n_tok), F32), vm((8, n_tok), F32), vm((7, 8, n_tok), F32), vm((2, half, CHUNK), F32),
                sem((12,)), sem((N_BLK,)), sem((N_BLK,)), sem((N_X,)), sem((N_X,)),
                sem((12 + SPLITS,)), sem((12 + SPLITS,)), sem((1,)), sem((1,)), sem((4,)), sem((4,)), sem((10,)), sem((10,)),
                sem((SPLITS,)), sem((SPLITS,))],
            compiler_params=pltpu.CompilerParams(collective_id=0, has_side_effects=True, vmem_limit_bytes=50 * 1024 * 1024),
            name='layer',
        )(x_in.reshape(tok), positions, freq, d_y.reshape(tok), ln_gamma[None], w_q, w_g, w_u, w_k, w_v, w_o, w_d)

        y_out, d_x, d_gamma, d_wq, d_wg, d_wu, d_wk, d_wv, d_wo, d_wd = pl.pallas_call(
            grad_kernel,
            out_shape=[jax.ShapeDtypeStruct(tok, BF16), jax.ShapeDtypeStruct(tok, BF16), jax.ShapeDtypeStruct((1, d_local), F32)]
            + [jax.ShapeDtypeStruct(w.shape, F32) for w in (w_q, w_g, w_u, w_k, w_v, w_o, w_d)],
            in_specs=[vmem_spec] * 9,
            out_specs=[any_spec, any_spec, vmem_spec] + [any_spec] * 7,
            scratch_shapes=[vm((d_local, n_tok), BF16), vm((12, d_local, BLK), F32), sem((12, 2)), sem((4,))],
            compiler_params=pltpu.CompilerParams(vmem_limit_bytes=40 * 1024 * 1024),
            name='weight_grads',
        )(*kept)
        return (y_out.reshape(x_in.shape), d_x.reshape(x_in.shape), d_gamma.reshape(d_local),
                d_wq, d_wg, d_wu, d_wk, d_wv, d_wo, d_wd)

    return jax.shard_map(local_layer, mesh=mesh, in_specs=in_specs, out_specs=out_specs, check_vma=False)
```

```python
import functools

import jax
import jax.numpy as jnp
import numpy as np
from jax import lax
from jax.experimental import pallas as pl
from jax.experimental.pallas import tpu as pltpu
from jax.sharding import PartitionSpec as P

EPS = 1e-6
ROPE_BASE = 10000.0
F32 = jnp.float32
BF16 = jnp.bfloat16
MESH = pl.DeviceIdType.MESH

BLK = 512
CHUNK = 1024
B_DATTN, B_DACT_LO, B_QKV, B_GU, B_DACT_HI, N_BLK = 0, 2, 6, 9, 25, 29
X_UNITS = ((0, 1), (1, 1), (2, 2), (4, 2), (6, 2), (9, 4), (13, 4), (17, 4), (21, 4), (25, 2))
SPLITS = 8
X_KV = len(X_UNITS)
X_LAST = X_KV + 1
N_X = X_LAST + SPLITS


def dot(a, b, dims):
    return lax.dot_general(a, b, (dims, ((), ())), preferred_element_type=F32)


def mm(a, b):
    return dot(a, b, ((1,), (0,)))


def mm_bt(a, b):
    return dot(a, b, ((1,), (1,)))


def mm_at(a, b):
    return dot(a, b, ((0,), (0,)))


def rope(first, second, cos_t, sin_t):
    return first * cos_t - second * sin_t, second * cos_t + first * sin_t


def layer_kernel(d_model, x_hbm, pos_hbm, freq_hbm, dy_hbm, gamma_hbm, wq_hbm, wg_hbm, wu_hbm, wk_hbm, wv_hbm, wo_hbm, wd_hbm,
                 y_o, dx_o, dgamma_ref, nrm_t, attn_v, md, dq_v, dkv_v, dy_v, tiles,
                 pos_ref, freq_ref, gamma_ref, nrm_v, x_v, wqkv_v, wg_v, wu_v, wo_v, wd_v,
                 keep, send, rcore, chip, rx, packed, dkv_part, dkv_rx, kv_acc,
                 xhat_v, inv_v, cos_v, sin_v, br_v, dh_v, y_snd, y_rx, dh_snd, dh_rx,
                 st_snd, st_rx, st_sum, bst_snd, bst_rx, factors,
                 ld_sem, cs, cr, xs, xr, gs, gr, ps, pr, ts, tr, ss, sr, ds, dr):
    tx = lax.axis_index('tx')
    ty = lax.axis_index('ty')
    core = lax.rem(tx, 2)
    near = {'tx': tx + 1 - 2 * core}
    across = {'tx': lax.rem(tx + 2, 4)}
    far = {'tx': lax.rem(tx + 1 - 2 * core + 2, 4)}
    other_ty = {'ty': 1 - ty}
    peers = [near, across, far, other_ty] + [{'tx': p['tx'], 'ty': 1 - ty} for p in (near, across, far)]
    n_tok = x_v.shape[0]
    half = n_tok // 2
    mine = pl.multiple_of(core * half, half)
    other = pl.multiple_of((1 - core) * half, half)
    head_dim = 256
    q_width = wo_v.shape[0]
    heads = q_width // head_dim
    piece = half // SPLITS

    def load(i, src, dst):
        return pltpu.make_async_copy(src, dst, ld_sem.at[i])

    d_half = wd_v.shape[0] // 2
    loads = [
        load(0, dy_hbm.at[pl.ds(mine, half)], dy_v.at[0:half]),
        load(1, dy_hbm.at[pl.ds(other, half)], dy_v.at[half:n_tok]),
        load(2, wo_hbm, wo_v),
        load(3, x_hbm.at[pl.ds(mine, half)], x_v.at[0:half]),
        load(4, x_hbm.at[pl.ds(other, half)], x_v.at[half:n_tok]),
        load(5, wd_hbm.at[0:d_half], wd_v.at[0:d_half]),
        load(6, wq_hbm, wqkv_v.at[:, 0:q_width]),
        load(7, wk_hbm, wqkv_v.at[:, q_width:q_width + head_dim]),
        load(8, wv_hbm, wqkv_v.at[:, q_width + head_dim:q_width + 2 * head_dim]),
        load(9, wg_hbm, wg_v),
        load(10, wu_hbm, wu_v),
        load(11, wd_hbm.at[d_half:2 * d_half], wd_v.at[d_half:2 * d_half]),
        load(12, gamma_hbm, gamma_ref),
        load(13, pos_hbm, pos_ref),
        load(14, freq_hbm, freq_ref),
    ]
    for ld in loads[:5]:
        ld.start()

    barrier = pltpu.get_barrier_semaphore()
    for peer in peers:
        pl.semaphore_signal(barrier, inc=1, device_id=peer, device_id_type=MESH)
    for ld in loads[:3]:
        ld.wait()
    for ld in loads[5:]:
        ld.start()

    def remote(src, dst, send_sem, recv_sem, peer):
        return pltpu.make_async_remote_copy(src_ref=src, dst_ref=dst, send_sem=send_sem, recv_sem=recv_sem,
                                            device_id=peer, device_id_type=MESH)

    def core_copy(b):
        return remote(send.at[b], rcore.at[b], cs.at[b], cr.at[b], near)

    def x_copy(u):
        if u >= X_LAST:
            rows = pl.ds((u - X_LAST) * piece, piece)
            return remote(chip.at[pl.ds(N_BLK - 2, 2), rows], rx.at[pl.ds(N_BLK - 2, 2), rows], xs.at[u], xr.at[u], across)
        if u == X_KV:
            cols = pl.ds(pl.multiple_of(ty * head_dim, head_dim), head_dim)
            return remote(chip.at[B_QKV + 2, :, cols], rx.at[B_QKV + 2, :, cols], xs.at[u], xr.at[u], across)
        start, count = X_UNITS[u]
        return remote(chip.at[pl.ds(start, count)], rx.at[pl.ds(start, count)], xs.at[u], xr.at[u], across)

    def put(b, part):
        keep[b] = part[:half]
        send[b] = part[half:].astype(BF16)
        core_copy(b).start()

    def issue_bwd(b, w_ref, row):
        put(b, mm_bt(dy_v[...], w_ref[pl.ds(row, BLK), :]))

    def issue_fwd(b, w_ref, col):
        put(b, mm(nrm_v[...], w_ref[:, pl.ds(col, BLK)]))

    def combine(b):
        core_copy(b).wait_recv()
        chip[b] = (keep[b] + rcore[b].astype(F32)).astype(BF16)

    def total(b):
        return chip[b].astype(F32) + rx[b].astype(F32)

    part = mm_bt(dy_v[...], wo_v[0:BLK, :])
    keep[0] = part[:half]
    send[0] = part[half:].astype(BF16)
    pl.semaphore_wait(barrier, len(peers))
    core_copy(0).start()
    issue_bwd(1, wo_v, BLK)

    def rows_of(col_a, col_b):
        lane = lax.broadcasted_iota(jnp.int32, (half, 128), 1)
        return jnp.where(lane == 0, col_a, col_b).T[0:8]

    def stats_copies(snd, got, base, to):
        return [remote(snd, got.at[i], ss.at[base + i], sr.at[base + i], peer) for i, peer in enumerate(to)]

    def stats_put(snd, col_a, col_b):
        for lo, at in ((0, mine), (half, other)):
            snd[:, pl.ds(at, half)] = rows_of(col_a[lo:lo + half], col_b[lo:lo + half])

    def stats_columns(rows_ref):
        cols = []
        for i in range(2):
            parts = [jnp.broadcast_to(rows_ref[i:i + 1, pl.ds(at, half)], (128, half)).T[:, 0:1] for at in (mine, other)]
            cols.append(jnp.concatenate(parts, axis=0))
        return cols

    loads[3].wait()
    loads[4].wait()
    x_f = x_v[...].astype(F32)
    stats_put(st_snd, jnp.sum(x_f, axis=1, keepdims=True), jnp.sum(x_f * x_f, axis=1, keepdims=True))
    fwd_stats = stats_copies(st_snd, st_rx, 0, (near, across, far))
    for copy in fwd_stats:
        copy.start()

    combine(0)
    x_copy(0).start()
    combine(1)
    x_copy(1).start()

    loads[5].wait()
    for i in range(4):
        issue_bwd(B_DACT_LO + i, wd_v, i * BLK)
        if i >= 1:
            combine(B_DACT_LO + i - 1)
        if i == 2:
            x_copy(2).start()
    combine(B_DACT_LO + 3)
    x_copy(3).start()

    loads[12].wait()
    for copy in fwd_stats:
        copy.wait_recv()
    st_sum[...] = (st_snd[...] + st_rx[0]) + (st_rx[1] + st_rx[2])
    sum_x, sum_xx = stats_columns(st_sum)
    tok_mean = sum_x / d_model
    inv_std = lax.rsqrt(sum_xx / d_model - tok_mean * tok_mean + EPS)
    inv_v[...] = jnp.broadcast_to(inv_std, (n_tok, 128))
    x_hat = (x_v[...].astype(F32) - tok_mean) * inv_std
    xhat_v[...] = x_hat
    nrm_v[...] = (x_hat * gamma_ref[...]).astype(BF16)

    for i in range(6, 9):
        loads[i].wait()
    for i in range(3):
        issue_fwd(B_QKV + i, wqkv_v, i * BLK)
    for i in (2, 0, 1):
        combine(B_QKV + i)
        if i == 2:
            x_copy(X_KV).start()
    x_copy(4).start()

    loads[9].wait()
    loads[10].wait()
    for k in range(4):
        def gu_issue(j, carry, k=k):
            col = pl.multiple_of(k * CHUNK + j * BLK, BLK)
            issue_fwd(B_GU + 4 * k + j, wg_v, col)
            issue_fwd(B_GU + 4 * k + 2 + j, wu_v, col)
            return carry

        def gu_combine(j, carry, k=k):
            combine(B_GU + 4 * k + j)
            return carry

        lax.fori_loop(0, 2, gu_issue, 0)
        lax.fori_loop(0, 4, gu_combine, 0)
        x_copy(5 + k).start()

    loads[11].wait()

    def hi_issue(j, carry):
        issue_bwd(B_DACT_HI + j, wd_v, pl.multiple_of(d_half + j * BLK, BLK))
        return carry

    lax.fori_loop(0, 4, hi_issue, 0)
    for j in range(4):
        combine(B_DACT_HI + j)
        if j == 1:
            x_copy(9).start()
    for r in range(SPLITS):
        x_copy(X_LAST + r).start()

    nrm_t[...] = nrm_v[...].T

    loads[13].wait()
    loads[14].wait()
    freq = freq_ref[...]
    for lo, at in ((0, mine), (half, other)):
        pos_col = jnp.broadcast_to(pos_ref[0:1, pl.ds(at, half)].astype(F32), (128, half)).T
        angles = pos_col * freq
        cos_v[lo:lo + half] = jnp.cos(angles)
        sin_v[lo:lo + half] = jnp.sin(angles)

    packed_copy = remote(packed.at[0:half], packed.at[half:n_tok], ps.at[0], pr.at[0], near)
    x_copy(0).wait_recv()
    x_copy(1).wait_recv()
    for j in range(2):
        packed[0:half, q_width + 512 + j * BLK:q_width + 512 + (j + 1) * BLK] = total(B_DATTN + j).astype(BF16)
    x_copy(4).wait_recv()
    cos_h, sin_h = cos_v[0:half], sin_v[0:half]
    for j in range(2):
        blk = total(B_QKV + j)
        for h in range(2):
            lo = h * head_dim
            first, second = rope(blk[:, lo:lo + 128], blk[:, lo + 128:lo + 256], cos_h, sin_h)
            packed[0:half, j * BLK + lo:j * BLK + lo + 128] = first.astype(BF16)
            packed[0:half, j * BLK + lo + 128:j * BLK + lo + 256] = second.astype(BF16)
    x_copy(X_KV).wait_recv()
    kv_cols = pl.ds(pl.multiple_of(ty * head_dim, head_dim), head_dim)
    blk = chip[B_QKV + 2, :, kv_cols].astype(F32) + rx[B_QKV + 2, :, kv_cols].astype(F32)
    first, second = rope(blk[:, 0:128], blk[:, 128:256], cos_h, sin_h)
    kv_mine = jnp.where(ty == 0, jnp.concatenate([first, second], axis=1), blk).astype(BF16)
    kv_dst = packed.at[0:half, pl.ds(pl.multiple_of(q_width + ty * head_dim, head_dim), head_dim)]
    kv_dst[...] = kv_mine
    kv_copy = remote(kv_dst, kv_dst, ts.at[3], tr.at[3], other_ty)
    kv_copy.start()
    kv_copy.wait_recv()
    packed_copy.start()
    packed_copy.wait_recv()

    row_i = lax.rem(lax.broadcasted_iota(jnp.int32, (n_tok, n_tok), 0) + core * half, n_tok)
    col_i = lax.rem(lax.broadcasted_iota(jnp.int32, (n_tok, n_tok), 1) + core * half, n_tok)
    scale = head_dim ** -0.5
    kv_acc[...] = jnp.zeros_like(kv_acc)

    def head_step(h, carry):
        cols = pl.ds(pl.multiple_of(h * head_dim, head_dim), head_dim)
        q_h = packed[:, cols]
        da_h = packed[:, pl.ds(pl.multiple_of(q_width + 512 + h * head_dim, head_dim), head_dim)]
        k_rot = packed[:, q_width:q_width + 256]
        v_val = packed[:, q_width + 256:q_width + 512]
        scores = jnp.where(row_i >= col_i, mm_bt(q_h, k_rot) * scale, -1e30)
        exps = jnp.exp(scores - jnp.max(scores, axis=1, keepdims=True))
        probs_f = exps / jnp.sum(exps, axis=1, keepdims=True)
        probs = probs_f.astype(BF16)
        attn_v[:, cols] = mm(probs, v_val).astype(BF16)
        d_probs = mm_bt(da_h, v_val).astype(BF16).astype(F32)
        d_scores = (probs_f * (d_probs - jnp.sum(d_probs * probs_f, axis=1, keepdims=True)) * scale).astype(BF16)
        dq_h = mm(d_scores, k_rot).astype(BF16).astype(F32)
        first, second = rope(dq_h[:, 0:128], dq_h[:, 128:256], cos_v[...], -sin_v[...])
        dq_v[:, pl.ds(pl.multiple_of(h * head_dim, head_dim), 128)] = first.astype(BF16)
        dq_v[:, pl.ds(pl.multiple_of(h * head_dim + 128, 128), 128)] = second.astype(BF16)
        kv_acc[:, 0:256] += mm_at(d_scores, q_h)
        kv_acc[:, 256:512] += mm_at(probs, da_h)
        return carry

    lax.fori_loop(0, heads, head_step, 0)
    dkv_part[...] = kv_acc[...].astype(BF16)
    dkv_copy = remote(dkv_part, dkv_rx, ts.at[0], tr.at[0], other_ty)
    dkv_copy.start()
    br_v[...] = mm(attn_v[...], wo_v[...])
    dh_v[...] = mm_bt(dq_v[...], wqkv_v[:, 0:q_width])

    for j in range(2):
        tiles[j] = mm(nrm_t[...], dq_v[:, j * BLK:(j + 1) * BLK])
        tiles[2 + j] = mm_at(attn_v[:, j * BLK:(j + 1) * BLK], dy_v[...])

    def piece_copy(r):
        return remote(md.at[3, 1:3, r * piece:(r + 1) * piece], md.at[3, 1:3, half + r * piece:half + (r + 1) * piece],
                      gs.at[12 + r], gr.at[12 + r], near)

    def gather_copy(k, i):
        return remote(md.at[k, i, 0:half], md.at[k, i, half:n_tok], gs.at[3 * k + i], gr.at[3 * k + i], near)

    def dact_block(k, j):
        return B_DACT_LO + 2 * k + j if k < 2 else B_DACT_HI + 2 * (k - 2) + j

    def gated(k, want_act, want_grad):
        def step(r, carry):
            rows = pl.ds(pl.multiple_of(r * 16, 16), 16)
            for j in range(2):
                bg, bu, bd = B_GU + 4 * k + j, B_GU + 4 * k + 2 + j, dact_block(k, j)
                gate = (chip[bg, rows].astype(F32) + rx[bg, rows].astype(F32)).astype(BF16).astype(F32)
                up = (chip[bu, rows].astype(F32) + rx[bu, rows].astype(F32)).astype(BF16).astype(F32)
                sig = jax.nn.sigmoid(gate)
                silu = gate * sig
                cols = slice(j * BLK, (j + 1) * BLK)
                if want_act:
                    md[k, 0, rows, cols] = (silu * up).astype(BF16)
                if k == 3:
                    factors[0, rows, cols] = up * sig * (1.0 + gate * (1.0 - sig))
                    factors[1, rows, cols] = silu
                if want_grad:
                    d_act = (chip[bd, rows].astype(F32) + rx[bd, rows].astype(F32)).astype(BF16).astype(F32)
                    md[k, 1, rows, cols] = (d_act * up * sig * (1.0 + gate * (1.0 - sig))).astype(BF16)
                    md[k, 2, rows, cols] = (d_act * silu).astype(BF16)
            return carry

        lax.fori_loop(0, half // 16, step, 0)
        for i in ((0,) if want_act else ()) + ((1, 2) if want_grad else ()):
            gather_copy(k, i).start()

    def use_act(k):
        gather_copy(k, 0).wait_recv()
        br_v[...] += mm(md[k, 0], wd_v[k * CHUNK:(k + 1) * CHUNK, :])

    def use_grad(k):
        for i in (1, 2):
            gather_copy(k, i).wait_recv()
        dh_v[...] += (mm_bt(md[k, 1], wg_v[:, k * CHUNK:(k + 1) * CHUNK])
                      + mm_bt(md[k, 2], wu_v[:, k * CHUNK:(k + 1) * CHUNK]))

    x_copy(2).wait_recv()
    x_copy(3).wait_recv()
    for k in range(2):
        x_copy(5 + k).wait_recv()
        gated(k, True, True)
        use_act(k)
        use_grad(k)
        if k == 0:
            dkv_copy.wait_recv()
            d_k = dkv_part[:, 0:256].astype(F32) + dkv_rx[:, 0:256].astype(F32)
            d_k = d_k.astype(BF16).astype(F32)
            first, second = rope(d_k[:, 0:128], d_k[:, 128:256], cos_v[...], -sin_v[...])
            dkv_v[:, 0:128] = first.astype(BF16)
            dkv_v[:, 128:256] = second.astype(BF16)
            dkv_v[:, 256:512] = (dkv_part[:, 256:512].astype(F32) + dkv_rx[:, 256:512].astype(F32)).astype(BF16)
            dh_v[...] += 0.5 * mm_bt(dkv_v[...], wqkv_v[:, q_width:q_width + 512])
            tiles[4] = mm(nrm_t[...], dkv_v[...])
            for j in range(2):
                tiles[5 + j] = mm_at(md[0, 0, :, j * BLK:(j + 1) * BLK], dy_v[...])
    for k in (2, 3):
        x_copy(5 + k).wait_recv()
        gated(k, True, False)
        use_act(k)
    y_snd[...] = br_v[...].astype(BF16)
    y_copy = remote(y_snd, y_rx, ts.at[1], tr.at[1], other_ty)
    y_copy.start()
    x_copy(9).wait_recv()
    gated(2, False, True)

    def dh_copy(r):
        return remote(dh_snd.at[r], dh_rx.at[r], ds.at[r], dr.at[r], other_ty)

    def both(ref, r):
        return jnp.concatenate([ref[r * piece:(r + 1) * piece], ref[half + r * piece:half + (r + 1) * piece]], axis=0)

    sums = []

    def piece_grad(r):
        x_copy(X_LAST + r).wait_recv()
        rows = slice(r * piece, (r + 1) * piece)
        for j in range(2):
            cols = slice(j * BLK, (j + 1) * BLK)
            b = dact_block(3, j)
            d_act = (chip[b, rows].astype(F32) + rx[b, rows].astype(F32)).astype(BF16).astype(F32)
            for i in range(2):
                md[3, 1 + i, rows, cols] = (d_act * factors[i, rows, cols]).astype(BF16)
        piece_copy(r).start()

    def piece_dh(r):
        piece_copy(r).wait_recv()
        part = both(dh_v, r) + mm_bt(both(md.at[3, 1], r), wg_v[:, 3 * CHUNK:4 * CHUNK]) + mm_bt(both(md.at[3, 2], r), wu_v[:, 3 * CHUNK:4 * CHUNK])
        part_b = part.astype(BF16)
        dh_snd[r] = part_b
        dh_copy(r).start()
        d_hat = part_b.astype(F32) * gamma_ref[...]
        sums.append((jnp.sum(d_hat, axis=1, keepdims=True), jnp.sum(d_hat * both(xhat_v, r), axis=1, keepdims=True)))

    piece_grad(0)
    use_grad(2)
    for r in range(1, SPLITS):
        piece_grad(r)
        piece_dh(r - 1)
    piece_dh(SPLITS - 1)
    cols = [jnp.concatenate([sums[r][i][:piece] for r in range(SPLITS)] + [sums[r][i][piece:] for r in range(SPLITS)], axis=0) for i in range(2)]
    stats_put(bst_snd, cols[0], cols[1])
    bwd_stats = stats_copies(bst_snd, bst_rx, 3, peers)
    for copy in bwd_stats:
        copy.start()

    y_copy.wait_recv()
    y_o[...] = (x_v[...].astype(F32) + (y_snd[...].astype(F32) + y_rx[...].astype(F32))).astype(BF16)

    d_gamma = jnp.zeros_like(dgamma_ref)
    for r in range(SPLITS):
        dh_copy(r).wait_recv()
        d_nrm = dh_snd[r].astype(F32) + dh_rx[r].astype(F32)
        d_gamma = d_gamma + jnp.sum(d_nrm * both(xhat_v, r), axis=0, keepdims=True)
        dh_v[r * piece:(r + 1) * piece] = d_nrm[:piece]
        dh_v[half + r * piece:half + (r + 1) * piece] = d_nrm[piece:]
    dgamma_ref[...] = d_gamma
    for copy in bwd_stats:
        copy.wait_recv()
    st_sum[...] = ((bst_snd[...] + bst_rx[0]) + (bst_rx[1] + bst_rx[2])) + ((bst_rx[3] + bst_rx[4]) + (bst_rx[5] + bst_rx[6]))
    sum_d, sum_dx = stats_columns(st_sum)
    d_hat = dh_v[...] * gamma_ref[...]
    d_x = dy_v[...].astype(F32) + inv_v[:, 0:1] * (d_hat - sum_d / d_model - xhat_v[...] * (sum_dx / d_model))
    dx_o[...] = d_x.astype(BF16)

    def drain(b, carry):
        core_copy(b).wait_send()
        return carry

    lax.fori_loop(0, N_BLK, drain, 0)
    for u in range(N_X):
        x_copy(u).wait_send()
    for k in range(4):
        for i in range(3 if k < 3 else 1):
            gather_copy(k, i).wait_send()
    for r in range(SPLITS):
        piece_copy(r).wait_send()
        dh_copy(r).wait_send()
    for copy in [packed_copy, dkv_copy, y_copy, kv_copy] + fwd_stats + bwd_stats:
        copy.wait_send()


def grad_kernel(y_v, dx_v, dgamma_in, nrm_t, attn_v, md, dq_v, dkv_v, dy_v, tiles,
                y_hbm, dx_hbm, dgamma_ref, dwq_hbm, dwg_hbm, dwu_hbm, dwk_hbm, dwv_hbm, dwo_hbm, dwd_hbm,
                ring, out_sem, cp_sem):
    width, n_tok = nrm_t.shape
    half = n_tok // 2
    n_ring = ring.shape[0]
    core = lax.rem(lax.axis_index('tx'), 2)
    mine = pl.multiple_of(core * half, half)
    other = pl.multiple_of((1 - core) * half, half)
    hand_out = [pltpu.make_async_copy(src.at[lo:lo + half], dst.at[pl.ds(at, half)], cp_sem.at[i])
                for i, (src, dst, lo, at) in enumerate(((y_v, y_hbm, 0, mine), (y_v, y_hbm, half, other), (dx_v, dx_hbm, 0, mine), (dx_v, dx_hbm, half, other)))]
    for cp in hand_out:
        cp.start()
    dgamma_ref[...] = dgamma_in[...]

    ready = [(0, dwq_hbm.at[:, 0:BLK]), (1, dwq_hbm.at[:, BLK:2 * BLK]), (2, dwo_hbm.at[0:BLK, :]), (3, dwo_hbm.at[BLK:2 * BLK, :]),
             (5, dwd_hbm.at[0:BLK, :]), (6, dwd_hbm.at[BLK:2 * BLK, :])]
    ready = [(tiles.at[i], dst) for i, dst in ready] + [(tiles.at[4, :, 0:256], dwk_hbm), (tiles.at[4, :, 256:512], dwv_hbm)]
    for i, (src, dst) in enumerate(ready):
        hand_out.append(pltpu.make_async_copy(src, dst, cp_sem.at[4 + i]))
        hand_out[-1].start()

    flight = []

    def emit(value, dsts):
        t = len(flight)
        slot = t % n_ring
        if t >= n_ring:
            for cp in flight[t - n_ring]:
                cp.wait()
        ring[slot] = value
        copies = [pltpu.make_async_copy(ring.at[slot, :, lo:hi], dst, out_sem.at[slot, i]) for i, (lo, hi, dst) in enumerate(dsts)]
        for cp in copies:
            cp.start()
        flight.append(copies)

    def columns(grads, col, out, to):
        emit(mm(nrm_t[...], grads[:, col:col + BLK]), [(0, BLK, out.at[:, to:to + BLK])])

    def rows(acts, col, out, to):
        emit(mm_at(acts[:, col:col + width], dy_v[...]), [(0, BLK, out.at[to:to + width, :])])

    for k in range(4):
        for j in range(2):
            columns(md.at[k, 1], j * BLK, dwg_hbm, k * CHUNK + j * BLK)
        for j in range(2):
            columns(md.at[k, 2], j * BLK, dwu_hbm, k * CHUNK + j * BLK)
        for j in range(2 if k > 0 else 0):
            rows(md.at[k, 0], j * BLK, dwd_hbm, k * CHUNK + j * BLK)
    for copies in flight[-n_ring:]:
        for cp in copies:
            cp.wait()
    for cp in hand_out:
        cp.wait()


def solution(mesh):
    tx_size = mesh.shape['tx']
    tok_spec = P('dp', None, 'tx')
    in_specs = (tok_spec, P('dp', None), tok_spec, P('tx'), P('tx', 'ty'), P('tx', 'ty'), P('tx', 'ty'),
                P('tx', None), P('tx', None), P('ty', 'tx'), P('ty', 'tx'))
    out_specs = (tok_spec, tok_spec, P(('dp', 'tx')), P(('dp', 'tx'), 'ty'), P(('dp', 'tx'), 'ty'), P(('dp', 'tx'), 'ty'),
                 P(('dp', 'tx'), None), P(('dp', 'tx'), None), P(('dp', 'ty'), 'tx'), P(('dp', 'ty'), 'tx'))

    def local_layer(x_in, positions, d_y, ln_gamma, w_q, w_g, w_u, w_k, w_v, w_o, w_d):
        _, n_tok, d_local = x_in.shape
        half = n_tok // 2
        d_model = d_local * tx_size
        head_dim = w_k.shape[1]
        q_width = w_q.shape[1]
        d_ff = w_g.shape[1]
        freq = jnp.asarray((ROPE_BASE ** (-2.0 * np.arange(head_dim // 2) / head_dim)).astype(np.float32)[None])
        any_spec = pl.BlockSpec(memory_space=pl.ANY)
        vmem_spec = pl.BlockSpec(memory_space=pltpu.VMEM)
        tok = (n_tok, d_local)
        sem = pltpu.SemaphoreType.DMA
        vm = pltpu.VMEM
        kept = pl.pallas_call(
            functools.partial(layer_kernel, d_model),
            out_shape=[vm(tok, BF16), vm(tok, BF16), vm((1, d_local), F32), vm((d_local, n_tok), BF16), vm((n_tok, q_width), BF16),
                       vm((4, 3, n_tok, CHUNK), BF16), vm((n_tok, q_width), BF16), vm((n_tok, 2 * head_dim), BF16), vm(tok, BF16),
                       vm((7, BLK, BLK), F32)],
            in_specs=[any_spec] * 12,
            out_specs=[vmem_spec] * 10,
            scratch_shapes=[
                vm((1, n_tok), jnp.int32), vm((1, head_dim // 2), F32), vm((1, d_local), F32), vm(tok, BF16),
                vm(tok, BF16), vm((d_local, q_width + 2 * head_dim), BF16), vm((d_local, d_ff), BF16), vm((d_local, d_ff), BF16),
                vm((q_width, d_local), BF16), vm((d_ff, d_local), BF16),
                vm((N_BLK, half, BLK), F32), vm((N_BLK, half, BLK), BF16), vm((N_BLK, half, BLK), BF16),
                vm((N_BLK, half, BLK), BF16), vm((N_BLK, half, BLK), BF16), vm((n_tok, 2 * q_width + 2 * head_dim), BF16),
                vm((n_tok, 512), BF16), vm((n_tok, 512), BF16), vm((n_tok, 512), F32),
                vm(tok, F32), vm((n_tok, 128), F32), vm((n_tok, 128), F32), vm((n_tok, 128), F32), vm(tok, F32), vm(tok, F32),
                vm(tok, BF16), vm(tok, BF16), vm((SPLITS, n_tok // SPLITS, d_local), BF16), vm((SPLITS, n_tok // SPLITS, d_local), BF16),
                vm((8, n_tok), F32), vm((3, 8, n_tok), F32), vm((8, n_tok), F32), vm((8, n_tok), F32), vm((7, 8, n_tok), F32), vm((2, half, CHUNK), F32),
                sem((15,)), sem((N_BLK,)), sem((N_BLK,)), sem((N_X,)), sem((N_X,)),
                sem((12 + SPLITS,)), sem((12 + SPLITS,)), sem((1,)), sem((1,)), sem((4,)), sem((4,)), sem((10,)), sem((10,)),
                sem((SPLITS,)), sem((SPLITS,))],
            compiler_params=pltpu.CompilerParams(collective_id=0, has_side_effects=True, vmem_limit_bytes=46 * 1024 * 1024),
            name='layer',
        )(x_in.reshape(tok), positions, freq, d_y.reshape(tok), ln_gamma[None], w_q, w_g, w_u, w_k, w_v, w_o, w_d)

        y_out, d_x, d_gamma, d_wq, d_wg, d_wu, d_wk, d_wv, d_wo, d_wd = pl.pallas_call(
            grad_kernel,
            out_shape=[jax.ShapeDtypeStruct(tok, BF16), jax.ShapeDtypeStruct(tok, BF16), jax.ShapeDtypeStruct((1, d_local), F32)]
            + [jax.ShapeDtypeStruct(w.shape, F32) for w in (w_q, w_g, w_u, w_k, w_v, w_o, w_d)],
            in_specs=[vmem_spec] * 10,
            out_specs=[any_spec, any_spec, vmem_spec] + [any_spec] * 7,
            scratch_shapes=[vm((10, d_local, BLK), F32), sem((10, 2)), sem((12,))],
            compiler_params=pltpu.CompilerParams(vmem_limit_bytes=30 * 1024 * 1024),
            name='weight_grads',
        )(*kept)
        return (y_out.reshape(x_in.shape), d_x.reshape(x_in.shape), d_gamma.reshape(d_local),
                d_wq, d_wg, d_wu, d_wk, d_wv, d_wo, d_wd)

    return jax.shard_map(local_layer, mesh=mesh, in_specs=in_specs, out_specs=out_specs, check_vma=False)
```

```python
import functools

import jax
import jax.numpy as jnp
import numpy as np
from jax import lax
from jax.experimental import pallas as pl
from jax.experimental.pallas import tpu as pltpu
from jax.sharding import PartitionSpec as P

EPS = 1e-6
ROPE_BASE = 10000.0
F32 = jnp.float32
BF16 = jnp.bfloat16
MESH = pl.DeviceIdType.MESH

BLK = 512
CHUNK = 1024
B_DATTN, B_DACT_LO, B_QKV, B_GU, B_DACT_HI, N_BLK = 0, 2, 6, 9, 25, 29
X_UNITS = ((0, 1), (1, 1), (2, 2), (4, 2), (6, 2), (9, 4), (13, 4), (17, 4), (21, 4), (25, 2))
SPLITS = 4
X_KV = len(X_UNITS)
X_LAST = X_KV + 1
N_X = X_LAST + SPLITS


def dot(a, b, dims):
    return lax.dot_general(a, b, (dims, ((), ())), preferred_element_type=F32)


def mm(a, b):
    return dot(a, b, ((1,), (0,)))


def mm_bt(a, b):
    return dot(a, b, ((1,), (1,)))


def mm_at(a, b):
    return dot(a, b, ((0,), (0,)))


def rope(first, second, cos_t, sin_t):
    return first * cos_t - second * sin_t, second * cos_t + first * sin_t


def layer_kernel(d_model, x_hbm, pos_hbm, freq_hbm, dy_hbm, gamma_hbm, wq_hbm, wg_hbm, wu_hbm, wk_hbm, wv_hbm, wo_hbm, wd_hbm,
                 y_o, dx_o, dgamma_ref, nrm_t, attn_v, md, dq_v, dkv_v, dy_v, tiles,
                 pos_ref, freq_ref, gamma_ref, nrm_v, x_v, wqkv_v, wg_v, wu_v, wo_v, wd_v,
                 keep, send, rcore, chip, rx, packed, dkv_part, dkv_rx, kv_acc,
                 xhat_v, inv_v, cos_v, sin_v, br_v, dh_v, y_snd, y_rx, dh_snd, dh_rx,
                 st_snd, st_rx, st_sum, bst_snd, bst_rx, factors,
                 ld_sem, cs, cr, xs, xr, gs, gr, ps, pr, ts, tr, ss, sr, ds, dr):
    tx = lax.axis_index('tx')
    ty = lax.axis_index('ty')
    core = lax.rem(tx, 2)
    near = {'tx': tx + 1 - 2 * core}
    across = {'tx': lax.rem(tx + 2, 4)}
    far = {'tx': lax.rem(tx + 1 - 2 * core + 2, 4)}
    other_ty = {'ty': 1 - ty}
    peers = [near, across, far, other_ty] + [{'tx': p['tx'], 'ty': 1 - ty} for p in (near, across, far)]
    n_tok = x_v.shape[0]
    half = n_tok // 2
    mine = pl.multiple_of(core * half, half)
    other = pl.multiple_of((1 - core) * half, half)
    head_dim = 256
    q_width = wo_v.shape[0]
    heads = q_width // head_dim
    piece = half // SPLITS

    def load(i, src, dst):
        return pltpu.make_async_copy(src, dst, ld_sem.at[i])

    d_half = wd_v.shape[0] // 2
    loads = [
        load(0, dy_hbm.at[pl.ds(mine, half)], dy_v.at[0:half]),
        load(1, dy_hbm.at[pl.ds(other, half)], dy_v.at[half:n_tok]),
        load(2, wo_hbm, wo_v),
        load(3, x_hbm.at[pl.ds(mine, half)], x_v.at[0:half]),
        load(4, x_hbm.at[pl.ds(other, half)], x_v.at[half:n_tok]),
        load(5, wd_hbm.at[0:d_half], wd_v.at[0:d_half]),
        load(6, wq_hbm, wqkv_v.at[:, 0:q_width]),
        load(7, wk_hbm, wqkv_v.at[:, q_width:q_width + head_dim]),
        load(8, wv_hbm, wqkv_v.at[:, q_width + head_dim:q_width + 2 * head_dim]),
        load(9, wg_hbm, wg_v),
        load(10, wu_hbm, wu_v),
        load(11, wd_hbm.at[d_half:2 * d_half], wd_v.at[d_half:2 * d_half]),
        load(12, gamma_hbm, gamma_ref),
        load(13, pos_hbm, pos_ref),
        load(14, freq_hbm, freq_ref),
    ]
    for ld in loads[:5]:
        ld.start()

    barrier = pltpu.get_barrier_semaphore()
    for peer in peers:
        pl.semaphore_signal(barrier, inc=1, device_id=peer, device_id_type=MESH)
    for ld in loads[:3]:
        ld.wait()
    for ld in loads[5:]:
        ld.start()

    def remote(src, dst, send_sem, recv_sem, peer):
        return pltpu.make_async_remote_copy(src_ref=src, dst_ref=dst, send_sem=send_sem, recv_sem=recv_sem,
                                            device_id=peer, device_id_type=MESH)

    def core_copy(b):
        return remote(send.at[b], rcore.at[b], cs.at[b], cr.at[b], near)

    def x_copy(u):
        if u >= X_LAST:
            rows = pl.ds((u - X_LAST) * piece, piece)
            return remote(chip.at[pl.ds(N_BLK - 2, 2), rows], rx.at[pl.ds(N_BLK - 2, 2), rows], xs.at[u], xr.at[u], across)
        if u == X_KV:
            cols = pl.ds(pl.multiple_of(ty * head_dim, head_dim), head_dim)
            return remote(chip.at[B_QKV + 2, :, cols], rx.at[B_QKV + 2, :, cols], xs.at[u], xr.at[u], across)
        start, count = X_UNITS[u]
        return remote(chip.at[pl.ds(start, count)], rx.at[pl.ds(start, count)], xs.at[u], xr.at[u], across)

    def put(b, part):
        keep[b] = part[:half]
        send[b] = part[half:].astype(BF16)
        core_copy(b).start()

    def issue_bwd(b, w_ref, row):
        put(b, mm_bt(dy_v[...], w_ref[pl.ds(row, BLK), :]))

    def issue_fwd(b, w_ref, col):
        put(b, mm(nrm_v[...], w_ref[:, pl.ds(col, BLK)]))

    def combine(b):
        core_copy(b).wait_recv()
        chip[b] = (keep[b] + rcore[b].astype(F32)).astype(BF16)

    def total(b):
        return chip[b].astype(F32) + rx[b].astype(F32)

    part = mm_bt(dy_v[...], wo_v[0:BLK, :])
    keep[0] = part[:half]
    send[0] = part[half:].astype(BF16)
    pl.semaphore_wait(barrier, len(peers))
    core_copy(0).start()
    issue_bwd(1, wo_v, BLK)

    def rows_of(col_a, col_b):
        lane = lax.broadcasted_iota(jnp.int32, (half, 128), 1)
        return jnp.where(lane == 0, col_a, col_b).T[0:8]

    def stats_copies(snd, got, base, to):
        return [remote(snd, got.at[i], ss.at[base + i], sr.at[base + i], peer) for i, peer in enumerate(to)]

    def stats_put(snd, col_a, col_b):
        for lo, at in ((0, mine), (half, other)):
            snd[:, pl.ds(at, half)] = rows_of(col_a[lo:lo + half], col_b[lo:lo + half])

    def stats_columns(rows_ref):
        cols = []
        for i in range(2):
            parts = [jnp.broadcast_to(rows_ref[i:i + 1, pl.ds(at, half)], (128, half)).T[:, 0:1] for at in (mine, other)]
            cols.append(jnp.concatenate(parts, axis=0))
        return cols

    loads[3].wait()
    loads[4].wait()
    x_f = x_v[...].astype(F32)
    stats_put(st_snd, jnp.sum(x_f, axis=1, keepdims=True), jnp.sum(x_f * x_f, axis=1, keepdims=True))
    fwd_stats = stats_copies(st_snd, st_rx, 0, (near, across, far))
    for copy in fwd_stats:
        copy.start()

    combine(0)
    x_copy(0).start()
    combine(1)
    x_copy(1).start()

    loads[5].wait()
    for i in range(4):
        issue_bwd(B_DACT_LO + i, wd_v, i * BLK)
        if i >= 1:
            combine(B_DACT_LO + i - 1)
        if i == 2:
            x_copy(2).start()
    combine(B_DACT_LO + 3)
    x_copy(3).start()

    loads[12].wait()
    for copy in fwd_stats:
        copy.wait_recv()
    st_sum[...] = (st_snd[...] + st_rx[0]) + (st_rx[1] + st_rx[2])
    sum_x, sum_xx = stats_columns(st_sum)
    tok_mean = sum_x / d_model
    inv_std = lax.rsqrt(sum_xx / d_model - tok_mean * tok_mean + EPS)
    inv_v[...] = jnp.broadcast_to(inv_std, (n_tok, 128))
    x_hat = (x_v[...].astype(F32) - tok_mean) * inv_std
    xhat_v[...] = x_hat
    nrm_v[...] = (x_hat * gamma_ref[...]).astype(BF16)

    for i in range(6, 9):
        loads[i].wait()
    for i in range(3):
        issue_fwd(B_QKV + i, wqkv_v, i * BLK)
    for i in (2, 0, 1):
        combine(B_QKV + i)
        if i == 2:
            x_copy(X_KV).start()
    x_copy(4).start()

    loads[9].wait()
    loads[10].wait()
    for k in range(4):
        def gu_issue(j, carry, k=k):
            col = pl.multiple_of(k * CHUNK + j * BLK, BLK)
            issue_fwd(B_GU + 4 * k + j, wg_v, col)
            issue_fwd(B_GU + 4 * k + 2 + j, wu_v, col)
            return carry

        def gu_combine(j, carry, k=k):
            combine(B_GU + 4 * k + j)
            return carry

        lax.fori_loop(0, 2, gu_issue, 0)
        lax.fori_loop(0, 4, gu_combine, 0)
        x_copy(5 + k).start()

    loads[11].wait()

    def hi_issue(j, carry):
        issue_bwd(B_DACT_HI + j, wd_v, pl.multiple_of(d_half + j * BLK, BLK))
        return carry

    lax.fori_loop(0, 4, hi_issue, 0)
    for j in range(4):
        combine(B_DACT_HI + j)
        if j == 1:
            x_copy(9).start()
    for r in range(SPLITS):
        x_copy(X_LAST + r).start()

    nrm_t[...] = nrm_v[...].T

    loads[13].wait()
    loads[14].wait()
    freq = freq_ref[...]
    for lo, at in ((0, mine), (half, other)):
        pos_col = jnp.broadcast_to(pos_ref[0:1, pl.ds(at, half)].astype(F32), (128, half)).T
        angles = pos_col * freq
        cos_v[lo:lo + half] = jnp.cos(angles)
        sin_v[lo:lo + half] = jnp.sin(angles)

    packed_copy = remote(packed.at[0:half], packed.at[half:n_tok], ps.at[0], pr.at[0], near)
    x_copy(0).wait_recv()
    x_copy(1).wait_recv()
    for j in range(2):
        packed[0:half, q_width + 512 + j * BLK:q_width + 512 + (j + 1) * BLK] = total(B_DATTN + j).astype(BF16)
    x_copy(4).wait_recv()
    cos_h, sin_h = cos_v[0:half], sin_v[0:half]
    for j in range(2):
        blk = total(B_QKV + j)
        for h in range(2):
            lo = h * head_dim
            first, second = rope(blk[:, lo:lo + 128], blk[:, lo + 128:lo + 256], cos_h, sin_h)
            packed[0:half, j * BLK + lo:j * BLK + lo + 128] = first.astype(BF16)
            packed[0:half, j * BLK + lo + 128:j * BLK + lo + 256] = second.astype(BF16)
    x_copy(X_KV).wait_recv()
    kv_cols = pl.ds(pl.multiple_of(ty * head_dim, head_dim), head_dim)
    blk = chip[B_QKV + 2, :, kv_cols].astype(F32) + rx[B_QKV + 2, :, kv_cols].astype(F32)
    first, second = rope(blk[:, 0:128], blk[:, 128:256], cos_h, sin_h)
    kv_mine = jnp.where(ty == 0, jnp.concatenate([first, second], axis=1), blk).astype(BF16)
    kv_dst = packed.at[0:half, pl.ds(pl.multiple_of(q_width + ty * head_dim, head_dim), head_dim)]
    kv_dst[...] = kv_mine
    kv_copy = remote(kv_dst, kv_dst, ts.at[3], tr.at[3], other_ty)
    kv_copy.start()
    kv_copy.wait_recv()
    packed_copy.start()
    packed_copy.wait_recv()

    row_i = lax.rem(lax.broadcasted_iota(jnp.int32, (n_tok, n_tok), 0) + core * half, n_tok)
    col_i = lax.rem(lax.broadcasted_iota(jnp.int32, (n_tok, n_tok), 1) + core * half, n_tok)
    scale = head_dim ** -0.5
    kv_acc[...] = jnp.zeros_like(kv_acc)

    def head_step(h, carry):
        cols = pl.ds(pl.multiple_of(h * head_dim, head_dim), head_dim)
        q_h = packed[:, cols]
        da_h = packed[:, pl.ds(pl.multiple_of(q_width + 512 + h * head_dim, head_dim), head_dim)]
        k_rot = packed[:, q_width:q_width + 256]
        v_val = packed[:, q_width + 256:q_width + 512]
        scores = jnp.where(row_i >= col_i, mm_bt(q_h, k_rot) * scale, -1e30)
        exps = jnp.exp(scores - jnp.max(scores, axis=1, keepdims=True))
        probs_f = exps / jnp.sum(exps, axis=1, keepdims=True)
        probs = probs_f.astype(BF16)
        attn_v[:, cols] = mm(probs, v_val).astype(BF16)
        d_probs = mm_bt(da_h, v_val).astype(BF16).astype(F32)
        d_scores = (probs_f * (d_probs - jnp.sum(d_probs * probs_f, axis=1, keepdims=True)) * scale).astype(BF16)
        dq_h = mm(d_scores, k_rot).astype(BF16).astype(F32)
        first, second = rope(dq_h[:, 0:128], dq_h[:, 128:256], cos_v[...], -sin_v[...])
        dq_v[:, pl.ds(pl.multiple_of(h * head_dim, head_dim), 128)] = first.astype(BF16)
        dq_v[:, pl.ds(pl.multiple_of(h * head_dim + 128, 128), 128)] = second.astype(BF16)
        kv_acc[:, 0:256] += mm_at(d_scores, q_h)
        kv_acc[:, 256:512] += mm_at(probs, da_h)
        return carry

    lax.fori_loop(0, heads, head_step, 0)
    dkv_part[...] = kv_acc[...].astype(BF16)
    dkv_copy = remote(dkv_part, dkv_rx, ts.at[0], tr.at[0], other_ty)
    dkv_copy.start()
    br_v[...] = mm(attn_v[...], wo_v[...])
    dh_v[...] = mm_bt(dq_v[...], wqkv_v[:, 0:q_width])

    for j in range(2):
        tiles[j] = mm(nrm_t[...], dq_v[:, j * BLK:(j + 1) * BLK])
        tiles[2 + j] = mm_at(attn_v[:, j * BLK:(j + 1) * BLK], dy_v[...])

    def piece_copy(r):
        return remote(md.at[3, 1:3, r * piece:(r + 1) * piece], md.at[3, 1:3, half + r * piece:half + (r + 1) * piece],
                      gs.at[12 + r], gr.at[12 + r], near)

    def gather_copy(k, i):
        return remote(md.at[k, i, 0:half], md.at[k, i, half:n_tok], gs.at[3 * k + i], gr.at[3 * k + i], near)

    def dact_block(k, j):
        return B_DACT_LO + 2 * k + j if k < 2 else B_DACT_HI + 2 * (k - 2) + j

    def gated(k, want_act, want_grad):
        def step(r, carry):
            rows = pl.ds(pl.multiple_of(r * 16, 16), 16)
            for j in range(2):
                bg, bu, bd = B_GU + 4 * k + j, B_GU + 4 * k + 2 + j, dact_block(k, j)
                gate = (chip[bg, rows].astype(F32) + rx[bg, rows].astype(F32)).astype(BF16).astype(F32)
                up = (chip[bu, rows].astype(F32) + rx[bu, rows].astype(F32)).astype(BF16).astype(F32)
                sig = jax.nn.sigmoid(gate)
                silu = gate * sig
                cols = slice(j * BLK, (j + 1) * BLK)
                if want_act:
                    md[k, 0, rows, cols] = (silu * up).astype(BF16)
                if k == 3:
                    factors[0, rows, cols] = up * sig * (1.0 + gate * (1.0 - sig))
                    factors[1, rows, cols] = silu
                if want_grad:
                    d_act = (chip[bd, rows].astype(F32) + rx[bd, rows].astype(F32)).astype(BF16).astype(F32)
                    md[k, 1, rows, cols] = (d_act * up * sig * (1.0 + gate * (1.0 - sig))).astype(BF16)
                    md[k, 2, rows, cols] = (d_act * silu).astype(BF16)
            return carry

        lax.fori_loop(0, half // 16, step, 0)
        for i in ((0,) if want_act else ()) + ((1, 2) if want_grad else ()):
            gather_copy(k, i).start()

    def use_act(k):
        gather_copy(k, 0).wait_recv()
        br_v[...] += mm(md[k, 0], wd_v[k * CHUNK:(k + 1) * CHUNK, :])

    def use_grad(k):
        for i in (1, 2):
            gather_copy(k, i).wait_recv()
        dh_v[...] += (mm_bt(md[k, 1], wg_v[:, k * CHUNK:(k + 1) * CHUNK])
                      + mm_bt(md[k, 2], wu_v[:, k * CHUNK:(k + 1) * CHUNK]))

    x_copy(2).wait_recv()
    x_copy(3).wait_recv()
    for k in range(2):
        x_copy(5 + k).wait_recv()
        gated(k, True, True)
        use_act(k)
        use_grad(k)
        if k == 0:
            dkv_copy.wait_recv()
            d_k = dkv_part[:, 0:256].astype(F32) + dkv_rx[:, 0:256].astype(F32)
            d_k = d_k.astype(BF16).astype(F32)
            first, second = rope(d_k[:, 0:128], d_k[:, 128:256], cos_v[...], -sin_v[...])
            dkv_v[:, 0:128] = first.astype(BF16)
            dkv_v[:, 128:256] = second.astype(BF16)
            dkv_v[:, 256:512] = (dkv_part[:, 256:512].astype(F32) + dkv_rx[:, 256:512].astype(F32)).astype(BF16)
            dh_v[...] += 0.5 * mm_bt(dkv_v[...], wqkv_v[:, q_width:q_width + 512])
            tiles[4] = mm(nrm_t[...], dkv_v[...])
            for j in range(2):
                tiles[5 + j] = mm_at(md[0, 0, :, j * BLK:(j + 1) * BLK], dy_v[...])
    for k in (2, 3):
        x_copy(5 + k).wait_recv()
        gated(k, True, False)
        use_act(k)
    y_snd[...] = br_v[...].astype(BF16)
    y_copy = remote(y_snd, y_rx, ts.at[1], tr.at[1], other_ty)
    y_copy.start()
    x_copy(9).wait_recv()
    gated(2, False, True)

    def dh_copy(r):
        return remote(dh_snd.at[r], dh_rx.at[r], ds.at[r], dr.at[r], other_ty)

    def both(ref, r):
        return jnp.concatenate([ref[r * piece:(r + 1) * piece], ref[half + r * piece:half + (r + 1) * piece]], axis=0)

    sums = []

    def piece_grad(r):
        x_copy(X_LAST + r).wait_recv()
        rows = slice(r * piece, (r + 1) * piece)
        for j in range(2):
            cols = slice(j * BLK, (j + 1) * BLK)
            b = dact_block(3, j)
            d_act = (chip[b, rows].astype(F32) + rx[b, rows].astype(F32)).astype(BF16).astype(F32)
            for i in range(2):
                md[3, 1 + i, rows, cols] = (d_act * factors[i, rows, cols]).astype(BF16)
        piece_copy(r).start()

    def piece_dh(r):
        piece_copy(r).wait_recv()
        part = both(dh_v, r) + mm_bt(both(md.at[3, 1], r), wg_v[:, 3 * CHUNK:4 * CHUNK]) + mm_bt(both(md.at[3, 2], r), wu_v[:, 3 * CHUNK:4 * CHUNK])
        part_b = part.astype(BF16)
        dh_snd[r] = part_b
        dh_copy(r).start()
        d_hat = part_b.astype(F32) * gamma_ref[...]
        sums.append((jnp.sum(d_hat, axis=1, keepdims=True), jnp.sum(d_hat * both(xhat_v, r), axis=1, keepdims=True)))

    piece_grad(0)
    use_grad(2)
    for r in range(1, SPLITS):
        piece_grad(r)
        piece_dh(r - 1)
    piece_dh(SPLITS - 1)
    cols = [jnp.concatenate([sums[r][i][:piece] for r in range(SPLITS)] + [sums[r][i][piece:] for r in range(SPLITS)], axis=0) for i in range(2)]
    stats_put(bst_snd, cols[0], cols[1])
    bwd_stats = stats_copies(bst_snd, bst_rx, 3, peers)
    for copy in bwd_stats:
        copy.start()

    y_copy.wait_recv()
    y_o[...] = (x_v[...].astype(F32) + (y_snd[...].astype(F32) + y_rx[...].astype(F32))).astype(BF16)

    d_gamma = jnp.zeros_like(dgamma_ref)
    for r in range(SPLITS):
        dh_copy(r).wait_recv()
        d_nrm = dh_snd[r].astype(F32) + dh_rx[r].astype(F32)
        d_gamma = d_gamma + jnp.sum(d_nrm * both(xhat_v, r), axis=0, keepdims=True)
        dh_v[r * piece:(r + 1) * piece] = d_nrm[:piece]
        dh_v[half + r * piece:half + (r + 1) * piece] = d_nrm[piece:]
    dgamma_ref[...] = d_gamma
    for copy in bwd_stats:
        copy.wait_recv()
    st_sum[...] = ((bst_snd[...] + bst_rx[0]) + (bst_rx[1] + bst_rx[2])) + ((bst_rx[3] + bst_rx[4]) + (bst_rx[5] + bst_rx[6]))
    sum_d, sum_dx = stats_columns(st_sum)
    d_hat = dh_v[...] * gamma_ref[...]
    d_x = dy_v[...].astype(F32) + inv_v[:, 0:1] * (d_hat - sum_d / d_model - xhat_v[...] * (sum_dx / d_model))
    dx_o[...] = d_x.astype(BF16)

    def drain(b, carry):
        core_copy(b).wait_send()
        return carry

    lax.fori_loop(0, N_BLK, drain, 0)
    for u in range(N_X):
        x_copy(u).wait_send()
    for k in range(4):
        for i in range(3 if k < 3 else 1):
            gather_copy(k, i).wait_send()
    for r in range(SPLITS):
        piece_copy(r).wait_send()
        dh_copy(r).wait_send()
    for copy in [packed_copy, dkv_copy, y_copy, kv_copy] + fwd_stats + bwd_stats:
        copy.wait_send()


def grad_kernel(y_v, dx_v, dgamma_in, nrm_t, attn_v, md, dq_v, dkv_v, dy_v, tiles,
                y_hbm, dx_hbm, dgamma_ref, dwq_hbm, dwg_hbm, dwu_hbm, dwk_hbm, dwv_hbm, dwo_hbm, dwd_hbm,
                ring, wide, out_sem, cp_sem):
    width, n_tok = nrm_t.shape
    half = n_tok // 2
    core = lax.rem(lax.axis_index('tx'), 2)
    mine = pl.multiple_of(core * half, half)
    other = pl.multiple_of((1 - core) * half, half)
    hand_out = [pltpu.make_async_copy(src.at[lo:lo + half], dst.at[pl.ds(at, half)], cp_sem.at[i])
                for i, (src, dst, lo, at) in enumerate(((y_v, y_hbm, 0, mine), (y_v, y_hbm, half, other), (dx_v, dx_hbm, 0, mine), (dx_v, dx_hbm, half, other)))]
    for cp in hand_out:
        cp.start()
    dgamma_ref[...] = dgamma_in[...]

    ready = [(0, dwq_hbm.at[:, 0:BLK]), (1, dwq_hbm.at[:, BLK:2 * BLK]), (2, dwo_hbm.at[0:BLK, :]), (3, dwo_hbm.at[BLK:2 * BLK, :]),
             (5, dwd_hbm.at[0:BLK, :]), (6, dwd_hbm.at[BLK:2 * BLK, :])]
    ready = [(tiles.at[i], dst) for i, dst in ready] + [(tiles.at[4, :, 0:256], dwk_hbm), (tiles.at[4, :, 256:512], dwv_hbm)]
    for i, (src, dst) in enumerate(ready):
        hand_out.append(pltpu.make_async_copy(src, dst, cp_sem.at[4 + i]))
        hand_out[-1].start()

    def put(src, dst, i):
        hand_out.append(pltpu.make_async_copy(src, dst, out_sem.at[i]))
        hand_out[-1].start()

    for t in range(6):
        k, j = 1 + t // 2, t % 2
        ring[t] = mm_at(md[k, 0, :, j * BLK:(j + 1) * BLK], dy_v[...])
        put(ring.at[t], dwd_hbm.at[k * CHUNK + j * BLK:k * CHUNK + (j + 1) * BLK, :], t)
    n_row = 128
    for i, (out, at) in enumerate(((dwg_hbm, 6), (dwu_hbm, 10))):
        for k in range(4):
            for j in range(2):
                lo = k * CHUNK + j * BLK
                wide[i, :, lo:lo + BLK] = mm(nrm_t[...], md[k, 1 + i, :, j * BLK:(j + 1) * BLK])
        for r in range(width // n_row):
            put(wide.at[i, r * n_row:(r + 1) * n_row], out.at[r * n_row:(r + 1) * n_row], at + r)
    for cp in hand_out:
        cp.wait()


def solution(mesh):
    tx_size = mesh.shape['tx']
    tok_spec = P('dp', None, 'tx')
    in_specs = (tok_spec, P('dp', None), tok_spec, P('tx'), P('tx', 'ty'), P('tx', 'ty'), P('tx', 'ty'),
                P('tx', None), P('tx', None), P('ty', 'tx'), P('ty', 'tx'))
    out_specs = (tok_spec, tok_spec, P(('dp', 'tx')), P(('dp', 'tx'), 'ty'), P(('dp', 'tx'), 'ty'), P(('dp', 'tx'), 'ty'),
                 P(('dp', 'tx'), None), P(('dp', 'tx'), None), P(('dp', 'ty'), 'tx'), P(('dp', 'ty'), 'tx'))

    def local_layer(x_in, positions, d_y, ln_gamma, w_q, w_g, w_u, w_k, w_v, w_o, w_d):
        _, n_tok, d_local = x_in.shape
        half = n_tok // 2
        d_model = d_local * tx_size
        head_dim = w_k.shape[1]
        q_width = w_q.shape[1]
        d_ff = w_g.shape[1]
        freq = jnp.asarray((ROPE_BASE ** (-2.0 * np.arange(head_dim // 2) / head_dim)).astype(np.float32)[None])
        any_spec = pl.BlockSpec(memory_space=pl.ANY)
        vmem_spec = pl.BlockSpec(memory_space=pltpu.VMEM)
        tok = (n_tok, d_local)
        sem = pltpu.SemaphoreType.DMA
        vm = pltpu.VMEM
        kept = pl.pallas_call(
            functools.partial(layer_kernel, d_model),
            out_shape=[vm(tok, BF16), vm(tok, BF16), vm((1, d_local), F32), vm((d_local, n_tok), BF16), vm((n_tok, q_width), BF16),
                       vm((4, 3, n_tok, CHUNK), BF16), vm((n_tok, q_width), BF16), vm((n_tok, 2 * head_dim), BF16), vm(tok, BF16),
                       vm((7, BLK, BLK), F32)],
            in_specs=[any_spec] * 12,
            out_specs=[vmem_spec] * 10,
            scratch_shapes=[
                vm((1, n_tok), jnp.int32), vm((1, head_dim // 2), F32), vm((1, d_local), F32), vm(tok, BF16),
                vm(tok, BF16), vm((d_local, q_width + 2 * head_dim), BF16), vm((d_local, d_ff), BF16), vm((d_local, d_ff), BF16),
                vm((q_width, d_local), BF16), vm((d_ff, d_local), BF16),
                vm((N_BLK, half, BLK), F32), vm((N_BLK, half, BLK), BF16), vm((N_BLK, half, BLK), BF16),
                vm((N_BLK, half, BLK), BF16), vm((N_BLK, half, BLK), BF16), vm((n_tok, 2 * q_width + 2 * head_dim), BF16),
                vm((n_tok, 512), BF16), vm((n_tok, 512), BF16), vm((n_tok, 512), F32),
                vm(tok, F32), vm((n_tok, 128), F32), vm((n_tok, 128), F32), vm((n_tok, 128), F32), vm(tok, F32), vm(tok, F32),
                vm(tok, BF16), vm(tok, BF16), vm((SPLITS, n_tok // SPLITS, d_local), BF16), vm((SPLITS, n_tok // SPLITS, d_local), BF16),
                vm((8, n_tok), F32), vm((3, 8, n_tok), F32), vm((8, n_tok), F32), vm((8, n_tok), F32), vm((7, 8, n_tok), F32), vm((2, half, CHUNK), F32),
                sem((15,)), sem((N_BLK,)), sem((N_BLK,)), sem((N_X,)), sem((N_X,)),
                sem((12 + SPLITS,)), sem((12 + SPLITS,)), sem((1,)), sem((1,)), sem((4,)), sem((4,)), sem((10,)), sem((10,)),
                sem((SPLITS,)), sem((SPLITS,))],
            compiler_params=pltpu.CompilerParams(collective_id=0, has_side_effects=True, vmem_limit_bytes=46 * 1024 * 1024),
            name='layer',
        )(x_in.reshape(tok), positions, freq, d_y.reshape(tok), ln_gamma[None], w_q, w_g, w_u, w_k, w_v, w_o, w_d)

        y_out, d_x, d_gamma, d_wq, d_wg, d_wu, d_wk, d_wv, d_wo, d_wd = pl.pallas_call(
            grad_kernel,
            out_shape=[jax.ShapeDtypeStruct(tok, BF16), jax.ShapeDtypeStruct(tok, BF16), jax.ShapeDtypeStruct((1, d_local), F32)]
            + [jax.ShapeDtypeStruct(w.shape, F32) for w in (w_q, w_g, w_u, w_k, w_v, w_o, w_d)],
            in_specs=[vmem_spec] * 10,
            out_specs=[any_spec, any_spec, vmem_spec] + [any_spec] * 7,
            scratch_shapes=[vm((6, d_local, BLK), F32), vm((2, d_local, d_ff), F32), sem((14,)), sem((12,))],
            compiler_params=pltpu.CompilerParams(vmem_limit_bytes=30 * 1024 * 1024),
            name='weight_grads',
        )(*kept)
        return (y_out.reshape(x_in.shape), d_x.reshape(x_in.shape), d_gamma.reshape(d_local),
                d_wq, d_wg, d_wu, d_wk, d_wv, d_wo, d_wd)

    return jax.shard_map(local_layer, mesh=mesh, in_specs=in_specs, out_specs=out_specs, check_vma=False)
```

```python
import functools

import jax
import jax.numpy as jnp
import numpy as np
from jax import lax
from jax.experimental import pallas as pl
from jax.experimental.pallas import tpu as pltpu
from jax.sharding import PartitionSpec as P

EPS = 1e-6
ROPE_BASE = 10000.0
F32 = jnp.float32
BF16 = jnp.bfloat16
MESH = pl.DeviceIdType.MESH

BLK = 512
CHUNK = 1024
B_DATTN, B_DACT_LO, B_QKV, B_GU, B_DACT_HI, N_BLK = 0, 2, 6, 9, 25, 29
X_UNITS = ((0, 1), (1, 1), (2, 2), (4, 2), (6, 2), (9, 4), (13, 4), (17, 4), (21, 4), (25, 2))
PIECES = ((0, 16), (16, 32), (48, 32), (80, 32), (112, 16))
SPLITS = len(PIECES)
X_KV = len(X_UNITS)
X_LAST = X_KV + 1
N_X = X_LAST + SPLITS


def dot(a, b, dims):
    return lax.dot_general(a, b, (dims, ((), ())), preferred_element_type=F32)


def mm(a, b):
    return dot(a, b, ((1,), (0,)))


def mm_bt(a, b):
    return dot(a, b, ((1,), (1,)))


def mm_at(a, b):
    return dot(a, b, ((0,), (0,)))


def rope(first, second, cos_t, sin_t):
    return first * cos_t - second * sin_t, second * cos_t + first * sin_t


def layer_kernel(d_model, x_hbm, pos_hbm, freq_hbm, dy_hbm, gamma_hbm, wq_hbm, wg_hbm, wu_hbm, wk_hbm, wv_hbm, wo_hbm, wd_hbm,
                 y_o, dx_o, dgamma_ref, nrm_t, attn_v, md, dq_v, dkv_v, dy_v, tiles,
                 pos_ref, freq_ref, gamma_ref, nrm_v, x_v, wqkv_v, wg_v, wu_v, wo_v, wd_v,
                 keep, send, rcore, chip, rx, packed, dkv_part, dkv_rx, kv_acc,
                 xhat_v, inv_v, cos_v, sin_v, br_v, dh_v, y_snd, y_rx, dh_snd, dh_rx,
                 st_snd, st_rx, st_sum, bst_snd, bst_rx, factors,
                 ld_sem, cs, cr, xs, xr, gs, gr, ps, pr, ts, tr, ss, sr, ds, dr):
    tx = lax.axis_index('tx')
    ty = lax.axis_index('ty')
    core = lax.rem(tx, 2)
    near = {'tx': tx + 1 - 2 * core}
    across = {'tx': lax.rem(tx + 2, 4)}
    far = {'tx': lax.rem(tx + 1 - 2 * core + 2, 4)}
    other_ty = {'ty': 1 - ty}
    peers = [near, across, far, other_ty] + [{'tx': p['tx'], 'ty': 1 - ty} for p in (near, across, far)]
    n_tok = x_v.shape[0]
    half = n_tok // 2
    mine = pl.multiple_of(core * half, half)
    other = pl.multiple_of((1 - core) * half, half)
    head_dim = 256
    q_width = wo_v.shape[0]
    heads = q_width // head_dim

    def load(i, src, dst):
        return pltpu.make_async_copy(src, dst, ld_sem.at[i])

    d_half = wd_v.shape[0] // 2
    loads = [
        load(0, dy_hbm.at[pl.ds(mine, half)], dy_v.at[0:half]),
        load(1, dy_hbm.at[pl.ds(other, half)], dy_v.at[half:n_tok]),
        load(2, wo_hbm.at[0:BLK], wo_v.at[0:BLK]),
        load(3, x_hbm.at[pl.ds(mine, half)], x_v.at[0:half]),
        load(4, x_hbm.at[pl.ds(other, half)], x_v.at[half:n_tok]),
        load(5, wd_hbm.at[0:d_half], wd_v.at[0:d_half]),
        load(6, wq_hbm, wqkv_v.at[:, 0:q_width]),
        load(7, wk_hbm, wqkv_v.at[:, q_width:q_width + head_dim]),
        load(8, wv_hbm, wqkv_v.at[:, q_width + head_dim:q_width + 2 * head_dim]),
        load(9, wg_hbm, wg_v),
        load(10, wu_hbm, wu_v),
        load(11, wd_hbm.at[d_half:2 * d_half], wd_v.at[d_half:2 * d_half]),
        load(12, gamma_hbm, gamma_ref),
        load(13, pos_hbm, pos_ref),
        load(14, freq_hbm, freq_ref),
        load(15, wo_hbm.at[BLK:q_width], wo_v.at[BLK:q_width]),
    ]
    for i in (0, 1, 2, 15, 3, 4):
        loads[i].start()

    barrier = pltpu.get_barrier_semaphore()
    for peer in peers:
        pl.semaphore_signal(barrier, inc=1, device_id=peer, device_id_type=MESH)
    for ld in loads[:3]:
        ld.wait()
    for ld in loads[5:15]:
        ld.start()

    def remote(src, dst, send_sem, recv_sem, peer):
        return pltpu.make_async_remote_copy(src_ref=src, dst_ref=dst, send_sem=send_sem, recv_sem=recv_sem,
                                            device_id=peer, device_id_type=MESH)

    def core_copy(b):
        return remote(send.at[b], rcore.at[b], cs.at[b], cr.at[b], near)

    def x_copy(u):
        if u >= X_LAST:
            rows = pl.ds(*PIECES[u - X_LAST])
            return remote(chip.at[pl.ds(N_BLK - 2, 2), rows], rx.at[pl.ds(N_BLK - 2, 2), rows], xs.at[u], xr.at[u], across)
        if u == X_KV:
            cols = pl.ds(pl.multiple_of(ty * head_dim, head_dim), head_dim)
            return remote(chip.at[B_QKV + 2, :, cols], rx.at[B_QKV + 2, :, cols], xs.at[u], xr.at[u], across)
        start, count = X_UNITS[u]
        return remote(chip.at[pl.ds(start, count)], rx.at[pl.ds(start, count)], xs.at[u], xr.at[u], across)

    def put(b, part):
        keep[b] = part[:half]
        send[b] = part[half:].astype(BF16)
        core_copy(b).start()

    def issue_bwd(b, w_ref, row):
        put(b, mm_bt(dy_v[...], w_ref[pl.ds(row, BLK), :]))

    def issue_fwd(b, w_ref, col):
        put(b, mm(nrm_v[...], w_ref[:, pl.ds(col, BLK)]))

    def combine(b):
        core_copy(b).wait_recv()
        chip[b] = (keep[b] + rcore[b].astype(F32)).astype(BF16)

    def total(b):
        return chip[b].astype(F32) + rx[b].astype(F32)

    part = mm_bt(dy_v[...], wo_v[0:BLK, :])
    keep[0] = part[:half]
    send[0] = part[half:].astype(BF16)
    pl.semaphore_wait(barrier, len(peers))
    core_copy(0).start()
    loads[15].wait()
    issue_bwd(1, wo_v, BLK)

    def rows_of(col_a, col_b):
        lane = lax.broadcasted_iota(jnp.int32, (half, 128), 1)
        return jnp.where(lane == 0, col_a, col_b).T[0:8]

    def stats_copies(snd, got, base, to):
        return [remote(snd, got.at[i], ss.at[base + i], sr.at[base + i], peer) for i, peer in enumerate(to)]

    def stats_put(snd, col_a, col_b):
        for lo, at in ((0, mine), (half, other)):
            snd[:, pl.ds(at, half)] = rows_of(col_a[lo:lo + half], col_b[lo:lo + half])

    def stats_columns(rows_ref):
        cols = []
        for i in range(2):
            parts = [jnp.broadcast_to(rows_ref[i:i + 1, pl.ds(at, half)], (128, half)).T[:, 0:1] for at in (mine, other)]
            cols.append(jnp.concatenate(parts, axis=0))
        return cols

    loads[3].wait()
    loads[4].wait()
    x_f = x_v[...].astype(F32)
    stats_put(st_snd, jnp.sum(x_f, axis=1, keepdims=True), jnp.sum(x_f * x_f, axis=1, keepdims=True))
    fwd_stats = stats_copies(st_snd, st_rx, 0, (near, across, far))
    for copy in fwd_stats:
        copy.start()

    combine(0)
    x_copy(0).start()
    combine(1)
    x_copy(1).start()

    loads[5].wait()
    for i in range(4):
        issue_bwd(B_DACT_LO + i, wd_v, i * BLK)
        if i >= 1:
            combine(B_DACT_LO + i - 1)
        if i == 2:
            x_copy(2).start()
    combine(B_DACT_LO + 3)
    x_copy(3).start()

    loads[12].wait()
    for copy in fwd_stats:
        copy.wait_recv()
    st_sum[...] = (st_snd[...] + st_rx[0]) + (st_rx[1] + st_rx[2])
    sum_x, sum_xx = stats_columns(st_sum)
    tok_mean = sum_x / d_model
    inv_std = lax.rsqrt(sum_xx / d_model - tok_mean * tok_mean + EPS)
    inv_v[...] = jnp.broadcast_to(inv_std, (n_tok, 128))
    x_hat = (x_v[...].astype(F32) - tok_mean) * inv_std
    xhat_v[...] = x_hat
    nrm_v[...] = (x_hat * gamma_ref[...]).astype(BF16)

    for i in range(6, 9):
        loads[i].wait()
    for i in range(3):
        issue_fwd(B_QKV + i, wqkv_v, i * BLK)
    for i in (2, 0, 1):
        combine(B_QKV + i)
        if i == 2:
            x_copy(X_KV).start()
    x_copy(4).start()

    loads[9].wait()
    loads[10].wait()
    for k in range(4):
        def gu_issue(j, carry, k=k):
            col = pl.multiple_of(k * CHUNK + j * BLK, BLK)
            issue_fwd(B_GU + 4 * k + j, wg_v, col)
            issue_fwd(B_GU + 4 * k + 2 + j, wu_v, col)
            return carry

        def gu_combine(j, carry, k=k):
            combine(B_GU + 4 * k + j)
            return carry

        lax.fori_loop(0, 2, gu_issue, 0)
        lax.fori_loop(0, 4, gu_combine, 0)
        x_copy(5 + k).start()

    loads[11].wait()

    def hi_issue(j, carry):
        issue_bwd(B_DACT_HI + j, wd_v, pl.multiple_of(d_half + j * BLK, BLK))
        return carry

    lax.fori_loop(0, 4, hi_issue, 0)
    for j in range(4):
        combine(B_DACT_HI + j)
        if j == 1:
            x_copy(9).start()
    for r in range(SPLITS):
        x_copy(X_LAST + r).start()

    nrm_t[...] = nrm_v[...].T

    loads[13].wait()
    loads[14].wait()
    freq = freq_ref[...]
    for lo, at in ((0, mine), (half, other)):
        pos_col = jnp.broadcast_to(pos_ref[0:1, pl.ds(at, half)].astype(F32), (128, half)).T
        angles = pos_col * freq
        cos_v[lo:lo + half] = jnp.cos(angles)
        sin_v[lo:lo + half] = jnp.sin(angles)

    packed_copy = remote(packed.at[0:half], packed.at[half:n_tok], ps.at[0], pr.at[0], near)
    x_copy(0).wait_recv()
    x_copy(1).wait_recv()
    for j in range(2):
        packed[0:half, q_width + 512 + j * BLK:q_width + 512 + (j + 1) * BLK] = total(B_DATTN + j).astype(BF16)
    x_copy(4).wait_recv()
    cos_h, sin_h = cos_v[0:half], sin_v[0:half]
    for j in range(2):
        blk = total(B_QKV + j)
        for h in range(2):
            lo = h * head_dim
            first, second = rope(blk[:, lo:lo + 128], blk[:, lo + 128:lo + 256], cos_h, sin_h)
            packed[0:half, j * BLK + lo:j * BLK + lo + 128] = first.astype(BF16)
            packed[0:half, j * BLK + lo + 128:j * BLK + lo + 256] = second.astype(BF16)
    x_copy(X_KV).wait_recv()
    kv_cols = pl.ds(pl.multiple_of(ty * head_dim, head_dim), head_dim)
    blk = chip[B_QKV + 2, :, kv_cols].astype(F32) + rx[B_QKV + 2, :, kv_cols].astype(F32)
    first, second = rope(blk[:, 0:128], blk[:, 128:256], cos_h, sin_h)
    kv_mine = jnp.where(ty == 0, jnp.concatenate([first, second], axis=1), blk).astype(BF16)
    kv_dst = packed.at[0:half, pl.ds(pl.multiple_of(q_width + ty * head_dim, head_dim), head_dim)]
    kv_dst[...] = kv_mine
    kv_copy = remote(kv_dst, kv_dst, ts.at[3], tr.at[3], other_ty)
    kv_copy.start()
    kv_copy.wait_recv()
    packed_copy.start()
    packed_copy.wait_recv()

    row_i = lax.rem(lax.broadcasted_iota(jnp.int32, (n_tok, n_tok), 0) + core * half, n_tok)
    col_i = lax.rem(lax.broadcasted_iota(jnp.int32, (n_tok, n_tok), 1) + core * half, n_tok)
    scale = head_dim ** -0.5
    kv_acc[...] = jnp.zeros_like(kv_acc)

    def head_step(h, carry):
        cols = pl.ds(pl.multiple_of(h * head_dim, head_dim), head_dim)
        q_h = packed[:, cols]
        da_h = packed[:, pl.ds(pl.multiple_of(q_width + 512 + h * head_dim, head_dim), head_dim)]
        k_rot = packed[:, q_width:q_width + 256]
        v_val = packed[:, q_width + 256:q_width + 512]
        scores = jnp.where(row_i >= col_i, mm_bt(q_h, k_rot) * scale, -1e30)
        exps = jnp.exp(scores - jnp.max(scores, axis=1, keepdims=True))
        probs_f = exps / jnp.sum(exps, axis=1, keepdims=True)
        probs = probs_f.astype(BF16)
        attn_v[:, cols] = mm(probs, v_val).astype(BF16)
        d_probs = mm_bt(da_h, v_val).astype(BF16).astype(F32)
        d_scores = (probs_f * (d_probs - jnp.sum(d_probs * probs_f, axis=1, keepdims=True)) * scale).astype(BF16)
        dq_h = mm(d_scores, k_rot).astype(BF16).astype(F32)
        first, second = rope(dq_h[:, 0:128], dq_h[:, 128:256], cos_v[...], -sin_v[...])
        dq_v[:, pl.ds(pl.multiple_of(h * head_dim, head_dim), 128)] = first.astype(BF16)
        dq_v[:, pl.ds(pl.multiple_of(h * head_dim + 128, 128), 128)] = second.astype(BF16)
        kv_acc[:, 0:256] += mm_at(d_scores, q_h)
        kv_acc[:, 256:512] += mm_at(probs, da_h)
        return carry

    lax.fori_loop(0, heads, head_step, 0)
    dkv_part[...] = kv_acc[...].astype(BF16)
    dkv_copy = remote(dkv_part, dkv_rx, ts.at[0], tr.at[0], other_ty)
    dkv_copy.start()
    br_v[...] = mm(attn_v[...], wo_v[...])
    dh_v[...] = mm_bt(dq_v[...], wqkv_v[:, 0:q_width])

    for j in range(2):
        tiles[j] = mm(nrm_t[...], dq_v[:, j * BLK:(j + 1) * BLK])
        tiles[2 + j] = mm_at(attn_v[:, j * BLK:(j + 1) * BLK], dy_v[...])

    def piece_copy(r):
        lo, size = PIECES[r]
        return remote(md.at[3, 1:3, lo:lo + size], md.at[3, 1:3, half + lo:half + lo + size], gs.at[12 + r], gr.at[12 + r], near)

    def gather_copy(k, i):
        return remote(md.at[k, i, 0:half], md.at[k, i, half:n_tok], gs.at[3 * k + i], gr.at[3 * k + i], near)

    def dact_block(k, j):
        return B_DACT_LO + 2 * k + j if k < 2 else B_DACT_HI + 2 * (k - 2) + j

    def gated(k, want_act, want_grad):
        def step(r, carry):
            rows = pl.ds(pl.multiple_of(r * 16, 16), 16)
            for j in range(2):
                bg, bu, bd = B_GU + 4 * k + j, B_GU + 4 * k + 2 + j, dact_block(k, j)
                gate = (chip[bg, rows].astype(F32) + rx[bg, rows].astype(F32)).astype(BF16).astype(F32)
                up = (chip[bu, rows].astype(F32) + rx[bu, rows].astype(F32)).astype(BF16).astype(F32)
                sig = jax.nn.sigmoid(gate)
                silu = gate * sig
                cols = slice(j * BLK, (j + 1) * BLK)
                if want_act:
                    md[k, 0, rows, cols] = (silu * up).astype(BF16)
                if k == 3:
                    factors[0, rows, cols] = up * sig * (1.0 + gate * (1.0 - sig))
                    factors[1, rows, cols] = silu
                if want_grad:
                    d_act = (chip[bd, rows].astype(F32) + rx[bd, rows].astype(F32)).astype(BF16).astype(F32)
                    md[k, 1, rows, cols] = (d_act * up * sig * (1.0 + gate * (1.0 - sig))).astype(BF16)
                    md[k, 2, rows, cols] = (d_act * silu).astype(BF16)
            return carry

        lax.fori_loop(0, half // 16, step, 0)
        for i in ((0,) if want_act else ()) + ((1, 2) if want_grad else ()):
            gather_copy(k, i).start()

    def use_act(k):
        gather_copy(k, 0).wait_recv()
        br_v[...] += mm(md[k, 0], wd_v[k * CHUNK:(k + 1) * CHUNK, :])

    def use_grad(k):
        for i in (1, 2):
            gather_copy(k, i).wait_recv()
        dh_v[...] += (mm_bt(md[k, 1], wg_v[:, k * CHUNK:(k + 1) * CHUNK])
                      + mm_bt(md[k, 2], wu_v[:, k * CHUNK:(k + 1) * CHUNK]))

    x_copy(2).wait_recv()
    x_copy(3).wait_recv()
    for k in range(2):
        x_copy(5 + k).wait_recv()
        gated(k, True, True)
        use_act(k)
        use_grad(k)
        if k == 0:
            dkv_copy.wait_recv()
            d_k = dkv_part[:, 0:256].astype(F32) + dkv_rx[:, 0:256].astype(F32)
            d_k = d_k.astype(BF16).astype(F32)
            first, second = rope(d_k[:, 0:128], d_k[:, 128:256], cos_v[...], -sin_v[...])
            dkv_v[:, 0:128] = first.astype(BF16)
            dkv_v[:, 128:256] = second.astype(BF16)
            dkv_v[:, 256:512] = (dkv_part[:, 256:512].astype(F32) + dkv_rx[:, 256:512].astype(F32)).astype(BF16)
            dh_v[...] += 0.5 * mm_bt(dkv_v[...], wqkv_v[:, q_width:q_width + 512])
            tiles[4] = mm(nrm_t[...], dkv_v[...])
            for j in range(2):
                tiles[5 + j] = mm_at(md[0, 0, :, j * BLK:(j + 1) * BLK], dy_v[...])
    for k in (2, 3):
        x_copy(5 + k).wait_recv()
        gated(k, True, False)
        use_act(k)
    y_snd[...] = br_v[...].astype(BF16)
    y_copy = remote(y_snd, y_rx, ts.at[1], tr.at[1], other_ty)
    y_copy.start()
    x_copy(9).wait_recv()
    gated(2, False, True)

    def dh_copy(r):
        at = pl.ds(2 * PIECES[r][0], 2 * PIECES[r][1])
        return remote(dh_snd.at[at], dh_rx.at[at], ds.at[r], dr.at[r], other_ty)

    def both(ref, r):
        lo, size = PIECES[r]
        return jnp.concatenate([ref[lo:lo + size], ref[half + lo:half + lo + size]], axis=0)

    sums = []

    def piece_grad(r):
        x_copy(X_LAST + r).wait_recv()
        rows = slice(PIECES[r][0], PIECES[r][0] + PIECES[r][1])
        for j in range(2):
            cols = slice(j * BLK, (j + 1) * BLK)
            b = dact_block(3, j)
            d_act = (chip[b, rows].astype(F32) + rx[b, rows].astype(F32)).astype(BF16).astype(F32)
            for i in range(2):
                md[3, 1 + i, rows, cols] = (d_act * factors[i, rows, cols]).astype(BF16)
        piece_copy(r).start()

    def piece_dh(r):
        piece_copy(r).wait_recv()
        part = both(dh_v, r) + mm_bt(both(md.at[3, 1], r), wg_v[:, 3 * CHUNK:4 * CHUNK]) + mm_bt(both(md.at[3, 2], r), wu_v[:, 3 * CHUNK:4 * CHUNK])
        part_b = part.astype(BF16)
        dh_snd[2 * PIECES[r][0]:2 * (PIECES[r][0] + PIECES[r][1])] = part_b
        dh_copy(r).start()
        d_hat = part_b.astype(F32) * gamma_ref[...]
        sums.append((jnp.sum(d_hat, axis=1, keepdims=True), jnp.sum(d_hat * both(xhat_v, r), axis=1, keepdims=True)))

    piece_grad(0)
    use_grad(2)
    for r in range(1, SPLITS):
        piece_grad(r)
        piece_dh(r - 1)
    piece_dh(SPLITS - 1)
    cols = [jnp.concatenate([sums[r][i][:PIECES[r][1]] for r in range(SPLITS)] + [sums[r][i][PIECES[r][1]:] for r in range(SPLITS)], axis=0) for i in range(2)]
    stats_put(bst_snd, cols[0], cols[1])
    bwd_stats = stats_copies(bst_snd, bst_rx, 3, peers)
    for copy in bwd_stats:
        copy.start()

    y_copy.wait_recv()
    y_o[...] = (x_v[...].astype(F32) + (y_snd[...].astype(F32) + y_rx[...].astype(F32))).astype(BF16)

    def drain(b, carry):
        core_copy(b).wait_send()
        return carry

    lax.fori_loop(0, N_BLK, drain, 0)
    for u in range(N_X):
        x_copy(u).wait_send()
    for k in range(4):
        for i in range(3 if k < 3 else 1):
            gather_copy(k, i).wait_send()
    for r in range(SPLITS):
        piece_copy(r).wait_send()
    for copy in [packed_copy, dkv_copy, y_copy, kv_copy] + fwd_stats:
        copy.wait_send()

    d_gamma = jnp.zeros_like(dgamma_ref)
    for r in range(SPLITS):
        dh_copy(r).wait_recv()
        lo, size = PIECES[r]
        d_nrm = dh_snd[2 * lo:2 * (lo + size)].astype(F32) + dh_rx[2 * lo:2 * (lo + size)].astype(F32)
        d_gamma = d_gamma + jnp.sum(d_nrm * both(xhat_v, r), axis=0, keepdims=True)
        dh_v[lo:lo + size] = d_nrm[:size]
        dh_v[half + lo:half + lo + size] = d_nrm[size:]
    dgamma_ref[...] = d_gamma
    for copy in bwd_stats:
        copy.wait_recv()
    st_sum[...] = ((bst_snd[...] + bst_rx[0]) + (bst_rx[1] + bst_rx[2])) + ((bst_rx[3] + bst_rx[4]) + (bst_rx[5] + bst_rx[6]))
    sum_d, sum_dx = stats_columns(st_sum)
    d_hat = dh_v[...] * gamma_ref[...]
    d_x = dy_v[...].astype(F32) + inv_v[:, 0:1] * (d_hat - sum_d / d_model - xhat_v[...] * (sum_dx / d_model))
    dx_o[...] = d_x.astype(BF16)

    for r in range(SPLITS):
        dh_copy(r).wait_send()
    for copy in bwd_stats:
        copy.wait_send()


def grad_kernel(y_v, dx_v, dgamma_in, nrm_t, attn_v, md, dq_v, dkv_v, dy_v, tiles,
                y_hbm, dx_hbm, dgamma_hbm, dwq_hbm, dwg_hbm, dwu_hbm, dwk_hbm, dwv_hbm, dwo_hbm, dwd_hbm,
                ring, wide, out_sem, cp_sem):
    width, n_tok = nrm_t.shape
    half = n_tok // 2
    core = lax.rem(lax.axis_index('tx'), 2)
    mine = pl.multiple_of(core * half, half)
    other = pl.multiple_of((1 - core) * half, half)
    hand_out = [pltpu.make_async_copy(src.at[lo:lo + half], dst.at[pl.ds(at, half)], cp_sem.at[i])
                for i, (src, dst, lo, at) in enumerate(((y_v, y_hbm, 0, mine), (y_v, y_hbm, half, other), (dx_v, dx_hbm, 0, mine), (dx_v, dx_hbm, half, other)))]
    for cp in hand_out:
        cp.start()
    hand_out.append(pltpu.make_async_copy(dgamma_in, dgamma_hbm, cp_sem.at[12]))
    hand_out[-1].start()

    ready = [(0, dwq_hbm.at[:, 0:BLK]), (1, dwq_hbm.at[:, BLK:2 * BLK]), (2, dwo_hbm.at[0:BLK, :]), (3, dwo_hbm.at[BLK:2 * BLK, :]),
             (5, dwd_hbm.at[0:BLK, :]), (6, dwd_hbm.at[BLK:2 * BLK, :])]
    ready = [(tiles.at[i], dst) for i, dst in ready] + [(tiles.at[4, :, 0:256], dwk_hbm), (tiles.at[4, :, 256:512], dwv_hbm)]
    for i, (src, dst) in enumerate(ready):
        hand_out.append(pltpu.make_async_copy(src, dst, cp_sem.at[4 + i]))
        hand_out[-1].start()

    def put(src, dst, i):
        hand_out.append(pltpu.make_async_copy(src, dst, out_sem.at[i]))
        hand_out[-1].start()

    for t in range(6):
        k, j = 1 + t // 2, t % 2
        ring[t] = mm_at(md[k, 0, :, j * BLK:(j + 1) * BLK], dy_v[...])
        put(ring.at[t], dwd_hbm.at[k * CHUNK + j * BLK:k * CHUNK + (j + 1) * BLK, :], t)
    n_row = 128
    for i, (out, at) in enumerate(((dwg_hbm, 6), (dwu_hbm, 10))):
        for k in range(4):
            for j in range(2):
                lo = k * CHUNK + j * BLK
                wide[i, :, lo:lo + BLK] = mm(nrm_t[...], md[k, 1 + i, :, j * BLK:(j + 1) * BLK])
        for r in range(width // n_row):
            put(wide.at[i, r * n_row:(r + 1) * n_row], out.at[r * n_row:(r + 1) * n_row], at + r)
    for cp in hand_out:
        cp.wait()


def solution(mesh):
    tx_size = mesh.shape['tx']
    tok_spec = P('dp', None, 'tx')
    in_specs = (tok_spec, P('dp', None), tok_spec, P('tx'), P('tx', 'ty'), P('tx', 'ty'), P('tx', 'ty'),
                P('tx', None), P('tx', None), P('ty', 'tx'), P('ty', 'tx'))
    out_specs = (tok_spec, tok_spec, P(('dp', 'tx')), P(('dp', 'tx'), 'ty'), P(('dp', 'tx'), 'ty'), P(('dp', 'tx'), 'ty'),
                 P(('dp', 'tx'), None), P(('dp', 'tx'), None), P(('dp', 'ty'), 'tx'), P(('dp', 'ty'), 'tx'))

    def local_layer(x_in, positions, d_y, ln_gamma, w_q, w_g, w_u, w_k, w_v, w_o, w_d):
        _, n_tok, d_local = x_in.shape
        half = n_tok // 2
        d_model = d_local * tx_size
        head_dim = w_k.shape[1]
        q_width = w_q.shape[1]
        d_ff = w_g.shape[1]
        freq = jnp.asarray((ROPE_BASE ** (-2.0 * np.arange(head_dim // 2) / head_dim)).astype(np.float32)[None])
        any_spec = pl.BlockSpec(memory_space=pl.ANY)
        vmem_spec = pl.BlockSpec(memory_space=pltpu.VMEM)
        tok = (n_tok, d_local)
        sem = pltpu.SemaphoreType.DMA
        vm = pltpu.VMEM
        kept = pl.pallas_call(
            functools.partial(layer_kernel, d_model),
            out_shape=[vm(tok, BF16), vm(tok, BF16), vm((1, d_local), F32), vm((d_local, n_tok), BF16), vm((n_tok, q_width), BF16),
                       vm((4, 3, n_tok, CHUNK), BF16), vm((n_tok, q_width), BF16), vm((n_tok, 2 * head_dim), BF16), vm(tok, BF16),
                       vm((7, BLK, BLK), F32)],
            in_specs=[any_spec] * 12,
            out_specs=[vmem_spec] * 10,
            scratch_shapes=[
                vm((1, n_tok), jnp.int32), vm((1, head_dim // 2), F32), vm((1, d_local), F32), vm(tok, BF16),
                vm(tok, BF16), vm((d_local, q_width + 2 * head_dim), BF16), vm((d_local, d_ff), BF16), vm((d_local, d_ff), BF16),
                vm((q_width, d_local), BF16), vm((d_ff, d_local), BF16),
                vm((N_BLK, half, BLK), F32), vm((N_BLK, half, BLK), BF16), vm((N_BLK, half, BLK), BF16),
                vm((N_BLK, half, BLK), BF16), vm((N_BLK, half, BLK), BF16), vm((n_tok, 2 * q_width + 2 * head_dim), BF16),
                vm((n_tok, 512), BF16), vm((n_tok, 512), BF16), vm((n_tok, 512), F32),
                vm(tok, F32), vm((n_tok, 128), F32), vm((n_tok, 128), F32), vm((n_tok, 128), F32), vm(tok, F32), vm(tok, F32),
                vm(tok, BF16), vm(tok, BF16), vm(tok, BF16), vm(tok, BF16),
                vm((8, n_tok), F32), vm((3, 8, n_tok), F32), vm((8, n_tok), F32), vm((8, n_tok), F32), vm((7, 8, n_tok), F32), vm((2, half, CHUNK), F32),
                sem((16,)), sem((N_BLK,)), sem((N_BLK,)), sem((N_X,)), sem((N_X,)),
                sem((12 + SPLITS,)), sem((12 + SPLITS,)), sem((1,)), sem((1,)), sem((4,)), sem((4,)), sem((10,)), sem((10,)),
                sem((SPLITS,)), sem((SPLITS,))],
            compiler_params=pltpu.CompilerParams(collective_id=0, has_side_effects=True, vmem_limit_bytes=46 * 1024 * 1024),
            name='layer',
        )(x_in.reshape(tok), positions, freq, d_y.reshape(tok), ln_gamma[None], w_q, w_g, w_u, w_k, w_v, w_o, w_d)

        y_out, d_x, d_gamma, d_wq, d_wg, d_wu, d_wk, d_wv, d_wo, d_wd = pl.pallas_call(
            grad_kernel,
            out_shape=[jax.ShapeDtypeStruct(tok, BF16), jax.ShapeDtypeStruct(tok, BF16), jax.ShapeDtypeStruct((1, d_local), F32)]
            + [jax.ShapeDtypeStruct(w.shape, F32) for w in (w_q, w_g, w_u, w_k, w_v, w_o, w_d)],
            in_specs=[vmem_spec] * 10,
            out_specs=[any_spec] * 10,
            scratch_shapes=[vm((6, d_local, BLK), F32), vm((2, d_local, d_ff), F32), sem((14,)), sem((13,))],
            compiler_params=pltpu.CompilerParams(vmem_limit_bytes=30 * 1024 * 1024),
            name='weight_grads',
        )(*kept)
        return (y_out.reshape(x_in.shape), d_x.reshape(x_in.shape), d_gamma.reshape(d_local),
                d_wq, d_wg, d_wu, d_wk, d_wv, d_wo, d_wd)

    return jax.shard_map(local_layer, mesh=mesh, in_specs=in_specs, out_specs=out_specs, check_vma=False)
```

```python
import functools

import jax
import jax.numpy as jnp
import numpy as np
from jax import lax
from jax.experimental import pallas as pl
from jax.experimental.pallas import tpu as pltpu
from jax.sharding import PartitionSpec as P

EPS = 1e-6
ROPE_BASE = 10000.0
F32 = jnp.float32
BF16 = jnp.bfloat16
MESH = pl.DeviceIdType.MESH

BLK = 512
CHUNK = 1024
B_DATTN, B_DACT_LO, B_QKV, B_GU, B_DACT_HI, N_BLK = 0, 2, 4, 7, 23, 29
X_UNITS = ((0, 1), (1, 1), (2, 2), (4, 2), (7, 4), (11, 4), (15, 4), (19, 4), (23, 2), (25, 2))
PIECES = ((0, 16), (16, 32), (48, 32), (80, 32), (112, 16))
SPLITS = len(PIECES)
X_KV = len(X_UNITS)
X_LAST = X_KV + 1
N_X = X_LAST + SPLITS


def dot(a, b, dims):
    return lax.dot_general(a, b, (dims, ((), ())), preferred_element_type=F32)


def mm(a, b):
    return dot(a, b, ((1,), (0,)))


def mm_bt(a, b):
    return dot(a, b, ((1,), (1,)))


def mm_at(a, b):
    return dot(a, b, ((0,), (0,)))


def rope(first, second, cos_t, sin_t):
    return first * cos_t - second * sin_t, second * cos_t + first * sin_t


def layer_kernel(d_model, x_hbm, pos_hbm, freq_hbm, dy_hbm, gamma_hbm, wq_hbm, wg_hbm, wu_hbm, wk_hbm, wv_hbm, wo_hbm, wd_hbm,
                 y_o, dx_o, dgamma_ref, nrm_t, attn_v, md, dq_v, dkv_v, dy_v, tiles,
                 pos_ref, freq_ref, gamma_ref, nrm_v, x_v, wqkv_v, wg_v, wu_v, wo_v, wd_v,
                 keep, send, rcore, chip, rx, packed, dkv_part, dkv_rx, kv_acc,
                 xhat_v, inv_v, cos_v, sin_v, br_v, dh_v, y_snd, y_rx, dh_snd, dh_rx,
                 st_snd, st_rx, st_sum, bst_snd, bst_rx, factors,
                 ld_sem, cs, cr, xs, xr, gs, gr, ps, pr, ts, tr, ss, sr, ds, dr):
    tx = lax.axis_index('tx')
    ty = lax.axis_index('ty')
    core = lax.rem(tx, 2)
    near = {'tx': tx + 1 - 2 * core}
    across = {'tx': lax.rem(tx + 2, 4)}
    far = {'tx': lax.rem(tx + 1 - 2 * core + 2, 4)}
    other_ty = {'ty': 1 - ty}
    peers = [near, across, far, other_ty] + [{'tx': p['tx'], 'ty': 1 - ty} for p in (near, across, far)]
    n_tok = x_v.shape[0]
    half = n_tok // 2
    mine = pl.multiple_of(core * half, half)
    other = pl.multiple_of((1 - core) * half, half)
    head_dim = 256
    q_width = wo_v.shape[0]
    heads = q_width // head_dim

    def load(i, src, dst):
        return pltpu.make_async_copy(src, dst, ld_sem.at[i])

    loads = [
        load(0, dy_hbm.at[pl.ds(mine, half)], dy_v.at[0:half]),
        load(1, dy_hbm.at[pl.ds(other, half)], dy_v.at[half:n_tok]),
        load(2, wo_hbm.at[0:BLK], wo_v.at[0:BLK]),
        load(3, x_hbm.at[pl.ds(mine, half)], x_v.at[0:half]),
        load(4, x_hbm.at[pl.ds(other, half)], x_v.at[half:n_tok]),
        load(5, wd_hbm.at[0:CHUNK], wd_v.at[0:CHUNK]),
        load(6, wq_hbm, wqkv_v.at[:, 0:q_width]),
        load(7, wk_hbm, wqkv_v.at[:, q_width:q_width + head_dim]),
        load(8, wv_hbm, wqkv_v.at[:, q_width + head_dim:q_width + 2 * head_dim]),
        load(9, wg_hbm, wg_v),
        load(10, wu_hbm, wu_v),
        load(11, wd_hbm.at[CHUNK:4 * CHUNK], wd_v.at[CHUNK:4 * CHUNK]),
        load(12, gamma_hbm, gamma_ref),
        load(13, pos_hbm, pos_ref),
        load(14, freq_hbm, freq_ref),
        load(15, wo_hbm.at[BLK:q_width], wo_v.at[BLK:q_width]),
    ]
    for i in (0, 1, 2, 15, 3, 4, 5):
        loads[i].start()

    barrier = pltpu.get_barrier_semaphore()
    for peer in peers:
        pl.semaphore_signal(barrier, inc=1, device_id=peer, device_id_type=MESH)
    for ld in loads[:3]:
        ld.wait()
    for i in (12, 6, 7, 8):
        loads[i].start()

    def remote(src, dst, send_sem, recv_sem, peer):
        return pltpu.make_async_remote_copy(src_ref=src, dst_ref=dst, send_sem=send_sem, recv_sem=recv_sem,
                                            device_id=peer, device_id_type=MESH)

    def core_copy(b):
        return remote(send.at[b], rcore.at[b], cs.at[b], cr.at[b], near)

    def x_copy(u):
        if u >= X_LAST:
            rows = pl.ds(*PIECES[u - X_LAST])
            return remote(chip.at[pl.ds(N_BLK - 2, 2), rows], rx.at[pl.ds(N_BLK - 2, 2), rows], xs.at[u], xr.at[u], across)
        if u == X_KV:
            cols = pl.ds(pl.multiple_of(ty * head_dim, head_dim), head_dim)
            return remote(chip.at[B_QKV + 2, :, cols], rx.at[B_QKV + 2, :, cols], xs.at[u], xr.at[u], across)
        start, count = X_UNITS[u]
        return remote(chip.at[pl.ds(start, count)], rx.at[pl.ds(start, count)], xs.at[u], xr.at[u], across)

    def put(b, part):
        keep[b] = part[:half]
        send[b] = part[half:].astype(BF16)
        core_copy(b).start()

    def issue_bwd(b, w_ref, row):
        put(b, mm_bt(dy_v[...], w_ref[pl.ds(row, BLK), :]))

    def issue_fwd(b, w_ref, col):
        put(b, mm(nrm_v[...], w_ref[:, pl.ds(col, BLK)]))

    def combine(b):
        core_copy(b).wait_recv()
        chip[b] = (keep[b] + rcore[b].astype(F32)).astype(BF16)

    def total(b):
        return chip[b].astype(F32) + rx[b].astype(F32)

    part = mm_bt(dy_v[...], wo_v[0:BLK, :])
    keep[0] = part[:half]
    send[0] = part[half:].astype(BF16)
    pl.semaphore_wait(barrier, len(peers))
    core_copy(0).start()
    loads[15].wait()
    issue_bwd(1, wo_v, BLK)

    def rows_of(col_a, col_b):
        lane = lax.broadcasted_iota(jnp.int32, (half, 128), 1)
        return jnp.where(lane == 0, col_a, col_b).T[0:8]

    def stats_copies(snd, got, base, to):
        return [remote(snd, got.at[i], ss.at[base + i], sr.at[base + i], peer) for i, peer in enumerate(to)]

    def stats_put(snd, col_a, col_b):
        for lo, at in ((0, mine), (half, other)):
            snd[:, pl.ds(at, half)] = rows_of(col_a[lo:lo + half], col_b[lo:lo + half])

    def stats_columns(rows_ref):
        cols = []
        for i in range(2):
            parts = [jnp.broadcast_to(rows_ref[i:i + 1, pl.ds(at, half)], (128, half)).T[:, 0:1] for at in (mine, other)]
            cols.append(jnp.concatenate(parts, axis=0))
        return cols

    loads[3].wait()
    loads[4].wait()
    for i in (9, 10, 11, 13, 14):
        loads[i].start()
    x_f = x_v[...].astype(F32)
    stats_put(st_snd, jnp.sum(x_f, axis=1, keepdims=True), jnp.sum(x_f * x_f, axis=1, keepdims=True))
    fwd_stats = stats_copies(st_snd, st_rx, 0, (near, across, far))
    for copy in fwd_stats:
        copy.start()

    combine(0)
    x_copy(0).start()
    combine(1)
    x_copy(1).start()

    loads[5].wait()
    for i in range(2):
        issue_bwd(B_DACT_LO + i, wd_v, i * BLK)
    for i in range(2):
        combine(B_DACT_LO + i)
    x_copy(2).start()

    loads[12].wait()
    for copy in fwd_stats:
        copy.wait_recv()
    st_sum[...] = (st_snd[...] + st_rx[0]) + (st_rx[1] + st_rx[2])
    sum_x, sum_xx = stats_columns(st_sum)
    tok_mean = sum_x / d_model
    inv_std = lax.rsqrt(sum_xx / d_model - tok_mean * tok_mean + EPS)
    inv_v[...] = jnp.broadcast_to(inv_std, (n_tok, 128))
    x_hat = (x_v[...].astype(F32) - tok_mean) * inv_std
    xhat_v[...] = x_hat
    nrm_v[...] = (x_hat * gamma_ref[...]).astype(BF16)

    for i in range(6, 9):
        loads[i].wait()
    for i in range(3):
        issue_fwd(B_QKV + i, wqkv_v, i * BLK)
    for i in (2, 0, 1):
        combine(B_QKV + i)
        if i == 2:
            x_copy(X_KV).start()
    x_copy(3).start()

    loads[9].wait()
    loads[10].wait()
    for k in range(4):
        def gu_issue(j, carry, k=k):
            col = pl.multiple_of(k * CHUNK + j * BLK, BLK)
            issue_fwd(B_GU + 4 * k + j, wg_v, col)
            issue_fwd(B_GU + 4 * k + 2 + j, wu_v, col)
            return carry

        def gu_combine(j, carry, k=k):
            combine(B_GU + 4 * k + j)
            return carry

        lax.fori_loop(0, 2, gu_issue, 0)
        lax.fori_loop(0, 4, gu_combine, 0)
        x_copy(4 + k).start()

    loads[11].wait()

    def hi_issue(j, carry):
        issue_bwd(B_DACT_HI + j, wd_v, pl.multiple_of(CHUNK + j * BLK, BLK))
        return carry

    lax.fori_loop(0, 6, hi_issue, 0)
    for j in range(6):
        combine(B_DACT_HI + j)
        if j == 1 or j == 3:
            x_copy(8 + j // 2).start()
    for r in range(SPLITS):
        x_copy(X_LAST + r).start()

    nrm_t[...] = nrm_v[...].T

    loads[13].wait()
    loads[14].wait()
    freq = freq_ref[...]
    for lo, at in ((0, mine), (half, other)):
        pos_col = jnp.broadcast_to(pos_ref[0:1, pl.ds(at, half)].astype(F32), (128, half)).T
        angles = pos_col * freq
        cos_v[lo:lo + half] = jnp.cos(angles)
        sin_v[lo:lo + half] = jnp.sin(angles)

    packed_copy = remote(packed.at[0:half], packed.at[half:n_tok], ps.at[0], pr.at[0], near)
    x_copy(0).wait_recv()
    x_copy(1).wait_recv()
    for j in range(2):
        packed[0:half, q_width + 512 + j * BLK:q_width + 512 + (j + 1) * BLK] = total(B_DATTN + j).astype(BF16)
    x_copy(3).wait_recv()
    cos_h, sin_h = cos_v[0:half], sin_v[0:half]
    for j in range(2):
        blk = total(B_QKV + j)
        for h in range(2):
            lo = h * head_dim
            first, second = rope(blk[:, lo:lo + 128], blk[:, lo + 128:lo + 256], cos_h, sin_h)
            packed[0:half, j * BLK + lo:j * BLK + lo + 128] = first.astype(BF16)
            packed[0:half, j * BLK + lo + 128:j * BLK + lo + 256] = second.astype(BF16)
    x_copy(X_KV).wait_recv()
    kv_cols = pl.ds(pl.multiple_of(ty * head_dim, head_dim), head_dim)
    blk = chip[B_QKV + 2, :, kv_cols].astype(F32) + rx[B_QKV + 2, :, kv_cols].astype(F32)
    first, second = rope(blk[:, 0:128], blk[:, 128:256], cos_h, sin_h)
    kv_mine = jnp.where(ty == 0, jnp.concatenate([first, second], axis=1), blk).astype(BF16)
    kv_dst = packed.at[0:half, pl.ds(pl.multiple_of(q_width + ty * head_dim, head_dim), head_dim)]
    kv_dst[...] = kv_mine
    kv_copy = remote(kv_dst, kv_dst, ts.at[3], tr.at[3], other_ty)
    kv_copy.start()
    kv_copy.wait_recv()
    packed_copy.start()
    packed_copy.wait_recv()

    row_i = lax.rem(lax.broadcasted_iota(jnp.int32, (n_tok, n_tok), 0) + core * half, n_tok)
    col_i = lax.rem(lax.broadcasted_iota(jnp.int32, (n_tok, n_tok), 1) + core * half, n_tok)
    scale = head_dim ** -0.5
    kv_acc[...] = jnp.zeros_like(kv_acc)

    def head_step(h, carry):
        cols = pl.ds(pl.multiple_of(h * head_dim, head_dim), head_dim)
        q_h = packed[:, cols]
        da_h = packed[:, pl.ds(pl.multiple_of(q_width + 512 + h * head_dim, head_dim), head_dim)]
        k_rot = packed[:, q_width:q_width + 256]
        v_val = packed[:, q_width + 256:q_width + 512]
        scores = jnp.where(row_i >= col_i, mm_bt(q_h, k_rot) * scale, -1e30)
        exps = jnp.exp(scores - jnp.max(scores, axis=1, keepdims=True))
        probs_f = exps / jnp.sum(exps, axis=1, keepdims=True)
        probs = probs_f.astype(BF16)
        attn_v[:, cols] = mm(probs, v_val).astype(BF16)
        d_probs = mm_bt(da_h, v_val).astype(BF16).astype(F32)
        d_scores = (probs_f * (d_probs - jnp.sum(d_probs * probs_f, axis=1, keepdims=True)) * scale).astype(BF16)
        dq_h = mm(d_scores, k_rot).astype(BF16).astype(F32)
        first, second = rope(dq_h[:, 0:128], dq_h[:, 128:256], cos_v[...], -sin_v[...])
        dq_v[:, pl.ds(pl.multiple_of(h * head_dim, head_dim), 128)] = first.astype(BF16)
        dq_v[:, pl.ds(pl.multiple_of(h * head_dim + 128, 128), 128)] = second.astype(BF16)
        kv_acc[:, 0:256] += mm_at(d_scores, q_h)
        kv_acc[:, 256:512] += mm_at(probs, da_h)
        return carry

    lax.fori_loop(0, heads, head_step, 0)
    dkv_part[...] = kv_acc[...].astype(BF16)
    dkv_copy = remote(dkv_part, dkv_rx, ts.at[0], tr.at[0], other_ty)
    dkv_copy.start()
    br_v[...] = mm(attn_v[...], wo_v[...])
    dh_v[...] = mm_bt(dq_v[...], wqkv_v[:, 0:q_width])

    for j in range(2):
        tiles[j] = mm(nrm_t[...], dq_v[:, j * BLK:(j + 1) * BLK])
        tiles[2 + j] = mm_at(attn_v[:, j * BLK:(j + 1) * BLK], dy_v[...])

    def piece_copy(r):
        lo, size = PIECES[r]
        return remote(md.at[3, 1:3, lo:lo + size], md.at[3, 1:3, half + lo:half + lo + size], gs.at[12 + r], gr.at[12 + r], near)

    def gather_copy(k, i):
        return remote(md.at[k, i, 0:half], md.at[k, i, half:n_tok], gs.at[3 * k + i], gr.at[3 * k + i], near)

    def dact_block(k, j):
        return B_DACT_LO + j if k == 0 else B_DACT_HI + 2 * (k - 1) + j

    def gated(k, want_act, want_grad):
        def step(r, carry):
            rows = pl.ds(pl.multiple_of(r * 16, 16), 16)
            for j in range(2):
                bg, bu, bd = B_GU + 4 * k + j, B_GU + 4 * k + 2 + j, dact_block(k, j)
                gate = (chip[bg, rows].astype(F32) + rx[bg, rows].astype(F32)).astype(BF16).astype(F32)
                up = (chip[bu, rows].astype(F32) + rx[bu, rows].astype(F32)).astype(BF16).astype(F32)
                sig = jax.nn.sigmoid(gate)
                silu = gate * sig
                cols = slice(j * BLK, (j + 1) * BLK)
                if want_act:
                    md[k, 0, rows, cols] = (silu * up).astype(BF16)
                if k == 3:
                    factors[0, rows, cols] = up * sig * (1.0 + gate * (1.0 - sig))
                    factors[1, rows, cols] = silu
                if want_grad:
                    d_act = (chip[bd, rows].astype(F32) + rx[bd, rows].astype(F32)).astype(BF16).astype(F32)
                    md[k, 1, rows, cols] = (d_act * up * sig * (1.0 + gate * (1.0 - sig))).astype(BF16)
                    md[k, 2, rows, cols] = (d_act * silu).astype(BF16)
            return carry

        lax.fori_loop(0, half // 16, step, 0)
        for i in ((0,) if want_act else ()) + ((1, 2) if want_grad else ()):
            gather_copy(k, i).start()

    def use_act(k):
        gather_copy(k, 0).wait_recv()
        br_v[...] += mm(md[k, 0], wd_v[k * CHUNK:(k + 1) * CHUNK, :])

    def use_grad(k):
        for i in (1, 2):
            gather_copy(k, i).wait_recv()
        dh_v[...] += (mm_bt(md[k, 1], wg_v[:, k * CHUNK:(k + 1) * CHUNK])
                      + mm_bt(md[k, 2], wu_v[:, k * CHUNK:(k + 1) * CHUNK]))

    x_copy(2).wait_recv()
    for k in range(4):
        x_copy(4 + k).wait_recv()
        gated(k, True, k == 0)
        use_act(k)
        if k == 0:
            use_grad(0)
            dkv_copy.wait_recv()
            d_k = dkv_part[:, 0:256].astype(F32) + dkv_rx[:, 0:256].astype(F32)
            d_k = d_k.astype(BF16).astype(F32)
            first, second = rope(d_k[:, 0:128], d_k[:, 128:256], cos_v[...], -sin_v[...])
            dkv_v[:, 0:128] = first.astype(BF16)
            dkv_v[:, 128:256] = second.astype(BF16)
            dkv_v[:, 256:512] = (dkv_part[:, 256:512].astype(F32) + dkv_rx[:, 256:512].astype(F32)).astype(BF16)
            dh_v[...] += 0.5 * mm_bt(dkv_v[...], wqkv_v[:, q_width:q_width + 512])
            tiles[4] = mm(nrm_t[...], dkv_v[...])
            for j in range(2):
                tiles[5 + j] = mm_at(md[0, 0, :, j * BLK:(j + 1) * BLK], dy_v[...])
    y_snd[...] = br_v[...].astype(BF16)
    y_copy = remote(y_snd, y_rx, ts.at[1], tr.at[1], other_ty)
    y_copy.start()
    x_copy(8).wait_recv()
    gated(1, False, True)
    use_grad(1)
    x_copy(9).wait_recv()
    gated(2, False, True)

    def dh_copy(r):
        at = pl.ds(2 * PIECES[r][0], 2 * PIECES[r][1])
        return remote(dh_snd.at[at], dh_rx.at[at], ds.at[r], dr.at[r], other_ty)

    def both(ref, r):
        lo, size = PIECES[r]
        return jnp.concatenate([ref[lo:lo + size], ref[half + lo:half + lo + size]], axis=0)

    sums = []

    def piece_grad(r):
        x_copy(X_LAST + r).wait_recv()
        rows = slice(PIECES[r][0], PIECES[r][0] + PIECES[r][1])
        for j in range(2):
            cols = slice(j * BLK, (j + 1) * BLK)
            b = dact_block(3, j)
            d_act = (chip[b, rows].astype(F32) + rx[b, rows].astype(F32)).astype(BF16).astype(F32)
            for i in range(2):
                md[3, 1 + i, rows, cols] = (d_act * factors[i, rows, cols]).astype(BF16)
        piece_copy(r).start()

    def piece_dh(r):
        piece_copy(r).wait_recv()
        part = both(dh_v, r) + mm_bt(both(md.at[3, 1], r), wg_v[:, 3 * CHUNK:4 * CHUNK]) + mm_bt(both(md.at[3, 2], r), wu_v[:, 3 * CHUNK:4 * CHUNK])
        part_b = part.astype(BF16)
        dh_snd[2 * PIECES[r][0]:2 * (PIECES[r][0] + PIECES[r][1])] = part_b
        dh_copy(r).start()
        d_hat = part_b.astype(F32) * gamma_ref[...]
        sums.append((jnp.sum(d_hat, axis=1, keepdims=True), jnp.sum(d_hat * both(xhat_v, r), axis=1, keepdims=True)))

    piece_grad(0)
    use_grad(2)
    for r in range(1, SPLITS):
        piece_grad(r)
        piece_dh(r - 1)
    piece_dh(SPLITS - 1)
    cols = [jnp.concatenate([sums[r][i][:PIECES[r][1]] for r in range(SPLITS)] + [sums[r][i][PIECES[r][1]:] for r in range(SPLITS)], axis=0) for i in range(2)]
    stats_put(bst_snd, cols[0], cols[1])
    bwd_stats = stats_copies(bst_snd, bst_rx, 3, peers)
    for copy in bwd_stats:
        copy.start()

    y_copy.wait_recv()
    y_o[...] = (x_v[...].astype(F32) + (y_snd[...].astype(F32) + y_rx[...].astype(F32))).astype(BF16)

    def drain(b, carry):
        core_copy(b).wait_send()
        return carry

    lax.fori_loop(0, N_BLK, drain, 0)
    for u in range(N_X):
        x_copy(u).wait_send()
    for k in range(4):
        for i in range(3 if k < 3 else 1):
            gather_copy(k, i).wait_send()
    for r in range(SPLITS):
        piece_copy(r).wait_send()
    for copy in [packed_copy, dkv_copy, y_copy, kv_copy] + fwd_stats:
        copy.wait_send()

    d_gamma = jnp.zeros_like(dgamma_ref)
    for r in range(SPLITS):
        dh_copy(r).wait_recv()
        lo, size = PIECES[r]
        d_nrm = dh_snd[2 * lo:2 * (lo + size)].astype(F32) + dh_rx[2 * lo:2 * (lo + size)].astype(F32)
        d_gamma = d_gamma + jnp.sum(d_nrm * both(xhat_v, r), axis=0, keepdims=True)
        dh_v[lo:lo + size] = d_nrm[:size]
        dh_v[half + lo:half + lo + size] = d_nrm[size:]
    dgamma_ref[...] = d_gamma
    for copy in bwd_stats:
        copy.wait_recv()
    st_sum[...] = ((bst_snd[...] + bst_rx[0]) + (bst_rx[1] + bst_rx[2])) + ((bst_rx[3] + bst_rx[4]) + (bst_rx[5] + bst_rx[6]))
    sum_d, sum_dx = stats_columns(st_sum)
    d_hat = dh_v[...] * gamma_ref[...]
    d_x = dy_v[...].astype(F32) + inv_v[:, 0:1] * (d_hat - sum_d / d_model - xhat_v[...] * (sum_dx / d_model))
    dx_o[...] = d_x.astype(BF16)

    for r in range(SPLITS):
        dh_copy(r).wait_send()
    for copy in bwd_stats:
        copy.wait_send()


def grad_kernel(y_v, dx_v, dgamma_in, nrm_t, attn_v, md, dq_v, dkv_v, dy_v, tiles,
                y_hbm, dx_hbm, dgamma_hbm, dwq_hbm, dwg_hbm, dwu_hbm, dwk_hbm, dwv_hbm, dwo_hbm, dwd_hbm,
                ring, wide, out_sem, cp_sem):
    width, n_tok = nrm_t.shape
    half = n_tok // 2
    core = lax.rem(lax.axis_index('tx'), 2)
    mine = pl.multiple_of(core * half, half)
    other = pl.multiple_of((1 - core) * half, half)
    hand_out = [pltpu.make_async_copy(src.at[lo:lo + half], dst.at[pl.ds(at, half)], cp_sem.at[i])
                for i, (src, dst, lo, at) in enumerate(((y_v, y_hbm, 0, mine), (y_v, y_hbm, half, other), (dx_v, dx_hbm, 0, mine), (dx_v, dx_hbm, half, other)))]
    for cp in hand_out:
        cp.start()
    hand_out.append(pltpu.make_async_copy(dgamma_in, dgamma_hbm, cp_sem.at[12]))
    hand_out[-1].start()

    ready = [(0, dwq_hbm.at[:, 0:BLK]), (1, dwq_hbm.at[:, BLK:2 * BLK]), (2, dwo_hbm.at[0:BLK, :]), (3, dwo_hbm.at[BLK:2 * BLK, :]),
             (5, dwd_hbm.at[0:BLK, :]), (6, dwd_hbm.at[BLK:2 * BLK, :])]
    ready = [(tiles.at[i], dst) for i, dst in ready] + [(tiles.at[4, :, 0:256], dwk_hbm), (tiles.at[4, :, 256:512], dwv_hbm)]
    for i, (src, dst) in enumerate(ready):
        hand_out.append(pltpu.make_async_copy(src, dst, cp_sem.at[4 + i]))
        hand_out[-1].start()

    def put(src, dst, i):
        hand_out.append(pltpu.make_async_copy(src, dst, out_sem.at[i]))
        hand_out[-1].start()

    for t in range(6):
        k, j = 1 + t // 2, t % 2
        ring[t] = mm_at(md[k, 0, :, j * BLK:(j + 1) * BLK], dy_v[...])
        put(ring.at[t], dwd_hbm.at[k * CHUNK + j * BLK:k * CHUNK + (j + 1) * BLK, :], t)
    n_row = 128
    for i, (out, at) in enumerate(((dwg_hbm, 6), (dwu_hbm, 10))):
        for k in range(4):
            for j in range(2):
                lo = k * CHUNK + j * BLK
                wide[i, :, lo:lo + BLK] = mm(nrm_t[...], md[k, 1 + i, :, j * BLK:(j + 1) * BLK])
        for r in range(width // n_row):
            put(wide.at[i, r * n_row:(r + 1) * n_row], out.at[r * n_row:(r + 1) * n_row], at + r)
    for cp in hand_out:
        cp.wait()


def solution(mesh):
    tx_size = mesh.shape['tx']
    tok_spec = P('dp', None, 'tx')
    in_specs = (tok_spec, P('dp', None), tok_spec, P('tx'), P('tx', 'ty'), P('tx', 'ty'), P('tx', 'ty'),
                P('tx', None), P('tx', None), P('ty', 'tx'), P('ty', 'tx'))
    out_specs = (tok_spec, tok_spec, P(('dp', 'tx')), P(('dp', 'tx'), 'ty'), P(('dp', 'tx'), 'ty'), P(('dp', 'tx'), 'ty'),
                 P(('dp', 'tx'), None), P(('dp', 'tx'), None), P(('dp', 'ty'), 'tx'), P(('dp', 'ty'), 'tx'))

    def local_layer(x_in, positions, d_y, ln_gamma, w_q, w_g, w_u, w_k, w_v, w_o, w_d):
        _, n_tok, d_local = x_in.shape
        half = n_tok // 2
        d_model = d_local * tx_size
        head_dim = w_k.shape[1]
        q_width = w_q.shape[1]
        d_ff = w_g.shape[1]
        freq = jnp.asarray((ROPE_BASE ** (-2.0 * np.arange(head_dim // 2) / head_dim)).astype(np.float32)[None])
        any_spec = pl.BlockSpec(memory_space=pl.ANY)
        vmem_spec = pl.BlockSpec(memory_space=pltpu.VMEM)
        tok = (n_tok, d_local)
        sem = pltpu.SemaphoreType.DMA
        vm = pltpu.VMEM
        kept = pl.pallas_call(
            functools.partial(layer_kernel, d_model),
            out_shape=[vm(tok, BF16), vm(tok, BF16), vm((1, d_local), F32), vm((d_local, n_tok), BF16), vm((n_tok, q_width), BF16),
                       vm((4, 3, n_tok, CHUNK), BF16), vm((n_tok, q_width), BF16), vm((n_tok, 2 * head_dim), BF16), vm(tok, BF16),
                       vm((7, BLK, BLK), F32)],
            in_specs=[any_spec] * 12,
            out_specs=[vmem_spec] * 10,
            scratch_shapes=[
                vm((1, n_tok), jnp.int32), vm((1, head_dim // 2), F32), vm((1, d_local), F32), vm(tok, BF16),
                vm(tok, BF16), vm((d_local, q_width + 2 * head_dim), BF16), vm((d_local, d_ff), BF16), vm((d_local, d_ff), BF16),
                vm((q_width, d_local), BF16), vm((d_ff, d_local), BF16),
                vm((N_BLK, half, BLK), F32), vm((N_BLK, half, BLK), BF16), vm((N_BLK, half, BLK), BF16),
                vm((N_BLK, half, BLK), BF16), vm((N_BLK, half, BLK), BF16), vm((n_tok, 2 * q_width + 2 * head_dim), BF16),
                vm((n_tok, 512), BF16), vm((n_tok, 512), BF16), vm((n_tok, 512), F32),
                vm(tok, F32), vm((n_tok, 128), F32), vm((n_tok, 128), F32), vm((n_tok, 128), F32), vm(tok, F32), vm(tok, F32),
                vm(tok, BF16), vm(tok, BF16), vm(tok, BF16), vm(tok, BF16),
                vm((8, n_tok), F32), vm((3, 8, n_tok), F32), vm((8, n_tok), F32), vm((8, n_tok), F32), vm((7, 8, n_tok), F32), vm((2, half, CHUNK), F32),
                sem((16,)), sem((N_BLK,)), sem((N_BLK,)), sem((N_X,)), sem((N_X,)),
                sem((12 + SPLITS,)), sem((12 + SPLITS,)), sem((1,)), sem((1,)), sem((4,)), sem((4,)), sem((10,)), sem((10,)),
                sem((SPLITS,)), sem((SPLITS,))],
            compiler_params=pltpu.CompilerParams(collective_id=0, has_side_effects=True, vmem_limit_bytes=46 * 1024 * 1024),
            name='layer',
        )(x_in.reshape(tok), positions, freq, d_y.reshape(tok), ln_gamma[None], w_q, w_g, w_u, w_k, w_v, w_o, w_d)

        y_out, d_x, d_gamma, d_wq, d_wg, d_wu, d_wk, d_wv, d_wo, d_wd = pl.pallas_call(
            grad_kernel,
            out_shape=[jax.ShapeDtypeStruct(tok, BF16), jax.ShapeDtypeStruct(tok, BF16), jax.ShapeDtypeStruct((1, d_local), F32)]
            + [jax.ShapeDtypeStruct(w.shape, F32) for w in (w_q, w_g, w_u, w_k, w_v, w_o, w_d)],
            in_specs=[vmem_spec] * 10,
            out_specs=[any_spec] * 10,
            scratch_shapes=[vm((6, d_local, BLK), F32), vm((2, d_local, d_ff), F32), sem((14,)), sem((13,))],
            compiler_params=pltpu.CompilerParams(vmem_limit_bytes=30 * 1024 * 1024),
            name='weight_grads',
        )(*kept)
        return (y_out.reshape(x_in.shape), d_x.reshape(x_in.shape), d_gamma.reshape(d_local),
                d_wq, d_wg, d_wu, d_wk, d_wv, d_wo, d_wd)

    return jax.shard_map(local_layer, mesh=mesh, in_specs=in_specs, out_specs=out_specs, check_vma=False)
```

```python
import functools

import jax
import jax.numpy as jnp
import numpy as np
from jax import lax
from jax.experimental import pallas as pl
from jax.experimental.pallas import tpu as pltpu
from jax.sharding import PartitionSpec as P

EPS = 1e-6
ROPE_BASE = 10000.0
F32 = jnp.float32
BF16 = jnp.bfloat16
MESH = pl.DeviceIdType.MESH

BLK = 512
CHUNK = 1024
B_DATTN, B_DACT_LO, B_QKV, B_GU, B_DACT_HI, N_BLK = 0, 2, 4, 7, 23, 29
X_UNITS = ((0, 1), (1, 1), (2, 2), (4, 2), (7, 4), (11, 4), (15, 4), (19, 4), (23, 2), (25, 2))
PIECES = ((0, 16), (16, 32), (48, 32), (80, 32), (112, 16))
SPLITS = len(PIECES)
EARLY = 128
X_KV = len(X_UNITS)
X_LAST = X_KV + 1
N_X = X_LAST + SPLITS


def dot(a, b, dims):
    return lax.dot_general(a, b, (dims, ((), ())), preferred_element_type=F32)


def mm(a, b):
    return dot(a, b, ((1,), (0,)))


def mm_bt(a, b):
    return dot(a, b, ((1,), (1,)))


def mm_at(a, b):
    return dot(a, b, ((0,), (0,)))


def rope(first, second, cos_t, sin_t):
    return first * cos_t - second * sin_t, second * cos_t + first * sin_t


def layer_kernel(d_model, x_hbm, pos_hbm, freq_hbm, dy_hbm, gamma_hbm, wq_hbm, wg_hbm, wu_hbm, wk_hbm, wv_hbm, wo_hbm, wd_hbm,
                 y_o, dx_o, dgamma_ref, nrm_t, attn_v, md, dq_v, dkv_v, dy_v, tiles,
                 pos_ref, freq_ref, gamma_ref, nrm_v, x_v, wqkv_v, wg_v, wu_v, wo_v, wd_v,
                 keep, send, rcore, chip, rx, packed, dkv_part, dkv_rx, kv_acc,
                 xhat_v, inv_v, cos_v, sin_v, br_v, dh_v, y_snd, y_rx, dh_snd, dh_rx,
                 st_snd, st_rx, st_sum, bst_snd, bst_rx, factors,
                 ld_sem, cs, cr, xs, xr, gs, gr, ps, pr, ts, tr, ss, sr, ds, dr, early_snd, early_rx, es, er):
    tx = lax.axis_index('tx')
    ty = lax.axis_index('ty')
    core = lax.rem(tx, 2)
    near = {'tx': tx + 1 - 2 * core}
    across = {'tx': lax.rem(tx + 2, 4)}
    far = {'tx': lax.rem(tx + 1 - 2 * core + 2, 4)}
    other_ty = {'ty': 1 - ty}
    peers = [near, across, far, other_ty] + [{'tx': p['tx'], 'ty': 1 - ty} for p in (near, across, far)]
    n_tok = x_v.shape[0]
    half = n_tok // 2
    mine = pl.multiple_of(core * half, half)
    other = pl.multiple_of((1 - core) * half, half)
    head_dim = 256
    q_width = wo_v.shape[0]
    heads = q_width // head_dim

    def load(i, src, dst):
        return pltpu.make_async_copy(src, dst, ld_sem.at[i])

    loads = [
        load(0, dy_hbm.at[pl.ds(mine, half)], dy_v.at[0:half]),
        load(1, dy_hbm.at[pl.ds(other, half)], dy_v.at[half:n_tok]),
        load(2, wo_hbm.at[0:BLK], wo_v.at[0:BLK]),
        load(3, x_hbm.at[pl.ds(mine, half)], x_v.at[0:half]),
        load(4, x_hbm.at[pl.ds(other, half)], x_v.at[half:n_tok]),
        load(5, wd_hbm.at[0:CHUNK], wd_v.at[0:CHUNK]),
        load(6, wq_hbm, wqkv_v.at[:, 0:q_width]),
        load(7, wk_hbm, wqkv_v.at[:, q_width:q_width + head_dim]),
        load(8, wv_hbm, wqkv_v.at[:, q_width + head_dim:q_width + 2 * head_dim]),
        load(9, wg_hbm, wg_v),
        load(10, wu_hbm, wu_v),
        load(11, wd_hbm.at[CHUNK:4 * CHUNK], wd_v.at[CHUNK:4 * CHUNK]),
        load(12, gamma_hbm, gamma_ref),
        load(13, pos_hbm, pos_ref),
        load(14, freq_hbm, freq_ref),
        load(15, wo_hbm.at[BLK:q_width], wo_v.at[BLK:q_width]),
    ]
    for i in (0, 1, 2, 15, 3, 4, 5):
        loads[i].start()

    barrier = pltpu.get_barrier_semaphore()
    for peer in peers:
        pl.semaphore_signal(barrier, inc=1, device_id=peer, device_id_type=MESH)
    for ld in loads[:3]:
        ld.wait()
    for i in (12, 6, 7, 8):
        loads[i].start()

    def remote(src, dst, send_sem, recv_sem, peer):
        return pltpu.make_async_remote_copy(src_ref=src, dst_ref=dst, send_sem=send_sem, recv_sem=recv_sem,
                                            device_id=peer, device_id_type=MESH)

    def core_copy(b):
        return remote(send.at[b], rcore.at[b], cs.at[b], cr.at[b], near)

    def x_copy(u):
        if u >= X_LAST:
            rows = pl.ds(*PIECES[u - X_LAST])
            return remote(chip.at[pl.ds(N_BLK - 2, 2), rows], rx.at[pl.ds(N_BLK - 2, 2), rows], xs.at[u], xr.at[u], across)
        if u == X_KV:
            cols = pl.ds(pl.multiple_of(ty * head_dim, head_dim), head_dim)
            return remote(chip.at[B_QKV + 2, :, cols], rx.at[B_QKV + 2, :, cols], xs.at[u], xr.at[u], across)
        if u == 0:
            return remote(chip.at[0, :, EARLY:BLK], rx.at[0, :, EARLY:BLK], xs.at[u], xr.at[u], across)
        start, count = X_UNITS[u]
        return remote(chip.at[pl.ds(start, count)], rx.at[pl.ds(start, count)], xs.at[u], xr.at[u], across)

    def put(b, part):
        keep[b] = part[:half]
        send[b] = part[half:].astype(BF16)
        core_copy(b).start()

    def issue_bwd(b, w_ref, row):
        put(b, mm_bt(dy_v[...], w_ref[pl.ds(row, BLK), :]))

    def issue_fwd(b, w_ref, col):
        put(b, mm(nrm_v[...], w_ref[:, pl.ds(col, BLK)]))

    def combine(b):
        core_copy(b).wait_recv()
        chip[b] = (keep[b] + rcore[b].astype(F32)).astype(BF16)

    def total(b):
        return chip[b].astype(F32) + rx[b].astype(F32)

    part = mm_bt(dy_v[...], wo_v[0:BLK, :])
    keep[0] = part[:half]
    send[0] = part[half:].astype(BF16)
    early_snd[...] = part[:, 0:EARLY].astype(BF16)
    pl.semaphore_wait(barrier, len(peers))
    early = [remote(early_snd.at[0:half], early_rx.at[0], es.at[0], er.at[0], across),
             remote(early_snd.at[half:n_tok], early_rx.at[1], es.at[1], er.at[1], far)]
    core_copy(0).start()
    for copy in early:
        copy.start()
    loads[15].wait()
    issue_bwd(1, wo_v, BLK)

    def rows_of(col_a, col_b):
        lane = lax.broadcasted_iota(jnp.int32, (half, 128), 1)
        return jnp.where(lane == 0, col_a, col_b).T[0:8]

    def stats_copies(snd, got, base, to):
        return [remote(snd, got.at[i], ss.at[base + i], sr.at[base + i], peer) for i, peer in enumerate(to)]

    def stats_put(snd, col_a, col_b):
        for lo, at in ((0, mine), (half, other)):
            snd[:, pl.ds(at, half)] = rows_of(col_a[lo:lo + half], col_b[lo:lo + half])

    def stats_columns(rows_ref):
        cols = []
        for i in range(2):
            parts = [jnp.broadcast_to(rows_ref[i:i + 1, pl.ds(at, half)], (128, half)).T[:, 0:1] for at in (mine, other)]
            cols.append(jnp.concatenate(parts, axis=0))
        return cols

    loads[3].wait()
    loads[4].wait()
    for i in (9, 10, 11, 13, 14):
        loads[i].start()
    x_f = x_v[...].astype(F32)
    stats_put(st_snd, jnp.sum(x_f, axis=1, keepdims=True), jnp.sum(x_f * x_f, axis=1, keepdims=True))
    fwd_stats = stats_copies(st_snd, st_rx, 0, (near, across, far))
    for copy in fwd_stats:
        copy.start()

    combine(0)
    x_copy(0).start()
    combine(1)
    x_copy(1).start()

    loads[5].wait()
    for i in range(2):
        issue_bwd(B_DACT_LO + i, wd_v, i * BLK)
    for i in range(2):
        combine(B_DACT_LO + i)
    x_copy(2).start()

    loads[12].wait()
    for copy in fwd_stats:
        copy.wait_recv()
    st_sum[...] = (st_snd[...] + st_rx[0]) + (st_rx[1] + st_rx[2])
    sum_x, sum_xx = stats_columns(st_sum)
    tok_mean = sum_x / d_model
    inv_std = lax.rsqrt(sum_xx / d_model - tok_mean * tok_mean + EPS)
    inv_v[...] = jnp.broadcast_to(inv_std, (n_tok, 128))
    x_hat = (x_v[...].astype(F32) - tok_mean) * inv_std
    xhat_v[...] = x_hat
    nrm_v[...] = (x_hat * gamma_ref[...]).astype(BF16)

    for i in range(6, 9):
        loads[i].wait()
    for i in range(3):
        issue_fwd(B_QKV + i, wqkv_v, i * BLK)
    for i in (2, 0, 1):
        combine(B_QKV + i)
        if i == 2:
            x_copy(X_KV).start()
    x_copy(3).start()

    loads[9].wait()
    loads[10].wait()
    for k in range(4):
        def gu_issue(j, carry, k=k):
            col = pl.multiple_of(k * CHUNK + j * BLK, BLK)
            issue_fwd(B_GU + 4 * k + j, wg_v, col)
            issue_fwd(B_GU + 4 * k + 2 + j, wu_v, col)
            return carry

        def gu_combine(j, carry, k=k):
            combine(B_GU + 4 * k + j)
            return carry

        lax.fori_loop(0, 2, gu_issue, 0)
        lax.fori_loop(0, 4, gu_combine, 0)
        x_copy(4 + k).start()

    loads[11].wait()

    def hi_issue(j, carry):
        issue_bwd(B_DACT_HI + j, wd_v, pl.multiple_of(CHUNK + j * BLK, BLK))
        return carry

    lax.fori_loop(0, 6, hi_issue, 0)
    for j in range(6):
        combine(B_DACT_HI + j)
        if j == 1 or j == 3:
            x_copy(8 + j // 2).start()
    for r in range(SPLITS):
        x_copy(X_LAST + r).start()

    nrm_t[...] = nrm_v[...].T

    loads[13].wait()
    loads[14].wait()
    freq = freq_ref[...]
    for lo, at in ((0, mine), (half, other)):
        pos_col = jnp.broadcast_to(pos_ref[0:1, pl.ds(at, half)].astype(F32), (128, half)).T
        angles = pos_col * freq
        cos_v[lo:lo + half] = jnp.cos(angles)
        sin_v[lo:lo + half] = jnp.sin(angles)

    packed_copy = remote(packed.at[0:half], packed.at[half:n_tok], ps.at[0], pr.at[0], near)
    x_copy(0).wait_recv()
    x_copy(1).wait_recv()
    for copy in early:
        copy.wait_recv()
    rx[0, :, 0:EARLY] = (early_rx[0].astype(F32) + early_rx[1].astype(F32)).astype(BF16)
    for j in range(2):
        packed[0:half, q_width + 512 + j * BLK:q_width + 512 + (j + 1) * BLK] = total(B_DATTN + j).astype(BF16)
    x_copy(3).wait_recv()
    cos_h, sin_h = cos_v[0:half], sin_v[0:half]
    for j in range(2):
        blk = total(B_QKV + j)
        for h in range(2):
            lo = h * head_dim
            first, second = rope(blk[:, lo:lo + 128], blk[:, lo + 128:lo + 256], cos_h, sin_h)
            packed[0:half, j * BLK + lo:j * BLK + lo + 128] = first.astype(BF16)
            packed[0:half, j * BLK + lo + 128:j * BLK + lo + 256] = second.astype(BF16)
    x_copy(X_KV).wait_recv()
    kv_cols = pl.ds(pl.multiple_of(ty * head_dim, head_dim), head_dim)
    blk = chip[B_QKV + 2, :, kv_cols].astype(F32) + rx[B_QKV + 2, :, kv_cols].astype(F32)
    first, second = rope(blk[:, 0:128], blk[:, 128:256], cos_h, sin_h)
    kv_mine = jnp.where(ty == 0, jnp.concatenate([first, second], axis=1), blk).astype(BF16)
    kv_dst = packed.at[0:half, pl.ds(pl.multiple_of(q_width + ty * head_dim, head_dim), head_dim)]
    kv_dst[...] = kv_mine
    kv_copy = remote(kv_dst, kv_dst, ts.at[3], tr.at[3], other_ty)
    kv_copy.start()
    kv_copy.wait_recv()
    packed_copy.start()
    packed_copy.wait_recv()

    row_i = lax.rem(lax.broadcasted_iota(jnp.int32, (n_tok, n_tok), 0) + core * half, n_tok)
    col_i = lax.rem(lax.broadcasted_iota(jnp.int32, (n_tok, n_tok), 1) + core * half, n_tok)
    scale = head_dim ** -0.5
    kv_acc[...] = jnp.zeros_like(kv_acc)

    def head_step(h, carry):
        cols = pl.ds(pl.multiple_of(h * head_dim, head_dim), head_dim)
        q_h = packed[:, cols]
        da_h = packed[:, pl.ds(pl.multiple_of(q_width + 512 + h * head_dim, head_dim), head_dim)]
        k_rot = packed[:, q_width:q_width + 256]
        v_val = packed[:, q_width + 256:q_width + 512]
        scores = jnp.where(row_i >= col_i, mm_bt(q_h, k_rot) * scale, -1e30)
        exps = jnp.exp(scores - jnp.max(scores, axis=1, keepdims=True))
        probs_f = exps / jnp.sum(exps, axis=1, keepdims=True)
        probs = probs_f.astype(BF16)
        attn_v[:, cols] = mm(probs, v_val).astype(BF16)
        d_probs = mm_bt(da_h, v_val).astype(BF16).astype(F32)
        d_scores = (probs_f * (d_probs - jnp.sum(d_probs * probs_f, axis=1, keepdims=True)) * scale).astype(BF16)
        dq_h = mm(d_scores, k_rot).astype(BF16).astype(F32)
        first, second = rope(dq_h[:, 0:128], dq_h[:, 128:256], cos_v[...], -sin_v[...])
        dq_v[:, pl.ds(pl.multiple_of(h * head_dim, head_dim), 128)] = first.astype(BF16)
        dq_v[:, pl.ds(pl.multiple_of(h * head_dim + 128, 128), 128)] = second.astype(BF16)
        kv_acc[:, 0:256] += mm_at(d_scores, q_h)
        kv_acc[:, 256:512] += mm_at(probs, da_h)
        return carry

    lax.fori_loop(0, heads, head_step, 0)
    dkv_part[...] = kv_acc[...].astype(BF16)
    dkv_copy = remote(dkv_part, dkv_rx, ts.at[0], tr.at[0], other_ty)
    dkv_copy.start()
    br_v[...] = mm(attn_v[...], wo_v[...])
    dh_v[...] = mm_bt(dq_v[...], wqkv_v[:, 0:q_width])

    for j in range(2):
        tiles[j] = mm(nrm_t[...], dq_v[:, j * BLK:(j + 1) * BLK])
        tiles[2 + j] = mm_at(attn_v[:, j * BLK:(j + 1) * BLK], dy_v[...])

    def piece_copy(r):
        lo, size = PIECES[r]
        return remote(md.at[3, 1:3, lo:lo + size], md.at[3, 1:3, half + lo:half + lo + size], gs.at[12 + r], gr.at[12 + r], near)

    def gather_copy(k, i):
        return remote(md.at[k, i, 0:half], md.at[k, i, half:n_tok], gs.at[3 * k + i], gr.at[3 * k + i], near)

    def dact_block(k, j):
        return B_DACT_LO + j if k == 0 else B_DACT_HI + 2 * (k - 1) + j

    def gated(k, want_act, want_grad):
        def step(r, carry):
            rows = pl.ds(pl.multiple_of(r * 16, 16), 16)
            for j in range(2):
                bg, bu, bd = B_GU + 4 * k + j, B_GU + 4 * k + 2 + j, dact_block(k, j)
                gate = (chip[bg, rows].astype(F32) + rx[bg, rows].astype(F32)).astype(BF16).astype(F32)
                up = (chip[bu, rows].astype(F32) + rx[bu, rows].astype(F32)).astype(BF16).astype(F32)
                sig = jax.nn.sigmoid(gate)
                silu = gate * sig
                cols = slice(j * BLK, (j + 1) * BLK)
                if want_act:
                    md[k, 0, rows, cols] = (silu * up).astype(BF16)
                if k == 3:
                    factors[0, rows, cols] = up * sig * (1.0 + gate * (1.0 - sig))
                    factors[1, rows, cols] = silu
                if want_grad:
                    d_act = (chip[bd, rows].astype(F32) + rx[bd, rows].astype(F32)).astype(BF16).astype(F32)
                    md[k, 1, rows, cols] = (d_act * up * sig * (1.0 + gate * (1.0 - sig))).astype(BF16)
                    md[k, 2, rows, cols] = (d_act * silu).astype(BF16)
            return carry

        lax.fori_loop(0, half // 16, step, 0)
        for i in ((0,) if want_act else ()) + ((1, 2) if want_grad else ()):
            gather_copy(k, i).start()

    def use_act(k):
        gather_copy(k, 0).wait_recv()
        br_v[...] += mm(md[k, 0], wd_v[k * CHUNK:(k + 1) * CHUNK, :])

    def use_grad(k):
        for i in (1, 2):
            gather_copy(k, i).wait_recv()
        dh_v[...] += (mm_bt(md[k, 1], wg_v[:, k * CHUNK:(k + 1) * CHUNK])
                      + mm_bt(md[k, 2], wu_v[:, k * CHUNK:(k + 1) * CHUNK]))

    x_copy(2).wait_recv()
    for k in range(4):
        x_copy(4 + k).wait_recv()
        gated(k, True, k == 0)
        use_act(k)
        if k == 0:
            use_grad(0)
            dkv_copy.wait_recv()
            d_k = dkv_part[:, 0:256].astype(F32) + dkv_rx[:, 0:256].astype(F32)
            d_k = d_k.astype(BF16).astype(F32)
            first, second = rope(d_k[:, 0:128], d_k[:, 128:256], cos_v[...], -sin_v[...])
            dkv_v[:, 0:128] = first.astype(BF16)
            dkv_v[:, 128:256] = second.astype(BF16)
            dkv_v[:, 256:512] = (dkv_part[:, 256:512].astype(F32) + dkv_rx[:, 256:512].astype(F32)).astype(BF16)
            dh_v[...] += 0.5 * mm_bt(dkv_v[...], wqkv_v[:, q_width:q_width + 512])
            tiles[4] = mm(nrm_t[...], dkv_v[...])
            for j in range(2):
                tiles[5 + j] = mm_at(md[0, 0, :, j * BLK:(j + 1) * BLK], dy_v[...])
    y_snd[...] = br_v[...].astype(BF16)
    y_copy = remote(y_snd, y_rx, ts.at[1], tr.at[1], other_ty)
    y_copy.start()
    x_copy(8).wait_recv()
    gated(1, False, True)
    use_grad(1)
    x_copy(9).wait_recv()
    gated(2, False, True)

    def dh_copy(r):
        at = pl.ds(2 * PIECES[r][0], 2 * PIECES[r][1])
        return remote(dh_snd.at[at], dh_rx.at[at], ds.at[r], dr.at[r], other_ty)

    def both(ref, r):
        lo, size = PIECES[r]
        return jnp.concatenate([ref[lo:lo + size], ref[half + lo:half + lo + size]], axis=0)

    sums = []

    def piece_grad(r):
        x_copy(X_LAST + r).wait_recv()
        rows = slice(PIECES[r][0], PIECES[r][0] + PIECES[r][1])
        for j in range(2):
            cols = slice(j * BLK, (j + 1) * BLK)
            b = dact_block(3, j)
            d_act = (chip[b, rows].astype(F32) + rx[b, rows].astype(F32)).astype(BF16).astype(F32)
            for i in range(2):
                md[3, 1 + i, rows, cols] = (d_act * factors[i, rows, cols]).astype(BF16)
        piece_copy(r).start()

    def piece_dh(r):
        piece_copy(r).wait_recv()
        part = both(dh_v, r) + mm_bt(both(md.at[3, 1], r), wg_v[:, 3 * CHUNK:4 * CHUNK]) + mm_bt(both(md.at[3, 2], r), wu_v[:, 3 * CHUNK:4 * CHUNK])
        part_b = part.astype(BF16)
        dh_snd[2 * PIECES[r][0]:2 * (PIECES[r][0] + PIECES[r][1])] = part_b
        dh_copy(r).start()
        d_hat = part_b.astype(F32) * gamma_ref[...]
        sums.append((jnp.sum(d_hat, axis=1, keepdims=True), jnp.sum(d_hat * both(xhat_v, r), axis=1, keepdims=True)))

    piece_grad(0)
    use_grad(2)
    for r in range(1, SPLITS):
        piece_grad(r)
        piece_dh(r - 1)
    piece_dh(SPLITS - 1)
    cols = [jnp.concatenate([sums[r][i][:PIECES[r][1]] for r in range(SPLITS)] + [sums[r][i][PIECES[r][1]:] for r in range(SPLITS)], axis=0) for i in range(2)]
    stats_put(bst_snd, cols[0], cols[1])
    bwd_stats = stats_copies(bst_snd, bst_rx, 3, peers)
    for copy in bwd_stats:
        copy.start()

    y_copy.wait_recv()
    y_o[...] = (x_v[...].astype(F32) + (y_snd[...].astype(F32) + y_rx[...].astype(F32))).astype(BF16)

    def drain(b, carry):
        core_copy(b).wait_send()
        return carry

    lax.fori_loop(0, N_BLK, drain, 0)
    for u in range(N_X):
        x_copy(u).wait_send()
    for k in range(4):
        for i in range(3 if k < 3 else 1):
            gather_copy(k, i).wait_send()
    for r in range(SPLITS):
        piece_copy(r).wait_send()
    for copy in [packed_copy, dkv_copy, y_copy, kv_copy] + early + fwd_stats:
        copy.wait_send()

    br_v[...] = inv_v[:, 0:1] * xhat_v[...]
    d_gamma = jnp.zeros_like(dgamma_ref)
    for r in range(SPLITS):
        dh_copy(r).wait_recv()
        lo, size = PIECES[r]
        d_nrm = dh_snd[2 * lo:2 * (lo + size)].astype(F32) + dh_rx[2 * lo:2 * (lo + size)].astype(F32)
        d_gamma = d_gamma + jnp.sum(d_nrm * both(xhat_v, r), axis=0, keepdims=True)
        base = both(dy_v, r).astype(F32) + both(inv_v, r)[:, 0:1] * (d_nrm * gamma_ref[...])
        dh_v[lo:lo + size] = base[:size]
        dh_v[half + lo:half + lo + size] = base[size:]
    dgamma_ref[...] = d_gamma
    for copy in bwd_stats:
        copy.wait_recv()
    st_sum[...] = ((bst_snd[...] + bst_rx[0]) + (bst_rx[1] + bst_rx[2])) + ((bst_rx[3] + bst_rx[4]) + (bst_rx[5] + bst_rx[6]))
    sum_d, sum_dx = stats_columns(st_sum)
    d_x = dh_v[...] - inv_v[:, 0:1] * (sum_d / d_model) - br_v[...] * (sum_dx / d_model)
    dx_o[...] = d_x.astype(BF16)

    for r in range(SPLITS):
        dh_copy(r).wait_send()
    for copy in bwd_stats:
        copy.wait_send()


def grad_kernel(y_v, dx_v, dgamma_in, nrm_t, attn_v, md, dq_v, dkv_v, dy_v, tiles,
                y_hbm, dx_hbm, dgamma_hbm, dwq_hbm, dwg_hbm, dwu_hbm, dwk_hbm, dwv_hbm, dwo_hbm, dwd_hbm,
                ring, wide, out_sem, cp_sem):
    width, n_tok = nrm_t.shape
    half = n_tok // 2
    core = lax.rem(lax.axis_index('tx'), 2)
    mine = pl.multiple_of(core * half, half)
    other = pl.multiple_of((1 - core) * half, half)
    hand_out = [pltpu.make_async_copy(src.at[lo:lo + half], dst.at[pl.ds(at, half)], cp_sem.at[i])
                for i, (src, dst, lo, at) in enumerate(((y_v, y_hbm, 0, mine), (y_v, y_hbm, half, other), (dx_v, dx_hbm, 0, mine), (dx_v, dx_hbm, half, other)))]
    for cp in hand_out:
        cp.start()
    hand_out.append(pltpu.make_async_copy(dgamma_in, dgamma_hbm, cp_sem.at[12]))
    hand_out[-1].start()

    ready = [(0, dwq_hbm.at[:, 0:BLK]), (1, dwq_hbm.at[:, BLK:2 * BLK]), (2, dwo_hbm.at[0:BLK, :]), (3, dwo_hbm.at[BLK:2 * BLK, :]),
             (5, dwd_hbm.at[0:BLK, :]), (6, dwd_hbm.at[BLK:2 * BLK, :])]
    ready = [(tiles.at[i], dst) for i, dst in ready] + [(tiles.at[4, :, 0:256], dwk_hbm), (tiles.at[4, :, 256:512], dwv_hbm)]
    for i, (src, dst) in enumerate(ready):
        hand_out.append(pltpu.make_async_copy(src, dst, cp_sem.at[4 + i]))
        hand_out[-1].start()

    def put(src, dst, i):
        hand_out.append(pltpu.make_async_copy(src, dst, out_sem.at[i]))
        hand_out[-1].start()

    for t in range(6):
        k, j = 1 + t // 2, t % 2
        ring[t] = mm_at(md[k, 0, :, j * BLK:(j + 1) * BLK], dy_v[...])
        put(ring.at[t], dwd_hbm.at[k * CHUNK + j * BLK:k * CHUNK + (j + 1) * BLK, :], t)
    n_row = 128
    for i, (out, at) in enumerate(((dwg_hbm, 6), (dwu_hbm, 10))):
        for k in range(4):
            for j in range(2):
                lo = k * CHUNK + j * BLK
                wide[i, :, lo:lo + BLK] = mm(nrm_t[...], md[k, 1 + i, :, j * BLK:(j + 1) * BLK])
        for r in range(width // n_row):
            put(wide.at[i, r * n_row:(r + 1) * n_row], out.at[r * n_row:(r + 1) * n_row], at + r)
    for cp in hand_out:
        cp.wait()


def solution(mesh):
    tx_size = mesh.shape['tx']
    tok_spec = P('dp', None, 'tx')
    in_specs = (tok_spec, P('dp', None), tok_spec, P('tx'), P('tx', 'ty'), P('tx', 'ty'), P('tx', 'ty'),
                P('tx', None), P('tx', None), P('ty', 'tx'), P('ty', 'tx'))
    out_specs = (tok_spec, tok_spec, P(('dp', 'tx')), P(('dp', 'tx'), 'ty'), P(('dp', 'tx'), 'ty'), P(('dp', 'tx'), 'ty'),
                 P(('dp', 'tx'), None), P(('dp', 'tx'), None), P(('dp', 'ty'), 'tx'), P(('dp', 'ty'), 'tx'))

    def local_layer(x_in, positions, d_y, ln_gamma, w_q, w_g, w_u, w_k, w_v, w_o, w_d):
        _, n_tok, d_local = x_in.shape
        half = n_tok // 2
        d_model = d_local * tx_size
        head_dim = w_k.shape[1]
        q_width = w_q.shape[1]
        d_ff = w_g.shape[1]
        freq = jnp.asarray((ROPE_BASE ** (-2.0 * np.arange(head_dim // 2) / head_dim)).astype(np.float32)[None])
        any_spec = pl.BlockSpec(memory_space=pl.ANY)
        vmem_spec = pl.BlockSpec(memory_space=pltpu.VMEM)
        tok = (n_tok, d_local)
        sem = pltpu.SemaphoreType.DMA
        vm = pltpu.VMEM
        kept = pl.pallas_call(
            functools.partial(layer_kernel, d_model),
            out_shape=[vm(tok, BF16), vm(tok, BF16), vm((1, d_local), F32), vm((d_local, n_tok), BF16), vm((n_tok, q_width), BF16),
                       vm((4, 3, n_tok, CHUNK), BF16), vm((n_tok, q_width), BF16), vm((n_tok, 2 * head_dim), BF16), vm(tok, BF16),
                       vm((7, BLK, BLK), F32)],
            in_specs=[any_spec] * 12,
            out_specs=[vmem_spec] * 10,
            scratch_shapes=[
                vm((1, n_tok), jnp.int32), vm((1, head_dim // 2), F32), vm((1, d_local), F32), vm(tok, BF16),
                vm(tok, BF16), vm((d_local, q_width + 2 * head_dim), BF16), vm((d_local, d_ff), BF16), vm((d_local, d_ff), BF16),
                vm((q_width, d_local), BF16), vm((d_ff, d_local), BF16),
                vm((N_BLK, half, BLK), F32), vm((N_BLK, half, BLK), BF16), vm((N_BLK, half, BLK), BF16),
                vm((N_BLK, half, BLK), BF16), vm((N_BLK, half, BLK), BF16), vm((n_tok, 2 * q_width + 2 * head_dim), BF16),
                vm((n_tok, 512), BF16), vm((n_tok, 512), BF16), vm((n_tok, 512), F32),
                vm(tok, F32), vm((n_tok, 128), F32), vm((n_tok, 128), F32), vm((n_tok, 128), F32), vm(tok, F32), vm(tok, F32),
                vm(tok, BF16), vm(tok, BF16), vm(tok, BF16), vm(tok, BF16),
                vm((8, n_tok), F32), vm((3, 8, n_tok), F32), vm((8, n_tok), F32), vm((8, n_tok), F32), vm((7, 8, n_tok), F32), vm((2, half, CHUNK), F32),
                sem((16,)), sem((N_BLK,)), sem((N_BLK,)), sem((N_X,)), sem((N_X,)),
                sem((12 + SPLITS,)), sem((12 + SPLITS,)), sem((1,)), sem((1,)), sem((4,)), sem((4,)), sem((10,)), sem((10,)),
                sem((SPLITS,)), sem((SPLITS,)), vm((n_tok, EARLY), BF16), vm((2, half, EARLY), BF16), sem((2,)), sem((2,))],
            compiler_params=pltpu.CompilerParams(collective_id=0, has_side_effects=True, vmem_limit_bytes=46 * 1024 * 1024),
            name='layer',
        )(x_in.reshape(tok), positions, freq, d_y.reshape(tok), ln_gamma[None], w_q, w_g, w_u, w_k, w_v, w_o, w_d)

        y_out, d_x, d_gamma, d_wq, d_wg, d_wu, d_wk, d_wv, d_wo, d_wd = pl.pallas_call(
            grad_kernel,
            out_shape=[jax.ShapeDtypeStruct(tok, BF16), jax.ShapeDtypeStruct(tok, BF16), jax.ShapeDtypeStruct((1, d_local), F32)]
            + [jax.ShapeDtypeStruct(w.shape, F32) for w in (w_q, w_g, w_u, w_k, w_v, w_o, w_d)],
            in_specs=[vmem_spec] * 10,
            out_specs=[any_spec] * 10,
            scratch_shapes=[vm((6, d_local, BLK), F32), vm((2, d_local, d_ff), F32), sem((14,)), sem((13,))],
            compiler_params=pltpu.CompilerParams(vmem_limit_bytes=30 * 1024 * 1024),
            name='weight_grads',
        )(*kept)
        return (y_out.reshape(x_in.shape), d_x.reshape(x_in.shape), d_gamma.reshape(d_local),
                d_wq, d_wg, d_wu, d_wk, d_wv, d_wo, d_wd)

    return jax.shard_map(local_layer, mesh=mesh, in_specs=in_specs, out_specs=out_specs, check_vma=False)
```

```python
import functools

import jax
import jax.numpy as jnp
import numpy as np
from jax import lax
from jax.experimental import pallas as pl
from jax.experimental.pallas import tpu as pltpu
from jax.sharding import PartitionSpec as P

EPS = 1e-6
ROPE_BASE = 10000.0
F32 = jnp.float32
BF16 = jnp.bfloat16
MESH = pl.DeviceIdType.MESH

BLK = 512
CHUNK = 1024
B_DATTN, B_DACT_LO, B_QKV, B_GU, B_DACT_HI, N_BLK = 0, 2, 4, 7, 23, 29
X_UNITS = ((0, 1), (1, 1), (2, 2), (4, 2), (7, 4), (11, 4), (15, 4), (19, 4), (23, 2), (25, 2))
PIECES = ((0, 16), (16, 32), (48, 32), (80, 32), (112, 16))
SPLITS = len(PIECES)
EARLY = 128
X_KV = len(X_UNITS)
X_LAST = X_KV + 1
N_X = X_LAST + SPLITS


def dot(a, b, dims):
    return lax.dot_general(a, b, (dims, ((), ())), preferred_element_type=F32)


def mm(a, b):
    return dot(a, b, ((1,), (0,)))


def mm_bt(a, b):
    return dot(a, b, ((1,), (1,)))


def mm_at(a, b):
    return dot(a, b, ((0,), (0,)))


def rope(first, second, cos_t, sin_t):
    return first * cos_t - second * sin_t, second * cos_t + first * sin_t


def layer_kernel(d_model, x_hbm, pos_hbm, freq_hbm, dy_hbm, gamma_hbm, wq_hbm, wg_hbm, wu_hbm, wk_hbm, wv_hbm, wo_hbm, wd_hbm,
                 y_o, dx_o, dgamma_ref, nrm_t, attn_v, md, dq_v, dkv_v, dy_v, tiles,
                 pos_ref, freq_ref, gamma_ref, nrm_v, x_v, wqkv_v, wg_v, wu_v, wo_v, wd_v,
                 keep, send, rcore, chip, rx, packed, dkv_part, dkv_rx, kv_acc,
                 xhat_v, inv_v, cos_v, sin_v, br_v, dh_v, y_snd, y_rx, dh_snd, dh_rx,
                 st_snd, st_rx, st_sum, bst_snd, bst_rx, factors,
                 ld_sem, cs, cr, xs, xr, gs, gr, ps, pr, ts, tr, ss, sr, ds, dr, early_snd, early_rx, es, er):
    tx = lax.axis_index('tx')
    ty = lax.axis_index('ty')
    core = lax.rem(tx, 2)
    near = {'tx': tx + 1 - 2 * core}
    across = {'tx': lax.rem(tx + 2, 4)}
    far = {'tx': lax.rem(tx + 1 - 2 * core + 2, 4)}
    other_ty = {'ty': 1 - ty}
    peers = [near, across, far, other_ty] + [{'tx': p['tx'], 'ty': 1 - ty} for p in (near, across, far)]
    close = peers[:5]
    n_tok = x_v.shape[0]
    half = n_tok // 2
    mine = pl.multiple_of(core * half, half)
    other = pl.multiple_of((1 - core) * half, half)
    head_dim = 256
    q_width = wo_v.shape[0]
    heads = q_width // head_dim

    def load(i, src, dst):
        return pltpu.make_async_copy(src, dst, ld_sem.at[i])

    loads = [
        load(0, dy_hbm.at[pl.ds(mine, half)], dy_v.at[0:half]),
        load(1, dy_hbm.at[pl.ds(other, half)], dy_v.at[half:n_tok]),
        load(2, wo_hbm.at[0:EARLY], wo_v.at[0:EARLY]),
        load(3, x_hbm.at[pl.ds(mine, half)], x_v.at[0:half]),
        load(4, x_hbm.at[pl.ds(other, half)], x_v.at[half:n_tok]),
        load(5, wd_hbm.at[0:CHUNK], wd_v.at[0:CHUNK]),
        load(6, wq_hbm, wqkv_v.at[:, 0:q_width]),
        load(7, wk_hbm, wqkv_v.at[:, q_width:q_width + head_dim]),
        load(8, wv_hbm, wqkv_v.at[:, q_width + head_dim:q_width + 2 * head_dim]),
        load(9, wg_hbm, wg_v),
        load(10, wu_hbm, wu_v),
        load(11, wd_hbm.at[CHUNK:4 * CHUNK], wd_v.at[CHUNK:4 * CHUNK]),
        load(12, gamma_hbm, gamma_ref),
        load(13, pos_hbm, pos_ref),
        load(14, freq_hbm, freq_ref),
        load(15, wo_hbm.at[BLK:q_width], wo_v.at[BLK:q_width]),
        load(16, wo_hbm.at[EARLY:BLK], wo_v.at[EARLY:BLK]),
    ]
    for i in (0, 1, 2, 16, 15, 3, 4, 5):
        loads[i].start()

    barrier = pltpu.get_barrier_semaphore()
    for peer in close:
        pl.semaphore_signal(barrier, inc=1, device_id=peer, device_id_type=MESH)
    for ld in loads[:3]:
        ld.wait()
    for i in (12, 6, 7, 8):
        loads[i].start()

    def remote(src, dst, send_sem, recv_sem, peer):
        return pltpu.make_async_remote_copy(src_ref=src, dst_ref=dst, send_sem=send_sem, recv_sem=recv_sem,
                                            device_id=peer, device_id_type=MESH)

    def core_copy(b):
        return remote(send.at[b], rcore.at[b], cs.at[b], cr.at[b], near)

    def x_copy(u):
        if u >= X_LAST:
            rows = pl.ds(*PIECES[u - X_LAST])
            return remote(chip.at[pl.ds(N_BLK - 2, 2), rows], rx.at[pl.ds(N_BLK - 2, 2), rows], xs.at[u], xr.at[u], across)
        if u == X_KV:
            cols = pl.ds(pl.multiple_of(ty * head_dim, head_dim), head_dim)
            return remote(chip.at[B_QKV + 2, :, cols], rx.at[B_QKV + 2, :, cols], xs.at[u], xr.at[u], across)
        if u == 0:
            return remote(chip.at[0, :, EARLY:BLK], rx.at[0, :, EARLY:BLK], xs.at[u], xr.at[u], across)
        start, count = X_UNITS[u]
        return remote(chip.at[pl.ds(start, count)], rx.at[pl.ds(start, count)], xs.at[u], xr.at[u], across)

    def put(b, part):
        keep[b] = part[:half]
        send[b] = part[half:].astype(BF16)
        core_copy(b).start()

    def issue_bwd(b, w_ref, row):
        put(b, mm_bt(dy_v[...], w_ref[pl.ds(row, BLK), :]))

    def issue_fwd(b, w_ref, col):
        put(b, mm(nrm_v[...], w_ref[:, pl.ds(col, BLK)]))

    def combine(b):
        core_copy(b).wait_recv()
        chip[b] = (keep[b] + rcore[b].astype(F32)).astype(BF16)

    def total(b):
        return chip[b].astype(F32) + rx[b].astype(F32)

    early_snd[...] = mm_bt(dy_v[...], wo_v[0:EARLY, :]).astype(BF16)
    pl.semaphore_wait(barrier, len(close))
    early = [remote(early_snd.at[0:half], early_rx.at[0], es.at[0], er.at[0], across),
             remote(early_snd.at[half:n_tok], early_rx.at[1], es.at[1], er.at[1], far)]
    for copy in early:
        copy.start()
    loads[16].wait()
    issue_bwd(0, wo_v, 0)
    loads[15].wait()
    issue_bwd(1, wo_v, BLK)

    def rows_of(col_a, col_b):
        lane = lax.broadcasted_iota(jnp.int32, (half, 128), 1)
        return jnp.where(lane == 0, col_a, col_b).T[0:8]

    def stats_copies(snd, got, base, to):
        return [remote(snd, got.at[i], ss.at[base + i], sr.at[base + i], peer) for i, peer in enumerate(to)]

    def stats_put(snd, col_a, col_b):
        for lo, at in ((0, mine), (half, other)):
            snd[:, pl.ds(at, half)] = rows_of(col_a[lo:lo + half], col_b[lo:lo + half])

    def stats_columns(rows_ref):
        cols = []
        for i in range(2):
            parts = [jnp.broadcast_to(rows_ref[i:i + 1, pl.ds(at, half)], (128, half)).T[:, 0:1] for at in (mine, other)]
            cols.append(jnp.concatenate(parts, axis=0))
        return cols

    loads[3].wait()
    loads[4].wait()
    for i in (9, 10, 11, 13, 14):
        loads[i].start()
    x_f = x_v[...].astype(F32)
    stats_put(st_snd, jnp.sum(x_f, axis=1, keepdims=True), jnp.sum(x_f * x_f, axis=1, keepdims=True))
    fwd_stats = stats_copies(st_snd, st_rx, 0, (near, across, far))
    for copy in fwd_stats:
        copy.start()

    combine(0)
    x_copy(0).start()
    combine(1)
    x_copy(1).start()

    loads[5].wait()
    for i in range(2):
        issue_bwd(B_DACT_LO + i, wd_v, i * BLK)
    for i in range(2):
        combine(B_DACT_LO + i)
    x_copy(2).start()

    loads[12].wait()
    for copy in fwd_stats:
        copy.wait_recv()
    st_sum[...] = (st_snd[...] + st_rx[0]) + (st_rx[1] + st_rx[2])
    sum_x, sum_xx = stats_columns(st_sum)
    tok_mean = sum_x / d_model
    inv_std = lax.rsqrt(sum_xx / d_model - tok_mean * tok_mean + EPS)
    inv_v[...] = jnp.broadcast_to(inv_std, (n_tok, 128))
    x_hat = (x_v[...].astype(F32) - tok_mean) * inv_std
    xhat_v[...] = x_hat
    nrm_v[...] = (x_hat * gamma_ref[...]).astype(BF16)

    for i in range(6, 9):
        loads[i].wait()
    for i in range(3):
        issue_fwd(B_QKV + i, wqkv_v, i * BLK)
    for i in (2, 0, 1):
        combine(B_QKV + i)
        if i == 2:
            x_copy(X_KV).start()
    x_copy(3).start()

    loads[9].wait()
    loads[10].wait()
    for k in range(4):
        def gu_issue(j, carry, k=k):
            col = pl.multiple_of(k * CHUNK + j * BLK, BLK)
            issue_fwd(B_GU + 4 * k + j, wg_v, col)
            issue_fwd(B_GU + 4 * k + 2 + j, wu_v, col)
            return carry

        def gu_combine(j, carry, k=k):
            combine(B_GU + 4 * k + j)
            return carry

        lax.fori_loop(0, 2, gu_issue, 0)
        lax.fori_loop(0, 4, gu_combine, 0)
        x_copy(4 + k).start()

    loads[11].wait()

    def hi_issue(j, carry):
        issue_bwd(B_DACT_HI + j, wd_v, pl.multiple_of(CHUNK + j * BLK, BLK))
        return carry

    lax.fori_loop(0, 6, hi_issue, 0)
    for j in range(6):
        combine(B_DACT_HI + j)
        if j == 1 or j == 3:
            x_copy(8 + j // 2).start()
    for r in range(SPLITS):
        x_copy(X_LAST + r).start()

    nrm_t[...] = nrm_v[...].T

    loads[13].wait()
    loads[14].wait()
    freq = freq_ref[...]
    for lo, at in ((0, mine), (half, other)):
        pos_col = jnp.broadcast_to(pos_ref[0:1, pl.ds(at, half)].astype(F32), (128, half)).T
        angles = pos_col * freq
        cos_v[lo:lo + half] = jnp.cos(angles)
        sin_v[lo:lo + half] = jnp.sin(angles)

    packed_copy = remote(packed.at[0:half], packed.at[half:n_tok], ps.at[0], pr.at[0], near)
    x_copy(0).wait_recv()
    x_copy(1).wait_recv()
    for copy in early:
        copy.wait_recv()
    rx[0, :, 0:EARLY] = (early_rx[0].astype(F32) + early_rx[1].astype(F32)).astype(BF16)
    for j in range(2):
        packed[0:half, q_width + 512 + j * BLK:q_width + 512 + (j + 1) * BLK] = total(B_DATTN + j).astype(BF16)
    x_copy(3).wait_recv()
    cos_h, sin_h = cos_v[0:half], sin_v[0:half]
    for j in range(2):
        blk = total(B_QKV + j)
        for h in range(2):
            lo = h * head_dim
            first, second = rope(blk[:, lo:lo + 128], blk[:, lo + 128:lo + 256], cos_h, sin_h)
            packed[0:half, j * BLK + lo:j * BLK + lo + 128] = first.astype(BF16)
            packed[0:half, j * BLK + lo + 128:j * BLK + lo + 256] = second.astype(BF16)
    x_copy(X_KV).wait_recv()
    kv_cols = pl.ds(pl.multiple_of(ty * head_dim, head_dim), head_dim)
    blk = chip[B_QKV + 2, :, kv_cols].astype(F32) + rx[B_QKV + 2, :, kv_cols].astype(F32)
    first, second = rope(blk[:, 0:128], blk[:, 128:256], cos_h, sin_h)
    kv_mine = jnp.where(ty == 0, jnp.concatenate([first, second], axis=1), blk).astype(BF16)
    kv_dst = packed.at[0:half, pl.ds(pl.multiple_of(q_width + ty * head_dim, head_dim), head_dim)]
    kv_dst[...] = kv_mine
    kv_copy = remote(kv_dst, kv_dst, ts.at[3], tr.at[3], other_ty)
    kv_copy.start()
    kv_copy.wait_recv()
    packed_copy.start()
    packed_copy.wait_recv()

    row_i = lax.rem(lax.broadcasted_iota(jnp.int32, (n_tok, n_tok), 0) + core * half, n_tok)
    col_i = lax.rem(lax.broadcasted_iota(jnp.int32, (n_tok, n_tok), 1) + core * half, n_tok)
    scale = head_dim ** -0.5
    kv_acc[...] = jnp.zeros_like(kv_acc)

    def head_step(h, carry):
        cols = pl.ds(pl.multiple_of(h * head_dim, head_dim), head_dim)
        q_h = packed[:, cols]
        da_h = packed[:, pl.ds(pl.multiple_of(q_width + 512 + h * head_dim, head_dim), head_dim)]
        k_rot = packed[:, q_width:q_width + 256]
        v_val = packed[:, q_width + 256:q_width + 512]
        scores = jnp.where(row_i >= col_i, mm_bt(q_h, k_rot) * scale, -1e30)
        exps = jnp.exp(scores - jnp.max(scores, axis=1, keepdims=True))
        probs_f = exps / jnp.sum(exps, axis=1, keepdims=True)
        probs = probs_f.astype(BF16)
        attn_v[:, cols] = mm(probs, v_val).astype(BF16)
        d_probs = mm_bt(da_h, v_val).astype(BF16).astype(F32)
        d_scores = (probs_f * (d_probs - jnp.sum(d_probs * probs_f, axis=1, keepdims=True)) * scale).astype(BF16)
        dq_h = mm(d_scores, k_rot).astype(BF16).astype(F32)
        first, second = rope(dq_h[:, 0:128], dq_h[:, 128:256], cos_v[...], -sin_v[...])
        dq_v[:, pl.ds(pl.multiple_of(h * head_dim, head_dim), 128)] = first.astype(BF16)
        dq_v[:, pl.ds(pl.multiple_of(h * head_dim + 128, 128), 128)] = second.astype(BF16)
        kv_acc[:, 0:256] += mm_at(d_scores, q_h)
        kv_acc[:, 256:512] += mm_at(probs, da_h)
        return carry

    lax.fori_loop(0, heads, head_step, 0)
    dkv_part[...] = kv_acc[...].astype(BF16)
    dkv_copy = remote(dkv_part, dkv_rx, ts.at[0], tr.at[0], other_ty)
    dkv_copy.start()
    br_v[...] = mm(attn_v[...], wo_v[...])
    dh_v[...] = mm_bt(dq_v[...], wqkv_v[:, 0:q_width])

    for j in range(2):
        tiles[j] = mm(nrm_t[...], dq_v[:, j * BLK:(j + 1) * BLK])
        tiles[2 + j] = mm_at(attn_v[:, j * BLK:(j + 1) * BLK], dy_v[...])

    def piece_copy(r):
        lo, size = PIECES[r]
        return remote(md.at[3, 1:3, lo:lo + size], md.at[3, 1:3, half + lo:half + lo + size], gs.at[12 + r], gr.at[12 + r], near)

    def gather_copy(k, i):
        return remote(md.at[k, i, 0:half], md.at[k, i, half:n_tok], gs.at[3 * k + i], gr.at[3 * k + i], near)

    def dact_block(k, j):
        return B_DACT_LO + j if k == 0 else B_DACT_HI + 2 * (k - 1) + j

    def gated(k, want_act, want_grad):
        def step(r, carry):
            rows = pl.ds(pl.multiple_of(r * 16, 16), 16)
            for j in range(2):
                bg, bu, bd = B_GU + 4 * k + j, B_GU + 4 * k + 2 + j, dact_block(k, j)
                gate = (chip[bg, rows].astype(F32) + rx[bg, rows].astype(F32)).astype(BF16).astype(F32)
                up = (chip[bu, rows].astype(F32) + rx[bu, rows].astype(F32)).astype(BF16).astype(F32)
                sig = jax.nn.sigmoid(gate)
                silu = gate * sig
                cols = slice(j * BLK, (j + 1) * BLK)
                if want_act:
                    md[k, 0, rows, cols] = (silu * up).astype(BF16)
                if k == 3:
                    factors[0, rows, cols] = up * sig * (1.0 + gate * (1.0 - sig))
                    factors[1, rows, cols] = silu
                if want_grad:
                    d_act = (chip[bd, rows].astype(F32) + rx[bd, rows].astype(F32)).astype(BF16).astype(F32)
                    md[k, 1, rows, cols] = (d_act * up * sig * (1.0 + gate * (1.0 - sig))).astype(BF16)
                    md[k, 2, rows, cols] = (d_act * silu).astype(BF16)
            return carry

        lax.fori_loop(0, half // 16, step, 0)
        for i in ((0,) if want_act else ()) + ((1, 2) if want_grad else ()):
            gather_copy(k, i).start()

    def use_act(k):
        gather_copy(k, 0).wait_recv()
        br_v[...] += mm(md[k, 0], wd_v[k * CHUNK:(k + 1) * CHUNK, :])

    def use_grad(k):
        for i in (1, 2):
            gather_copy(k, i).wait_recv()
        dh_v[...] += (mm_bt(md[k, 1], wg_v[:, k * CHUNK:(k + 1) * CHUNK])
                      + mm_bt(md[k, 2], wu_v[:, k * CHUNK:(k + 1) * CHUNK]))

    x_copy(2).wait_recv()
    for k in range(4):
        x_copy(4 + k).wait_recv()
        gated(k, True, k == 0)
        use_act(k)
        if k == 0:
            use_grad(0)
            dkv_copy.wait_recv()
            d_k = dkv_part[:, 0:256].astype(F32) + dkv_rx[:, 0:256].astype(F32)
            d_k = d_k.astype(BF16).astype(F32)
            first, second = rope(d_k[:, 0:128], d_k[:, 128:256], cos_v[...], -sin_v[...])
            dkv_v[:, 0:128] = first.astype(BF16)
            dkv_v[:, 128:256] = second.astype(BF16)
            dkv_v[:, 256:512] = (dkv_part[:, 256:512].astype(F32) + dkv_rx[:, 256:512].astype(F32)).astype(BF16)
            dh_v[...] += 0.5 * mm_bt(dkv_v[...], wqkv_v[:, q_width:q_width + 512])
            tiles[4] = mm(nrm_t[...], dkv_v[...])
            for j in range(2):
                tiles[5 + j] = mm_at(md[0, 0, :, j * BLK:(j + 1) * BLK], dy_v[...])
    y_snd[...] = br_v[...].astype(BF16)
    y_copy = remote(y_snd, y_rx, ts.at[1], tr.at[1], other_ty)
    y_copy.start()
    x_copy(8).wait_recv()
    gated(1, False, True)
    use_grad(1)
    x_copy(9).wait_recv()
    gated(2, False, True)

    def dh_copy(r):
        at = pl.ds(2 * PIECES[r][0], 2 * PIECES[r][1])
        return remote(dh_snd.at[at], dh_rx.at[at], ds.at[r], dr.at[r], other_ty)

    def both(ref, r):
        lo, size = PIECES[r]
        return jnp.concatenate([ref[lo:lo + size], ref[half + lo:half + lo + size]], axis=0)

    sums = []

    def piece_grad(r):
        x_copy(X_LAST + r).wait_recv()
        rows = slice(PIECES[r][0], PIECES[r][0] + PIECES[r][1])
        for j in range(2):
            cols = slice(j * BLK, (j + 1) * BLK)
            b = dact_block(3, j)
            d_act = (chip[b, rows].astype(F32) + rx[b, rows].astype(F32)).astype(BF16).astype(F32)
            for i in range(2):
                md[3, 1 + i, rows, cols] = (d_act * factors[i, rows, cols]).astype(BF16)
        piece_copy(r).start()

    def piece_dh(r):
        piece_copy(r).wait_recv()
        part = both(dh_v, r) + mm_bt(both(md.at[3, 1], r), wg_v[:, 3 * CHUNK:4 * CHUNK]) + mm_bt(both(md.at[3, 2], r), wu_v[:, 3 * CHUNK:4 * CHUNK])
        part_b = part.astype(BF16)
        dh_snd[2 * PIECES[r][0]:2 * (PIECES[r][0] + PIECES[r][1])] = part_b
        dh_copy(r).start()
        d_hat = part_b.astype(F32) * gamma_ref[...]
        sums.append((jnp.sum(d_hat, axis=1, keepdims=True), jnp.sum(d_hat * both(xhat_v, r), axis=1, keepdims=True)))

    piece_grad(0)
    use_grad(2)
    for r in range(1, SPLITS):
        piece_grad(r)
        piece_dh(r - 1)
    piece_dh(SPLITS - 1)
    cols = [jnp.concatenate([sums[r][i][:PIECES[r][1]] for r in range(SPLITS)] + [sums[r][i][PIECES[r][1]:] for r in range(SPLITS)], axis=0) for i in range(2)]
    stats_put(bst_snd, cols[0], cols[1])
    bwd_stats = stats_copies(bst_snd, bst_rx, 3, peers)
    for copy in bwd_stats:
        copy.start()

    y_copy.wait_recv()
    y_o[...] = (x_v[...].astype(F32) + (y_snd[...].astype(F32) + y_rx[...].astype(F32))).astype(BF16)

    def drain(b, carry):
        core_copy(b).wait_send()
        return carry

    lax.fori_loop(0, N_BLK, drain, 0)
    for u in range(N_X):
        x_copy(u).wait_send()
    for k in range(4):
        for i in range(3 if k < 3 else 1):
            gather_copy(k, i).wait_send()
    for r in range(SPLITS):
        piece_copy(r).wait_send()
    for copy in [packed_copy, dkv_copy, y_copy, kv_copy] + early + fwd_stats:
        copy.wait_send()

    br_v[...] = inv_v[:, 0:1] * xhat_v[...]
    d_gamma = jnp.zeros_like(dgamma_ref)
    for r in range(SPLITS):
        dh_copy(r).wait_recv()
        lo, size = PIECES[r]
        d_nrm = dh_snd[2 * lo:2 * (lo + size)].astype(F32) + dh_rx[2 * lo:2 * (lo + size)].astype(F32)
        d_gamma = d_gamma + jnp.sum(d_nrm * both(xhat_v, r), axis=0, keepdims=True)
        base = both(dy_v, r).astype(F32) + both(inv_v, r)[:, 0:1] * (d_nrm * gamma_ref[...])
        dh_v[lo:lo + size] = base[:size]
        dh_v[half + lo:half + lo + size] = base[size:]
    dgamma_ref[...] = d_gamma
    for copy in bwd_stats:
        copy.wait_recv()
    st_sum[...] = ((bst_snd[...] + bst_rx[0]) + (bst_rx[1] + bst_rx[2])) + ((bst_rx[3] + bst_rx[4]) + (bst_rx[5] + bst_rx[6]))
    sum_d, sum_dx = stats_columns(st_sum)
    d_x = dh_v[...] - inv_v[:, 0:1] * (sum_d / d_model) - br_v[...] * (sum_dx / d_model)
    dx_o[...] = d_x.astype(BF16)

    for r in range(SPLITS):
        dh_copy(r).wait_send()
    for copy in bwd_stats:
        copy.wait_send()


def grad_kernel(y_v, dx_v, dgamma_in, nrm_t, attn_v, md, dq_v, dkv_v, dy_v, tiles,
                y_hbm, dx_hbm, dgamma_hbm, dwq_hbm, dwg_hbm, dwu_hbm, dwk_hbm, dwv_hbm, dwo_hbm, dwd_hbm,
                ring, wide, out_sem, cp_sem):
    width, n_tok = nrm_t.shape
    half = n_tok // 2
    core = lax.rem(lax.axis_index('tx'), 2)
    mine = pl.multiple_of(core * half, half)
    other = pl.multiple_of((1 - core) * half, half)
    hand_out = [pltpu.make_async_copy(src.at[lo:lo + half], dst.at[pl.ds(at, half)], cp_sem.at[i])
                for i, (src, dst, lo, at) in enumerate(((y_v, y_hbm, 0, mine), (y_v, y_hbm, half, other), (dx_v, dx_hbm, 0, mine), (dx_v, dx_hbm, half, other)))]
    for cp in hand_out:
        cp.start()
    hand_out.append(pltpu.make_async_copy(dgamma_in, dgamma_hbm, cp_sem.at[12]))
    hand_out[-1].start()

    ready = [(0, dwq_hbm.at[:, 0:BLK]), (1, dwq_hbm.at[:, BLK:2 * BLK]), (2, dwo_hbm.at[0:BLK, :]), (3, dwo_hbm.at[BLK:2 * BLK, :]),
             (5, dwd_hbm.at[0:BLK, :]), (6, dwd_hbm.at[BLK:2 * BLK, :])]
    ready = [(tiles.at[i], dst) for i, dst in ready] + [(tiles.at[4, :, 0:256], dwk_hbm), (tiles.at[4, :, 256:512], dwv_hbm)]
    for i, (src, dst) in enumerate(ready):
        hand_out.append(pltpu.make_async_copy(src, dst, cp_sem.at[4 + i]))
        hand_out[-1].start()

    def put(src, dst, i):
        hand_out.append(pltpu.make_async_copy(src, dst, out_sem.at[i]))
        hand_out[-1].start()

    for t in range(6):
        k, j = 1 + t // 2, t % 2
        ring[t] = mm_at(md[k, 0, :, j * BLK:(j + 1) * BLK], dy_v[...])
        put(ring.at[t], dwd_hbm.at[k * CHUNK + j * BLK:k * CHUNK + (j + 1) * BLK, :], t)
    n_row = 128
    for i, (out, at) in enumerate(((dwg_hbm, 6), (dwu_hbm, 10))):
        for k in range(4):
            for j in range(2):
                lo = k * CHUNK + j * BLK
                wide[i, :, lo:lo + BLK] = mm(nrm_t[...], md[k, 1 + i, :, j * BLK:(j + 1) * BLK])
        for r in range(width // n_row):
            put(wide.at[i, r * n_row:(r + 1) * n_row], out.at[r * n_row:(r + 1) * n_row], at + r)
    for cp in hand_out:
        cp.wait()


def solution(mesh):
    tx_size = mesh.shape['tx']
    tok_spec = P('dp', None, 'tx')
    in_specs = (tok_spec, P('dp', None), tok_spec, P('tx'), P('tx', 'ty'), P('tx', 'ty'), P('tx', 'ty'),
                P('tx', None), P('tx', None), P('ty', 'tx'), P('ty', 'tx'))
    out_specs = (tok_spec, tok_spec, P(('dp', 'tx')), P(('dp', 'tx'), 'ty'), P(('dp', 'tx'), 'ty'), P(('dp', 'tx'), 'ty'),
                 P(('dp', 'tx'), None), P(('dp', 'tx'), None), P(('dp', 'ty'), 'tx'), P(('dp', 'ty'), 'tx'))

    def local_layer(x_in, positions, d_y, ln_gamma, w_q, w_g, w_u, w_k, w_v, w_o, w_d):
        _, n_tok, d_local = x_in.shape
        half = n_tok // 2
        d_model = d_local * tx_size
        head_dim = w_k.shape[1]
        q_width = w_q.shape[1]
        d_ff = w_g.shape[1]
        freq = jnp.asarray((ROPE_BASE ** (-2.0 * np.arange(head_dim // 2) / head_dim)).astype(np.float32)[None])
        any_spec = pl.BlockSpec(memory_space=pl.ANY)
        vmem_spec = pl.BlockSpec(memory_space=pltpu.VMEM)
        tok = (n_tok, d_local)
        sem = pltpu.SemaphoreType.DMA
        vm = pltpu.VMEM
        kept = pl.pallas_call(
            functools.partial(layer_kernel, d_model),
            out_shape=[vm(tok, BF16), vm(tok, BF16), vm((1, d_local), F32), vm((d_local, n_tok), BF16), vm((n_tok, q_width), BF16),
                       vm((4, 3, n_tok, CHUNK), BF16), vm((n_tok, q_width), BF16), vm((n_tok, 2 * head_dim), BF16), vm(tok, BF16),
                       vm((7, BLK, BLK), F32)],
            in_specs=[any_spec] * 12,
            out_specs=[vmem_spec] * 10,
            scratch_shapes=[
                vm((1, n_tok), jnp.int32), vm((1, head_dim // 2), F32), vm((1, d_local), F32), vm(tok, BF16),
                vm(tok, BF16), vm((d_local, q_width + 2 * head_dim), BF16), vm((d_local, d_ff), BF16), vm((d_local, d_ff), BF16),
                vm((q_width, d_local), BF16), vm((d_ff, d_local), BF16),
                vm((N_BLK, half, BLK), F32), vm((N_BLK, half, BLK), BF16), vm((N_BLK, half, BLK), BF16),
                vm((N_BLK, half, BLK), BF16), vm((N_BLK, half, BLK), BF16), vm((n_tok, 2 * q_width + 2 * head_dim), BF16),
                vm((n_tok, 512), BF16), vm((n_tok, 512), BF16), vm((n_tok, 512), F32),
                vm(tok, F32), vm((n_tok, 128), F32), vm((n_tok, 128), F32), vm((n_tok, 128), F32), vm(tok, F32), vm(tok, F32),
                vm(tok, BF16), vm(tok, BF16), vm(tok, BF16), vm(tok, BF16),
                vm((8, n_tok), F32), vm((3, 8, n_tok), F32), vm((8, n_tok), F32), vm((8, n_tok), F32), vm((7, 8, n_tok), F32), vm((2, half, CHUNK), F32),
                sem((17,)), sem((N_BLK,)), sem((N_BLK,)), sem((N_X,)), sem((N_X,)),
                sem((12 + SPLITS,)), sem((12 + SPLITS,)), sem((1,)), sem((1,)), sem((4,)), sem((4,)), sem((10,)), sem((10,)),
                sem((SPLITS,)), sem((SPLITS,)), vm((n_tok, EARLY), BF16), vm((2, half, EARLY), BF16), sem((2,)), sem((2,))],
            compiler_params=pltpu.CompilerParams(collective_id=0, has_side_effects=True, vmem_limit_bytes=46 * 1024 * 1024),
            name='layer',
        )(x_in.reshape(tok), positions, freq, d_y.reshape(tok), ln_gamma[None], w_q, w_g, w_u, w_k, w_v, w_o, w_d)

        y_out, d_x, d_gamma, d_wq, d_wg, d_wu, d_wk, d_wv, d_wo, d_wd = pl.pallas_call(
            grad_kernel,
            out_shape=[jax.ShapeDtypeStruct(tok, BF16), jax.ShapeDtypeStruct(tok, BF16), jax.ShapeDtypeStruct((1, d_local), F32)]
            + [jax.ShapeDtypeStruct(w.shape, F32) for w in (w_q, w_g, w_u, w_k, w_v, w_o, w_d)],
            in_specs=[vmem_spec] * 10,
            out_specs=[any_spec] * 10,
            scratch_shapes=[vm((6, d_local, BLK), F32), vm((2, d_local, d_ff), F32), sem((14,)), sem((13,))],
            compiler_params=pltpu.CompilerParams(vmem_limit_bytes=30 * 1024 * 1024),
            name='weight_grads',
        )(*kept)
        return (y_out.reshape(x_in.shape), d_x.reshape(x_in.shape), d_gamma.reshape(d_local),
                d_wq, d_wg, d_wu, d_wk, d_wv, d_wo, d_wd)

    return jax.shard_map(local_layer, mesh=mesh, in_specs=in_specs, out_specs=out_specs, check_vma=False)
```

```python
import functools

import jax
import jax.numpy as jnp
import numpy as np
from jax import lax
from jax.experimental import pallas as pl
from jax.experimental.pallas import tpu as pltpu
from jax.sharding import PartitionSpec as P

EPS = 1e-6
ROPE_BASE = 10000.0
F32 = jnp.float32
BF16 = jnp.bfloat16
MESH = pl.DeviceIdType.MESH

BLK = 512
CHUNK = 1024
B_DATTN, B_DACT_LO, B_QKV, B_GU, B_DACT_HI, N_BLK = 0, 2, 4, 7, 23, 29
X_UNITS = ((0, 1), (1, 1), (2, 2), (4, 2), (7, 4), (11, 4), (15, 4), (19, 4), (23, 2), (25, 2))
PIECES = ((0, 16), (16, 32), (48, 32), (80, 32), (112, 16))
SPLITS = len(PIECES)
EARLY = 128
X_KV = len(X_UNITS)
X_LAST = X_KV + 1
N_X = X_LAST + SPLITS


def dot(a, b, dims):
    return lax.dot_general(a, b, (dims, ((), ())), preferred_element_type=F32)


def mm(a, b):
    return dot(a, b, ((1,), (0,)))


def mm_bt(a, b):
    return dot(a, b, ((1,), (1,)))


def mm_at(a, b):
    return dot(a, b, ((0,), (0,)))


def rope(first, second, cos_t, sin_t):
    return first * cos_t - second * sin_t, second * cos_t + first * sin_t


def layer_kernel(d_model, x_hbm, pos_hbm, freq_hbm, dy_hbm, gamma_hbm, wq_hbm, wg_hbm, wu_hbm, wk_hbm, wv_hbm, wo_hbm, wd_hbm,
                 y_o, dx_o, dgamma_ref, nrm_t, attn_v, md, dq_v, dkv_v, dy_v, tiles,
                 pos_ref, freq_ref, gamma_ref, nrm_v, x_v, wqkv_v, wg_v, wu_v, wo_v, wd_v,
                 keep, send, rcore, chip, rx, packed, dkv_part, dkv_rx, kv_acc,
                 xhat_v, inv_v, cos_v, sin_v, br_v, dh_v, y_snd, y_rx, dh_snd, dh_rx,
                 st_snd, st_rx, st_sum, bst_snd, bst_rx, factors,
                 ld_sem, cs, cr, xs, xr, gs, gr, ps, pr, ts, tr, ss, sr, ds, dr, early_snd, early_rx, es, er):
    tx = lax.axis_index('tx')
    ty = lax.axis_index('ty')
    core = lax.rem(tx, 2)
    near = {'tx': tx + 1 - 2 * core}
    across = {'tx': lax.rem(tx + 2, 4)}
    far = {'tx': lax.rem(tx + 1 - 2 * core + 2, 4)}
    other_ty = {'ty': 1 - ty}
    peers = [near, across, far, other_ty] + [{'tx': p['tx'], 'ty': 1 - ty} for p in (near, across, far)]
    close = peers[:5]
    n_tok = x_v.shape[0]
    half = n_tok // 2
    mine = pl.multiple_of(core * half, half)
    other = pl.multiple_of((1 - core) * half, half)
    head_dim = 256
    q_width = wo_v.shape[0]
    heads = q_width // head_dim

    def load(i, src, dst):
        return pltpu.make_async_copy(src, dst, ld_sem.at[i])

    loads = [
        load(0, dy_hbm.at[pl.ds(mine, half)], dy_v.at[0:half]),
        load(1, dy_hbm.at[pl.ds(other, half)], dy_v.at[half:n_tok]),
        load(2, wo_hbm.at[0:EARLY], wo_v.at[0:EARLY]),
        load(3, x_hbm.at[pl.ds(mine, half)], x_v.at[0:half]),
        load(4, x_hbm.at[pl.ds(other, half)], x_v.at[half:n_tok]),
        load(5, wd_hbm.at[0:CHUNK], wd_v.at[0:CHUNK]),
        load(6, wq_hbm, wqkv_v.at[:, 0:q_width]),
        load(7, wk_hbm, wqkv_v.at[:, q_width:q_width + head_dim]),
        load(8, wv_hbm, wqkv_v.at[:, q_width + head_dim:q_width + 2 * head_dim]),
        load(9, wg_hbm, wg_v),
        load(10, wu_hbm, wu_v),
        load(11, wd_hbm.at[CHUNK:4 * CHUNK], wd_v.at[CHUNK:4 * CHUNK]),
        load(12, gamma_hbm, gamma_ref),
        load(13, pos_hbm, pos_ref),
        load(14, freq_hbm, freq_ref),
        load(15, wo_hbm.at[BLK:q_width], wo_v.at[BLK:q_width]),
        load(16, wo_hbm.at[EARLY:BLK], wo_v.at[EARLY:BLK]),
    ]
    for i in (0, 1, 2, 16, 15, 3, 4, 5):
        loads[i].start()

    barrier = pltpu.get_barrier_semaphore()
    for peer in close:
        pl.semaphore_signal(barrier, inc=1, device_id=peer, device_id_type=MESH)
    for ld in loads[:3]:
        ld.wait()
    for i in (12, 6, 7, 8):
        loads[i].start()

    def remote(src, dst, send_sem, recv_sem, peer):
        return pltpu.make_async_remote_copy(src_ref=src, dst_ref=dst, send_sem=send_sem, recv_sem=recv_sem,
                                            device_id=peer, device_id_type=MESH)

    def core_copy(b):
        return remote(send.at[b], rcore.at[b], cs.at[b], cr.at[b], near)

    def x_copy(u):
        if u >= X_LAST:
            rows = pl.ds(*PIECES[u - X_LAST])
            return remote(chip.at[pl.ds(N_BLK - 2, 2), rows], rx.at[pl.ds(N_BLK - 2, 2), rows], xs.at[u], xr.at[u], across)
        if u == X_KV:
            cols = pl.ds(pl.multiple_of(ty * head_dim, head_dim), head_dim)
            return remote(chip.at[B_QKV + 2, :, cols], rx.at[B_QKV + 2, :, cols], xs.at[u], xr.at[u], across)
        if u == 0:
            return remote(chip.at[0, :, EARLY:BLK], rx.at[0, :, EARLY:BLK], xs.at[u], xr.at[u], across)
        start, count = X_UNITS[u]
        return remote(chip.at[pl.ds(start, count)], rx.at[pl.ds(start, count)], xs.at[u], xr.at[u], across)

    def put(b, part):
        keep[b] = part[:half]
        send[b] = part[half:].astype(BF16)
        core_copy(b).start()

    def issue_bwd(b, w_ref, row):
        put(b, mm_bt(dy_v[...], w_ref[pl.ds(row, BLK), :]))

    def issue_fwd(b, w_ref, col):
        put(b, mm(nrm_v[...], w_ref[:, pl.ds(col, BLK)]))

    def combine(b):
        core_copy(b).wait_recv()
        chip[b] = (keep[b] + rcore[b].astype(F32)).astype(BF16)

    def total(b):
        return chip[b].astype(F32) + rx[b].astype(F32)

    early_snd[...] = mm_bt(dy_v[...], wo_v[0:EARLY, :]).astype(BF16)
    pl.semaphore_wait(barrier, len(close))
    early = [remote(early_snd.at[0:half], early_rx.at[0], es.at[0], er.at[0], across),
             remote(early_snd.at[half:n_tok], early_rx.at[1], es.at[1], er.at[1], far)]
    for copy in early:
        copy.start()
    loads[16].wait()
    issue_bwd(0, wo_v, 0)
    loads[15].wait()
    issue_bwd(1, wo_v, BLK)

    def rows_of(col_a, col_b):
        lane = lax.broadcasted_iota(jnp.int32, (half, 128), 1)
        return jnp.where(lane == 0, col_a, col_b).T[0:8]

    def stats_copies(snd, got, base, to):
        return [remote(snd, got.at[i], ss.at[base + i], sr.at[base + i], peer) for i, peer in enumerate(to)]

    def stats_put(snd, col_a, col_b):
        for lo, at in ((0, mine), (half, other)):
            snd[:, pl.ds(at, half)] = rows_of(col_a[lo:lo + half], col_b[lo:lo + half])

    def stats_columns(rows_ref):
        cols = []
        for i in range(2):
            parts = [jnp.broadcast_to(rows_ref[i:i + 1, pl.ds(at, half)], (128, half)).T[:, 0:1] for at in (mine, other)]
            cols.append(jnp.concatenate(parts, axis=0))
        return cols

    loads[3].wait()
    loads[4].wait()
    for i in (9, 10, 11, 13, 14):
        loads[i].start()
    x_f = x_v[...].astype(F32)
    stats_put(st_snd, jnp.sum(x_f, axis=1, keepdims=True), jnp.sum(x_f * x_f, axis=1, keepdims=True))
    fwd_stats = stats_copies(st_snd, st_rx, 0, (near, across, far))
    for copy in fwd_stats:
        copy.start()

    combine(0)
    x_copy(0).start()
    combine(1)
    x_copy(1).start()

    loads[5].wait()
    for i in range(2):
        issue_bwd(B_DACT_LO + i, wd_v, i * BLK)
    for i in range(2):
        combine(B_DACT_LO + i)
    x_copy(2).start()

    loads[12].wait()
    for copy in fwd_stats:
        copy.wait_recv()
    st_sum[...] = (st_snd[...] + st_rx[0]) + (st_rx[1] + st_rx[2])
    sum_x, sum_xx = stats_columns(st_sum)
    tok_mean = sum_x / d_model
    inv_std = lax.rsqrt(sum_xx / d_model - tok_mean * tok_mean + EPS)
    inv_v[...] = jnp.broadcast_to(inv_std, (n_tok, 128))
    x_hat = (x_v[...].astype(F32) - tok_mean) * inv_std
    xhat_v[...] = x_hat
    nrm_v[...] = (x_hat * gamma_ref[...]).astype(BF16)

    for i in range(6, 9):
        loads[i].wait()
    for i in range(3):
        issue_fwd(B_QKV + i, wqkv_v, i * BLK)
    for i in (2, 0, 1):
        combine(B_QKV + i)
        if i == 2:
            x_copy(X_KV).start()
    x_copy(3).start()

    loads[9].wait()
    loads[10].wait()
    for k in range(4):
        def gu_issue(j, carry, k=k):
            col = pl.multiple_of(k * CHUNK + j * BLK, BLK)
            issue_fwd(B_GU + 4 * k + j, wg_v, col)
            issue_fwd(B_GU + 4 * k + 2 + j, wu_v, col)
            return carry

        def gu_combine(j, carry, k=k):
            combine(B_GU + 4 * k + j)
            return carry

        lax.fori_loop(0, 2, gu_issue, 0)
        lax.fori_loop(0, 4, gu_combine, 0)
        x_copy(4 + k).start()

    loads[11].wait()

    def hi_issue(j, carry):
        issue_bwd(B_DACT_HI + j, wd_v, pl.multiple_of(CHUNK + j * BLK, BLK))
        return carry

    lax.fori_loop(0, 6, hi_issue, 0)
    for j in range(6):
        combine(B_DACT_HI + j)
        if j == 1 or j == 3:
            x_copy(8 + j // 2).start()
    for r in range(SPLITS):
        x_copy(X_LAST + r).start()

    nrm_t[...] = nrm_v[...].T

    loads[13].wait()
    loads[14].wait()
    freq = freq_ref[...]
    for lo, at in ((0, mine), (half, other)):
        pos_col = jnp.broadcast_to(pos_ref[0:1, pl.ds(at, half)].astype(F32), (128, half)).T
        angles = pos_col * freq
        cos_v[lo:lo + half] = jnp.cos(angles)
        sin_v[lo:lo + half] = jnp.sin(angles)

    packed_copy = remote(packed.at[0:half], packed.at[half:n_tok], ps.at[0], pr.at[0], near)
    x_copy(0).wait_recv()
    x_copy(1).wait_recv()
    for copy in early:
        copy.wait_recv()
    rx[0, :, 0:EARLY] = (early_rx[0].astype(F32) + early_rx[1].astype(F32)).astype(BF16)
    for j in range(2):
        packed[0:half, q_width + 512 + j * BLK:q_width + 512 + (j + 1) * BLK] = total(B_DATTN + j).astype(BF16)
    x_copy(3).wait_recv()
    cos_h, sin_h = cos_v[0:half], sin_v[0:half]
    for j in range(2):
        blk = total(B_QKV + j)
        for h in range(2):
            lo = h * head_dim
            first, second = rope(blk[:, lo:lo + 128], blk[:, lo + 128:lo + 256], cos_h, sin_h)
            packed[0:half, j * BLK + lo:j * BLK + lo + 128] = first.astype(BF16)
            packed[0:half, j * BLK + lo + 128:j * BLK + lo + 256] = second.astype(BF16)
    x_copy(X_KV).wait_recv()
    kv_cols = pl.ds(pl.multiple_of(ty * head_dim, head_dim), head_dim)
    blk = chip[B_QKV + 2, :, kv_cols].astype(F32) + rx[B_QKV + 2, :, kv_cols].astype(F32)
    first, second = rope(blk[:, 0:128], blk[:, 128:256], cos_h, sin_h)
    kv_mine = jnp.where(ty == 0, jnp.concatenate([first, second], axis=1), blk).astype(BF16)
    kv_dst = packed.at[0:half, pl.ds(pl.multiple_of(q_width + ty * head_dim, head_dim), head_dim)]
    kv_dst[...] = kv_mine
    kv_copy = remote(kv_dst, kv_dst, ts.at[3], tr.at[3], other_ty)
    kv_copy.start()
    kv_copy.wait_recv()
    packed_copy.start()
    packed_copy.wait_recv()

    row_i = lax.rem(lax.broadcasted_iota(jnp.int32, (n_tok, n_tok), 0) + core * half, n_tok)
    col_i = lax.rem(lax.broadcasted_iota(jnp.int32, (n_tok, n_tok), 1) + core * half, n_tok)
    scale = head_dim ** -0.5
    kv_acc[...] = jnp.zeros_like(kv_acc)

    def head_step(h, carry):
        cols = pl.ds(pl.multiple_of(h * head_dim, head_dim), head_dim)
        q_h = packed[:, cols]
        da_h = packed[:, pl.ds(pl.multiple_of(q_width + 512 + h * head_dim, head_dim), head_dim)]
        k_rot = packed[:, q_width:q_width + 256]
        v_val = packed[:, q_width + 256:q_width + 512]
        scores = jnp.where(row_i >= col_i, mm_bt(q_h, k_rot) * scale, -1e30)
        exps = jnp.exp(scores - jnp.max(scores, axis=1, keepdims=True))
        probs_f = exps / jnp.sum(exps, axis=1, keepdims=True)
        probs = probs_f.astype(BF16)
        attn_v[:, cols] = mm(probs, v_val).astype(BF16)
        d_probs = mm_bt(da_h, v_val).astype(BF16).astype(F32)
        d_scores = (probs_f * (d_probs - jnp.sum(d_probs * probs_f, axis=1, keepdims=True)) * scale).astype(BF16)
        dq_h = mm(d_scores, k_rot).astype(BF16).astype(F32)
        first, second = rope(dq_h[:, 0:128], dq_h[:, 128:256], cos_v[...], -sin_v[...])
        dq_v[:, pl.ds(pl.multiple_of(h * head_dim, head_dim), 128)] = first.astype(BF16)
        dq_v[:, pl.ds(pl.multiple_of(h * head_dim + 128, 128), 128)] = second.astype(BF16)
        kv_acc[:, 0:256] += mm_at(d_scores, q_h)
        kv_acc[:, 256:512] += mm_at(probs, da_h)
        return carry

    lax.fori_loop(0, heads, head_step, 0)
    dkv_part[...] = kv_acc[...].astype(BF16)
    dkv_copy = remote(dkv_part, dkv_rx, ts.at[0], tr.at[0], other_ty)
    dkv_copy.start()
    br_v[...] = mm(attn_v[...], wo_v[...])
    dh_v[...] = mm_bt(dq_v[...], wqkv_v[:, 0:q_width])

    for j in range(2):
        tiles[j] = mm(nrm_t[...], dq_v[:, j * BLK:(j + 1) * BLK])
        tiles[2 + j] = mm_at(attn_v[:, j * BLK:(j + 1) * BLK], dy_v[...])

    def piece_copy(r):
        lo, size = PIECES[r]
        return remote(md.at[3, 1:3, lo:lo + size], md.at[3, 1:3, half + lo:half + lo + size], gs.at[12 + r], gr.at[12 + r], near)

    def gather_copy(k, i):
        return remote(md.at[k, i, 0:half], md.at[k, i, half:n_tok], gs.at[3 * k + i], gr.at[3 * k + i], near)

    def dact_block(k, j):
        return B_DACT_LO + j if k == 0 else B_DACT_HI + 2 * (k - 1) + j

    def gated(k, want_act, want_grad):
        def step(r, carry):
            rows = pl.ds(pl.multiple_of(r * 16, 16), 16)
            for j in range(2):
                bg, bu, bd = B_GU + 4 * k + j, B_GU + 4 * k + 2 + j, dact_block(k, j)
                gate = (chip[bg, rows].astype(F32) + rx[bg, rows].astype(F32)).astype(BF16).astype(F32)
                up = (chip[bu, rows].astype(F32) + rx[bu, rows].astype(F32)).astype(BF16).astype(F32)
                sig = jax.nn.sigmoid(gate)
                silu = gate * sig
                cols = slice(j * BLK, (j + 1) * BLK)
                if want_act:
                    md[k, 0, rows, cols] = (silu * up).astype(BF16)
                if k >= 2:
                    factors[k - 2, 0, rows, cols] = up * sig * (1.0 + gate * (1.0 - sig))
                    factors[k - 2, 1, rows, cols] = silu
                if want_grad:
                    d_act = (chip[bd, rows].astype(F32) + rx[bd, rows].astype(F32)).astype(BF16).astype(F32)
                    md[k, 1, rows, cols] = (d_act * up * sig * (1.0 + gate * (1.0 - sig))).astype(BF16)
                    md[k, 2, rows, cols] = (d_act * silu).astype(BF16)
            return carry

        lax.fori_loop(0, half // 16, step, 0)
        for i in ((0,) if want_act else ()) + ((1, 2) if want_grad else ()):
            gather_copy(k, i).start()

    def use_act(k):
        gather_copy(k, 0).wait_recv()
        br_v[...] += mm(md[k, 0], wd_v[k * CHUNK:(k + 1) * CHUNK, :])

    def use_grad(k):
        for i in (1, 2):
            gather_copy(k, i).wait_recv()
        dh_v[...] += (mm_bt(md[k, 1], wg_v[:, k * CHUNK:(k + 1) * CHUNK])
                      + mm_bt(md[k, 2], wu_v[:, k * CHUNK:(k + 1) * CHUNK]))

    x_copy(2).wait_recv()
    for k in range(4):
        x_copy(4 + k).wait_recv()
        gated(k, True, k == 0)
        use_act(k)
        if k == 0:
            use_grad(0)
            dkv_copy.wait_recv()
            d_k = dkv_part[:, 0:256].astype(F32) + dkv_rx[:, 0:256].astype(F32)
            d_k = d_k.astype(BF16).astype(F32)
            first, second = rope(d_k[:, 0:128], d_k[:, 128:256], cos_v[...], -sin_v[...])
            dkv_v[:, 0:128] = first.astype(BF16)
            dkv_v[:, 128:256] = second.astype(BF16)
            dkv_v[:, 256:512] = (dkv_part[:, 256:512].astype(F32) + dkv_rx[:, 256:512].astype(F32)).astype(BF16)
            dh_v[...] += 0.5 * mm_bt(dkv_v[...], wqkv_v[:, q_width:q_width + 512])
            tiles[4] = mm(nrm_t[...], dkv_v[...])
            for j in range(2):
                tiles[5 + j] = mm_at(md[0, 0, :, j * BLK:(j + 1) * BLK], dy_v[...])
    y_snd[...] = br_v[...].astype(BF16)
    y_copy = remote(y_snd, y_rx, ts.at[1], tr.at[1], other_ty)
    y_copy.start()
    x_copy(8).wait_recv()
    gated(1, False, True)
    use_grad(1)
    x_copy(9).wait_recv()

    def scaled(k, rows):
        for j in range(2):
            cols = slice(j * BLK, (j + 1) * BLK)
            b = dact_block(k, j)
            d_act = (chip[b, rows].astype(F32) + rx[b, rows].astype(F32)).astype(BF16).astype(F32)
            for i in range(2):
                md[k, 1 + i, rows, cols] = (d_act * factors[k - 2, i, rows, cols]).astype(BF16)

    def scaled_step(r, carry):
        scaled(2, pl.ds(pl.multiple_of(r * 32, 32), 32))
        return carry

    lax.fori_loop(0, half // 32, scaled_step, 0)
    for i in (1, 2):
        gather_copy(2, i).start()

    def dh_copy(r):
        at = pl.ds(2 * PIECES[r][0], 2 * PIECES[r][1])
        return remote(dh_snd.at[at], dh_rx.at[at], ds.at[r], dr.at[r], other_ty)

    def both(ref, r):
        lo, size = PIECES[r]
        return jnp.concatenate([ref[lo:lo + size], ref[half + lo:half + lo + size]], axis=0)

    sums = []

    def piece_grad(r):
        x_copy(X_LAST + r).wait_recv()
        scaled(3, slice(PIECES[r][0], PIECES[r][0] + PIECES[r][1]))
        piece_copy(r).start()

    def piece_dh(r):
        piece_copy(r).wait_recv()
        part = both(dh_v, r) + mm_bt(both(md.at[3, 1], r), wg_v[:, 3 * CHUNK:4 * CHUNK]) + mm_bt(both(md.at[3, 2], r), wu_v[:, 3 * CHUNK:4 * CHUNK])
        part_b = part.astype(BF16)
        dh_snd[2 * PIECES[r][0]:2 * (PIECES[r][0] + PIECES[r][1])] = part_b
        dh_copy(r).start()
        d_hat = part_b.astype(F32) * gamma_ref[...]
        sums.append((jnp.sum(d_hat, axis=1, keepdims=True), jnp.sum(d_hat * both(xhat_v, r), axis=1, keepdims=True)))

    piece_grad(0)
    use_grad(2)
    for r in range(1, SPLITS):
        piece_grad(r)
        piece_dh(r - 1)
    piece_dh(SPLITS - 1)
    cols = [jnp.concatenate([sums[r][i][:PIECES[r][1]] for r in range(SPLITS)] + [sums[r][i][PIECES[r][1]:] for r in range(SPLITS)], axis=0) for i in range(2)]
    stats_put(bst_snd, cols[0], cols[1])
    bwd_stats = stats_copies(bst_snd, bst_rx, 3, peers)
    for copy in bwd_stats:
        copy.start()

    y_copy.wait_recv()
    y_o[...] = (x_v[...].astype(F32) + (y_snd[...].astype(F32) + y_rx[...].astype(F32))).astype(BF16)

    def drain(b, carry):
        core_copy(b).wait_send()
        return carry

    lax.fori_loop(0, N_BLK, drain, 0)
    for u in range(N_X):
        x_copy(u).wait_send()
    for k in range(4):
        for i in range(3 if k < 3 else 1):
            gather_copy(k, i).wait_send()
    for r in range(SPLITS):
        piece_copy(r).wait_send()
    for copy in [packed_copy, dkv_copy, y_copy, kv_copy] + early + fwd_stats:
        copy.wait_send()

    br_v[...] = inv_v[:, 0:1] * xhat_v[...]
    d_gamma = jnp.zeros_like(dgamma_ref)
    for r in range(SPLITS):
        dh_copy(r).wait_recv()
        lo, size = PIECES[r]
        d_nrm = dh_snd[2 * lo:2 * (lo + size)].astype(F32) + dh_rx[2 * lo:2 * (lo + size)].astype(F32)
        d_gamma = d_gamma + jnp.sum(d_nrm * both(xhat_v, r), axis=0, keepdims=True)
        base = both(dy_v, r).astype(F32) + both(inv_v, r)[:, 0:1] * (d_nrm * gamma_ref[...])
        dh_v[lo:lo + size] = base[:size]
        dh_v[half + lo:half + lo + size] = base[size:]
    dgamma_ref[...] = d_gamma
    for copy in bwd_stats:
        copy.wait_recv()
    st_sum[...] = ((bst_snd[...] + bst_rx[0]) + (bst_rx[1] + bst_rx[2])) + ((bst_rx[3] + bst_rx[4]) + (bst_rx[5] + bst_rx[6]))
    sum_d, sum_dx = stats_columns(st_sum)
    d_x = dh_v[...] - inv_v[:, 0:1] * (sum_d / d_model) - br_v[...] * (sum_dx / d_model)
    dx_o[...] = d_x.astype(BF16)

    for r in range(SPLITS):
        dh_copy(r).wait_send()
    for copy in bwd_stats:
        copy.wait_send()


def grad_kernel(y_v, dx_v, dgamma_in, nrm_t, attn_v, md, dq_v, dkv_v, dy_v, tiles,
                y_hbm, dx_hbm, dgamma_hbm, dwq_hbm, dwg_hbm, dwu_hbm, dwk_hbm, dwv_hbm, dwo_hbm, dwd_hbm,
                ring, wide, out_sem, cp_sem):
    width, n_tok = nrm_t.shape
    half = n_tok // 2
    core = lax.rem(lax.axis_index('tx'), 2)
    mine = pl.multiple_of(core * half, half)
    other = pl.multiple_of((1 - core) * half, half)
    hand_out = [pltpu.make_async_copy(src.at[lo:lo + half], dst.at[pl.ds(at, half)], cp_sem.at[i])
                for i, (src, dst, lo, at) in enumerate(((y_v, y_hbm, 0, mine), (y_v, y_hbm, half, other), (dx_v, dx_hbm, 0, mine), (dx_v, dx_hbm, half, other)))]
    for cp in hand_out:
        cp.start()
    hand_out.append(pltpu.make_async_copy(dgamma_in, dgamma_hbm, cp_sem.at[12]))
    hand_out[-1].start()

    ready = [(0, dwq_hbm.at[:, 0:BLK]), (1, dwq_hbm.at[:, BLK:2 * BLK]), (2, dwo_hbm.at[0:BLK, :]), (3, dwo_hbm.at[BLK:2 * BLK, :]),
             (5, dwd_hbm.at[0:BLK, :]), (6, dwd_hbm.at[BLK:2 * BLK, :])]
    ready = [(tiles.at[i], dst) for i, dst in ready] + [(tiles.at[4, :, 0:256], dwk_hbm), (tiles.at[4, :, 256:512], dwv_hbm)]
    for i, (src, dst) in enumerate(ready):
        hand_out.append(pltpu.make_async_copy(src, dst, cp_sem.at[4 + i]))
        hand_out[-1].start(priority=len(hand_out) % 2)

    def put(src, dst, i):
        hand_out.append(pltpu.make_async_copy(src, dst, out_sem.at[i]))
        hand_out[-1].start(priority=len(hand_out) % 2)

    for t in range(6):
        k, j = 1 + t // 2, t % 2
        ring[t] = mm_at(md[k, 0, :, j * BLK:(j + 1) * BLK], dy_v[...])
        put(ring.at[t], dwd_hbm.at[k * CHUNK + j * BLK:k * CHUNK + (j + 1) * BLK, :], t)
    n_row = 128
    for i, (out, at) in enumerate(((dwg_hbm, 6), (dwu_hbm, 10))):
        for k in range(4):
            for j in range(2):
                lo = k * CHUNK + j * BLK
                wide[i, :, lo:lo + BLK] = mm(nrm_t[...], md[k, 1 + i, :, j * BLK:(j + 1) * BLK])
        for r in range(width // n_row):
            put(wide.at[i, r * n_row:(r + 1) * n_row], out.at[r * n_row:(r + 1) * n_row], at + r)
    for cp in hand_out:
        cp.wait()


def solution(mesh):
    tx_size = mesh.shape['tx']
    tok_spec = P('dp', None, 'tx')
    in_specs = (tok_spec, P('dp', None), tok_spec, P('tx'), P('tx', 'ty'), P('tx', 'ty'), P('tx', 'ty'),
                P('tx', None), P('tx', None), P('ty', 'tx'), P('ty', 'tx'))
    out_specs = (tok_spec, tok_spec, P(('dp', 'tx')), P(('dp', 'tx'), 'ty'), P(('dp', 'tx'), 'ty'), P(('dp', 'tx'), 'ty'),
                 P(('dp', 'tx'), None), P(('dp', 'tx'), None), P(('dp', 'ty'), 'tx'), P(('dp', 'ty'), 'tx'))

    def local_layer(x_in, positions, d_y, ln_gamma, w_q, w_g, w_u, w_k, w_v, w_o, w_d):
        _, n_tok, d_local = x_in.shape
        half = n_tok // 2
        d_model = d_local * tx_size
        head_dim = w_k.shape[1]
        q_width = w_q.shape[1]
        d_ff = w_g.shape[1]
        freq = jnp.asarray((ROPE_BASE ** (-2.0 * np.arange(head_dim // 2) / head_dim)).astype(np.float32)[None])
        any_spec = pl.BlockSpec(memory_space=pl.ANY)
        vmem_spec = pl.BlockSpec(memory_space=pltpu.VMEM)
        tok = (n_tok, d_local)
        sem = pltpu.SemaphoreType.DMA
        vm = pltpu.VMEM
        kept = pl.pallas_call(
            functools.partial(layer_kernel, d_model),
            out_shape=[vm(tok, BF16), vm(tok, BF16), vm((1, d_local), F32), vm((d_local, n_tok), BF16), vm((n_tok, q_width), BF16),
                       vm((4, 3, n_tok, CHUNK), BF16), vm((n_tok, q_width), BF16), vm((n_tok, 2 * head_dim), BF16), vm(tok, BF16),
                       vm((7, BLK, BLK), F32)],
            in_specs=[any_spec] * 12,
            out_specs=[vmem_spec] * 10,
            scratch_shapes=[
                vm((1, n_tok), jnp.int32), vm((1, head_dim // 2), F32), vm((1, d_local), F32), vm(tok, BF16),
                vm(tok, BF16), vm((d_local, q_width + 2 * head_dim), BF16), vm((d_local, d_ff), BF16), vm((d_local, d_ff), BF16),
                vm((q_width, d_local), BF16), vm((d_ff, d_local), BF16),
                vm((N_BLK, half, BLK), F32), vm((N_BLK, half, BLK), BF16), vm((N_BLK, half, BLK), BF16),
                vm((N_BLK, half, BLK), BF16), vm((N_BLK, half, BLK), BF16), vm((n_tok, 2 * q_width + 2 * head_dim), BF16),
                vm((n_tok, 512), BF16), vm((n_tok, 512), BF16), vm((n_tok, 512), F32),
                vm(tok, F32), vm((n_tok, 128), F32), vm((n_tok, 128), F32), vm((n_tok, 128), F32), vm(tok, F32), vm(tok, F32),
                vm(tok, BF16), vm(tok, BF16), vm(tok, BF16), vm(tok, BF16),
                vm((8, n_tok), F32), vm((3, 8, n_tok), F32), vm((8, n_tok), F32), vm((8, n_tok), F32), vm((7, 8, n_tok), F32), vm((2, 2, half, CHUNK), F32),
                sem((17,)), sem((N_BLK,)), sem((N_BLK,)), sem((N_X,)), sem((N_X,)),
                sem((12 + SPLITS,)), sem((12 + SPLITS,)), sem((1,)), sem((1,)), sem((4,)), sem((4,)), sem((10,)), sem((10,)),
                sem((SPLITS,)), sem((SPLITS,)), vm((n_tok, EARLY), BF16), vm((2, half, EARLY), BF16), sem((2,)), sem((2,))],
            compiler_params=pltpu.CompilerParams(collective_id=0, has_side_effects=True, vmem_limit_bytes=47 * 1024 * 1024),
            name='layer',
        )(x_in.reshape(tok), positions, freq, d_y.reshape(tok), ln_gamma[None], w_q, w_g, w_u, w_k, w_v, w_o, w_d)

        y_out, d_x, d_gamma, d_wq, d_wg, d_wu, d_wk, d_wv, d_wo, d_wd = pl.pallas_call(
            grad_kernel,
            out_shape=[jax.ShapeDtypeStruct(tok, BF16), jax.ShapeDtypeStruct(tok, BF16), jax.ShapeDtypeStruct((1, d_local), F32)]
            + [jax.ShapeDtypeStruct(w.shape, F32) for w in (w_q, w_g, w_u, w_k, w_v, w_o, w_d)],
            in_specs=[vmem_spec] * 10,
            out_specs=[any_spec] * 10,
            scratch_shapes=[vm((6, d_local, BLK), F32), vm((2, d_local, d_ff), F32), sem((14,)), sem((13,))],
            compiler_params=pltpu.CompilerParams(vmem_limit_bytes=30 * 1024 * 1024),
            name='weight_grads',
        )(*kept)
        return (y_out.reshape(x_in.shape), d_x.reshape(x_in.shape), d_gamma.reshape(d_local),
                d_wq, d_wg, d_wu, d_wk, d_wv, d_wo, d_wd)

    return jax.shard_map(local_layer, mesh=mesh, in_specs=in_specs, out_specs=out_specs, check_vma=False)
```

```python
import functools

import jax
import jax.numpy as jnp
import numpy as np
from jax import lax
from jax.experimental import pallas as pl
from jax.experimental.pallas import tpu as pltpu
from jax.sharding import PartitionSpec as P

EPS = 1e-6
ROPE_BASE = 10000.0
F32 = jnp.float32
BF16 = jnp.bfloat16
MESH = pl.DeviceIdType.MESH

BLK = 512
CHUNK = 1024
B_DATTN, B_DACT_LO, B_QKV, B_GU, B_DACT_HI, N_BLK = 0, 2, 4, 7, 23, 29
X_UNITS = ((0, 1), (1, 1), (2, 2), (4, 2), (7, 4), (11, 4), (15, 4), (19, 4), (23, 2), (25, 2))
PIECES = ((0, 32), (32, 32), (64, 32), (96, 32))
SPLITS = len(PIECES)
EARLY = 128
X_KV = len(X_UNITS)
X_LAST = X_KV + 1
N_X = X_LAST + SPLITS


def dot(a, b, dims):
    return lax.dot_general(a, b, (dims, ((), ())), preferred_element_type=F32)


def mm(a, b):
    return dot(a, b, ((1,), (0,)))


def mm_bt(a, b):
    return dot(a, b, ((1,), (1,)))


def mm_at(a, b):
    return dot(a, b, ((0,), (0,)))


def rope(first, second, cos_t, sin_t):
    return first * cos_t - second * sin_t, second * cos_t + first * sin_t


def layer_kernel(d_model, x_hbm, pos_hbm, freq_hbm, dy_hbm, gamma_hbm, wq_hbm, wg_hbm, wu_hbm, wk_hbm, wv_hbm, wo_hbm, wd_hbm,
                 y_o, dx_o, dgamma_ref, nrm_t, attn_v, md, dq_v, dkv_v, dy_v, tiles,
                 pos_ref, freq_ref, gamma_ref, nrm_v, x_v, wqkv_v, wg_v, wu_v, wo_v, wd_v,
                 keep, send, rcore, chip, rx, packed, dkv_part, dkv_rx, kv_acc,
                 xhat_v, inv_v, cos_v, sin_v, br_v, dh_v, y_snd, y_rx, dh_snd, dh_rx,
                 st_snd, st_rx, st_sum, bst_snd, bst_rx, factors,
                 ld_sem, cs, cr, xs, xr, gs, gr, ps, pr, ts, tr, ss, sr, ds, dr, early_snd, early_rx, es, er):
    tx = lax.axis_index('tx')
    ty = lax.axis_index('ty')
    core = lax.rem(tx, 2)
    near = {'tx': tx + 1 - 2 * core}
    across = {'tx': lax.rem(tx + 2, 4)}
    far = {'tx': lax.rem(tx + 1 - 2 * core + 2, 4)}
    other_ty = {'ty': 1 - ty}
    peers = [near, across, far, other_ty] + [{'tx': p['tx'], 'ty': 1 - ty} for p in (near, across, far)]
    close = peers[:5]
    n_tok = x_v.shape[0]
    half = n_tok // 2
    mine = pl.multiple_of(core * half, half)
    other = pl.multiple_of((1 - core) * half, half)
    head_dim = 256
    q_width = wo_v.shape[0]
    heads = q_width // head_dim

    def load(i, src, dst):
        return pltpu.make_async_copy(src, dst, ld_sem.at[i])

    loads = [
        load(0, dy_hbm.at[pl.ds(mine, half)], dy_v.at[0:half]),
        load(1, dy_hbm.at[pl.ds(other, half)], dy_v.at[half:n_tok]),
        load(2, wo_hbm.at[0:EARLY], wo_v.at[0:EARLY]),
        load(3, x_hbm.at[pl.ds(mine, half)], x_v.at[0:half]),
        load(4, x_hbm.at[pl.ds(other, half)], x_v.at[half:n_tok]),
        load(5, wd_hbm.at[0:CHUNK], wd_v.at[0:CHUNK]),
        load(6, wq_hbm, wqkv_v.at[:, 0:q_width]),
        load(7, wk_hbm, wqkv_v.at[:, q_width:q_width + head_dim]),
        load(8, wv_hbm, wqkv_v.at[:, q_width + head_dim:q_width + 2 * head_dim]),
        load(9, wg_hbm, wg_v),
        load(10, wu_hbm, wu_v),
        load(11, wd_hbm.at[CHUNK:4 * CHUNK], wd_v.at[CHUNK:4 * CHUNK]),
        load(12, gamma_hbm, gamma_ref),
        load(13, pos_hbm, pos_ref),
        load(14, freq_hbm, freq_ref),
        load(15, wo_hbm.at[BLK:q_width], wo_v.at[BLK:q_width]),
        load(16, wo_hbm.at[EARLY:BLK], wo_v.at[EARLY:BLK]),
    ]
    for i in (0, 1, 2, 16, 15, 3, 4, 5):
        loads[i].start()

    barrier = pltpu.get_barrier_semaphore()
    for peer in close:
        pl.semaphore_signal(barrier, inc=1, device_id=peer, device_id_type=MESH)
    for ld in loads[:3]:
        ld.wait()
    for i in (12, 6, 7, 8):
        loads[i].start()

    def remote(src, dst, send_sem, recv_sem, peer):
        return pltpu.make_async_remote_copy(src_ref=src, dst_ref=dst, send_sem=send_sem, recv_sem=recv_sem,
                                            device_id=peer, device_id_type=MESH)

    def core_copy(b):
        return remote(send.at[b], rcore.at[b], cs.at[b], cr.at[b], near)

    def x_copy(u):
        if u >= X_LAST:
            rows = pl.ds(*PIECES[u - X_LAST])
            return remote(chip.at[pl.ds(N_BLK - 2, 2), rows], rx.at[pl.ds(N_BLK - 2, 2), rows], xs.at[u], xr.at[u], across)
        if u == X_KV:
            cols = pl.ds(pl.multiple_of(ty * head_dim, head_dim), head_dim)
            return remote(chip.at[B_QKV + 2, :, cols], rx.at[B_QKV + 2, :, cols], xs.at[u], xr.at[u], across)
        if u == 0:
            return remote(chip.at[0, :, EARLY:BLK], rx.at[0, :, EARLY:BLK], xs.at[u], xr.at[u], across)
        start, count = X_UNITS[u]
        return remote(chip.at[pl.ds(start, count)], rx.at[pl.ds(start, count)], xs.at[u], xr.at[u], across)

    def put(b, part):
        keep[b] = part[:half]
        send[b] = part[half:].astype(BF16)
        core_copy(b).start()

    def issue_bwd(b, w_ref, row):
        put(b, mm_bt(dy_v[...], w_ref[pl.ds(row, BLK), :]))

    def issue_fwd(b, w_ref, col):
        put(b, mm(nrm_v[...], w_ref[:, pl.ds(col, BLK)]))

    def combine(b):
        core_copy(b).wait_recv()
        chip[b] = (keep[b] + rcore[b].astype(F32)).astype(BF16)

    def total(b):
        return chip[b].astype(F32) + rx[b].astype(F32)

    early_snd[...] = mm_bt(dy_v[...], wo_v[0:EARLY, :]).astype(BF16)
    pl.semaphore_wait(barrier, len(close))
    early = [remote(early_snd.at[0:half], early_rx.at[0], es.at[0], er.at[0], across),
             remote(early_snd.at[half:n_tok], early_rx.at[1], es.at[1], er.at[1], far)]
    for copy in early:
        copy.start()
    loads[16].wait()
    issue_bwd(0, wo_v, 0)
    loads[15].wait()
    issue_bwd(1, wo_v, BLK)

    def rows_of(col_a, col_b):
        lane = lax.broadcasted_iota(jnp.int32, (half, 128), 1)
        return jnp.where(lane == 0, col_a, col_b).T[0:8]

    def stats_copies(snd, got, base, to):
        return [remote(snd, got.at[i], ss.at[base + i], sr.at[base + i], peer) for i, peer in enumerate(to)]

    def stats_put(snd, col_a, col_b):
        for lo, at in ((0, mine), (half, other)):
            snd[:, pl.ds(at, half)] = rows_of(col_a[lo:lo + half], col_b[lo:lo + half])

    def stats_columns(rows_ref):
        cols = []
        for i in range(2):
            parts = [jnp.broadcast_to(rows_ref[i:i + 1, pl.ds(at, half)], (128, half)).T[:, 0:1] for at in (mine, other)]
            cols.append(jnp.concatenate(parts, axis=0))
        return cols

    loads[3].wait()
    loads[4].wait()
    for i in (9, 10, 11, 13, 14):
        loads[i].start()
    x_f = x_v[...].astype(F32)
    stats_put(st_snd, jnp.sum(x_f, axis=1, keepdims=True), jnp.sum(x_f * x_f, axis=1, keepdims=True))
    fwd_stats = stats_copies(st_snd, st_rx, 0, (near, across, far))
    for copy in fwd_stats:
        copy.start()

    combine(0)
    x_copy(0).start()
    combine(1)
    x_copy(1).start()

    loads[5].wait()
    for i in range(2):
        issue_bwd(B_DACT_LO + i, wd_v, i * BLK)
    for i in range(2):
        combine(B_DACT_LO + i)
    x_copy(2).start()

    loads[12].wait()
    for copy in fwd_stats:
        copy.wait_recv()
    st_sum[...] = (st_snd[...] + st_rx[0]) + (st_rx[1] + st_rx[2])
    sum_x, sum_xx = stats_columns(st_sum)
    tok_mean = sum_x / d_model
    inv_std = lax.rsqrt(sum_xx / d_model - tok_mean * tok_mean + EPS)
    inv_v[...] = jnp.broadcast_to(inv_std, (n_tok, 128))
    x_hat = (x_v[...].astype(F32) - tok_mean) * inv_std
    xhat_v[...] = x_hat
    nrm_v[...] = (x_hat * gamma_ref[...]).astype(BF16)

    for i in range(6, 9):
        loads[i].wait()
    for i in range(3):
        issue_fwd(B_QKV + i, wqkv_v, i * BLK)
    for i in (2, 0, 1):
        combine(B_QKV + i)
        if i == 2:
            x_copy(X_KV).start()
    x_copy(3).start()

    loads[9].wait()
    loads[10].wait()
    for k in range(4):
        def gu_issue(j, carry, k=k):
            col = pl.multiple_of(k * CHUNK + j * BLK, BLK)
            issue_fwd(B_GU + 4 * k + j, wg_v, col)
            issue_fwd(B_GU + 4 * k + 2 + j, wu_v, col)
            return carry

        def gu_combine(j, carry, k=k):
            combine(B_GU + 4 * k + j)
            return carry

        lax.fori_loop(0, 2, gu_issue, 0)
        lax.fori_loop(0, 4, gu_combine, 0)
        x_copy(4 + k).start()

    loads[11].wait()

    def hi_issue(j, carry):
        issue_bwd(B_DACT_HI + j, wd_v, pl.multiple_of(CHUNK + j * BLK, BLK))
        return carry

    lax.fori_loop(0, 6, hi_issue, 0)
    for j in range(6):
        combine(B_DACT_HI + j)
        if j == 1 or j == 3:
            x_copy(8 + j // 2).start()
    for r in range(SPLITS):
        x_copy(X_LAST + r).start()

    nrm_t[...] = nrm_v[...].T

    loads[13].wait()
    loads[14].wait()
    freq = freq_ref[...]
    for lo, at in ((0, mine), (half, other)):
        pos_col = jnp.broadcast_to(pos_ref[0:1, pl.ds(at, half)].astype(F32), (128, half)).T
        angles = pos_col * freq
        cos_v[lo:lo + half] = jnp.cos(angles)
        sin_v[lo:lo + half] = jnp.sin(angles)

    packed_copy = remote(packed.at[0:half], packed.at[half:n_tok], ps.at[0], pr.at[0], near)
    x_copy(0).wait_recv()
    x_copy(1).wait_recv()
    for copy in early:
        copy.wait_recv()
    rx[0, :, 0:EARLY] = (early_rx[0].astype(F32) + early_rx[1].astype(F32)).astype(BF16)
    for j in range(2):
        packed[0:half, q_width + 512 + j * BLK:q_width + 512 + (j + 1) * BLK] = total(B_DATTN + j).astype(BF16)
    x_copy(3).wait_recv()
    cos_h, sin_h = cos_v[0:half], sin_v[0:half]
    for j in range(2):
        blk = total(B_QKV + j)
        for h in range(2):
            lo = h * head_dim
            first, second = rope(blk[:, lo:lo + 128], blk[:, lo + 128:lo + 256], cos_h, sin_h)
            packed[0:half, j * BLK + lo:j * BLK + lo + 128] = first.astype(BF16)
            packed[0:half, j * BLK + lo + 128:j * BLK + lo + 256] = second.astype(BF16)
    x_copy(X_KV).wait_recv()
    kv_cols = pl.ds(pl.multiple_of(ty * head_dim, head_dim), head_dim)
    blk = chip[B_QKV + 2, :, kv_cols].astype(F32) + rx[B_QKV + 2, :, kv_cols].astype(F32)
    first, second = rope(blk[:, 0:128], blk[:, 128:256], cos_h, sin_h)
    kv_mine = jnp.where(ty == 0, jnp.concatenate([first, second], axis=1), blk).astype(BF16)
    kv_dst = packed.at[0:half, pl.ds(pl.multiple_of(q_width + ty * head_dim, head_dim), head_dim)]
    kv_dst[...] = kv_mine
    kv_copy = remote(kv_dst, kv_dst, ts.at[3], tr.at[3], other_ty)
    kv_copy.start()
    kv_copy.wait_recv()
    packed_copy.start()
    packed_copy.wait_recv()

    row_i = lax.rem(lax.broadcasted_iota(jnp.int32, (n_tok, n_tok), 0) + core * half, n_tok)
    col_i = lax.rem(lax.broadcasted_iota(jnp.int32, (n_tok, n_tok), 1) + core * half, n_tok)
    scale = head_dim ** -0.5
    kv_acc[...] = jnp.zeros_like(kv_acc)

    def head_step(h, carry):
        cols = pl.ds(pl.multiple_of(h * head_dim, head_dim), head_dim)
        q_h = packed[:, cols]
        da_h = packed[:, pl.ds(pl.multiple_of(q_width + 512 + h * head_dim, head_dim), head_dim)]
        k_rot = packed[:, q_width:q_width + 256]
        v_val = packed[:, q_width + 256:q_width + 512]
        scores = jnp.where(row_i >= col_i, mm_bt(q_h, k_rot) * scale, -1e30)
        exps = jnp.exp(scores - jnp.max(scores, axis=1, keepdims=True))
        probs_f = exps / jnp.sum(exps, axis=1, keepdims=True)
        probs = probs_f.astype(BF16)
        attn_v[:, cols] = mm(probs, v_val).astype(BF16)
        d_probs = mm_bt(da_h, v_val).astype(BF16).astype(F32)
        d_scores = (probs_f * (d_probs - jnp.sum(d_probs * probs_f, axis=1, keepdims=True)) * scale).astype(BF16)
        dq_h = mm(d_scores, k_rot).astype(BF16).astype(F32)
        first, second = rope(dq_h[:, 0:128], dq_h[:, 128:256], cos_v[...], -sin_v[...])
        dq_v[:, pl.ds(pl.multiple_of(h * head_dim, head_dim), 128)] = first.astype(BF16)
        dq_v[:, pl.ds(pl.multiple_of(h * head_dim + 128, 128), 128)] = second.astype(BF16)
        kv_acc[:, 0:256] += mm_at(d_scores, q_h)
        kv_acc[:, 256:512] += mm_at(probs, da_h)
        return carry

    lax.fori_loop(0, heads, head_step, 0)
    dkv_part[...] = kv_acc[...].astype(BF16)
    dkv_copy = remote(dkv_part, dkv_rx, ts.at[0], tr.at[0], other_ty)
    dkv_copy.start()
    br_v[...] = mm(attn_v[...], wo_v[...])
    dh_v[...] = mm_bt(dq_v[...], wqkv_v[:, 0:q_width])

    for j in range(2):
        tiles[j] = mm(nrm_t[...], dq_v[:, j * BLK:(j + 1) * BLK])
        tiles[2 + j] = mm_at(attn_v[:, j * BLK:(j + 1) * BLK], dy_v[...])

    def piece_copy(r):
        lo, size = PIECES[r]
        return remote(md.at[3, 1:3, lo:lo + size], md.at[3, 1:3, half + lo:half + lo + size], gs.at[12 + r], gr.at[12 + r], near)

    def gather_copy(k, i):
        return remote(md.at[k, i, 0:half], md.at[k, i, half:n_tok], gs.at[3 * k + i], gr.at[3 * k + i], near)

    def dact_block(k, j):
        return B_DACT_LO + j if k == 0 else B_DACT_HI + 2 * (k - 1) + j

    def gated(k, want_act, want_grad):
        def step(r, carry):
            rows = pl.ds(pl.multiple_of(r * 16, 16), 16)
            for j in range(2):
                bg, bu, bd = B_GU + 4 * k + j, B_GU + 4 * k + 2 + j, dact_block(k, j)
                gate = (chip[bg, rows].astype(F32) + rx[bg, rows].astype(F32)).astype(BF16).astype(F32)
                up = (chip[bu, rows].astype(F32) + rx[bu, rows].astype(F32)).astype(BF16).astype(F32)
                sig = jax.nn.sigmoid(gate)
                silu = gate * sig
                cols = slice(j * BLK, (j + 1) * BLK)
                if want_act:
                    md[k, 0, rows, cols] = (silu * up).astype(BF16)
                if k >= 2:
                    factors[k - 2, 0, rows, cols] = up * sig * (1.0 + gate * (1.0 - sig))
                    factors[k - 2, 1, rows, cols] = silu
                if want_grad:
                    d_act = (chip[bd, rows].astype(F32) + rx[bd, rows].astype(F32)).astype(BF16).astype(F32)
                    md[k, 1, rows, cols] = (d_act * up * sig * (1.0 + gate * (1.0 - sig))).astype(BF16)
                    md[k, 2, rows, cols] = (d_act * silu).astype(BF16)
            return carry

        lax.fori_loop(0, half // 16, step, 0)
        for i in ((0,) if want_act else ()) + ((1, 2) if want_grad else ()):
            gather_copy(k, i).start()

    def use_act(k):
        gather_copy(k, 0).wait_recv()
        br_v[...] += mm(md[k, 0], wd_v[k * CHUNK:(k + 1) * CHUNK, :])

    def use_grad(k):
        for i in (1, 2):
            gather_copy(k, i).wait_recv()
        dh_v[...] += (mm_bt(md[k, 1], wg_v[:, k * CHUNK:(k + 1) * CHUNK])
                      + mm_bt(md[k, 2], wu_v[:, k * CHUNK:(k + 1) * CHUNK]))

    x_copy(2).wait_recv()
    for k in range(4):
        x_copy(4 + k).wait_recv()
        gated(k, True, k == 0)
        use_act(k)
        if k == 0:
            use_grad(0)
            dkv_copy.wait_recv()
            d_k = dkv_part[:, 0:256].astype(F32) + dkv_rx[:, 0:256].astype(F32)
            d_k = d_k.astype(BF16).astype(F32)
            first, second = rope(d_k[:, 0:128], d_k[:, 128:256], cos_v[...], -sin_v[...])
            dkv_v[:, 0:128] = first.astype(BF16)
            dkv_v[:, 128:256] = second.astype(BF16)
            dkv_v[:, 256:512] = (dkv_part[:, 256:512].astype(F32) + dkv_rx[:, 256:512].astype(F32)).astype(BF16)
            dh_v[...] += 0.5 * mm_bt(dkv_v[...], wqkv_v[:, q_width:q_width + 512])
            tiles[4] = mm(nrm_t[...], dkv_v[...])
            for j in range(2):
                tiles[5 + j] = mm_at(md[0, 0, :, j * BLK:(j + 1) * BLK], dy_v[...])
    y_snd[...] = br_v[...].astype(BF16)
    y_copy = remote(y_snd, y_rx, ts.at[1], tr.at[1], other_ty)
    y_copy.start()
    x_copy(8).wait_recv()
    gated(1, False, True)
    use_grad(1)
    x_copy(9).wait_recv()

    def scaled(k, rows):
        for j in range(2):
            cols = slice(j * BLK, (j + 1) * BLK)
            b = dact_block(k, j)
            d_act = (chip[b, rows].astype(F32) + rx[b, rows].astype(F32)).astype(BF16).astype(F32)
            for i in range(2):
                md[k, 1 + i, rows, cols] = (d_act * factors[k - 2, i, rows, cols]).astype(BF16)

    def scaled_step(r, carry):
        scaled(2, pl.ds(pl.multiple_of(r * 32, 32), 32))
        return carry

    lax.fori_loop(0, half // 32, scaled_step, 0)
    for i in (1, 2):
        gather_copy(2, i).start()

    def dh_copy(r):
        at = pl.ds(2 * PIECES[r][0], 2 * PIECES[r][1])
        return remote(dh_snd.at[at], dh_rx.at[at], ds.at[r], dr.at[r], other_ty)

    def both(ref, r):
        lo, size = PIECES[r]
        return jnp.concatenate([ref[lo:lo + size], ref[half + lo:half + lo + size]], axis=0)

    sums = []

    def piece_grad(r):
        x_copy(X_LAST + r).wait_recv()
        scaled(3, slice(PIECES[r][0], PIECES[r][0] + PIECES[r][1]))
        piece_copy(r).start()

    def piece_dh(r):
        piece_copy(r).wait_recv()
        part = both(dh_v, r) + mm_bt(both(md.at[3, 1], r), wg_v[:, 3 * CHUNK:4 * CHUNK]) + mm_bt(both(md.at[3, 2], r), wu_v[:, 3 * CHUNK:4 * CHUNK])
        part_b = part.astype(BF16)
        dh_snd[2 * PIECES[r][0]:2 * (PIECES[r][0] + PIECES[r][1])] = part_b
        dh_copy(r).start()
        d_hat = part_b.astype(F32) * gamma_ref[...]
        sums.append((jnp.sum(d_hat, axis=1, keepdims=True), jnp.sum(d_hat * both(xhat_v, r), axis=1, keepdims=True)))

    piece_grad(0)
    use_grad(2)
    piece_dh(0)
    piece_grad(1)
    for r in range(2, SPLITS):
        piece_grad(r)
        piece_dh(r - 1)
    piece_dh(SPLITS - 1)
    cols = [jnp.concatenate([sums[r][i][:PIECES[r][1]] for r in range(SPLITS)] + [sums[r][i][PIECES[r][1]:] for r in range(SPLITS)], axis=0) for i in range(2)]
    stats_put(bst_snd, cols[0], cols[1])
    bwd_stats = stats_copies(bst_snd, bst_rx, 3, peers)
    for copy in bwd_stats:
        copy.start()

    y_copy.wait_recv()
    y_o[...] = (x_v[...].astype(F32) + (y_snd[...].astype(F32) + y_rx[...].astype(F32))).astype(BF16)

    def drain(b, carry):
        core_copy(b).wait_send()
        return carry

    lax.fori_loop(0, N_BLK, drain, 0)
    for u in range(N_X):
        x_copy(u).wait_send()
    for k in range(4):
        for i in range(3 if k < 3 else 1):
            gather_copy(k, i).wait_send()
    for r in range(SPLITS):
        piece_copy(r).wait_send()
    for copy in [packed_copy, dkv_copy, y_copy, kv_copy] + early + fwd_stats:
        copy.wait_send()

    br_v[...] = inv_v[:, 0:1] * xhat_v[...]
    d_gamma = jnp.zeros_like(dgamma_ref)
    for r in range(SPLITS):
        dh_copy(r).wait_recv()
        lo, size = PIECES[r]
        d_nrm = dh_snd[2 * lo:2 * (lo + size)].astype(F32) + dh_rx[2 * lo:2 * (lo + size)].astype(F32)
        d_gamma = d_gamma + jnp.sum(d_nrm * both(xhat_v, r), axis=0, keepdims=True)
        base = both(dy_v, r).astype(F32) + both(inv_v, r)[:, 0:1] * (d_nrm * gamma_ref[...])
        dh_v[lo:lo + size] = base[:size]
        dh_v[half + lo:half + lo + size] = base[size:]
    dgamma_ref[...] = d_gamma
    for copy in bwd_stats:
        copy.wait_recv()
    st_sum[...] = ((bst_snd[...] + bst_rx[0]) + (bst_rx[1] + bst_rx[2])) + ((bst_rx[3] + bst_rx[4]) + (bst_rx[5] + bst_rx[6]))
    sum_d, sum_dx = stats_columns(st_sum)
    d_x = dh_v[...] - inv_v[:, 0:1] * (sum_d / d_model) - br_v[...] * (sum_dx / d_model)
    dx_o[...] = d_x.astype(BF16)

    for r in range(SPLITS):
        dh_copy(r).wait_send()
    for copy in bwd_stats:
        copy.wait_send()


def grad_kernel(y_v, dx_v, dgamma_in, nrm_t, attn_v, md, dq_v, dkv_v, dy_v, tiles,
                y_hbm, dx_hbm, dgamma_hbm, dwq_hbm, dwg_hbm, dwu_hbm, dwk_hbm, dwv_hbm, dwo_hbm, dwd_hbm,
                ring, wide, out_sem, cp_sem):
    width, n_tok = nrm_t.shape
    half = n_tok // 2
    core = lax.rem(lax.axis_index('tx'), 2)
    mine = pl.multiple_of(core * half, half)
    other = pl.multiple_of((1 - core) * half, half)
    hand_out = [pltpu.make_async_copy(src.at[lo:lo + half], dst.at[pl.ds(at, half)], cp_sem.at[i])
                for i, (src, dst, lo, at) in enumerate(((y_v, y_hbm, 0, mine), (y_v, y_hbm, half, other), (dx_v, dx_hbm, 0, mine), (dx_v, dx_hbm, half, other)))]
    for cp in hand_out:
        cp.start()
    hand_out.append(pltpu.make_async_copy(dgamma_in, dgamma_hbm, cp_sem.at[12]))
    hand_out[-1].start()

    ready = [(0, dwq_hbm.at[:, 0:BLK]), (1, dwq_hbm.at[:, BLK:2 * BLK]), (2, dwo_hbm.at[0:BLK, :]), (3, dwo_hbm.at[BLK:2 * BLK, :]),
             (5, dwd_hbm.at[0:BLK, :]), (6, dwd_hbm.at[BLK:2 * BLK, :])]
    ready = [(tiles.at[i], dst) for i, dst in ready] + [(tiles.at[4, :, 0:256], dwk_hbm), (tiles.at[4, :, 256:512], dwv_hbm)]
    for i, (src, dst) in enumerate(ready):
        hand_out.append(pltpu.make_async_copy(src, dst, cp_sem.at[4 + i]))
        hand_out[-1].start(priority=len(hand_out) % 2)

    def put(src, dst, i):
        hand_out.append(pltpu.make_async_copy(src, dst, out_sem.at[i]))
        hand_out[-1].start(priority=len(hand_out) % 2)

    for t in range(6):
        k, j = 1 + t // 2, t % 2
        ring[t] = mm_at(md[k, 0, :, j * BLK:(j + 1) * BLK], dy_v[...])
        put(ring.at[t], dwd_hbm.at[k * CHUNK + j * BLK:k * CHUNK + (j + 1) * BLK, :], t)
    n_row = 256
    for i, (out, at) in enumerate(((dwg_hbm, 6), (dwu_hbm, 10))):
        for k in range(4):
            for j in range(2):
                lo = k * CHUNK + j * BLK
                wide[i, :, lo:lo + BLK] = mm(nrm_t[...], md[k, 1 + i, :, j * BLK:(j + 1) * BLK])
        for r in range(width // n_row):
            put(wide.at[i, r * n_row:(r + 1) * n_row], out.at[r * n_row:(r + 1) * n_row], at + r)
    for cp in hand_out:
        cp.wait()


def solution(mesh):
    tx_size = mesh.shape['tx']
    tok_spec = P('dp', None, 'tx')
    in_specs = (tok_spec, P('dp', None), tok_spec, P('tx'), P('tx', 'ty'), P('tx', 'ty'), P('tx', 'ty'),
                P('tx', None), P('tx', None), P('ty', 'tx'), P('ty', 'tx'))
    out_specs = (tok_spec, tok_spec, P(('dp', 'tx')), P(('dp', 'tx'), 'ty'), P(('dp', 'tx'), 'ty'), P(('dp', 'tx'), 'ty'),
                 P(('dp', 'tx'), None), P(('dp', 'tx'), None), P(('dp', 'ty'), 'tx'), P(('dp', 'ty'), 'tx'))

    def local_layer(x_in, positions, d_y, ln_gamma, w_q, w_g, w_u, w_k, w_v, w_o, w_d):
        _, n_tok, d_local = x_in.shape
        half = n_tok // 2
        d_model = d_local * tx_size
        head_dim = w_k.shape[1]
        q_width = w_q.shape[1]
        d_ff = w_g.shape[1]
        freq = jnp.asarray((ROPE_BASE ** (-2.0 * np.arange(head_dim // 2) / head_dim)).astype(np.float32)[None])
        any_spec = pl.BlockSpec(memory_space=pl.ANY)
        vmem_spec = pl.BlockSpec(memory_space=pltpu.VMEM)
        tok = (n_tok, d_local)
        sem = pltpu.SemaphoreType.DMA
        vm = pltpu.VMEM
        kept = pl.pallas_call(
            functools.partial(layer_kernel, d_model),
            out_shape=[vm(tok, BF16), vm(tok, BF16), vm((1, d_local), F32), vm((d_local, n_tok), BF16), vm((n_tok, q_width), BF16),
                       vm((4, 3, n_tok, CHUNK), BF16), vm((n_tok, q_width), BF16), vm((n_tok, 2 * head_dim), BF16), vm(tok, BF16),
                       vm((7, BLK, BLK), F32)],
            in_specs=[any_spec] * 12,
            out_specs=[vmem_spec] * 10,
            scratch_shapes=[
                vm((1, n_tok), jnp.int32), vm((1, head_dim // 2), F32), vm((1, d_local), F32), vm(tok, BF16),
                vm(tok, BF16), vm((d_local, q_width + 2 * head_dim), BF16), vm((d_local, d_ff), BF16), vm((d_local, d_ff), BF16),
                vm((q_width, d_local), BF16), vm((d_ff, d_local), BF16),
                vm((N_BLK, half, BLK), F32), vm((N_BLK, half, BLK), BF16), vm((N_BLK, half, BLK), BF16),
                vm((N_BLK, half, BLK), BF16), vm((N_BLK, half, BLK), BF16), vm((n_tok, 2 * q_width + 2 * head_dim), BF16),
                vm((n_tok, 512), BF16), vm((n_tok, 512), BF16), vm((n_tok, 512), F32),
                vm(tok, F32), vm((n_tok, 128), F32), vm((n_tok, 128), F32), vm((n_tok, 128), F32), vm(tok, F32), vm(tok, F32),
                vm(tok, BF16), vm(tok, BF16), vm(tok, BF16), vm(tok, BF16),
                vm((8, n_tok), F32), vm((3, 8, n_tok), F32), vm((8, n_tok), F32), vm((8, n_tok), F32), vm((7, 8, n_tok), F32), vm((2, 2, half, CHUNK), F32),
                sem((17,)), sem((N_BLK,)), sem((N_BLK,)), sem((N_X,)), sem((N_X,)),
                sem((12 + SPLITS,)), sem((12 + SPLITS,)), sem((1,)), sem((1,)), sem((4,)), sem((4,)), sem((10,)), sem((10,)),
                sem((SPLITS,)), sem((SPLITS,)), vm((n_tok, EARLY), BF16), vm((2, half, EARLY), BF16), sem((2,)), sem((2,))],
            compiler_params=pltpu.CompilerParams(collective_id=0, has_side_effects=True, vmem_limit_bytes=47 * 1024 * 1024),
            name='layer',
        )(x_in.reshape(tok), positions, freq, d_y.reshape(tok), ln_gamma[None], w_q, w_g, w_u, w_k, w_v, w_o, w_d)

        y_out, d_x, d_gamma, d_wq, d_wg, d_wu, d_wk, d_wv, d_wo, d_wd = pl.pallas_call(
            grad_kernel,
            out_shape=[jax.ShapeDtypeStruct(tok, BF16), jax.ShapeDtypeStruct(tok, BF16), jax.ShapeDtypeStruct((1, d_local), F32)]
            + [jax.ShapeDtypeStruct(w.shape, F32) for w in (w_q, w_g, w_u, w_k, w_v, w_o, w_d)],
            in_specs=[vmem_spec] * 10,
            out_specs=[any_spec] * 10,
            scratch_shapes=[vm((6, d_local, BLK), F32), vm((2, d_local, d_ff), F32), sem((14,)), sem((13,))],
            compiler_params=pltpu.CompilerParams(vmem_limit_bytes=30 * 1024 * 1024),
            name='weight_grads',
        )(*kept)
        return (y_out.reshape(x_in.shape), d_x.reshape(x_in.shape), d_gamma.reshape(d_local),
                d_wq, d_wg, d_wu, d_wk, d_wv, d_wo, d_wd)

    return jax.shard_map(local_layer, mesh=mesh, in_specs=in_specs, out_specs=out_specs, check_vma=False)
```

```python
import functools

import jax
import jax.numpy as jnp
import numpy as np
from jax import lax
from jax.experimental import pallas as pl
from jax.experimental.pallas import tpu as pltpu
from jax.sharding import PartitionSpec as P

EPS = 1e-6
ROPE_BASE = 10000.0
F32 = jnp.float32
BF16 = jnp.bfloat16
MESH = pl.DeviceIdType.MESH

BLK = 512
CHUNK = 1024
B_DATTN, B_DACT_LO, B_QKV, B_GU, B_DACT_HI, N_BLK = 0, 2, 4, 7, 23, 29
X_UNITS = ((0, 1), (1, 1), (2, 2), (4, 2), (7, 4), (11, 4), (15, 4), (19, 4), (23, 2), (25, 2))
PIECES = ((0, 16), (16, 32), (48, 32), (80, 32), (112, 16))
SPLITS = len(PIECES)
EARLY = 128
X_KV = len(X_UNITS)
X_LAST = X_KV + 1
N_X = X_LAST + SPLITS


def dot(a, b, dims):
    return lax.dot_general(a, b, (dims, ((), ())), preferred_element_type=F32)


def mm(a, b):
    return dot(a, b, ((1,), (0,)))


def mm_bt(a, b):
    return dot(a, b, ((1,), (1,)))


def mm_at(a, b):
    return dot(a, b, ((0,), (0,)))


def rope(first, second, cos_t, sin_t):
    return first * cos_t - second * sin_t, second * cos_t + first * sin_t


def layer_kernel(d_model, x_hbm, pos_hbm, freq_hbm, dy_hbm, gamma_hbm, wq_hbm, wg_hbm, wu_hbm, wk_hbm, wv_hbm, wo_hbm, wd_hbm,
                 y_o, dx_o, dgamma_ref, nrm_t, attn_v, md, dq_v, dkv_v, dy_v, tiles,
                 pos_ref, freq_ref, gamma_ref, nrm_v, x_v, wqkv_v, wg_v, wu_v, wo_v, wd_v,
                 keep, send, rcore, chip, rx, packed, dkv_part, dkv_rx, kv_acc,
                 xhat_v, inv_v, cos_v, sin_v, br_v, dh_v, y_snd, y_rx, dh_snd, dh_rx,
                 st_snd, st_rx, st_sum, bst_snd, bst_rx, factors,
                 ld_sem, cs, cr, xs, xr, gs, gr, ps, pr, ts, tr, ss, sr, ds, dr, early_snd, early_rx, es, er):
    tx = lax.axis_index('tx')
    ty = lax.axis_index('ty')
    core = lax.rem(tx, 2)
    near = {'tx': tx + 1 - 2 * core}
    across = {'tx': lax.rem(tx + 2, 4)}
    far = {'tx': lax.rem(tx + 1 - 2 * core + 2, 4)}
    other_ty = {'ty': 1 - ty}
    peers = [near, across, far, other_ty] + [{'tx': p['tx'], 'ty': 1 - ty} for p in (near, across, far)]
    close = peers[:5]
    n_tok = x_v.shape[0]
    half = n_tok // 2
    mine = pl.multiple_of(core * half, half)
    other = pl.multiple_of((1 - core) * half, half)
    head_dim = 256
    q_width = wo_v.shape[0]
    heads = q_width // head_dim

    def load(i, src, dst):
        return pltpu.make_async_copy(src, dst, ld_sem.at[i])

    loads = [
        load(0, dy_hbm.at[pl.ds(mine, half)], dy_v.at[0:half]),
        load(1, dy_hbm.at[pl.ds(other, half)], dy_v.at[half:n_tok]),
        load(2, wo_hbm.at[0:EARLY], wo_v.at[0:EARLY]),
        load(3, x_hbm.at[pl.ds(mine, half)], x_v.at[0:half]),
        load(4, x_hbm.at[pl.ds(other, half)], x_v.at[half:n_tok]),
        load(5, wd_hbm.at[0:CHUNK], wd_v.at[0:CHUNK]),
        load(6, wq_hbm, wqkv_v.at[:, 0:q_width]),
        load(7, wk_hbm, wqkv_v.at[:, q_width:q_width + head_dim]),
        load(8, wv_hbm, wqkv_v.at[:, q_width + head_dim:q_width + 2 * head_dim]),
        load(9, wg_hbm, wg_v),
        load(10, wu_hbm, wu_v),
        load(11, wd_hbm.at[CHUNK:4 * CHUNK], wd_v.at[CHUNK:4 * CHUNK]),
        load(12, gamma_hbm, gamma_ref),
        load(13, pos_hbm, pos_ref),
        load(14, freq_hbm, freq_ref),
        load(15, wo_hbm.at[BLK:q_width], wo_v.at[BLK:q_width]),
        load(16, wo_hbm.at[EARLY:BLK], wo_v.at[EARLY:BLK]),
    ]
    for i in (0, 1, 2, 16, 15, 3, 4, 5):
        loads[i].start()

    barrier = pltpu.get_barrier_semaphore()
    for peer in close:
        pl.semaphore_signal(barrier, inc=1, device_id=peer, device_id_type=MESH)
    for ld in loads[:3]:
        ld.wait()
    for i in (12, 6, 7, 8):
        loads[i].start()

    def remote(src, dst, send_sem, recv_sem, peer):
        return pltpu.make_async_remote_copy(src_ref=src, dst_ref=dst, send_sem=send_sem, recv_sem=recv_sem,
                                            device_id=peer, device_id_type=MESH)

    def core_copy(b):
        return remote(send.at[b], rcore.at[b], cs.at[b], cr.at[b], near)

    def x_copy(u):
        if u >= X_LAST:
            rows = pl.ds(*PIECES[u - X_LAST])
            return remote(chip.at[pl.ds(N_BLK - 2, 2), rows], rx.at[pl.ds(N_BLK - 2, 2), rows], xs.at[u], xr.at[u], across)
        if u == X_KV:
            cols = pl.ds(pl.multiple_of(ty * head_dim, head_dim), head_dim)
            return remote(chip.at[B_QKV + 2, :, cols], rx.at[B_QKV + 2, :, cols], xs.at[u], xr.at[u], across)
        if u == 0:
            return remote(chip.at[0, :, EARLY:BLK], rx.at[0, :, EARLY:BLK], xs.at[u], xr.at[u], across)
        start, count = X_UNITS[u]
        return remote(chip.at[pl.ds(start, count)], rx.at[pl.ds(start, count)], xs.at[u], xr.at[u], across)

    def put(b, part):
        keep[b] = part[:half]
        send[b] = part[half:].astype(BF16)
        core_copy(b).start()

    def issue_bwd(b, w_ref, row):
        put(b, mm_bt(dy_v[...], w_ref[pl.ds(row, BLK), :]))

    def issue_fwd(b, w_ref, col):
        put(b, mm(nrm_v[...], w_ref[:, pl.ds(col, BLK)]))

    def combine(b):
        core_copy(b).wait_recv()
        chip[b] = (keep[b] + rcore[b].astype(F32)).astype(BF16)

    def total(b):
        return chip[b].astype(F32) + rx[b].astype(F32)

    early_snd[...] = mm_bt(dy_v[...], wo_v[0:EARLY, :]).astype(BF16)
    pl.semaphore_wait(barrier, len(close))
    early = [remote(early_snd.at[0:half], early_rx.at[0], es.at[0], er.at[0], across),
             remote(early_snd.at[half:n_tok], early_rx.at[1], es.at[1], er.at[1], far)]
    for copy in early:
        copy.start()
    loads[16].wait()
    issue_bwd(0, wo_v, 0)
    loads[15].wait()
    issue_bwd(1, wo_v, BLK)

    def rows_of(col_a, col_b):
        lane = lax.broadcasted_iota(jnp.int32, (half, 128), 1)
        return jnp.where(lane == 0, col_a, col_b).T[0:8]

    def stats_copies(snd, got, base, to):
        return [remote(snd, got.at[i], ss.at[base + i], sr.at[base + i], peer) for i, peer in enumerate(to)]

    def stats_put(snd, col_a, col_b):
        for lo, at in ((0, mine), (half, other)):
            snd[:, pl.ds(at, half)] = rows_of(col_a[lo:lo + half], col_b[lo:lo + half])

    def stats_columns(rows_ref):
        cols = []
        for i in range(2):
            parts = [jnp.broadcast_to(rows_ref[i:i + 1, pl.ds(at, half)], (128, half)).T[:, 0:1] for at in (mine, other)]
            cols.append(jnp.concatenate(parts, axis=0))
        return cols

    loads[3].wait()
    loads[4].wait()
    for i in (9, 10, 11, 13, 14):
        loads[i].start()
    x_f = x_v[...].astype(F32)
    stats_put(st_snd, jnp.sum(x_f, axis=1, keepdims=True), jnp.sum(x_f * x_f, axis=1, keepdims=True))
    fwd_stats = stats_copies(st_snd, st_rx, 0, (near, across, far))
    for copy in fwd_stats:
        copy.start()

    combine(0)
    x_copy(0).start()
    combine(1)
    x_copy(1).start()

    loads[5].wait()
    for i in range(2):
        issue_bwd(B_DACT_LO + i, wd_v, i * BLK)
    for i in range(2):
        combine(B_DACT_LO + i)
    x_copy(2).start()

    loads[12].wait()
    for copy in fwd_stats:
        copy.wait_recv()
    st_sum[...] = (st_snd[...] + st_rx[0]) + (st_rx[1] + st_rx[2])
    sum_x, sum_xx = stats_columns(st_sum)
    tok_mean = sum_x / d_model
    inv_std = lax.rsqrt(sum_xx / d_model - tok_mean * tok_mean + EPS)
    inv_v[...] = jnp.broadcast_to(inv_std, (n_tok, 128))
    x_hat = (x_v[...].astype(F32) - tok_mean) * inv_std
    xhat_v[...] = x_hat
    nrm_v[...] = (x_hat * gamma_ref[...]).astype(BF16)

    for i in range(6, 9):
        loads[i].wait()
    for i in range(3):
        issue_fwd(B_QKV + i, wqkv_v, i * BLK)
    for i in (2, 0, 1):
        combine(B_QKV + i)
        if i == 2:
            x_copy(X_KV).start()
    x_copy(3).start()

    loads[9].wait()
    loads[10].wait()
    for k in range(4):
        def gu_issue(j, carry, k=k):
            col = pl.multiple_of(k * CHUNK + j * BLK, BLK)
            issue_fwd(B_GU + 4 * k + j, wg_v, col)
            issue_fwd(B_GU + 4 * k + 2 + j, wu_v, col)
            return carry

        def gu_combine(j, carry, k=k):
            combine(B_GU + 4 * k + j)
            return carry

        lax.fori_loop(0, 2, gu_issue, 0)
        lax.fori_loop(0, 4, gu_combine, 0)
        x_copy(4 + k).start()

    loads[11].wait()

    def hi_issue(j, carry):
        issue_bwd(B_DACT_HI + j, wd_v, pl.multiple_of(CHUNK + j * BLK, BLK))
        return carry

    lax.fori_loop(0, 6, hi_issue, 0)
    for j in range(6):
        combine(B_DACT_HI + j)
        if j == 1 or j == 3:
            x_copy(8 + j // 2).start()
    for r in range(SPLITS):
        x_copy(X_LAST + r).start()

    nrm_t[...] = nrm_v[...].T

    loads[13].wait()
    loads[14].wait()
    freq = freq_ref[...]
    for lo, at in ((0, mine), (half, other)):
        pos_col = jnp.broadcast_to(pos_ref[0:1, pl.ds(at, half)].astype(F32), (128, half)).T
        angles = pos_col * freq
        cos_v[lo:lo + half] = jnp.cos(angles)
        sin_v[lo:lo + half] = jnp.sin(angles)

    packed_copy = remote(packed.at[0:half], packed.at[half:n_tok], ps.at[0], pr.at[0], near)
    x_copy(0).wait_recv()
    x_copy(1).wait_recv()
    for copy in early:
        copy.wait_recv()
    rx[0, :, 0:EARLY] = (early_rx[0].astype(F32) + early_rx[1].astype(F32)).astype(BF16)
    for j in range(2):
        packed[0:half, q_width + 512 + j * BLK:q_width + 512 + (j + 1) * BLK] = total(B_DATTN + j).astype(BF16)
    x_copy(3).wait_recv()
    cos_h, sin_h = cos_v[0:half], sin_v[0:half]
    for j in range(2):
        blk = total(B_QKV + j)
        for h in range(2):
            lo = h * head_dim
            first, second = rope(blk[:, lo:lo + 128], blk[:, lo + 128:lo + 256], cos_h, sin_h)
            packed[0:half, j * BLK + lo:j * BLK + lo + 128] = first.astype(BF16)
            packed[0:half, j * BLK + lo + 128:j * BLK + lo + 256] = second.astype(BF16)
    x_copy(X_KV).wait_recv()
    kv_cols = pl.ds(pl.multiple_of(ty * head_dim, head_dim), head_dim)
    blk = chip[B_QKV + 2, :, kv_cols].astype(F32) + rx[B_QKV + 2, :, kv_cols].astype(F32)
    first, second = rope(blk[:, 0:128], blk[:, 128:256], cos_h, sin_h)
    kv_mine = jnp.where(ty == 0, jnp.concatenate([first, second], axis=1), blk).astype(BF16)
    kv_dst = packed.at[0:half, pl.ds(pl.multiple_of(q_width + ty * head_dim, head_dim), head_dim)]
    kv_dst[...] = kv_mine
    kv_copy = remote(kv_dst, kv_dst, ts.at[3], tr.at[3], other_ty)
    kv_copy.start()
    kv_copy.wait_recv()
    packed_copy.start()
    packed_copy.wait_recv()

    row_i = lax.rem(lax.broadcasted_iota(jnp.int32, (n_tok, n_tok), 0) + core * half, n_tok)
    col_i = lax.rem(lax.broadcasted_iota(jnp.int32, (n_tok, n_tok), 1) + core * half, n_tok)
    scale = head_dim ** -0.5
    kv_acc[...] = jnp.zeros_like(kv_acc)

    def head_step(h, carry):
        cols = pl.ds(pl.multiple_of(h * head_dim, head_dim), head_dim)
        q_h = packed[:, cols]
        da_h = packed[:, pl.ds(pl.multiple_of(q_width + 512 + h * head_dim, head_dim), head_dim)]
        k_rot = packed[:, q_width:q_width + 256]
        v_val = packed[:, q_width + 256:q_width + 512]
        scores = jnp.where(row_i >= col_i, mm_bt(q_h, k_rot) * scale, -1e30)
        exps = jnp.exp(scores - jnp.max(scores, axis=1, keepdims=True))
        probs_f = exps / jnp.sum(exps, axis=1, keepdims=True)
        probs = probs_f.astype(BF16)
        attn_v[:, cols] = mm(probs, v_val).astype(BF16)
        d_probs = mm_bt(da_h, v_val).astype(BF16).astype(F32)
        d_scores = (probs_f * (d_probs - jnp.sum(d_probs * probs_f, axis=1, keepdims=True)) * scale).astype(BF16)
        dq_h = mm(d_scores, k_rot).astype(BF16).astype(F32)
        first, second = rope(dq_h[:, 0:128], dq_h[:, 128:256], cos_v[...], -sin_v[...])
        dq_v[:, pl.ds(pl.multiple_of(h * head_dim, head_dim), 128)] = first.astype(BF16)
        dq_v[:, pl.ds(pl.multiple_of(h * head_dim + 128, 128), 128)] = second.astype(BF16)
        kv_acc[:, 0:256] += mm_at(d_scores, q_h)
        kv_acc[:, 256:512] += mm_at(probs, da_h)
        return carry

    lax.fori_loop(0, heads, head_step, 0)
    dkv_part[...] = kv_acc[...].astype(BF16)
    dkv_copy = remote(dkv_part, dkv_rx, ts.at[0], tr.at[0], other_ty)
    dkv_copy.start()
    br_v[...] = mm(attn_v[...], wo_v[...])
    dh_v[...] = mm_bt(dq_v[...], wqkv_v[:, 0:q_width])

    for j in range(2):
        tiles[j] = mm(nrm_t[...], dq_v[:, j * BLK:(j + 1) * BLK])
        tiles[2 + j] = mm_at(attn_v[:, j * BLK:(j + 1) * BLK], dy_v[...])

    def piece_copy(r):
        lo, size = PIECES[r]
        return remote(md.at[3, 1:3, lo:lo + size], md.at[3, 1:3, half + lo:half + lo + size], gs.at[12 + r], gr.at[12 + r], near)

    def gather_copy(k, i):
        return remote(md.at[k, i, 0:half], md.at[k, i, half:n_tok], gs.at[3 * k + i], gr.at[3 * k + i], near)

    def dact_block(k, j):
        return B_DACT_LO + j if k == 0 else B_DACT_HI + 2 * (k - 1) + j

    def gated(k, want_act, want_grad):
        def step(r, carry):
            rows = pl.ds(pl.multiple_of(r * 16, 16), 16)
            for j in range(2):
                bg, bu, bd = B_GU + 4 * k + j, B_GU + 4 * k + 2 + j, dact_block(k, j)
                gate = (chip[bg, rows].astype(F32) + rx[bg, rows].astype(F32)).astype(BF16).astype(F32)
                up = (chip[bu, rows].astype(F32) + rx[bu, rows].astype(F32)).astype(BF16).astype(F32)
                sig = jax.nn.sigmoid(gate)
                silu = gate * sig
                cols = slice(j * BLK, (j + 1) * BLK)
                if want_act:
                    md[k, 0, rows, cols] = (silu * up).astype(BF16)
                if k >= 2:
                    factors[k - 2, 0, rows, cols] = up * sig * (1.0 + gate * (1.0 - sig))
                    factors[k - 2, 1, rows, cols] = silu
                if want_grad:
                    d_act = (chip[bd, rows].astype(F32) + rx[bd, rows].astype(F32)).astype(BF16).astype(F32)
                    md[k, 1, rows, cols] = (d_act * up * sig * (1.0 + gate * (1.0 - sig))).astype(BF16)
                    md[k, 2, rows, cols] = (d_act * silu).astype(BF16)
            return carry

        lax.fori_loop(0, half // 16, step, 0)
        for i in ((0,) if want_act else ()) + ((1, 2) if want_grad else ()):
            gather_copy(k, i).start()

    def use_act(k):
        gather_copy(k, 0).wait_recv()
        br_v[...] += mm(md[k, 0], wd_v[k * CHUNK:(k + 1) * CHUNK, :])

    def use_grad(k):
        for i in (1, 2):
            gather_copy(k, i).wait_recv()
        dh_v[...] += (mm_bt(md[k, 1], wg_v[:, k * CHUNK:(k + 1) * CHUNK])
                      + mm_bt(md[k, 2], wu_v[:, k * CHUNK:(k + 1) * CHUNK]))

    x_copy(2).wait_recv()
    for k in range(4):
        x_copy(4 + k).wait_recv()
        gated(k, True, k == 0)
        use_act(k)
        if k == 0:
            use_grad(0)
            dkv_copy.wait_recv()
            d_k = dkv_part[:, 0:256].astype(F32) + dkv_rx[:, 0:256].astype(F32)
            d_k = d_k.astype(BF16).astype(F32)
            first, second = rope(d_k[:, 0:128], d_k[:, 128:256], cos_v[...], -sin_v[...])
            dkv_v[:, 0:128] = first.astype(BF16)
            dkv_v[:, 128:256] = second.astype(BF16)
            dkv_v[:, 256:512] = (dkv_part[:, 256:512].astype(F32) + dkv_rx[:, 256:512].astype(F32)).astype(BF16)
            dh_v[...] += 0.5 * mm_bt(dkv_v[...], wqkv_v[:, q_width:q_width + 512])
            tiles[4] = mm(nrm_t[...], dkv_v[...])
            for j in range(2):
                tiles[5 + j] = mm_at(md[0, 0, :, j * BLK:(j + 1) * BLK], dy_v[...])
    y_snd[...] = br_v[...].astype(BF16)
    y_copy = remote(y_snd, y_rx, ts.at[1], tr.at[1], other_ty)
    y_copy.start()
    x_copy(8).wait_recv()
    gated(1, False, True)
    use_grad(1)
    x_copy(9).wait_recv()

    def scaled(k, rows, which=(0, 1)):
        for j in range(2):
            cols = slice(j * BLK, (j + 1) * BLK)
            b = dact_block(k, j)
            d_act = (chip[b, rows].astype(F32) + rx[b, rows].astype(F32)).astype(BF16).astype(F32)
            for i in which:
                md[k, 1 + i, rows, cols] = (d_act * factors[k - 2, i, rows, cols]).astype(BF16)

    for i in range(2):
        def scaled_step(r, carry, i=i):
            scaled(2, pl.ds(pl.multiple_of(r * 32, 32), 32), (i,))
            return carry

        lax.fori_loop(0, half // 32, scaled_step, 0)
        gather_copy(2, 1 + i).start()

    def dh_copy(r):
        at = pl.ds(2 * PIECES[r][0], 2 * PIECES[r][1])
        return remote(dh_snd.at[at], dh_rx.at[at], ds.at[r], dr.at[r], other_ty)

    def both(ref, r):
        lo, size = PIECES[r]
        return jnp.concatenate([ref[lo:lo + size], ref[half + lo:half + lo + size]], axis=0)

    sums = []

    def piece_grad(r):
        x_copy(X_LAST + r).wait_recv()
        scaled(3, slice(PIECES[r][0], PIECES[r][0] + PIECES[r][1]))
        piece_copy(r).start()

    def piece_dh(r):
        piece_copy(r).wait_recv()
        part = both(dh_v, r) + mm_bt(both(md.at[3, 1], r), wg_v[:, 3 * CHUNK:4 * CHUNK]) + mm_bt(both(md.at[3, 2], r), wu_v[:, 3 * CHUNK:4 * CHUNK])
        part_b = part.astype(BF16)
        dh_snd[2 * PIECES[r][0]:2 * (PIECES[r][0] + PIECES[r][1])] = part_b
        dh_copy(r).start()
        d_hat = part_b.astype(F32) * gamma_ref[...]
        sums.append((jnp.sum(d_hat, axis=1, keepdims=True), jnp.sum(d_hat * both(xhat_v, r), axis=1, keepdims=True)))

    piece_grad(0)
    for i, weight in ((1, wg_v), (2, wu_v)):
        gather_copy(2, i).wait_recv()
        dh_v[...] += mm_bt(md[2, i], weight[:, 2 * CHUNK:3 * CHUNK])
    for r in range(1, SPLITS):
        piece_grad(r)
        piece_dh(r - 1)
    piece_dh(SPLITS - 1)
    cols = [jnp.concatenate([sums[r][i][:PIECES[r][1]] for r in range(SPLITS)] + [sums[r][i][PIECES[r][1]:] for r in range(SPLITS)], axis=0) for i in range(2)]
    stats_put(bst_snd, cols[0], cols[1])
    bwd_stats = stats_copies(bst_snd, bst_rx, 3, peers)
    for copy in bwd_stats:
        copy.start()

    y_copy.wait_recv()
    y_o[...] = (x_v[...].astype(F32) + (y_snd[...].astype(F32) + y_rx[...].astype(F32))).astype(BF16)

    def drain(b, carry):
        core_copy(b).wait_send()
        return carry

    lax.fori_loop(0, N_BLK, drain, 0)
    for u in range(N_X):
        x_copy(u).wait_send()
    for k in range(4):
        for i in range(3 if k < 3 else 1):
            gather_copy(k, i).wait_send()
    for r in range(SPLITS):
        piece_copy(r).wait_send()
    for copy in [packed_copy, dkv_copy, y_copy, kv_copy] + early + fwd_stats:
        copy.wait_send()

    br_v[...] = inv_v[:, 0:1] * xhat_v[...]
    d_gamma = jnp.zeros_like(dgamma_ref)
    for r in range(SPLITS):
        dh_copy(r).wait_recv()
        lo, size = PIECES[r]
        d_nrm = dh_snd[2 * lo:2 * (lo + size)].astype(F32) + dh_rx[2 * lo:2 * (lo + size)].astype(F32)
        d_gamma = d_gamma + jnp.sum(d_nrm * both(xhat_v, r), axis=0, keepdims=True)
        base = both(dy_v, r).astype(F32) + both(inv_v, r)[:, 0:1] * (d_nrm * gamma_ref[...])
        dh_v[lo:lo + size] = base[:size]
        dh_v[half + lo:half + lo + size] = base[size:]
    dgamma_ref[...] = d_gamma
    for copy in bwd_stats:
        copy.wait_recv()
    st_sum[...] = ((bst_snd[...] + bst_rx[0]) + (bst_rx[1] + bst_rx[2])) + ((bst_rx[3] + bst_rx[4]) + (bst_rx[5] + bst_rx[6]))
    sum_d, sum_dx = stats_columns(st_sum)
    d_x = dh_v[...] - inv_v[:, 0:1] * (sum_d / d_model) - br_v[...] * (sum_dx / d_model)
    dx_o[...] = d_x.astype(BF16)

    for r in range(SPLITS):
        dh_copy(r).wait_send()
    for copy in bwd_stats:
        copy.wait_send()


def grad_kernel(y_v, dx_v, dgamma_in, nrm_t, attn_v, md, dq_v, dkv_v, dy_v, tiles,
                y_hbm, dx_hbm, dgamma_hbm, dwq_hbm, dwg_hbm, dwu_hbm, dwk_hbm, dwv_hbm, dwo_hbm, dwd_hbm,
                ring, wide, out_sem, cp_sem):
    width, n_tok = nrm_t.shape
    half = n_tok // 2
    core = lax.rem(lax.axis_index('tx'), 2)
    mine = pl.multiple_of(core * half, half)
    other = pl.multiple_of((1 - core) * half, half)
    hand_out = [pltpu.make_async_copy(src.at[lo:lo + half], dst.at[pl.ds(at, half)], cp_sem.at[i])
                for i, (src, dst, lo, at) in enumerate(((y_v, y_hbm, 0, mine), (y_v, y_hbm, half, other), (dx_v, dx_hbm, 0, mine), (dx_v, dx_hbm, half, other)))]
    for cp in hand_out:
        cp.start()
    hand_out.append(pltpu.make_async_copy(dgamma_in, dgamma_hbm, cp_sem.at[12]))
    hand_out[-1].start()

    ready = [(0, dwq_hbm.at[:, 0:BLK]), (1, dwq_hbm.at[:, BLK:2 * BLK]), (2, dwo_hbm.at[0:BLK, :]), (3, dwo_hbm.at[BLK:2 * BLK, :]),
             (5, dwd_hbm.at[0:BLK, :]), (6, dwd_hbm.at[BLK:2 * BLK, :])]
    ready = [(tiles.at[i], dst) for i, dst in ready] + [(tiles.at[4, :, 0:256], dwk_hbm), (tiles.at[4, :, 256:512], dwv_hbm)]
    for i, (src, dst) in enumerate(ready):
        hand_out.append(pltpu.make_async_copy(src, dst, cp_sem.at[4 + i]))
        hand_out[-1].start(priority=len(hand_out) % 2)

    def put(src, dst, i):
        hand_out.append(pltpu.make_async_copy(src, dst, out_sem.at[i]))
        hand_out[-1].start(priority=len(hand_out) % 2)

    for t in range(6):
        k, j = 1 + t // 2, t % 2
        ring[t] = mm_at(md[k, 0, :, j * BLK:(j + 1) * BLK], dy_v[...])
        put(ring.at[t], dwd_hbm.at[k * CHUNK + j * BLK:k * CHUNK + (j + 1) * BLK, :], t)
    n_row = 128
    for i, (out, at) in enumerate(((dwg_hbm, 6), (dwu_hbm, 10))):
        for k in range(4):
            for j in range(2):
                lo = k * CHUNK + j * BLK
                wide[i, :, lo:lo + BLK] = mm(nrm_t[...], md[k, 1 + i, :, j * BLK:(j + 1) * BLK])
        for r in range(width // n_row):
            put(wide.at[i, r * n_row:(r + 1) * n_row], out.at[r * n_row:(r + 1) * n_row], at + r)
    for cp in hand_out:
        cp.wait()


def solution(mesh):
    tx_size = mesh.shape['tx']
    tok_spec = P('dp', None, 'tx')
    in_specs = (tok_spec, P('dp', None), tok_spec, P('tx'), P('tx', 'ty'), P('tx', 'ty'), P('tx', 'ty'),
                P('tx', None), P('tx', None), P('ty', 'tx'), P('ty', 'tx'))
    out_specs = (tok_spec, tok_spec, P(('dp', 'tx')), P(('dp', 'tx'), 'ty'), P(('dp', 'tx'), 'ty'), P(('dp', 'tx'), 'ty'),
                 P(('dp', 'tx'), None), P(('dp', 'tx'), None), P(('dp', 'ty'), 'tx'), P(('dp', 'ty'), 'tx'))

    def local_layer(x_in, positions, d_y, ln_gamma, w_q, w_g, w_u, w_k, w_v, w_o, w_d):
        _, n_tok, d_local = x_in.shape
        half = n_tok // 2
        d_model = d_local * tx_size
        head_dim = w_k.shape[1]
        q_width = w_q.shape[1]
        d_ff = w_g.shape[1]
        freq = jnp.asarray((ROPE_BASE ** (-2.0 * np.arange(head_dim // 2) / head_dim)).astype(np.float32)[None])
        any_spec = pl.BlockSpec(memory_space=pl.ANY)
        vmem_spec = pl.BlockSpec(memory_space=pltpu.VMEM)
        tok = (n_tok, d_local)
        sem = pltpu.SemaphoreType.DMA
        vm = pltpu.VMEM
        kept = pl.pallas_call(
            functools.partial(layer_kernel, d_model),
            out_shape=[vm(tok, BF16), vm(tok, BF16), vm((1, d_local), F32), vm((d_local, n_tok), BF16), vm((n_tok, q_width), BF16),
                       vm((4, 3, n_tok, CHUNK), BF16), vm((n_tok, q_width), BF16), vm((n_tok, 2 * head_dim), BF16), vm(tok, BF16),
                       vm((7, BLK, BLK), F32)],
            in_specs=[any_spec] * 12,
            out_specs=[vmem_spec] * 10,
            scratch_shapes=[
                vm((1, n_tok), jnp.int32), vm((1, head_dim // 2), F32), vm((1, d_local), F32), vm(tok, BF16),
                vm(tok, BF16), vm((d_local, q_width + 2 * head_dim), BF16), vm((d_local, d_ff), BF16), vm((d_local, d_ff), BF16),
                vm((q_width, d_local), BF16), vm((d_ff, d_local), BF16),
                vm((N_BLK, half, BLK), F32), vm((N_BLK, half, BLK), BF16), vm((N_BLK, half, BLK), BF16),
                vm((N_BLK, half, BLK), BF16), vm((N_BLK, half, BLK), BF16), vm((n_tok, 2 * q_width + 2 * head_dim), BF16),
                vm((n_tok, 512), BF16), vm((n_tok, 512), BF16), vm((n_tok, 512), F32),
                vm(tok, F32), vm((n_tok, 128), F32), vm((n_tok, 128), F32), vm((n_tok, 128), F32), vm(tok, F32), vm(tok, F32),
                vm(tok, BF16), vm(tok, BF16), vm(tok, BF16), vm(tok, BF16),
                vm((8, n_tok), F32), vm((3, 8, n_tok), F32), vm((8, n_tok), F32), vm((8, n_tok), F32), vm((7, 8, n_tok), F32), vm((2, 2, half, CHUNK), F32),
                sem((17,)), sem((N_BLK,)), sem((N_BLK,)), sem((N_X,)), sem((N_X,)),
                sem((12 + SPLITS,)), sem((12 + SPLITS,)), sem((1,)), sem((1,)), sem((4,)), sem((4,)), sem((10,)), sem((10,)),
                sem((SPLITS,)), sem((SPLITS,)), vm((n_tok, EARLY), BF16), vm((2, half, EARLY), BF16), sem((2,)), sem((2,))],
            compiler_params=pltpu.CompilerParams(collective_id=0, has_side_effects=True, vmem_limit_bytes=47 * 1024 * 1024),
            name='layer',
        )(x_in.reshape(tok), positions, freq, d_y.reshape(tok), ln_gamma[None], w_q, w_g, w_u, w_k, w_v, w_o, w_d)

        y_out, d_x, d_gamma, d_wq, d_wg, d_wu, d_wk, d_wv, d_wo, d_wd = pl.pallas_call(
            grad_kernel,
            out_shape=[jax.ShapeDtypeStruct(tok, BF16), jax.ShapeDtypeStruct(tok, BF16), jax.ShapeDtypeStruct((1, d_local), F32)]
            + [jax.ShapeDtypeStruct(w.shape, F32) for w in (w_q, w_g, w_u, w_k, w_v, w_o, w_d)],
            in_specs=[vmem_spec] * 10,
            out_specs=[any_spec] * 10,
            scratch_shapes=[vm((6, d_local, BLK), F32), vm((2, d_local, d_ff), F32), sem((14,)), sem((13,))],
            compiler_params=pltpu.CompilerParams(vmem_limit_bytes=30 * 1024 * 1024),
            name='weight_grads',
        )(*kept)
        return (y_out.reshape(x_in.shape), d_x.reshape(x_in.shape), d_gamma.reshape(d_local),
                d_wq, d_wg, d_wu, d_wk, d_wv, d_wo, d_wd)

    return jax.shard_map(local_layer, mesh=mesh, in_specs=in_specs, out_specs=out_specs, check_vma=False)
```

```python
import functools

import jax
import jax.numpy as jnp
import numpy as np
from jax import lax
from jax.experimental import pallas as pl
from jax.experimental.pallas import tpu as pltpu
from jax.sharding import PartitionSpec as P

EPS = 1e-6
ROPE_BASE = 10000.0
F32 = jnp.float32
BF16 = jnp.bfloat16
MESH = pl.DeviceIdType.MESH

BLK = 512
CHUNK = 1024
B_DATTN, B_DACT_LO, B_QKV, B_GU, B_DACT_HI, N_BLK = 0, 2, 4, 7, 23, 29
X_UNITS = ((0, 1), (1, 1), (2, 2), (4, 2), (7, 4), (11, 4), (15, 4), (19, 4), (23, 2), (25, 2))
PIECES = ((0, 16), (16, 32), (48, 32), (80, 32), (112, 16))
SPLITS = len(PIECES)
EARLY = 128
X_KV = len(X_UNITS)
X_LAST = X_KV + 1
N_X = X_LAST + SPLITS


def dot(a, b, dims):
    return lax.dot_general(a, b, (dims, ((), ())), preferred_element_type=F32)


def mm(a, b):
    return dot(a, b, ((1,), (0,)))


def mm_bt(a, b):
    return dot(a, b, ((1,), (1,)))


def mm_at(a, b):
    return dot(a, b, ((0,), (0,)))


def rope(first, second, cos_t, sin_t):
    return first * cos_t - second * sin_t, second * cos_t + first * sin_t


def layer_kernel(d_model, x_hbm, pos_hbm, freq_hbm, dy_hbm, gamma_hbm, wq_hbm, wg_hbm, wu_hbm, wk_hbm, wv_hbm, wo_hbm, wd_hbm,
                 y_o, dx_o, dgamma_ref, nrm_t, attn_v, md, dq_v, dkv_v, dy_v, tiles,
                 pos_ref, freq_ref, gamma_ref, nrm_v, x_v, wqkv_v, wg_v, wu_v, wo_v, wd_v,
                 keep, send, rcore, chip, rx, packed, dkv_part, dkv_rx, kv_acc,
                 xhat_v, inv_v, cos_v, sin_v, br_v, dh_v, y_snd, y_rx, dh_snd, dh_rx,
                 st_snd, st_rx, st_sum, bst_snd, bst_rx, factors,
                 ld_sem, cs, cr, xs, xr, gs, gr, ps, pr, ts, tr, ss, sr, ds, dr, early_snd, early_rx, es, er):
    tx = lax.axis_index('tx')
    ty = lax.axis_index('ty')
    core = lax.rem(tx, 2)
    near = {'tx': tx + 1 - 2 * core}
    across = {'tx': lax.rem(tx + 2, 4)}
    far = {'tx': lax.rem(tx + 1 - 2 * core + 2, 4)}
    other_ty = {'ty': 1 - ty}
    peers = [near, across, far, other_ty] + [{'tx': p['tx'], 'ty': 1 - ty} for p in (near, across, far)]
    close = peers[:5]
    n_tok = x_v.shape[0]
    half = n_tok // 2
    mine = pl.multiple_of(core * half, half)
    other = pl.multiple_of((1 - core) * half, half)
    head_dim = 256
    q_width = wo_v.shape[0]
    heads = q_width // head_dim

    def load(i, src, dst):
        return pltpu.make_async_copy(src, dst, ld_sem.at[i])

    loads = [
        load(0, dy_hbm.at[pl.ds(mine, half)], dy_v.at[0:half]),
        load(1, dy_hbm.at[pl.ds(other, half)], dy_v.at[half:n_tok]),
        load(2, wo_hbm.at[0:EARLY], wo_v.at[0:EARLY]),
        load(3, x_hbm.at[pl.ds(mine, half)], x_v.at[0:half]),
        load(4, x_hbm.at[pl.ds(other, half)], x_v.at[half:n_tok]),
        load(5, wd_hbm.at[0:CHUNK], wd_v.at[0:CHUNK]),
        load(6, wq_hbm, wqkv_v.at[:, 0:q_width]),
        load(7, wk_hbm, wqkv_v.at[:, q_width:q_width + head_dim]),
        load(8, wv_hbm, wqkv_v.at[:, q_width + head_dim:q_width + 2 * head_dim]),
        load(9, wg_hbm, wg_v),
        load(10, wu_hbm, wu_v),
        load(11, wd_hbm.at[CHUNK:4 * CHUNK], wd_v.at[CHUNK:4 * CHUNK]),
        load(12, gamma_hbm, gamma_ref),
        load(13, pos_hbm, pos_ref),
        load(14, freq_hbm, freq_ref),
        load(15, wo_hbm.at[BLK:q_width], wo_v.at[BLK:q_width]),
        load(16, wo_hbm.at[EARLY:BLK], wo_v.at[EARLY:BLK]),
    ]
    for i in (0, 1, 2, 16, 15, 3, 4, 5):
        loads[i].start()

    barrier = pltpu.get_barrier_semaphore()
    for peer in close:
        pl.semaphore_signal(barrier, inc=1, device_id=peer, device_id_type=MESH)
    for ld in loads[:3]:
        ld.wait()
    for i in (12, 6, 7, 8):
        loads[i].start()

    def remote(src, dst, send_sem, recv_sem, peer):
        return pltpu.make_async_remote_copy(src_ref=src, dst_ref=dst, send_sem=send_sem, recv_sem=recv_sem,
                                            device_id=peer, device_id_type=MESH)

    def core_copy(b):
        return remote(send.at[b], rcore.at[b], cs.at[b], cr.at[b], near)

    def x_copy(u):
        if u >= X_LAST:
            rows = pl.ds(*PIECES[u - X_LAST])
            return remote(chip.at[pl.ds(N_BLK - 2, 2), rows], rx.at[pl.ds(N_BLK - 2, 2), rows], xs.at[u], xr.at[u], across)
        if u == X_KV:
            cols = pl.ds(pl.multiple_of(ty * head_dim, head_dim), head_dim)
            return remote(chip.at[B_QKV + 2, :, cols], rx.at[B_QKV + 2, :, cols], xs.at[u], xr.at[u], across)
        if u == 0:
            return remote(chip.at[0, :, EARLY:BLK], rx.at[0, :, EARLY:BLK], xs.at[u], xr.at[u], across)
        start, count = X_UNITS[u]
        return remote(chip.at[pl.ds(start, count)], rx.at[pl.ds(start, count)], xs.at[u], xr.at[u], across)

    def put(b, part):
        keep[b] = part[:half]
        send[b] = part[half:].astype(BF16)
        core_copy(b).start()

    def issue_bwd(b, w_ref, row):
        put(b, mm_bt(dy_v[...], w_ref[pl.ds(row, BLK), :]))

    def issue_fwd(b, w_ref, col):
        put(b, mm(nrm_v[...], w_ref[:, pl.ds(col, BLK)]))

    def combine(b):
        core_copy(b).wait_recv()
        chip[b] = (keep[b] + rcore[b].astype(F32)).astype(BF16)

    def total(b):
        return chip[b].astype(F32) + rx[b].astype(F32)

    early_snd[...] = mm_bt(dy_v[...], wo_v[0:EARLY, :]).astype(BF16)
    pl.semaphore_wait(barrier, len(close))
    early = [remote(early_snd.at[0:half], early_rx.at[0], es.at[0], er.at[0], across),
             remote(early_snd.at[half:n_tok], early_rx.at[1], es.at[1], er.at[1], far)]
    for copy in early:
        copy.start()
    loads[16].wait()
    issue_bwd(0, wo_v, 0)
    loads[15].wait()
    issue_bwd(1, wo_v, BLK)

    def rows_of(col_a, col_b):
        lane = lax.broadcasted_iota(jnp.int32, (half, 128), 1)
        return jnp.where(lane == 0, col_a, col_b).T[0:8]

    def stats_copies(snd, got, base, to):
        return [remote(snd, got.at[i], ss.at[base + i], sr.at[base + i], peer) for i, peer in enumerate(to)]

    def stats_put(snd, col_a, col_b):
        for lo, at in ((0, mine), (half, other)):
            snd[:, pl.ds(at, half)] = rows_of(col_a[lo:lo + half], col_b[lo:lo + half])

    def stats_columns(rows_ref):
        cols = []
        for i in range(2):
            parts = [jnp.broadcast_to(rows_ref[i:i + 1, pl.ds(at, half)], (128, half)).T[:, 0:1] for at in (mine, other)]
            cols.append(jnp.concatenate(parts, axis=0))
        return cols

    loads[3].wait()
    loads[4].wait()
    for i in (9, 10, 11, 13, 14):
        loads[i].start()
    x_f = x_v[...].astype(F32)
    stats_put(st_snd, jnp.sum(x_f, axis=1, keepdims=True), jnp.sum(x_f * x_f, axis=1, keepdims=True))
    fwd_stats = stats_copies(st_snd, st_rx, 0, (near, across, far))
    for copy in fwd_stats:
        copy.start()

    combine(0)
    x_copy(0).start()
    combine(1)
    x_copy(1).start()

    loads[5].wait()
    for i in range(2):
        issue_bwd(B_DACT_LO + i, wd_v, i * BLK)
    for i in range(2):
        combine(B_DACT_LO + i)
    x_copy(2).start()

    loads[12].wait()
    for copy in fwd_stats:
        copy.wait_recv()
    st_sum[...] = (st_snd[...] + st_rx[0]) + (st_rx[1] + st_rx[2])
    sum_x, sum_xx = stats_columns(st_sum)
    tok_mean = sum_x / d_model
    inv_std = lax.rsqrt(sum_xx / d_model - tok_mean * tok_mean + EPS)
    inv_v[...] = jnp.broadcast_to(inv_std, (n_tok, 128))
    x_hat = (x_v[...].astype(F32) - tok_mean) * inv_std
    xhat_v[...] = x_hat
    nrm_v[...] = (x_hat * gamma_ref[...]).astype(BF16)

    for i in range(6, 9):
        loads[i].wait()
    for i in range(3):
        issue_fwd(B_QKV + i, wqkv_v, i * BLK)
    for i in (2, 0, 1):
        combine(B_QKV + i)
        if i == 2:
            x_copy(X_KV).start()
    x_copy(3).start()

    loads[9].wait()
    loads[10].wait()
    for k in range(4):
        def gu_issue(j, carry, k=k):
            col = pl.multiple_of(k * CHUNK + j * BLK, BLK)
            issue_fwd(B_GU + 4 * k + j, wg_v, col)
            issue_fwd(B_GU + 4 * k + 2 + j, wu_v, col)
            return carry

        def gu_combine(j, carry, k=k):
            combine(B_GU + 4 * k + j)
            return carry

        lax.fori_loop(0, 2, gu_issue, 0)
        lax.fori_loop(0, 4, gu_combine, 0)
        x_copy(4 + k).start()

    loads[11].wait()

    def hi_issue(j, carry):
        issue_bwd(B_DACT_HI + j, wd_v, pl.multiple_of(CHUNK + j * BLK, BLK))
        return carry

    lax.fori_loop(0, 6, hi_issue, 0)
    for j in range(6):
        combine(B_DACT_HI + j)
        if j == 1 or j == 3:
            x_copy(8 + j // 2).start()
    for r in range(SPLITS):
        x_copy(X_LAST + r).start()

    nrm_t[...] = nrm_v[...].T

    loads[13].wait()
    loads[14].wait()
    freq = freq_ref[...]
    for lo, at in ((0, mine), (half, other)):
        pos_col = jnp.broadcast_to(pos_ref[0:1, pl.ds(at, half)].astype(F32), (128, half)).T
        angles = pos_col * freq
        cos_v[lo:lo + half] = jnp.cos(angles)
        sin_v[lo:lo + half] = jnp.sin(angles)

    packed_copy = remote(packed.at[0:half], packed.at[half:n_tok], ps.at[0], pr.at[0], near)
    x_copy(0).wait_recv()
    x_copy(1).wait_recv()
    for copy in early:
        copy.wait_recv()
    rx[0, :, 0:EARLY] = (early_rx[0].astype(F32) + early_rx[1].astype(F32)).astype(BF16)
    for j in range(2):
        packed[0:half, q_width + 512 + j * BLK:q_width + 512 + (j + 1) * BLK] = total(B_DATTN + j).astype(BF16)
    x_copy(3).wait_recv()
    cos_h, sin_h = cos_v[0:half], sin_v[0:half]
    for j in range(2):
        blk = total(B_QKV + j)
        for h in range(2):
            lo = h * head_dim
            first, second = rope(blk[:, lo:lo + 128], blk[:, lo + 128:lo + 256], cos_h, sin_h)
            packed[0:half, j * BLK + lo:j * BLK + lo + 128] = first.astype(BF16)
            packed[0:half, j * BLK + lo + 128:j * BLK + lo + 256] = second.astype(BF16)
    x_copy(X_KV).wait_recv()
    kv_cols = pl.ds(pl.multiple_of(ty * head_dim, head_dim), head_dim)
    blk = chip[B_QKV + 2, :, kv_cols].astype(F32) + rx[B_QKV + 2, :, kv_cols].astype(F32)
    first, second = rope(blk[:, 0:128], blk[:, 128:256], cos_h, sin_h)
    kv_mine = jnp.where(ty == 0, jnp.concatenate([first, second], axis=1), blk).astype(BF16)
    kv_dst = packed.at[0:half, pl.ds(pl.multiple_of(q_width + ty * head_dim, head_dim), head_dim)]
    kv_dst[...] = kv_mine
    kv_copy = remote(kv_dst, kv_dst, ts.at[3], tr.at[3], other_ty)
    kv_copy.start()
    kv_copy.wait_recv()
    packed_copy.start()
    packed_copy.wait_recv()

    row_i = lax.rem(lax.broadcasted_iota(jnp.int32, (n_tok, n_tok), 0) + core * half, n_tok)
    col_i = lax.rem(lax.broadcasted_iota(jnp.int32, (n_tok, n_tok), 1) + core * half, n_tok)
    scale = head_dim ** -0.5
    kv_acc[...] = jnp.zeros_like(kv_acc)

    def head_step(h, carry):
        cols = pl.ds(pl.multiple_of(h * head_dim, head_dim), head_dim)
        q_h = packed[:, cols]
        da_h = packed[:, pl.ds(pl.multiple_of(q_width + 512 + h * head_dim, head_dim), head_dim)]
        k_rot = packed[:, q_width:q_width + 256]
        v_val = packed[:, q_width + 256:q_width + 512]
        scores = jnp.where(row_i >= col_i, mm_bt(q_h, k_rot) * scale, -1e30)
        exps = jnp.exp(scores - jnp.max(scores, axis=1, keepdims=True))
        probs_f = exps / jnp.sum(exps, axis=1, keepdims=True)
        probs = probs_f.astype(BF16)
        attn_v[:, cols] = mm(probs, v_val).astype(BF16)
        d_probs = mm_bt(da_h, v_val).astype(BF16).astype(F32)
        d_scores = (probs_f * (d_probs - jnp.sum(d_probs * probs_f, axis=1, keepdims=True)) * scale).astype(BF16)
        dq_h = mm(d_scores, k_rot).astype(BF16).astype(F32)
        first, second = rope(dq_h[:, 0:128], dq_h[:, 128:256], cos_v[...], -sin_v[...])
        dq_v[:, pl.ds(pl.multiple_of(h * head_dim, head_dim), 128)] = first.astype(BF16)
        dq_v[:, pl.ds(pl.multiple_of(h * head_dim + 128, 128), 128)] = second.astype(BF16)
        kv_acc[:, 0:256] += mm_at(d_scores, q_h)
        kv_acc[:, 256:512] += mm_at(probs, da_h)
        return carry

    lax.fori_loop(0, heads, head_step, 0)
    dkv_part[...] = kv_acc[...].astype(BF16)
    dkv_copy = remote(dkv_part, dkv_rx, ts.at[0], tr.at[0], other_ty)
    dkv_copy.start()
    br_v[...] = mm(attn_v[...], wo_v[...])
    dh_v[...] = mm_bt(dq_v[...], wqkv_v[:, 0:q_width])

    for j in range(2):
        tiles[j] = mm(nrm_t[...], dq_v[:, j * BLK:(j + 1) * BLK])
        tiles[2 + j] = mm_at(attn_v[:, j * BLK:(j + 1) * BLK], dy_v[...])

    def piece_copy(r):
        lo, size = PIECES[r]
        return remote(md.at[3, 1:3, lo:lo + size], md.at[3, 1:3, half + lo:half + lo + size], gs.at[12 + r], gr.at[12 + r], near)

    def gather_copy(k, i):
        return remote(md.at[k, i, 0:half], md.at[k, i, half:n_tok], gs.at[3 * k + i], gr.at[3 * k + i], near)

    def dact_block(k, j):
        return B_DACT_LO + j if k == 0 else B_DACT_HI + 2 * (k - 1) + j

    def gated(k, want_act, want_grad):
        def step(r, carry):
            rows = pl.ds(pl.multiple_of(r * 16, 16), 16)
            for j in range(2):
                bg, bu, bd = B_GU + 4 * k + j, B_GU + 4 * k + 2 + j, dact_block(k, j)
                gate = (chip[bg, rows].astype(F32) + rx[bg, rows].astype(F32)).astype(BF16).astype(F32)
                up = (chip[bu, rows].astype(F32) + rx[bu, rows].astype(F32)).astype(BF16).astype(F32)
                sig = jax.nn.sigmoid(gate)
                silu = gate * sig
                cols = slice(j * BLK, (j + 1) * BLK)
                if want_act:
                    md[k, 0, rows, cols] = (silu * up).astype(BF16)
                if k >= 2:
                    factors[k - 2, 0, rows, cols] = up * sig * (1.0 + gate * (1.0 - sig))
                    factors[k - 2, 1, rows, cols] = silu
                if want_grad:
                    d_act = (chip[bd, rows].astype(F32) + rx[bd, rows].astype(F32)).astype(BF16).astype(F32)
                    md[k, 1, rows, cols] = (d_act * up * sig * (1.0 + gate * (1.0 - sig))).astype(BF16)
                    md[k, 2, rows, cols] = (d_act * silu).astype(BF16)
            return carry

        lax.fori_loop(0, half // 16, step, 0)
        for i in ((0,) if want_act else ()) + ((1, 2) if want_grad else ()):
            gather_copy(k, i).start()

    def use_act(k):
        gather_copy(k, 0).wait_recv()
        br_v[...] += mm(md[k, 0], wd_v[k * CHUNK:(k + 1) * CHUNK, :])

    def use_grad(k):
        for i in (1, 2):
            gather_copy(k, i).wait_recv()
        dh_v[...] += (mm_bt(md[k, 1], wg_v[:, k * CHUNK:(k + 1) * CHUNK])
                      + mm_bt(md[k, 2], wu_v[:, k * CHUNK:(k + 1) * CHUNK]))

    x_copy(2).wait_recv()
    for k in range(4):
        x_copy(4 + k).wait_recv()
        gated(k, True, k == 0)
        use_act(k)
        if k == 0:
            use_grad(0)
            dkv_copy.wait_recv()
            d_k = dkv_part[:, 0:256].astype(F32) + dkv_rx[:, 0:256].astype(F32)
            d_k = d_k.astype(BF16).astype(F32)
            first, second = rope(d_k[:, 0:128], d_k[:, 128:256], cos_v[...], -sin_v[...])
            dkv_v[:, 0:128] = first.astype(BF16)
            dkv_v[:, 128:256] = second.astype(BF16)
            dkv_v[:, 256:512] = (dkv_part[:, 256:512].astype(F32) + dkv_rx[:, 256:512].astype(F32)).astype(BF16)
            dh_v[...] += 0.5 * mm_bt(dkv_v[...], wqkv_v[:, q_width:q_width + 512])
            tiles[4] = mm(nrm_t[...], dkv_v[...])
            for j in range(2):
                tiles[5 + j] = mm_at(md[0, 0, :, j * BLK:(j + 1) * BLK], dy_v[...])
    y_snd[...] = br_v[...].astype(BF16)
    y_copy = remote(y_snd, y_rx, ts.at[1], tr.at[1], other_ty)
    y_copy.start()
    x_copy(8).wait_recv()
    gated(1, False, True)
    use_grad(1)
    x_copy(9).wait_recv()

    def scaled(k, rows, which=(0, 1)):
        for j in range(2):
            cols = slice(j * BLK, (j + 1) * BLK)
            b = dact_block(k, j)
            d_act = (chip[b, rows].astype(F32) + rx[b, rows].astype(F32)).astype(BF16).astype(F32)
            for i in which:
                md[k, 1 + i, rows, cols] = (d_act * factors[k - 2, i, rows, cols]).astype(BF16)

    for i in range(2):
        def scaled_step(r, carry, i=i):
            scaled(2, pl.ds(pl.multiple_of(r * 32, 32), 32), (i,))
            return carry

        lax.fori_loop(0, half // 32, scaled_step, 0)
        gather_copy(2, 1 + i).start()

    def dh_copy(r):
        at = pl.ds(2 * PIECES[r][0], 2 * PIECES[r][1])
        return remote(dh_snd.at[at], dh_rx.at[at], ds.at[r], dr.at[r], other_ty)

    def both(ref, r):
        lo, size = PIECES[r]
        return jnp.concatenate([ref[lo:lo + size], ref[half + lo:half + lo + size]], axis=0)

    sums = []

    def piece_grad(r):
        x_copy(X_LAST + r).wait_recv()
        scaled(3, slice(PIECES[r][0], PIECES[r][0] + PIECES[r][1]))
        piece_copy(r).start()

    def piece_dh(r):
        piece_copy(r).wait_recv()
        part = both(dh_v, r) + mm_bt(both(md.at[3, 1], r), wg_v[:, 3 * CHUNK:4 * CHUNK]) + mm_bt(both(md.at[3, 2], r), wu_v[:, 3 * CHUNK:4 * CHUNK])
        part_b = part.astype(BF16)
        dh_snd[2 * PIECES[r][0]:2 * (PIECES[r][0] + PIECES[r][1])] = part_b
        dh_copy(r).start()

    def piece_sums(r):
        d_hat = dh_snd[2 * PIECES[r][0]:2 * (PIECES[r][0] + PIECES[r][1])].astype(F32) * gamma_ref[...]
        sums.append((jnp.sum(d_hat, axis=1, keepdims=True), jnp.sum(d_hat * both(xhat_v, r), axis=1, keepdims=True)))

    piece_grad(0)
    for i, weight in ((1, wg_v), (2, wu_v)):
        gather_copy(2, i).wait_recv()
        dh_v[...] += mm_bt(md[2, i], weight[:, 2 * CHUNK:3 * CHUNK])
    for r in range(1, SPLITS):
        piece_grad(r)
        piece_dh(r - 1)
    for r in range(SPLITS - 1):
        piece_sums(r)
    piece_dh(SPLITS - 1)
    piece_sums(SPLITS - 1)
    cols = [jnp.concatenate([sums[r][i][:PIECES[r][1]] for r in range(SPLITS)] + [sums[r][i][PIECES[r][1]:] for r in range(SPLITS)], axis=0) for i in range(2)]
    stats_put(bst_snd, cols[0], cols[1])
    bwd_stats = stats_copies(bst_snd, bst_rx, 3, peers)
    for copy in bwd_stats:
        copy.start()

    y_copy.wait_recv()
    y_o[...] = (x_v[...].astype(F32) + (y_snd[...].astype(F32) + y_rx[...].astype(F32))).astype(BF16)

    def drain(b, carry):
        core_copy(b).wait_send()
        return carry

    lax.fori_loop(0, N_BLK, drain, 0)
    for u in range(N_X):
        x_copy(u).wait_send()
    for k in range(4):
        for i in range(3 if k < 3 else 1):
            gather_copy(k, i).wait_send()
    for r in range(SPLITS):
        piece_copy(r).wait_send()
    for copy in [packed_copy, dkv_copy, y_copy, kv_copy] + early + fwd_stats:
        copy.wait_send()

    br_v[...] = inv_v[:, 0:1] * xhat_v[...]
    d_gamma = jnp.zeros_like(dgamma_ref)
    for r in range(SPLITS):
        dh_copy(r).wait_recv()
        lo, size = PIECES[r]
        d_nrm = dh_snd[2 * lo:2 * (lo + size)].astype(F32) + dh_rx[2 * lo:2 * (lo + size)].astype(F32)
        d_gamma = d_gamma + jnp.sum(d_nrm * both(xhat_v, r), axis=0, keepdims=True)
        base = both(dy_v, r).astype(F32) + both(inv_v, r)[:, 0:1] * (d_nrm * gamma_ref[...])
        dh_v[lo:lo + size] = base[:size]
        dh_v[half + lo:half + lo + size] = base[size:]
    dgamma_ref[...] = d_gamma
    for copy in bwd_stats:
        copy.wait_recv()
    st_sum[...] = ((bst_snd[...] + bst_rx[0]) + (bst_rx[1] + bst_rx[2])) + ((bst_rx[3] + bst_rx[4]) + (bst_rx[5] + bst_rx[6]))
    sum_d, sum_dx = stats_columns(st_sum)
    d_x = dh_v[...] - inv_v[:, 0:1] * (sum_d / d_model) - br_v[...] * (sum_dx / d_model)
    dx_o[...] = d_x.astype(BF16)

    for r in range(SPLITS):
        dh_copy(r).wait_send()
    for copy in bwd_stats:
        copy.wait_send()


def grad_kernel(y_v, dx_v, dgamma_in, nrm_t, attn_v, md, dq_v, dkv_v, dy_v, tiles,
                y_hbm, dx_hbm, dgamma_hbm, dwq_hbm, dwg_hbm, dwu_hbm, dwk_hbm, dwv_hbm, dwo_hbm, dwd_hbm,
                ring, wide, out_sem, cp_sem):
    width, n_tok = nrm_t.shape
    half = n_tok // 2
    core = lax.rem(lax.axis_index('tx'), 2)
    mine = pl.multiple_of(core * half, half)
    other = pl.multiple_of((1 - core) * half, half)
    hand_out = [pltpu.make_async_copy(src.at[lo:lo + half], dst.at[pl.ds(at, half)], cp_sem.at[i])
                for i, (src, dst, lo, at) in enumerate(((y_v, y_hbm, 0, mine), (y_v, y_hbm, half, other), (dx_v, dx_hbm, 0, mine), (dx_v, dx_hbm, half, other)))]
    for cp in hand_out:
        cp.start()
    hand_out.append(pltpu.make_async_copy(dgamma_in, dgamma_hbm, cp_sem.at[12]))
    hand_out[-1].start()

    ready = [(0, dwq_hbm.at[:, 0:BLK]), (1, dwq_hbm.at[:, BLK:2 * BLK]), (2, dwo_hbm.at[0:BLK, :]), (3, dwo_hbm.at[BLK:2 * BLK, :]),
             (5, dwd_hbm.at[0:BLK, :]), (6, dwd_hbm.at[BLK:2 * BLK, :])]
    ready = [(tiles.at[i], dst) for i, dst in ready] + [(tiles.at[4, :, 0:256], dwk_hbm), (tiles.at[4, :, 256:512], dwv_hbm)]
    for i, (src, dst) in enumerate(ready):
        hand_out.append(pltpu.make_async_copy(src, dst, cp_sem.at[4 + i]))
        hand_out[-1].start(priority=len(hand_out) % 2)

    def put(src, dst, i):
        hand_out.append(pltpu.make_async_copy(src, dst, out_sem.at[i]))
        hand_out[-1].start(priority=len(hand_out) % 2)

    for t in range(6):
        k, j = 1 + t // 2, t % 2
        ring[t] = mm_at(md[k, 0, :, j * BLK:(j + 1) * BLK], dy_v[...])
        put(ring.at[t], dwd_hbm.at[k * CHUNK + j * BLK:k * CHUNK + (j + 1) * BLK, :], t)
    n_row = 128
    for i, (out, at) in enumerate(((dwg_hbm, 6), (dwu_hbm, 10))):
        for k in range(4):
            for j in range(2):
                lo = k * CHUNK + j * BLK
                wide[i, :, lo:lo + BLK] = mm(nrm_t[...], md[k, 1 + i, :, j * BLK:(j + 1) * BLK])
        for r in range(width // n_row):
            put(wide.at[i, r * n_row:(r + 1) * n_row], out.at[r * n_row:(r + 1) * n_row], at + r)
    for cp in hand_out:
        cp.wait()


def solution(mesh):
    tx_size = mesh.shape['tx']
    tok_spec = P('dp', None, 'tx')
    in_specs = (tok_spec, P('dp', None), tok_spec, P('tx'), P('tx', 'ty'), P('tx', 'ty'), P('tx', 'ty'),
                P('tx', None), P('tx', None), P('ty', 'tx'), P('ty', 'tx'))
    out_specs = (tok_spec, tok_spec, P(('dp', 'tx')), P(('dp', 'tx'), 'ty'), P(('dp', 'tx'), 'ty'), P(('dp', 'tx'), 'ty'),
                 P(('dp', 'tx'), None), P(('dp', 'tx'), None), P(('dp', 'ty'), 'tx'), P(('dp', 'ty'), 'tx'))

    def local_layer(x_in, positions, d_y, ln_gamma, w_q, w_g, w_u, w_k, w_v, w_o, w_d):
        _, n_tok, d_local = x_in.shape
        half = n_tok // 2
        d_model = d_local * tx_size
        head_dim = w_k.shape[1]
        q_width = w_q.shape[1]
        d_ff = w_g.shape[1]
        freq = jnp.asarray((ROPE_BASE ** (-2.0 * np.arange(head_dim // 2) / head_dim)).astype(np.float32)[None])
        any_spec = pl.BlockSpec(memory_space=pl.ANY)
        vmem_spec = pl.BlockSpec(memory_space=pltpu.VMEM)
        tok = (n_tok, d_local)
        sem = pltpu.SemaphoreType.DMA
        vm = pltpu.VMEM
        kept = pl.pallas_call(
            functools.partial(layer_kernel, d_model),
            out_shape=[vm(tok, BF16), vm(tok, BF16), vm((1, d_local), F32), vm((d_local, n_tok), BF16), vm((n_tok, q_width), BF16),
                       vm((4, 3, n_tok, CHUNK), BF16), vm((n_tok, q_width), BF16), vm((n_tok, 2 * head_dim), BF16), vm(tok, BF16),
                       vm((7, BLK, BLK), F32)],
            in_specs=[any_spec] * 12,
            out_specs=[vmem_spec] * 10,
            scratch_shapes=[
                vm((1, n_tok), jnp.int32), vm((1, head_dim // 2), F32), vm((1, d_local), F32), vm(tok, BF16),
                vm(tok, BF16), vm((d_local, q_width + 2 * head_dim), BF16), vm((d_local, d_ff), BF16), vm((d_local, d_ff), BF16),
                vm((q_width, d_local), BF16), vm((d_ff, d_local), BF16),
                vm((N_BLK, half, BLK), F32), vm((N_BLK, half, BLK), BF16), vm((N_BLK, half, BLK), BF16),
                vm((N_BLK, half, BLK), BF16), vm((N_BLK, half, BLK), BF16), vm((n_tok, 2 * q_width + 2 * head_dim), BF16),
                vm((n_tok, 512), BF16), vm((n_tok, 512), BF16), vm((n_tok, 512), F32),
                vm(tok, F32), vm((n_tok, 128), F32), vm((n_tok, 128), F32), vm((n_tok, 128), F32), vm(tok, F32), vm(tok, F32),
                vm(tok, BF16), vm(tok, BF16), vm(tok, BF16), vm(tok, BF16),
                vm((8, n_tok), F32), vm((3, 8, n_tok), F32), vm((8, n_tok), F32), vm((8, n_tok), F32), vm((7, 8, n_tok), F32), vm((2, 2, half, CHUNK), F32),
                sem((17,)), sem((N_BLK,)), sem((N_BLK,)), sem((N_X,)), sem((N_X,)),
                sem((12 + SPLITS,)), sem((12 + SPLITS,)), sem((1,)), sem((1,)), sem((4,)), sem((4,)), sem((10,)), sem((10,)),
                sem((SPLITS,)), sem((SPLITS,)), vm((n_tok, EARLY), BF16), vm((2, half, EARLY), BF16), sem((2,)), sem((2,))],
            compiler_params=pltpu.CompilerParams(collective_id=0, has_side_effects=True, vmem_limit_bytes=47 * 1024 * 1024),
            name='layer',
        )(x_in.reshape(tok), positions, freq, d_y.reshape(tok), ln_gamma[None], w_q, w_g, w_u, w_k, w_v, w_o, w_d)

        y_out, d_x, d_gamma, d_wq, d_wg, d_wu, d_wk, d_wv, d_wo, d_wd = pl.pallas_call(
            grad_kernel,
            out_shape=[jax.ShapeDtypeStruct(tok, BF16), jax.ShapeDtypeStruct(tok, BF16), jax.ShapeDtypeStruct((1, d_local), F32)]
            + [jax.ShapeDtypeStruct(w.shape, F32) for w in (w_q, w_g, w_u, w_k, w_v, w_o, w_d)],
            in_specs=[vmem_spec] * 10,
            out_specs=[any_spec] * 10,
            scratch_shapes=[vm((6, d_local, BLK), F32), vm((2, d_local, d_ff), F32), sem((14,)), sem((13,))],
            compiler_params=pltpu.CompilerParams(vmem_limit_bytes=30 * 1024 * 1024),
            name='weight_grads',
        )(*kept)
        return (y_out.reshape(x_in.shape), d_x.reshape(x_in.shape), d_gamma.reshape(d_local),
                d_wq, d_wg, d_wu, d_wk, d_wv, d_wo, d_wd)

    return jax.shard_map(local_layer, mesh=mesh, in_specs=in_specs, out_specs=out_specs, check_vma=False)
```
